32 devices in a mesh: dp: 1 (over z), cp: 4 (over y), tp: 8 (over x, core).
Axes of the slice: x: 4, y: 4, z: 1, core: 2. Of those that a mesh axis runs over, the one named last changes fastest.
The devices are a block of a 4x4x8 slice.
Arguments:
- x_tok: bfloat16 [16384, 2048], P(('dp', 'cp', 'tp'))
- w_q: bfloat16 [2048, 16, 128], P(None, 'tp')
- w_k: bfloat16 [2048, 16, 128], P(None, 'tp')
- w_v: bfloat16 [2048, 16, 128], P(None, 'tp')
- w_o: bfloat16 [16, 128, 2048], P('tp')
- expert_ids: int32 [16384, 8], P(('dp', 'cp', 'tp'))
- gate_wts: float32 [16384, 8], P(('dp', 'cp', 'tp'))
- w_gate: bfloat16 [128, 2048, 512], P(('cp', 'tp'))
- w_up: bfloat16 [128, 2048, 512], P(('cp', 'tp'))
- w_down: bfloat16 [128, 512, 2048], P(('cp', 'tp'))
Outputs:
- output: bfloat16 [16384, 2048], P(('dp', 'cp', 'tp'))
All inputs are finite; a program needn't handle non-finite values.
Results may differ from the reference program's by a relative error of at most 0.0115601.
Values are sent between devices in bfloat16 or wider.
A program may use at most 768 MiB of HBM per device.

```python
import math
import jax
import jax.numpy as jnp
from jax import lax

TOK_DEV = 512
CP = 4
TP = 8
HID = 2048
FFN = 1024
HEADS = 16
KV_HEADS = 16
HEAD = 128
EXPERTS = 64
TOP = 8

SEQ = TOK_DEV * CP * TP
BLOCKS = CP * TP
PAIRS = CP * TP // 2
LOCAL = EXPERTS // PAIRS
HALF_FFN = FFN // 2
GROUP = HEADS // KV_HEADS


def token_positions():
    half_len = SEQ // CP
    chunk_len = half_len // 2
    row_ids = jnp.arange(SEQ)
    cp_rank = row_ids // half_len
    in_half = row_ids % half_len
    return jnp.where(in_half < chunk_len, cp_rank * chunk_len + in_half, (2 * CP - 1 - cp_rank) * chunk_len + in_half - chunk_len)


def draw_routing(route_key):
    perm_key, label_key = jax.random.split(route_key)
    tok_order = jax.vmap(lambda one_key: jax.random.permutation(one_key, TOK_DEV))(jax.random.split(perm_key, BLOCKS))
    relabel = jax.vmap(lambda one_key: jax.random.permutation(one_key, EXPERTS))(jax.random.split(label_key, BLOCKS))
    raw_ids = (tok_order[:, :, None] + jnp.arange(TOP)[None, None, :]) % EXPERTS
    picked = jax.vmap(lambda label_map, raw_set: label_map[raw_set])(relabel, raw_ids)
    return picked.reshape(SEQ, TOP).astype(jnp.int32)


def setup_inputs(seed: int = 0, part: int = 0) -> dict:
    part_key = jax.random.fold_in(jax.random.key(seed), part)
    key_x, key_route, key_gate = jax.random.split(part_key, 3)
    weight_keys = jax.random.split(jax.random.key(seed + 1), 7)
    score_gain = math.sqrt(max(math.log(SEQ / 8.0), 1.0))
    in_scale = 1.0 / math.sqrt(HID)
    x_tok = jax.random.normal(key_x, (SEQ, HID), jnp.float32).astype(jnp.bfloat16)
    w_q = (jax.random.normal(weight_keys[0], (HID, HEADS, HEAD), jnp.float32) * (score_gain * in_scale)).astype(jnp.bfloat16)
    w_k = (jax.random.normal(weight_keys[1], (HID, KV_HEADS, HEAD), jnp.float32) * in_scale).astype(jnp.bfloat16)
    w_v = (jax.random.normal(weight_keys[2], (HID, KV_HEADS, HEAD), jnp.float32) * in_scale).astype(jnp.bfloat16)
    w_o = (jax.random.normal(weight_keys[3], (HEADS, HEAD, HID), jnp.float32) * (2.0 / math.sqrt(HEADS * HEAD))).astype(jnp.bfloat16)
    w_gate = (jax.random.normal(weight_keys[4], (2 * EXPERTS, HID, HALF_FFN), jnp.float32) * in_scale).astype(jnp.bfloat16)
    w_up = (jax.random.normal(weight_keys[5], (2 * EXPERTS, HID, HALF_FFN), jnp.float32) * in_scale).astype(jnp.bfloat16)
    w_down = (jax.random.normal(weight_keys[6], (2 * EXPERTS, HALF_FFN, HID), jnp.float32) * (2.0 / math.sqrt(FFN))).astype(jnp.bfloat16)
    gate_raw = jax.random.uniform(key_gate, (SEQ, TOP), jnp.float32, 1.0, 3.0)
    gate_wts = gate_raw / jnp.sum(gate_raw, axis=1, keepdims=True)
    expert_ids = draw_routing(key_route)
    return {"x_tok": x_tok, "w_q": w_q, "w_k": w_k, "w_v": w_v, "w_o": w_o, "expert_ids": expert_ids, "gate_wts": gate_wts, "w_gate": w_gate, "w_up": w_up, "w_down": w_down}


def reference(x_tok, w_q, w_k, w_v, w_o, expert_ids, gate_wts, w_gate, w_up, w_down):
    q_all = jnp.dot(x_tok, w_q.reshape(HID, HEADS * HEAD), preferred_element_type=jnp.float32).astype(jnp.bfloat16)
    k_all = jnp.dot(x_tok, w_k.reshape(HID, KV_HEADS * HEAD), preferred_element_type=jnp.float32).astype(jnp.bfloat16)
    v_all = jnp.dot(x_tok, w_v.reshape(HID, KV_HEADS * HEAD), preferred_element_type=jnp.float32).astype(jnp.bfloat16)
    q_blocks = q_all.reshape(BLOCKS, TOK_DEV, KV_HEADS, GROUP, HEAD)
    positions = token_positions()
    pos_blocks = positions.reshape(BLOCKS, TOK_DEV)
    keys_f = k_all.reshape(SEQ, KV_HEADS, HEAD).astype(jnp.float32)
    vals_f = v_all.reshape(SEQ, KV_HEADS, HEAD).astype(jnp.float32)
    score_scale = HEAD ** -0.5

    def attend(blk_item):
        q_blk, q_pos = blk_item
        scores = jnp.einsum("qgrd,kgd->grqk", q_blk.astype(jnp.float32), keys_f) * score_scale
        allowed = q_pos[:, None] >= positions[None, :]
        scores = jnp.where(allowed[None, None], scores, -jnp.inf)
        row_peak = jnp.max(scores, axis=-1, keepdims=True)
        prob_vals = jnp.exp(scores - row_peak)
        row_sum = jnp.sum(prob_vals, axis=-1)
        mixed_vals = jnp.einsum("grqk,kgd->qgrd", prob_vals.astype(jnp.bfloat16).astype(jnp.float32), vals_f)
        return (mixed_vals / jnp.moveaxis(row_sum, -1, 0)[..., None]).astype(jnp.bfloat16)

    attn_out = lax.map(attend, (q_blocks, pos_blocks)).reshape(SEQ, HEADS * HEAD)
    h_tok = (x_tok.astype(jnp.float32) + jnp.dot(attn_out, w_o.reshape(HEADS * HEAD, HID), preferred_element_type=jnp.float32)).astype(jnp.bfloat16)

    full_gate = w_gate.reshape(PAIRS, 2, LOCAL, HID, HALF_FFN).transpose(0, 2, 3, 1, 4).reshape(EXPERTS, HID, FFN)
    full_up = w_up.reshape(PAIRS, 2, LOCAL, HID, HALF_FFN).transpose(0, 2, 3, 1, 4).reshape(EXPERTS, HID, FFN)
    full_down = w_down.reshape(PAIRS, 2, LOCAL, HALF_FFN, HID).transpose(0, 2, 1, 3, 4).reshape(EXPERTS, FFN, HID)
    flat_ids = expert_ids.reshape(-1)
    sort_order = jnp.argsort(flat_ids, stable=True)
    per_expert = SEQ * TOP // EXPERTS
    tok_rows = (sort_order // TOP).reshape(EXPERTS, per_expert)

    def run_expert(expert_item):
        rows_e, gate_e, up_e, down_e = expert_item
        tokens = h_tok[rows_e]
        gate_pre = jnp.dot(tokens, gate_e, preferred_element_type=jnp.float32)
        up_pre = jnp.dot(tokens, up_e, preferred_element_type=jnp.float32)
        hidden = (jax.nn.silu(gate_pre) * up_pre).astype(jnp.bfloat16)
        return jnp.dot(hidden, down_e, preferred_element_type=jnp.float32).astype(jnp.bfloat16)

    z_sorted = lax.map(run_expert, (tok_rows, full_gate, full_up, full_down)).reshape(SEQ * TOP, HID)
    back_order = jnp.argsort(sort_order)
    z_choice = z_sorted[back_order].reshape(SEQ, TOP, HID)
    y_acc = h_tok.astype(jnp.float32)
    for choice in range(TOP):
        y_acc = y_acc + gate_wts[:, choice:choice + 1] * z_choice[:, choice].astype(jnp.float32)
    return y_acc.astype(jnp.bfloat16)
```

```python
import functools

import jax
import jax.numpy as jnp
from jax import lax
from jax.experimental import pallas as pl
from jax.experimental.pallas import tpu as pltpu
from jax.sharding import PartitionSpec as P

MESH = pl.DeviceIdType.MESH
VMEM_LIMIT = 66_000_000


def peer_of(step, cp_pos, tp_pos, n_cp, n_tp, sign):
    n_x = n_tp // 2
    flip = step % 2
    off_x = (step // 2) % n_x
    off_y = (off_x + step // n_tp) % n_cp
    if sign < 0:
        off_x = n_x - off_x
        off_y = n_cp - off_y
    to_cp = (cp_pos + off_y) % n_cp
    to_tp = ((tp_pos // 2 + off_x) % n_x) * 2 + (tp_pos % 2 + flip) % 2
    return to_cp, to_tp


def mesh_id(cp_pos, tp_pos):
    return {"cp": cp_pos, "tp": tp_pos}


def moe_kernel(n_cp, n_tp, group, h_hbm, rank_ref, gate_ref, wg_hbm, wu_hbm, wd_hbm, wgx_hbm, wux_hbm, wdx_hbm,
               y_ref, rx_hbm, rz_hbm,
               h_buf, wg_buf, wu_buf, wd_buf, stage, x_buf, z_buf, acc, parts,
               w_sem, in_sem, x_sem, z_sem, sx_sem, rx_sem, sz_sem, rz_sem):
    n_dev = n_cp * n_tp
    tok_dev, hid = h_buf.shape
    cap = stage.shape[1] // 2
    half_f = wg_buf.shape[3]
    cp_pos, tp_pos = lax.axis_index("cp"), lax.axis_index("tp")
    core = tp_pos % 2

    def signal_peer(step, carry):
        to_cp, to_tp = peer_of(step, cp_pos, tp_pos, n_cp, n_tp, 1)
        pl.semaphore_signal(pltpu.get_barrier_semaphore(), inc=1, device_id=mesh_id(to_cp, to_tp), device_id_type=MESH)
        return carry

    h_copy = pltpu.make_async_copy(h_hbm, h_buf, in_sem)
    h_copy.start()
    w_copies = []
    for slot, (own, other, buf) in enumerate(((wg_hbm, wgx_hbm, wg_buf), (wu_hbm, wux_hbm, wu_buf), (wd_hbm, wdx_hbm, wd_buf))):
        w_copies.append(pltpu.make_async_copy(own.at[pl.ds(2 * core, 2)], buf.at[0], w_sem.at[2 * slot]))
        w_copies.append(pltpu.make_async_copy(other, buf.at[1], w_sem.at[2 * slot + 1]))
    for one in w_copies:
        one.start()
    lax.fori_loop(1, n_dev, signal_peer, 0)
    pl.semaphore_wait(pltpu.get_barrier_semaphore(), n_dev - 1)
    h_copy.wait()

    slots = lax.broadcasted_iota(jnp.int32, (cap, tok_dev), 0).astype(jnp.float32)

    def gather_rows(step):
        to_cp, to_tp = peer_of(step, cp_pos, tp_pos, n_cp, n_tp, 1)
        first = 2 * (to_cp * n_tp + to_tp)
        picks = [jnp.where(rank_ref[pl.ds(first + i, 1), :] == slots, 1.0, 0.0) for i in range(2)]
        pick = jnp.concatenate(picks, axis=0).astype(jnp.bfloat16)
        stage[step] = jnp.dot(pick, h_buf[...], preferred_element_type=jnp.float32).astype(jnp.bfloat16)

    def x_send(step):
        to_cp, to_tp = peer_of(step, cp_pos, tp_pos, n_cp, n_tp, 1)
        return pltpu.make_async_remote_copy(stage.at[step], rx_hbm.at[step], sx_sem.at[step], rx_sem.at[step],
                                            device_id=mesh_id(to_cp, to_tp), device_id_type=MESH)

    def z_send(step):
        to_cp, to_tp = peer_of(step, cp_pos, tp_pos, n_cp, n_tp, -1)
        return pltpu.make_async_remote_copy(stage.at[step], rz_hbm.at[step], sz_sem.at[step], rz_sem.at[step],
                                            device_id=mesh_id(to_cp, to_tp), device_id_type=MESH)

    self_x = pltpu.make_async_copy(stage.at[0], rx_hbm.at[0], rx_sem.at[0])
    self_z = pltpu.make_async_copy(stage.at[0], rz_hbm.at[0], rz_sem.at[0])

    gather_rows(0)
    gather_rows(1)
    self_x.start()

    def gather_step(step, carry):
        gather_rows(step)
        x_send(step - 1).start()
        return carry

    lax.fori_loop(2, n_dev, gather_step, 0)

    gate_all = gate_ref[...]
    high = gate_all.astype(jnp.bfloat16).astype(jnp.float32)
    rest = gate_all - high
    mid = rest.astype(jnp.bfloat16).astype(jnp.float32)
    parts[0] = high
    parts[1] = mid
    parts[2] = rest - mid
    x_send(n_dev - 1).start()
    acc[...] = h_buf[...].astype(jnp.float32)
    for one in w_copies:
        one.wait()

    rows = group * cap
    n_cols = min(512, hid)

    def expert_rows(place, i):
        x_rows = x_buf[:, pl.ds(i * cap, cap), :].reshape(rows, hid)
        hidden = []
        for half in range(2):
            gate_pre = jnp.dot(x_rows, wg_buf[half, i], preferred_element_type=jnp.float32)
            up_pre = jnp.dot(x_rows, wu_buf[half, i], preferred_element_type=jnp.float32)
            hidden.append((gate_pre * (1.0 / (1.0 + jnp.exp(-gate_pre))) * up_pre).astype(jnp.bfloat16))
        for col in range(0, hid, n_cols):
            z_rows = (jnp.dot(hidden[0], wd_buf[0, i, :, pl.ds(col, n_cols)], preferred_element_type=jnp.float32)
                      + jnp.dot(hidden[1], wd_buf[1, i, :, pl.ds(col, n_cols)], preferred_element_type=jnp.float32))
            stage[pl.ds(place, group), pl.ds(i * cap, cap), pl.ds(col, n_cols)] = z_rows.astype(jnp.bfloat16).reshape(group, cap, n_cols)

    def expert_group(g, carry):
        place = g * group
        for q in range(group):
            @pl.when(place + q == 0)
            def _():
                self_x.wait()

            @pl.when(place + q > 0)
            def _():
                x_send(place + q).wait_recv()
        for q in range(group):
            pltpu.make_async_copy(rx_hbm.at[place + q], x_buf.at[q], x_sem.at[q]).start()
        for q in range(group):
            pltpu.make_async_copy(rx_hbm.at[place + q], x_buf.at[q], x_sem.at[q]).wait()
        for q in range(group):
            @pl.when(place + q > 0)
            def _():
                x_send(place + q).wait_send()
        for i in range(2):
            expert_rows(place, i)
        for q in range(group):
            @pl.when(place + q == 0)
            def _():
                self_z.start()

            @pl.when(place + q > 0)
            def _():
                z_send(place + q).start()
        return carry

    lax.fori_loop(0, n_dev // group, expert_group, 0)

    def combine_pair(j, carry):
        @pl.when(j == 0)
        def _():
            self_z.wait()

        @pl.when(j > 0)
        def _():
            z_send(2 * j).wait_recv()
        z_send(2 * j + 1).wait_recv()
        z_copy = pltpu.make_async_copy(rz_hbm.at[pl.ds(2 * j, 2)], z_buf, z_sem)
        z_copy.start()
        weights = [[], [], []]
        for q in range(2):
            to_cp, to_tp = peer_of(2 * j + q, cp_pos, tp_pos, n_cp, n_tp, 1)
            first = 2 * (to_cp * n_tp + to_tp)
            for i in range(2):
                chosen = rank_ref[pl.ds(first + i, 1), :] == slots
                for part in range(3):
                    weights[part].append(jnp.where(chosen, parts[part, pl.ds(first + i, 1), :], 0.0))
        weights = [jnp.concatenate(w, axis=0).astype(jnp.bfloat16) for w in weights]
        z_copy.wait()
        for col in range(0, hid, n_cols):
            z_rows = z_buf[:, :, pl.ds(col, n_cols)].reshape(4 * cap, n_cols)
            total = None
            for part in range(3):
                term = lax.dot_general(weights[part], z_rows, (((0,), (0,)), ((), ())), preferred_element_type=jnp.float32)
                total = term if total is None else total + term
            acc[:, pl.ds(col, n_cols)] += total
        return carry

    lax.fori_loop(0, n_dev // 2, combine_pair, 0)
    y_ref[...] = acc[...].astype(jnp.bfloat16)

    def drain(step, carry):
        z_send(step).wait_send()
        return carry

    lax.fori_loop(1, n_dev, drain, 0)


def moe_call(n_cp, n_tp, cap, h_loc, rank_rows, gate_rows, w_gate, w_up, w_down, wg_other, wu_other, wd_other):
    n_dev = n_cp * n_tp
    tok_dev, hid = h_loc.shape
    half_f = w_gate.shape[2]
    group = 4
    any_spec = pl.BlockSpec(memory_space=pl.ANY)
    vmem_spec = pl.BlockSpec(memory_space=pltpu.VMEM)
    slab = jax.ShapeDtypeStruct((n_dev, 2 * cap, hid), jnp.bfloat16)
    flops = 2 * n_dev * 2 * cap * hid * 2 * half_f * 3
    y_loc, _, _ = pl.pallas_call(
        functools.partial(moe_kernel, n_cp, n_tp, group),
        name="routed_experts",
        out_shape=(jax.ShapeDtypeStruct((tok_dev, hid), jnp.bfloat16), slab, slab),
        in_specs=[any_spec, vmem_spec, vmem_spec] + [any_spec] * 6,
        out_specs=(vmem_spec, any_spec, any_spec),
        scratch_shapes=[
            pltpu.VMEM((tok_dev, hid), jnp.bfloat16),
            pltpu.VMEM((2, 2, hid, half_f), jnp.bfloat16),
            pltpu.VMEM((2, 2, hid, half_f), jnp.bfloat16),
            pltpu.VMEM((2, 2, half_f, hid), jnp.bfloat16),
            pltpu.VMEM((n_dev, 2 * cap, hid), jnp.bfloat16),
            pltpu.VMEM((group, 2 * cap, hid), jnp.bfloat16),
            pltpu.VMEM((2, 2 * cap, hid), jnp.bfloat16),
            pltpu.VMEM((tok_dev, hid), jnp.float32),
            pltpu.VMEM((3,) + rank_rows.shape, jnp.float32),
            pltpu.SemaphoreType.DMA((6,)),
            pltpu.SemaphoreType.DMA,
            pltpu.SemaphoreType.DMA((group,)),
            pltpu.SemaphoreType.DMA,
            pltpu.SemaphoreType.DMA((n_dev,)),
            pltpu.SemaphoreType.DMA((n_dev,)),
            pltpu.SemaphoreType.DMA((n_dev,)),
            pltpu.SemaphoreType.DMA((n_dev,)),
        ],
        compiler_params=pltpu.CompilerParams(collective_id=2, has_side_effects=True, vmem_limit_bytes=VMEM_LIMIT),
        cost_estimate=pl.CostEstimate(flops=flops, bytes_accessed=2**27, transcendentals=0),
    )(h_loc, rank_rows, gate_rows, w_gate, w_up, w_down, wg_other, wu_other, wd_other)
    return y_loc


def routing_rows(ids_loc, gates_loc, n_experts):
    tok_dev = ids_loc.shape[0]
    chosen = ids_loc.T[None, :, :] == jnp.arange(n_experts, dtype=ids_loc.dtype)[:, None, None]
    mask = jnp.any(chosen, axis=1)
    gate_rows = jnp.sum(jnp.where(chosen, gates_loc.T[None, :, :], 0.0), axis=1)
    before = jnp.triu(jnp.ones((tok_dev, tok_dev), jnp.bfloat16), 1)
    rank = jnp.dot(mask.astype(jnp.bfloat16), before, preferred_element_type=jnp.float32)
    return jnp.where(mask, rank, -1.0), gate_rows


def seq_positions(cp_index, n_cp, half_len):
    chunk_len = half_len // 2
    in_half = jnp.arange(half_len)
    return jnp.where(in_half < chunk_len, cp_index * chunk_len + in_half, (2 * n_cp - 1 - cp_index) * chunk_len + in_half - chunk_len)


def attend_block(q_loc, k_blk, v_blk, q_pos, k_pos, run_max, run_sum, run_acc):
    head_dim = q_loc.shape[-1]
    scores = jnp.einsum("qgrd,kgd->grqk", q_loc, k_blk, preferred_element_type=jnp.float32) * (head_dim ** -0.5)
    allowed = q_pos[:, None] >= k_pos[None, :]
    scores = jnp.where(allowed, scores, -1e30)
    new_max = jnp.maximum(run_max, jnp.max(scores, axis=-1))
    prob_vals = jnp.exp(scores - new_max[..., None])
    rescale = jnp.exp(run_max - new_max)
    new_sum = run_sum * rescale + jnp.sum(prob_vals, axis=-1)
    new_acc = run_acc * rescale[..., None] + jnp.einsum("grqk,kgd->grqd", prob_vals.astype(jnp.bfloat16), v_blk, preferred_element_type=jnp.float32)
    return new_max, new_sum, new_acc


def solution(mesh):
    n_cp = mesh.shape["cp"]
    n_tp = mesh.shape["tp"]
    row_spec = P(("dp", "cp", "tp"), None)
    head_spec = P(None, "tp", None)
    expert_spec = P(("cp", "tp"), None, None)

    def device_step(x_loc, w_q, w_k, w_v, w_o, ids_loc, gates_loc, w_gate, w_up, w_down):
        tok_dev, hid_dim = x_loc.shape
        top_k = ids_loc.shape[1]
        kv_loc = w_k.shape[1]
        head_dim = w_q.shape[2]
        grp_size = w_q.shape[1] // kv_loc
        local_exp = w_gate.shape[0]
        n_experts = local_exp * n_cp * n_tp // 2
        capacity = top_k * tok_dev // n_experts
        cp_index = lax.axis_index("cp")
        tp_index = lax.axis_index("tp")

        x_half = lax.all_gather(x_loc, "tp", axis=0, tiled=True)
        half_len = x_half.shape[0]
        q_loc = jnp.einsum("sh,hnd->snd", x_half, w_q, preferred_element_type=jnp.float32).astype(jnp.bfloat16).reshape(half_len, kv_loc, grp_size, head_dim)
        k_cur = jnp.einsum("sh,hnd->snd", x_half, w_k, preferred_element_type=jnp.float32).astype(jnp.bfloat16)
        v_cur = jnp.einsum("sh,hnd->snd", x_half, w_v, preferred_element_type=jnp.float32).astype(jnp.bfloat16)
        q_pos = seq_positions(cp_index, n_cp, half_len)
        init_max = jnp.full((kv_loc, grp_size, half_len), -1e30, jnp.float32)
        init_sum = jnp.zeros((kv_loc, grp_size, half_len), jnp.float32)
        init_acc = jnp.zeros((kv_loc, grp_size, half_len, head_dim), jnp.float32)
        first_state = attend_block(q_loc, k_cur, v_cur, q_pos, q_pos, init_max, init_sum, init_acc)
        shift_perm = [(src_dev, (src_dev + 1) % n_cp) for src_dev in range(n_cp)]

        def kv_step(step_idx, kv_state):
            k_blk, v_blk, cur_max, cur_sum, cur_acc = kv_state
            k_blk = lax.ppermute(k_blk, "cp", shift_perm)
            v_blk = lax.ppermute(v_blk, "cp", shift_perm)
            k_pos = seq_positions((cp_index - step_idx) % n_cp, n_cp, half_len)
            cur_max, cur_sum, cur_acc = attend_block(q_loc, k_blk, v_blk, q_pos, k_pos, cur_max, cur_sum, cur_acc)
            return k_blk, v_blk, cur_max, cur_sum, cur_acc

        kv_state = lax.fori_loop(1, n_cp, kv_step, (k_cur, v_cur) + first_state)
        attn_out = (kv_state[4] / kv_state[3][..., None]).astype(jnp.bfloat16)
        w_o_view = w_o.reshape(kv_loc, grp_size, head_dim, hid_dim)
        attn_part = jnp.einsum("grqd,grdh->qh", attn_out, w_o_view, preferred_element_type=jnp.float32)
        attn_rows = lax.psum_scatter(attn_part, "tp", scatter_dimension=0, tiled=True)
        h_loc = (x_loc.astype(jnp.float32) + attn_rows).astype(jnp.bfloat16)

        rank_rows, gate_rows = routing_rows(ids_loc, gates_loc, n_experts)
        keep = local_exp // 2
        give = (1 - tp_index % 2) * keep
        pair_perm = [(dev_idx, dev_idx ^ 1) for dev_idx in range(n_tp)]
        others = [lax.ppermute(lax.dynamic_slice_in_dim(w, give, keep, axis=0), "tp", pair_perm) for w in (w_gate, w_up, w_down)]
        return moe_call(n_cp, n_tp, capacity, h_loc, rank_rows, gate_rows, w_gate, w_up, w_down, *others)

    return jax.shard_map(device_step, mesh=mesh, in_specs=(row_spec, head_spec, head_spec, head_spec, P("tp", None, None), row_spec, row_spec, expert_spec, expert_spec, expert_spec), out_specs=row_spec, check_vma=False)
```

```python
import functools

import jax
import jax.numpy as jnp
from jax import lax
from jax.experimental import pallas as pl
from jax.experimental.pallas import tpu as pltpu
from jax.sharding import PartitionSpec as P

MESH = pl.DeviceIdType.MESH
VMEM_LIMIT = 66_000_000


def peer_of(step, cp_pos, tp_pos, n_cp, n_tp, sign):
    n_x = n_tp // 2
    flip = step % 2
    off_x = (step // 2) % n_x
    off_y = (off_x + step // n_tp) % n_cp
    if sign < 0:
        off_x = n_x - off_x
        off_y = n_cp - off_y
    to_cp = (cp_pos + off_y) % n_cp
    to_tp = ((tp_pos // 2 + off_x) % n_x) * 2 + (tp_pos % 2 + flip) % 2
    return to_cp, to_tp


def mesh_id(cp_pos, tp_pos):
    return {"cp": cp_pos, "tp": tp_pos}


def moe_kernel(n_cp, n_tp, group, h_hbm, rank_ref, gate_ref, wg_hbm, wu_hbm, wd_hbm, wgx_hbm, wux_hbm, wdx_hbm,
               y_ref, rx_hbm, rz_hbm,
               h_buf, wg_buf, wu_buf, wd_buf, stage, x_buf, z_buf, acc, parts,
               w_sem, in_sem, x_sem, z_sem, sx_sem, rx_sem, sz_sem, rz_sem):
    n_dev = n_cp * n_tp
    tok_dev, hid = h_buf.shape
    cap = stage.shape[1] // 2
    half_f = wg_buf.shape[3]
    cp_pos, tp_pos = lax.axis_index("cp"), lax.axis_index("tp")
    core = tp_pos % 2

    def signal_peer(step, carry):
        to_cp, to_tp = peer_of(step, cp_pos, tp_pos, n_cp, n_tp, 1)
        pl.semaphore_signal(pltpu.get_barrier_semaphore(), inc=1, device_id=mesh_id(to_cp, to_tp), device_id_type=MESH)
        return carry

    h_copy = pltpu.make_async_copy(h_hbm, h_buf, in_sem)
    h_copy.start()
    w_copies = []
    for slot, (own, other, buf) in enumerate(((wg_hbm, wgx_hbm, wg_buf), (wu_hbm, wux_hbm, wu_buf), (wd_hbm, wdx_hbm, wd_buf))):
        w_copies.append(pltpu.make_async_copy(own.at[pl.ds(2 * core, 2)], buf.at[0], w_sem.at[2 * slot]))
        w_copies.append(pltpu.make_async_copy(other, buf.at[1], w_sem.at[2 * slot + 1]))
    for one in w_copies:
        one.start()
    lax.fori_loop(1, n_dev, signal_peer, 0)
    pl.semaphore_wait(pltpu.get_barrier_semaphore(), n_dev - 1)
    h_copy.wait()

    slots = lax.broadcasted_iota(jnp.int32, (cap, tok_dev), 0).astype(jnp.float32)

    def gather_rows(step):
        to_cp, to_tp = peer_of(step, cp_pos, tp_pos, n_cp, n_tp, 1)
        first = 2 * (to_cp * n_tp + to_tp)
        picks = [jnp.where(rank_ref[pl.ds(first + i, 1), :] == slots, 1.0, 0.0) for i in range(2)]
        pick = jnp.concatenate(picks, axis=0).astype(jnp.bfloat16)
        stage[step] = jnp.dot(pick, h_buf[...], preferred_element_type=jnp.float32).astype(jnp.bfloat16)

    def x_send(step):
        to_cp, to_tp = peer_of(step, cp_pos, tp_pos, n_cp, n_tp, 1)
        return pltpu.make_async_remote_copy(stage.at[step], rx_hbm.at[step], sx_sem.at[step], rx_sem.at[step],
                                            device_id=mesh_id(to_cp, to_tp), device_id_type=MESH)

    def z_send(step):
        to_cp, to_tp = peer_of(step, cp_pos, tp_pos, n_cp, n_tp, -1)
        return pltpu.make_async_remote_copy(stage.at[step], rz_hbm.at[step], sz_sem.at[step], rz_sem.at[step],
                                            device_id=mesh_id(to_cp, to_tp), device_id_type=MESH)

    self_x = pltpu.make_async_copy(stage.at[0], rx_hbm.at[0], rx_sem.at[0])
    self_z = pltpu.make_async_copy(stage.at[0], rz_hbm.at[0], rz_sem.at[0])

    gather_rows(0)
    gather_rows(1)
    self_x.start()

    def gather_step(step, carry):
        gather_rows(step)
        x_send(step - 1).start()
        return carry

    lax.fori_loop(2, n_dev, gather_step, 0)

    gate_all = gate_ref[...]
    high = gate_all.astype(jnp.bfloat16).astype(jnp.float32)
    rest = gate_all - high
    mid = rest.astype(jnp.bfloat16).astype(jnp.float32)
    parts[0] = high
    parts[1] = mid
    parts[2] = rest - mid
    x_send(n_dev - 1).start()
    acc[...] = h_buf[...].astype(jnp.float32)
    for one in w_copies:
        one.wait()

    rows = group * cap
    n_cols = min(512, hid)

    def expert_rows(place, i):
        x_rows = x_buf[:, pl.ds(i * cap, cap), :].reshape(rows, hid)
        hidden = []
        for half in range(2):
            gate_pre = jnp.dot(x_rows, wg_buf[half, i], preferred_element_type=jnp.float32)
            up_pre = jnp.dot(x_rows, wu_buf[half, i], preferred_element_type=jnp.float32)
            hidden.append((gate_pre * (1.0 / (1.0 + jnp.exp(-gate_pre))) * up_pre).astype(jnp.bfloat16))
        for col in range(0, hid, n_cols):
            z_rows = (jnp.dot(hidden[0], wd_buf[0, i, :, pl.ds(col, n_cols)], preferred_element_type=jnp.float32)
                      + jnp.dot(hidden[1], wd_buf[1, i, :, pl.ds(col, n_cols)], preferred_element_type=jnp.float32))
            stage[pl.ds(place, group), pl.ds(i * cap, cap), pl.ds(col, n_cols)] = z_rows.astype(jnp.bfloat16).reshape(group, cap, n_cols)

    def expert_group(g, carry):
        place = g * group
        for q in range(group):
            @pl.when(place + q == 0)
            def _():
                self_x.wait()

            @pl.when(place + q > 0)
            def _():
                x_send(place + q).wait_recv()
        for q in range(group):
            pltpu.make_async_copy(rx_hbm.at[place + q], x_buf.at[q], x_sem.at[q]).start()
        for q in range(group):
            pltpu.make_async_copy(rx_hbm.at[place + q], x_buf.at[q], x_sem.at[q]).wait()
        for q in range(group):
            @pl.when(place + q > 0)
            def _():
                x_send(place + q).wait_send()
        for i in range(2):
            expert_rows(place, i)
        for q in range(group):
            @pl.when(place + q == 0)
            def _():
                self_z.start()

            @pl.when(place + q > 0)
            def _():
                z_send(place + q).start()
        return carry

    lax.fori_loop(0, n_dev // group, expert_group, 0)

    def combine_pair(j, carry):
        @pl.when(j == 0)
        def _():
            self_z.wait()

        @pl.when(j > 0)
        def _():
            z_send(2 * j).wait_recv()
        z_send(2 * j + 1).wait_recv()
        z_copy = pltpu.make_async_copy(rz_hbm.at[pl.ds(2 * j, 2)], z_buf, z_sem)
        z_copy.start()
        weights = [[], [], []]
        for q in range(2):
            to_cp, to_tp = peer_of(2 * j + q, cp_pos, tp_pos, n_cp, n_tp, 1)
            first = 2 * (to_cp * n_tp + to_tp)
            for i in range(2):
                chosen = rank_ref[pl.ds(first + i, 1), :] == slots
                for part in range(3):
                    weights[part].append(jnp.where(chosen, parts[part, pl.ds(first + i, 1), :], 0.0))
        weights = [jnp.concatenate(w, axis=0).astype(jnp.bfloat16) for w in weights]
        z_copy.wait()
        for col in range(0, hid, n_cols):
            z_rows = z_buf[:, :, pl.ds(col, n_cols)].reshape(4 * cap, n_cols)
            total = None
            for part in range(3):
                term = lax.dot_general(weights[part], z_rows, (((0,), (0,)), ((), ())), preferred_element_type=jnp.float32)
                total = term if total is None else total + term
            acc[:, pl.ds(col, n_cols)] += total
        return carry

    lax.fori_loop(0, n_dev // 2, combine_pair, 0)
    y_ref[...] = acc[...].astype(jnp.bfloat16)

    def drain(step, carry):
        z_send(step).wait_send()
        return carry

    lax.fori_loop(1, n_dev, drain, 0)


def moe_call(n_cp, n_tp, cap, h_loc, rank_rows, gate_rows, w_gate, w_up, w_down, wg_other, wu_other, wd_other):
    n_dev = n_cp * n_tp
    tok_dev, hid = h_loc.shape
    half_f = w_gate.shape[2]
    cap = 8 * tok_dev // rank_rows.shape[0]
    group = 4
    any_spec = pl.BlockSpec(memory_space=pl.ANY)
    vmem_spec = pl.BlockSpec(memory_space=pltpu.VMEM)
    slab = jax.ShapeDtypeStruct((n_dev, 2 * cap, hid), jnp.bfloat16)
    flops = 2 * n_dev * 2 * cap * hid * 2 * half_f * 3
    y_loc, _, _ = pl.pallas_call(
        functools.partial(moe_kernel, n_cp, n_tp, group),
        name="routed_experts",
        out_shape=(jax.ShapeDtypeStruct((tok_dev, hid), jnp.bfloat16), slab, slab),
        in_specs=[any_spec, vmem_spec, vmem_spec] + [any_spec] * 6,
        out_specs=(vmem_spec, any_spec, any_spec),
        scratch_shapes=[
            pltpu.VMEM((tok_dev, hid), jnp.bfloat16),
            pltpu.VMEM((2, 2, hid, half_f), jnp.bfloat16),
            pltpu.VMEM((2, 2, hid, half_f), jnp.bfloat16),
            pltpu.VMEM((2, 2, half_f, hid), jnp.bfloat16),
            pltpu.VMEM((n_dev, 2 * cap, hid), jnp.bfloat16),
            pltpu.VMEM((group, 2 * cap, hid), jnp.bfloat16),
            pltpu.VMEM((2, 2 * cap, hid), jnp.bfloat16),
            pltpu.VMEM((tok_dev, hid), jnp.float32),
            pltpu.VMEM((3,) + rank_rows.shape, jnp.float32),
            pltpu.SemaphoreType.DMA((6,)),
            pltpu.SemaphoreType.DMA,
            pltpu.SemaphoreType.DMA((group,)),
            pltpu.SemaphoreType.DMA,
            pltpu.SemaphoreType.DMA((n_dev,)),
            pltpu.SemaphoreType.DMA((n_dev,)),
            pltpu.SemaphoreType.DMA((n_dev,)),
            pltpu.SemaphoreType.DMA((n_dev,)),
        ],
        compiler_params=pltpu.CompilerParams(collective_id=2, has_side_effects=True, vmem_limit_bytes=VMEM_LIMIT),
        cost_estimate=pl.CostEstimate(flops=flops, bytes_accessed=2**27, transcendentals=0),
    )(h_loc, rank_rows, gate_rows, w_gate, w_up, w_down, wg_other, wu_other, wd_other)
    return y_loc


def routing_rows(ids_loc, gates_loc, n_experts):
    tok_dev = ids_loc.shape[0]
    chosen = ids_loc.T[None, :, :] == jnp.arange(n_experts, dtype=ids_loc.dtype)[:, None, None]
    mask = jnp.any(chosen, axis=1)
    gate_rows = jnp.sum(jnp.where(chosen, gates_loc.T[None, :, :], 0.0), axis=1)
    before = jnp.triu(jnp.ones((tok_dev, tok_dev), jnp.bfloat16), 1)
    rank = jnp.dot(mask.astype(jnp.bfloat16), before, preferred_element_type=jnp.float32)
    return jnp.where(mask, rank, -1.0), gate_rows


def block_of(cp_pos, tp_pos, n_cp, n_tp):
    per_chunk = n_tp // 2
    late = tp_pos // per_chunk
    chunk = late * (2 * n_cp - 1 - cp_pos) + (1 - late) * cp_pos
    return chunk * per_chunk + tp_pos % per_chunk


def owner_of(block, n_cp, n_tp):
    per_chunk = n_tp // 2
    chunk = block // per_chunk
    late = chunk // n_cp
    return late * (2 * n_cp - 1 - chunk) + (1 - late) * chunk, late * per_chunk + block % per_chunk


def front_kernel(n_cp, n_tp, x_hbm, w_ref, k_hbm, vt_hbm, q_hbm, x_buf, q_st, k_st, vt_st,
                 own_sem, ring_sem, pair_sem, rx_sem, sk_sem, sv_sem, sq_sem, kv_sem, rq_sem, sf_sem, rf_sem):
    n_x = n_tp // 2
    tok_dev, hid = x_hbm.shape
    half = tok_dev // 2
    head_dim = k_hbm.shape[1]
    n_loc = q_st.shape[1]
    chunk_len = tok_dev * n_x
    cp_pos, tp_pos = lax.axis_index("cp"), lax.axis_index("tp")
    x_pos, core = tp_pos // 2, tp_pos % 2
    sibling = 2 * x_pos + 1 - core
    barrier = pltpu.get_barrier_semaphore()

    def slot_at(off, flip):
        return 2 * ((x_pos + off + n_x) % n_x) + (core + flip) % 2

    own_copy = pltpu.make_async_copy(x_hbm, x_buf.at[tp_pos], own_sem)
    own_copy.start()
    for step in (1, n_x - 1):
        pl.semaphore_signal(barrier, inc=1, device_id=mesh_id(cp_pos, slot_at(step, 0)), device_id_type=MESH)
    for step in range(1, 2 * n_cp):
        pl.semaphore_signal(barrier, inc=1, device_id=mesh_id((cp_pos + step // 2) % n_cp, 2 * x_pos + (core + step) % 2), device_id_type=MESH)
    pl.semaphore_wait(barrier, 2 * n_cp + 1)

    def own_send(part, to_tp, sem):
        rows = pl.ds(part * half, half)
        return pltpu.make_async_remote_copy(x_hbm.at[rows], x_buf.at[tp_pos, rows], sem, rx_sem.at[tp_pos, part],
                                            device_id=mesh_id(cp_pos, to_tp), device_id_type=MESH)

    def pass_on(slot, part, to_tp, sem):
        rows = pl.ds(pl.multiple_of(part * half, half), half)
        return pltpu.make_async_remote_copy(x_buf.at[slot, rows], x_buf.at[slot, rows], sem, rx_sem.at[slot, part],
                                            device_id=mesh_id(cp_pos, to_tp), device_id_type=MESH)

    for i, (part, off) in enumerate(((0, 1), (1, -1), (1, 1), (0, -1))):
        own_send(part, slot_at(off, 0), ring_sem.at[i]).start()
    for part in range(2):
        own_send(part, sibling, pair_sem.at[part]).start()

    def place_of(step):
        wave, other, side = step // 4, (step // 2) % 2, step % 2
        near = ((wave + 1) // 2) % 2
        swap = (wave // 2) * (1 - wave // 3)
        off = near * (2 * side - 1) + 2 * (wave // 3)
        return slot_at(off, other), side + swap * (1 - 2 * side), off

    def outputs_of(step):
        slot, part, _ = place_of(step)
        block = block_of(cp_pos, slot, n_cp, n_tp)
        pos = block * tok_dev + part * half
        q_core = ((block % 4 + 1) // 2) % 2
        q_pos = (2 * (block // 4) + (block % 4) // 2) * tok_dev + part * half
        pos, q_pos = pl.multiple_of(pos, half), pl.multiple_of(q_pos, half)
        for i in range(n_loc):
            to_cp = n_loc * core + i
            for src, dst, s_sem, r_sem, to_core in (
                (k_st.at[step, i], k_hbm.at[pl.ds(pos, half)], sk_sem.at[i], kv_sem.at[cp_pos], 0),
                (vt_st.at[step, i], vt_hbm.at[:, pl.ds(pos, half)], sv_sem.at[i], kv_sem.at[cp_pos], 1),
                (q_st.at[step, i], q_hbm.at[pl.ds(q_pos, half)], sq_sem.at[i, q_core], rq_sem.at[cp_pos], q_core),
            ):
                here = jnp.logical_and(to_cp == cp_pos, to_core == core)

                @pl.when(here)
                def _():
                    pltpu.make_async_copy(src, dst, r_sem).start()

                @pl.when(jnp.logical_not(here))
                def _():
                    pltpu.make_async_remote_copy(src, dst, s_sem, r_sem, device_id=mesh_id(to_cp, 2 * x_pos + to_core),
                                                 device_id_type=MESH).start()

    def project(step, carry):
        slot, part, off = place_of(step)
        wave, other, side = step // 4, (step // 2) % 2, step % 2

        @pl.when(step == 0)
        def _():
            own_copy.wait()

        @pl.when(step > 1)
        def _():
            pass_on(slot, part, sibling, pair_sem.at[0]).wait_recv()

        @pl.when(jnp.logical_and(wave > 0, other == 0))
        def _():
            @pl.when(wave == 1)
            def _():
                pass_on(slot, part, slot_at(-off, 0), ring_sem.at[4 + side]).start()
            pass_on(slot, part, sibling, pair_sem.at[2 * wave + side]).start()

        x_rows = x_buf[slot, pl.ds(pl.multiple_of(part * half, half), half), :]
        qkv = jnp.dot(x_rows, w_ref[...], preferred_element_type=jnp.float32)
        for i in range(n_loc):
            q_st[step, i] = qkv[:, i * head_dim:(i + 1) * head_dim].astype(jnp.bfloat16)
            k_st[step, i] = qkv[:, (n_loc + i) * head_dim:(n_loc + i + 1) * head_dim].astype(jnp.bfloat16)
            vt_st[step, i] = qkv[:, (2 * n_loc + i) * head_dim:(2 * n_loc + i + 1) * head_dim].T.astype(jnp.bfloat16)

        @pl.when(step > 0)
        def _():
            outputs_of(step - 1)
        return carry

    n_steps = 2 * n_tp
    lax.fori_loop(0, n_steps, project, 0)
    outputs_of(n_steps - 1)

    def whole(ref, count, sem):
        return pltpu.make_async_copy(ref.at[pl.ds(0, count)], ref.at[pl.ds(0, count)], sem)

    def forward(y, place, core_id):
        chunk = y if place == 0 else 2 * n_cp - 1 - y
        cols = pl.ds(chunk * chunk_len, chunk_len)
        ref = k_hbm.at[cols] if core_id == 0 else vt_hbm.at[:, cols]
        return pltpu.make_async_remote_copy(ref, ref, sf_sem.at[2 * y + place], rf_sem.at[2 * y + place],
                                            device_id=mesh_id(cp_pos, sibling), device_id_type=MESH)

    for y in range(n_cp):
        whole(k_hbm, 2 * chunk_len, kv_sem.at[y]).wait()
        for core_id in range(2):
            @pl.when(core == core_id)
            def _():
                for place in range(2):
                    forward(y, place, core_id).start()
    for y in range(n_cp):
        whole(q_hbm, chunk_len, rq_sem.at[y]).wait()
    for i in range(4):
        own_send(0, sibling, ring_sem.at[i]).wait_send()
    for i in range(2):
        own_send(0, sibling, ring_sem.at[4 + i]).wait_send()
    for i in range(8):
        own_send(0, sibling, pair_sem.at[i]).wait_send()
    for i in range(n_loc):
        to_cp = n_loc * core + i
        for sem, to_core, count in ((sk_sem.at[i], 0, 2 * chunk_len), (sv_sem.at[i], 1, 2 * chunk_len),
                                    (sq_sem.at[i, 0], 0, chunk_len), (sq_sem.at[i, 1], 1, chunk_len)):
            @pl.when(jnp.logical_not(jnp.logical_and(to_cp == cp_pos, to_core == core)))
            def _():
                whole(k_hbm, count, sem).wait()
    for core_id in range(2):
        @pl.when(core == core_id)
        def _():
            for y in range(n_cp):
                for place in range(2):
                    forward(y, place, core_id).wait_send()
                    forward(y, place, 1 - core_id).wait_recv()


def front_call(n_cp, n_tp, x_loc, w_qkv, head_dim, n_loc):
    tok_dev, hid = x_loc.shape
    half = tok_dev // 2
    seq = tok_dev * n_cp * n_tp
    any_spec = pl.BlockSpec(memory_space=pl.ANY)
    n_steps = 2 * n_tp
    return pl.pallas_call(
        functools.partial(front_kernel, n_cp, n_tp),
        name="gather_project",
        out_shape=(jax.ShapeDtypeStruct((seq, head_dim), jnp.bfloat16), jax.ShapeDtypeStruct((head_dim, seq), jnp.bfloat16),
                   jax.ShapeDtypeStruct((seq // 2, head_dim), jnp.bfloat16)),
        in_specs=[any_spec, pl.BlockSpec(memory_space=pltpu.VMEM)],
        out_specs=(any_spec, any_spec, any_spec),
        scratch_shapes=[
            pltpu.VMEM((n_tp, tok_dev, hid), jnp.bfloat16),
            pltpu.VMEM((n_steps, n_loc, half, head_dim), jnp.bfloat16),
            pltpu.VMEM((n_steps, n_loc, half, head_dim), jnp.bfloat16),
            pltpu.VMEM((n_steps, n_loc, head_dim, half), jnp.bfloat16),
            pltpu.SemaphoreType.DMA,
            pltpu.SemaphoreType.DMA((6,)),
            pltpu.SemaphoreType.DMA((8,)),
            pltpu.SemaphoreType.DMA((n_tp, 2)),
            pltpu.SemaphoreType.DMA((n_loc,)),
            pltpu.SemaphoreType.DMA((n_loc,)),
            pltpu.SemaphoreType.DMA((n_loc, 2)),
            pltpu.SemaphoreType.DMA((n_cp,)),
            pltpu.SemaphoreType.DMA((n_cp,)),
            pltpu.SemaphoreType.DMA((2 * n_cp,)),
            pltpu.SemaphoreType.DMA((2 * n_cp,)),
        ],
        compiler_params=pltpu.CompilerParams(collective_id=0, has_side_effects=True, vmem_limit_bytes=VMEM_LIMIT),
        cost_estimate=pl.CostEstimate(flops=2 * n_tp * tok_dev * hid * w_qkv.shape[1], bytes_accessed=2**26, transcendentals=0),
    )(x_loc, w_qkv)


def attend_kernel(n_cp, n_tp, k_hbm, vt_hbm, q_hbm, x_hbm, wo_hbm, wg_hbm, wu_hbm, wd_hbm,
                  h_ref, o_hbm, wgx_hbm, wux_hbm, wdx_hbm,
                  k_buf, vt_buf, q_buf, qt_buf, o_st, o_buf, wo_buf, x_buf, s_even, s_odd, acc, m_ref, l_ref,
                  in_sem, so_sem, ro_sem, swo_sem, rwo_sem, sw_sem, rw_sem, o_sem):
    n_dev = n_cp * n_tp
    n_x = n_tp // 2
    tok_dev, hid = x_buf.shape
    head_dim = k_buf.shape[1]
    n_heads = o_buf.shape[0]
    cp_pos, tp_pos = lax.axis_index("cp"), lax.axis_index("tp")
    x_pos, core = tp_pos // 2, tp_pos % 2
    head = n_cp * x_pos + cp_pos
    scale = (head_dim ** -0.5) * 1.4426950408889634
    barrier = pltpu.get_barrier_semaphore()

    loads = [pltpu.make_async_copy(src, dst, in_sem.at[i]) for i, (src, dst) in enumerate(
        ((q_hbm, q_buf), (k_hbm, k_buf), (vt_hbm, vt_buf), (x_hbm, x_buf), (wo_hbm, wo_buf.at[tp_pos])))]
    for one in loads:
        one.start()

    def signal_peer(step, carry):
        to_cp, to_tp = peer_of(step, cp_pos, tp_pos, n_cp, n_tp, 1)
        pl.semaphore_signal(pltpu.get_barrier_semaphore(), inc=1, device_id=mesh_id(to_cp, to_tp), device_id_type=MESH)
        return carry

    lax.fori_loop(1, n_dev, signal_peer, 0)
    pl.semaphore_wait(barrier, n_dev - 1)

    def wo_send(step):
        return pltpu.make_async_remote_copy(wo_hbm, wo_buf.at[tp_pos], swo_sem.at[step], rwo_sem.at[step],
                                            device_id=mesh_id(cp_pos, (tp_pos + step) % n_tp), device_id_type=MESH)

    def wo_arrival(step):
        return pltpu.make_async_remote_copy(wo_hbm, wo_buf.at[(tp_pos + n_tp - step) % n_tp], swo_sem.at[step], rwo_sem.at[step],
                                            device_id=mesh_id(cp_pos, tp_pos), device_id_type=MESH)

    keep = wgx_hbm.shape[0]
    swaps = [pltpu.make_async_remote_copy(src.at[pl.ds((1 - core) * keep, keep)], dst, sw_sem.at[i], rw_sem.at[i],
                                          device_id=mesh_id(cp_pos, 2 * x_pos + 1 - core), device_id_type=MESH)
             for i, (src, dst) in enumerate(((wg_hbm, wgx_hbm), (wu_hbm, wux_hbm), (wd_hbm, wdx_hbm)))]
    for step in range(1, n_tp):
        wo_send(step).start()
    for one in swaps:
        one.start()
    for one in loads[:3]:
        one.wait()

    def update(s_vals, s_top, v_cols, lo, width):
        cols = pl.ds(lo, width)
        m_old = m_ref[:, cols]
        m_new = jnp.maximum(m_old, s_top)
        prob = jnp.exp2((s_vals - m_new) * scale)
        shrink = jnp.exp2((m_old - m_new) * scale)
        m_ref[:, cols] = m_new
        l_ref[:, cols] = l_ref[:, cols] * shrink + jnp.sum(prob, axis=0, keepdims=True)
        acc[:, cols] = acc[:, cols] * shrink + jnp.dot(v_cols, prob.astype(jnp.bfloat16), preferred_element_type=jnp.float32)

    def keys_at(block):
        return k_buf[pl.ds(pl.multiple_of(block * tok_dev, tok_dev), tok_dev), :]

    def values_at(block):
        return vt_buf[:, pl.ds(pl.multiple_of(block * tok_dev, tok_dev), tok_dev)]

    def query_pair(g, carry):
        q_rows = q_buf[pl.ds(pl.multiple_of(g * 2 * tok_dev, 2 * tok_dev), 2 * tok_dev), :]
        qt_buf[...] = q_rows.astype(jnp.float32).T.astype(jnp.bfloat16)
        m_ref[...] = jnp.full_like(m_ref, -1e30)
        l_ref[...] = jnp.zeros_like(l_ref)
        acc[...] = jnp.zeros_like(acc)
        for r in range(2):
            lo = r * tok_dev
            inner = (1 - core) * 3 * r + core * (1 + r)

            def near_scores(block):
                return jnp.dot(keys_at(block), qt_buf[:, pl.ds(lo, tok_dev)], preferred_element_type=jnp.float32)

            s_vals = near_scores(4 * g + inner)
            key_id = lax.broadcasted_iota(jnp.int32, s_vals.shape, 0)
            query_id = lax.broadcasted_iota(jnp.int32, s_vals.shape, 1)
            s_vals = jnp.where(key_id <= query_id, s_vals, -1e30)
            update(s_vals, jnp.max(s_vals, axis=0, keepdims=True), values_at(4 * g + inner), lo, tok_dev)

            def near_block(j, inner_carry):
                s_near = near_scores(4 * g + j)
                update(s_near, jnp.max(s_near, axis=0, keepdims=True), values_at(4 * g + j), lo, tok_dev)
                return inner_carry

            lax.fori_loop(0, inner, near_block, 0)

        def far_scores(block, s_ref):
            s_vals = jnp.dot(keys_at(block), qt_buf[...], preferred_element_type=jnp.float32)
            s_ref[...] = s_vals
            return jnp.max(s_vals, axis=0, keepdims=True)

        def far_pair(n, top_even):
            top_odd = far_scores(2 * n + 1, s_odd)
            update(s_even[...], top_even, values_at(2 * n), 0, 2 * tok_dev)
            top_next = far_scores(2 * n + 2, s_even)
            update(s_odd[...], top_odd, values_at(2 * n + 1), 0, 2 * tok_dev)
            return top_next

        lax.fori_loop(0, 2 * g, far_pair, far_scores(0, s_even))
        out = (acc[...] / l_ref[...]).T.astype(jnp.bfloat16)
        for r in range(2):
            o_st[2 * g + r] = out[r * tok_dev:(r + 1) * tok_dev]
            o_push(2 * g + r, "start")
        return carry

    def o_push(index, what):
        block = 4 * (index // 2) + (1 - core) * 3 * (index % 2) + core * (1 + index % 2)
        to_cp, to_tp = owner_of(block, n_cp, n_tp)
        here = jnp.logical_and(to_cp == cp_pos, to_tp == tp_pos)
        if what == "start":
            @pl.when(here)
            def _():
                pltpu.make_async_copy(o_st.at[index], o_hbm.at[head], ro_sem.at[head]).start()

        @pl.when(jnp.logical_not(here))
        def _():
            copy = pltpu.make_async_remote_copy(o_st.at[index], o_hbm.at[head], so_sem.at[index], ro_sem.at[head],
                                                device_id=mesh_id(to_cp, to_tp), device_id_type=MESH)
            if what == "start":
                copy.start()
            else:
                copy.wait_send()

    lax.fori_loop(0, n_dev // 4, query_pair, 0)

    for step in range(1, n_tp):
        wo_arrival(step).wait_recv()
    for one in loads[3:]:
        one.wait()
    for j in range(n_heads):
        pltpu.make_async_copy(o_hbm.at[j], o_hbm.at[j], ro_sem.at[j]).wait()
    o_load = pltpu.make_async_copy(o_hbm, o_buf, o_sem)
    o_load.start()
    o_load.wait()
    o_rows = jnp.concatenate([o_buf[j] for j in range(n_heads)], axis=1)
    n_cols = min(512, hid)

    for col in range(0, hid, n_cols):
        cols = pl.ds(col, n_cols)
        w_cols = wo_buf[:, :, cols].reshape(n_heads * head_dim, n_cols)
        h_ref[:, cols] = (x_buf[:, cols].astype(jnp.float32) + jnp.dot(o_rows, w_cols, preferred_element_type=jnp.float32)).astype(jnp.bfloat16)

    for step in range(1, n_tp):
        wo_send(step).wait_send()
    for one in swaps:
        one.wait()

    def drain(index, carry):
        o_push(index, "wait")
        return carry

    lax.fori_loop(0, n_dev // 2, drain, 0)


def attend_call(n_cp, n_tp, k_all, vt_all, q_all, x_loc, wo_loc, w_gate, w_up, w_down):
    n_dev = n_cp * n_tp
    tok_dev, hid = x_loc.shape
    seq, head_dim = k_all.shape
    n_heads = n_tp * wo_loc.shape[0] // head_dim
    keep = w_gate.shape[0] // 2
    any_spec = pl.BlockSpec(memory_space=pl.ANY)
    bf16 = jnp.bfloat16
    h_loc, _, wg_other, wu_other, wd_other = pl.pallas_call(
        functools.partial(attend_kernel, n_cp, n_tp),
        name="attend_heads",
        out_shape=(jax.ShapeDtypeStruct((tok_dev, hid), bf16), jax.ShapeDtypeStruct((n_heads, tok_dev, head_dim), bf16))
        + tuple(jax.ShapeDtypeStruct((keep,) + w.shape[1:], bf16) for w in (w_gate, w_up, w_down)),
        in_specs=[any_spec] * 8,
        out_specs=(pl.BlockSpec(memory_space=pltpu.VMEM),) + (any_spec,) * 4,
        scratch_shapes=[
            pltpu.VMEM((seq, head_dim), bf16),
            pltpu.VMEM((head_dim, seq), bf16),
            pltpu.VMEM((seq // 2, head_dim), bf16),
            pltpu.VMEM((head_dim, 2 * tok_dev), bf16),
            pltpu.VMEM((n_dev // 2, tok_dev, head_dim), bf16),
            pltpu.VMEM((n_heads, tok_dev, head_dim), bf16),
            pltpu.VMEM((n_tp,) + wo_loc.shape, bf16),
            pltpu.VMEM((tok_dev, hid), bf16),
            pltpu.VMEM((tok_dev, 2 * tok_dev), jnp.float32),
            pltpu.VMEM((tok_dev, 2 * tok_dev), jnp.float32),
            pltpu.VMEM((head_dim, 2 * tok_dev), jnp.float32),
            pltpu.VMEM((1, 2 * tok_dev), jnp.float32),
            pltpu.VMEM((1, 2 * tok_dev), jnp.float32),
            pltpu.SemaphoreType.DMA((5,)),
            pltpu.SemaphoreType.DMA((n_dev // 2,)),
            pltpu.SemaphoreType.DMA((n_heads,)),
            pltpu.SemaphoreType.DMA((n_tp,)),
            pltpu.SemaphoreType.DMA((n_tp,)),
            pltpu.SemaphoreType.DMA((3,)),
            pltpu.SemaphoreType.DMA((3,)),
            pltpu.SemaphoreType.DMA,
        ],
        compiler_params=pltpu.CompilerParams(collective_id=1, has_side_effects=True, vmem_limit_bytes=VMEM_LIMIT),
        cost_estimate=pl.CostEstimate(flops=2 * seq * seq * head_dim // 2, bytes_accessed=2**26, transcendentals=seq * seq // 4),
    )(k_all, vt_all, q_all, x_loc, wo_loc, w_gate, w_up, w_down)
    return h_loc, wg_other, wu_other, wd_other


def solution(mesh):
    n_cp = mesh.shape["cp"]
    n_tp = mesh.shape["tp"]
    row_spec = P(("dp", "cp", "tp"), None)
    head_spec = P(None, "tp", None)
    expert_spec = P(("cp", "tp"), None, None)

    def device_step(x_loc, w_q, w_k, w_v, w_o, ids_loc, gates_loc, w_gate, w_up, w_down):
        tok_dev, hid_dim = x_loc.shape
        n_loc, head_dim = w_q.shape[1:]
        n_experts = w_gate.shape[0] * n_cp * n_tp // 2
        capacity = ids_loc.shape[1] * tok_dev // n_experts
        w_qkv = jnp.concatenate([w.reshape(hid_dim, n_loc * head_dim) for w in (w_q, w_k, w_v)], axis=1)
        rank_rows, gate_rows = routing_rows(ids_loc, gates_loc, n_experts)
        k_all, vt_all, q_all = front_call(n_cp, n_tp, x_loc, w_qkv, head_dim, n_loc)
        h_loc, *others = attend_call(n_cp, n_tp, k_all, vt_all, q_all, x_loc, w_o.reshape(n_loc * head_dim, hid_dim), w_gate, w_up, w_down)
        return moe_call(n_cp, n_tp, capacity, h_loc, rank_rows, gate_rows, w_gate, w_up, w_down, *others)

    return jax.shard_map(device_step, mesh=mesh, in_specs=(row_spec, head_spec, head_spec, head_spec, P("tp", None, None), row_spec, row_spec, expert_spec, expert_spec, expert_spec), out_specs=row_spec, check_vma=False)
```

```python
import functools

import jax
import jax.numpy as jnp
from jax import lax
from jax.experimental import pallas as pl
from jax.experimental.pallas import tpu as pltpu
from jax.sharding import PartitionSpec as P

MESH = pl.DeviceIdType.MESH
PAIR = 2
BOTH = range(PAIR)
ROWS_ROWS = (((0,), (0,)), ((), ()))
VMEM_LIMIT = 66_000_000
PLACES = ((0, 0), (0, 1), (1, 0), (0, -1), (-1, 0), (1, 1), (0, 2), (2, 0), (1, 2), (2, 1), (2, -1), (-1, 2), (2, 2), (1, -1), (-1, 1), (-1, -1))
FIRST_FAR, N_FAR = 6, 7
SOURCES = (0, -1, 1, 2)


def peer_of(step, cp_pos, tp_pos, n_cp, n_tp):
    n_x = n_tp // PAIR
    off_x = (step // PAIR) % n_x
    off_y = (off_x + step // n_tp) % n_cp
    return (cp_pos + off_y) % n_cp, ((tp_pos // PAIR + off_x) % n_x) * 2 + (tp_pos % PAIR + step % PAIR) % PAIR


def mesh_id(cp_pos, tp_pos):
    return {"cp": cp_pos, "tp": tp_pos}


def enter_all(n_cp, n_tp):
    cp_pos, tp_pos = lax.axis_index("cp"), lax.axis_index("tp")

    def signal_peer(step, carry):
        to_cp, to_tp = peer_of(step, cp_pos, tp_pos, n_cp, n_tp)
        pl.semaphore_signal(pltpu.get_barrier_semaphore(), inc=1, device_id=mesh_id(to_cp, to_tp), device_id_type=MESH)
        return carry

    lax.fori_loop(1, n_cp * n_tp, signal_peer, 0)
    pl.semaphore_wait(pltpu.get_barrier_semaphore(), n_cp * n_tp - 1)


def pick(values, index):
    out = values[-1]
    for k, value in enumerate(values[:-1]):
        out = jnp.where(index == k, value, out)
    return out


def moe_kernel(n_cp, n_tp, group, h_hbm, rank_hbm, near_hbm, gate_ref, wg_hbm, wu_hbm, wd_hbm, wgx_hbm, wux_hbm, wdx_hbm,
               y_ref, rx_hbm, rl_hbm, rz_hbm, zl_hbm,
               h_buf, rank_buf, wg_buf, wu_buf, wd_buf, ring, own_stage, z_ring, x_buf, z_buf, acc, parts,
               w_sem, rank_sem, in_sem, x_sem, z_sem, hs_sem, hr_sem, ss_sem, rx_sem, rl_sem, fl_sem, sz_sem, rz_sem, zl_sem, fz_sem):
    n_x = n_tp // PAIR
    tok_dev, half_hid = h_buf.shape[2:]
    hid = PAIR * half_hid
    cap = ring.shape[3] // PAIR
    cp_pos, tp_pos = lax.axis_index("cp"), lax.axis_index("tp")
    x_pos, core = tp_pos // PAIR, tp_pos % PAIR
    half_tok = tok_dev // PAIR

    def at(off_y, off_x, flip):
        return (cp_pos + off_y + n_cp) % n_cp, PAIR * ((x_pos + off_x + n_x) % n_x) + (core + flip) % PAIR

    def line(place):
        return place[0] * n_tp + place[1]

    def send(src, dst, s_sem, r_sem, place):
        return pltpu.make_async_remote_copy(src, dst, s_sem, r_sem, device_id=mesh_id(*place), device_id_type=MESH)

    def await_bytes(ref, sem):
        pltpu.make_async_copy(ref, ref, sem).wait()

    h_loads = [pltpu.make_async_copy(h_hbm.at[part], h_buf.at[part, 0], in_sem.at[part]) for part in BOTH]
    rank_loads = []
    for part in BOTH:
        rank_loads.append(pltpu.make_async_copy(rank_hbm, rank_buf.at[part, 0], rank_sem.at[PAIR * part]))
        rank_loads.append(pltpu.make_async_copy(near_hbm.at[part, pl.ds(1, 3)], rank_buf.at[part, pl.ds(1, 3)], rank_sem.at[PAIR * part + 1]))
    w_loads = []
    for slot, (own, other, buf) in enumerate(((wg_hbm, wgx_hbm, wg_buf), (wu_hbm, wux_hbm, wu_buf), (wd_hbm, wdx_hbm, wd_buf))):
        w_loads.append(pltpu.make_async_copy(own.at[pl.ds(PAIR * core, 2)], buf.at[0], w_sem.at[PAIR * slot]))
        w_loads.append(pltpu.make_async_copy(other, buf.at[1], w_sem.at[PAIR * slot + 1]))
    for one in h_loads + rank_loads:
        one.start()
    enter_all(n_cp, n_tp)

    def along(part, off):
        return at(off, 0, 0) if part == 0 else at(0, off, 0)

    def across(part, off, flip):
        return at(0, off, flip) if part == 0 else at(off, 0, flip)

    def rows_of(piece):
        return pl.ds(piece * half_tok, half_tok)

    def spread(part, i):
        piece, off, slot = ((0, 1, 1), (1, -1, 2), (1, 1, 1), (0, -1, 2), (0, 1, 3), (1, -1, 3))[i]
        rows = rows_of(piece)
        src = h_hbm.at[part, rows] if i < 4 else h_buf.at[part, 1 if i == 4 else 2, rows]
        return send(src, h_buf.at[part, slot, rows], hs_sem.at[part, i], hr_sem.at[part, slot, piece], along(part, off))

    def await_h(part, slot, piece):
        await_bytes(h_buf.at[part, slot, rows_of(piece)], hr_sem.at[part, slot, piece])

    for i in range(4):
        for part in BOTH:
            spread(part, i).start()
    for one in w_loads:
        one.start()
    for one in h_loads + rank_loads:
        one.wait()

    slots = lax.broadcasted_iota(jnp.int32, (cap, tok_dev), 0).astype(jnp.float32)

    def gather_rows(part, stage, m):
        turn = m // PAIR
        off = turn + (turn // PAIR) * (5 - PAIR * turn)
        first = PAIR * line(across(part, off, m % PAIR))
        chosen = [jnp.where(rank_buf[part, stage, pl.ds(first + i, 1), :] == slots, 1.0, 0.0) for i in BOTH]
        chosen = jnp.concatenate(chosen, axis=0).astype(jnp.bfloat16)
        return jnp.dot(chosen, h_buf[part, stage], preferred_element_type=jnp.float32).astype(jnp.bfloat16)

    def source_line(part, stage, off):
        a = SOURCES[stage]
        return line(at(a, off, 0) if part == 0 else at(off, a, 0))

    def await_ring(part, stage):
        def one(m, carry):
            await_bytes(ring.at[part, stage % PAIR, m], ss_sem.at[part, stage % PAIR, m])
            return carry
        lax.fori_loop(1, 8, one, 0)

    def own_copy(part, stage):
        src_line = source_line(part, stage, 0)
        return pltpu.make_async_copy(own_stage.at[part, stage], rx_hbm.at[part, src_line], rx_sem.at[part, src_line])

    def run_stage(part, stage):
        side = stage % PAIR
        if stage >= 2:
            await_ring(part, stage)
        own_stage[part, stage] = gather_rows(part, stage, 0)

        def fill(m, carry):
            ring[part, side, m] = gather_rows(part, stage, m)
            return carry

        lax.fori_loop(1, 8, fill, 0)
        src_line = source_line(part, stage, 0)
        own_copy(part, stage).start()
        for m in (6, 7):
            for way, off in ((0, 1), (1, -1)):
                send(ring.at[part, side, m, pl.ds(way * cap, cap)], rl_hbm.at[part, way, stage, m % PAIR], ss_sem.at[part, side, m],
                     rl_sem.at[part, way, stage, m % PAIR], across(part, off, 0)).start()
        for m, off in ((2, 1), (4, -1), (3, 1), (5, -1), (1, 0)):
            send(ring.at[part, side, m], rx_hbm.at[part, src_line], ss_sem.at[part, side, m], rx_sem.at[part, src_line],
                 across(part, off, m % PAIR)).start()

    def relay(part, stage, way, flip):
        off = 1 - PAIR * way
        src_line = source_line(part, stage, -off)
        return send(rl_hbm.at[part, way, stage, flip], rx_hbm.at[part, src_line, pl.ds(way * cap, cap)], fl_sem.at[part, way, stage, flip],
                    rx_sem.at[part, src_line], across(part, off, flip))

    def run_relays(stage):
        for flip in BOTH:
            for way in BOTH:
                for part in BOTH:
                    await_bytes(rl_hbm.at[part, way, stage, flip], rl_sem.at[part, way, stage, flip])
                    relay(part, stage, way, flip).start()

    for part in BOTH:
        run_stage(part, 0)
    for part in BOTH:
        await_h(part, 1, 0)
        spread(part, 4).start()
    for part in BOTH:
        await_h(part, 2, 1)
        spread(part, 5).start()
    for part in BOTH:
        await_h(part, 1, 1)
        run_stage(part, 1)
    gate_all = gate_ref[...]
    high = gate_all.astype(jnp.bfloat16).astype(jnp.float32)
    rest = gate_all - high
    mid = rest.astype(jnp.bfloat16).astype(jnp.float32)
    parts[0] = high
    parts[1] = mid
    parts[2] = rest - mid
    for part in BOTH:
        acc[:, part * half_hid:(part + 1) * half_hid] = h_buf[part, 0].astype(jnp.float32)
    run_relays(0)
    for part in BOTH:
        await_h(part, 2, 0)
        run_stage(part, 2)
    run_relays(1)
    for part in BOTH:
        await_h(part, 3, 0)
        await_h(part, 3, 1)
        run_stage(part, 3)
    run_relays(2)
    for one in w_loads:
        one.wait()

    rows = group * cap
    n_cols = min(512, hid)
    n_groups = len(PLACES) // PAIR

    def expert_rows(slot, i):
        x_rows = x_buf[:, pl.ds(i * cap, cap), :].reshape(rows, hid)
        hidden = []
        for half in BOTH:
            gate_pre = jnp.dot(x_rows, wg_buf[half, i], preferred_element_type=jnp.float32)
            up_pre = jnp.dot(x_rows, wu_buf[half, i], preferred_element_type=jnp.float32)
            hidden.append((gate_pre * (1.0 / (1.0 + jnp.exp(-gate_pre))) * up_pre).astype(jnp.bfloat16))
        for col in range(0, hid, n_cols):
            z_rows = (jnp.dot(hidden[0], wd_buf[0, i, :, pl.ds(col, n_cols)], preferred_element_type=jnp.float32)
                      + jnp.dot(hidden[1], wd_buf[1, i, :, pl.ds(col, n_cols)], preferred_element_type=jnp.float32))
            z_ring[slot, :, pl.ds(i * cap, cap), pl.ds(col, n_cols)] = z_rows.astype(jnp.bfloat16).reshape(group, cap, n_cols)

    def place_at(g, q):
        off_y = pick([PLACES[PAIR * k + q // PAIR][0] for k in range(n_groups)], g)
        off_x = pick([PLACES[PAIR * k + q // PAIR][1] for k in range(n_groups)], g)
        return off_y, off_x

    my_line = line((cp_pos, tp_pos))

    def await_slot(slot):
        for q in range(group):
            await_bytes(z_ring.at[slot, q], sz_sem.at[slot, q])

    def expert_group(g, carry):
        slot = g % 3

        @pl.when(g == 2)
        def _():
            run_relays(3)

        sources = [line(at(*place_at(g, q), q % PAIR)) for q in range(group)]
        loads = []
        for q in range(group):
            for part in BOTH:
                await_bytes(rx_hbm.at[part, sources[q]], rx_sem.at[part, sources[q]])
                loads.append(pltpu.make_async_copy(rx_hbm.at[part, sources[q]], x_buf.at[q, :, pl.ds(part * half_hid, half_hid)], x_sem.at[part, q]))
                loads[-1].start()

        @pl.when(g >= 3)
        def _():
            await_slot(slot)
        for one in loads:
            one.wait()
        for i in BOTH:
            expert_rows(slot, i)
        for q in range(group):
            off_y, off_x = place_at(g, q)
            far = jnp.logical_or(off_y == 2, off_x == 2)
            alone = jnp.logical_and(g == 0, q == 0)

            @pl.when(alone)
            def _():
                pltpu.make_async_copy(z_ring.at[slot, q], rz_hbm.at[my_line], sz_sem.at[slot, q]).start()

            @pl.when(jnp.logical_not(jnp.logical_or(far, alone)))
            def _():
                send(z_ring.at[slot, q], rz_hbm.at[my_line], sz_sem.at[slot, q], rz_sem.at[my_line], at(off_y, off_x, q % PAIR)).start()

            @pl.when(far)
            def _():
                index = PAIR * g + q // PAIR - FIRST_FAR
                lead_y, lead_x = jnp.where(off_y == 2, 1, 0), jnp.where(off_x == 2, 1, 0)
                for way in BOTH:
                    sign = 1 - PAIR * way
                    send(z_ring.at[slot, q, pl.ds(way * cap, cap)], zl_hbm.at[index, q % PAIR, way], sz_sem.at[slot, q],
                         zl_sem.at[index, q % PAIR, way], at(sign * lead_y, sign * lead_x, 0)).start()
        return carry

    lax.fori_loop(0, n_groups, expert_group, 0)

    def z_relay(index, flip, way):
        off_y, off_x = PLACES[FIRST_FAR + index]
        sign = 1 - PAIR * way
        lead_y, lead_x = sign * (off_y == 2), sign * (off_x == 2)
        from_line = line(at(-lead_y, -lead_x, 0))
        to_y = sign if off_y == 2 else off_y
        to_x = sign if off_x == 2 else off_x
        return send(zl_hbm.at[index, flip, way], rz_hbm.at[from_line, pl.ds(way * cap, cap)], fz_sem.at[index, flip, way],
                    rz_sem.at[from_line], at(to_y, to_x, flip))

    def run_z_relays(first, count):
        for index in range(first, first + count):
            for flip in BOTH:
                for way in BOTH:
                    await_bytes(zl_hbm.at[index, flip, way], zl_sem.at[index, flip, way])
                    z_relay(index, flip, way).start()

    def combine(p, carry):
        off_y, off_x = pick([a for a, _ in PLACES], p), pick([b for _, b in PLACES], p)
        homes = [line(at(-off_y, -off_x, q)) for q in BOTH]
        loads = []
        for q in BOTH:
            @pl.when(jnp.logical_or(p > 0, q > 0))
            def _():
                await_bytes(rz_hbm.at[homes[q]], rz_sem.at[homes[q]])
            loads.append(pltpu.make_async_copy(rz_hbm.at[homes[q]], z_buf.at[q], z_sem.at[q]))
            loads[-1].start()
        weights = [[], [], []]
        for q in BOTH:
            for i in BOTH:
                row = pl.ds(PAIR * homes[q] + i, 1)
                chosen = rank_buf[0, 0, row, :] == slots
                for part in range(3):
                    weights[part].append(jnp.where(chosen, parts[part, row, :], 0.0))
        weights = [jnp.concatenate(w, axis=0).astype(jnp.bfloat16) for w in weights]
        for one in loads:
            one.wait()
        for col in range(0, hid, n_cols):
            z_rows = z_buf[:, :, pl.ds(col, n_cols)].reshape(4 * cap, n_cols)
            total = None
            for part in range(3):
                term = lax.dot_general(weights[part], z_rows, ROWS_ROWS, preferred_element_type=jnp.float32)
                total = term if total is None else total + term
            acc[:, pl.ds(col, n_cols)] += total
        return carry

    run_z_relays(0, 4)
    lax.fori_loop(0, FIRST_FAR, combine, 0)
    run_z_relays(4, N_FAR - 4)

    def combine_late(j, carry):
        first_late = FIRST_FAR + N_FAR
        n_late = len(PLACES) - first_late
        return combine(jnp.where(j < n_late, first_late + j, FIRST_FAR + j - n_late), carry)

    lax.fori_loop(0, len(PLACES) - FIRST_FAR, combine_late, 0)
    y_ref[...] = acc[...].astype(jnp.bfloat16)

    for part in BOTH:
        for i in range(6):
            spread(part, i).wait_send()
        for stage in (2, 3):
            await_ring(part, stage)
        for stage in range(4):
            for way in BOTH:
                for flip in BOTH:
                    relay(part, stage, way, flip).wait_send()
    for slot in range(3):
        await_slot(slot)
    for index in range(N_FAR):
        for flip in BOTH:
            for way in BOTH:
                z_relay(index, flip, way).wait_send()


def moe_call(n_cp, n_tp, cap, h_loc, rank_rows, near_rows, gate_rows, w_gate, w_up, w_down, wg_other, wu_other, wd_other):
    n_dev = n_cp * n_tp
    _, tok_dev, half_hid = h_loc.shape
    hid = PAIR * half_hid
    half_f = w_gate.shape[2]
    n_experts = rank_rows.shape[0]
    group = 4
    bf16 = jnp.bfloat16
    any_spec = pl.BlockSpec(memory_space=pl.ANY)
    vmem_spec = pl.BlockSpec(memory_space=pltpu.VMEM)
    dma = pltpu.SemaphoreType.DMA
    flops = PAIR * n_dev * PAIR * cap * hid * PAIR * half_f * 3
    return pl.pallas_call(
        functools.partial(moe_kernel, n_cp, n_tp, group),
        name="routed_experts",
        out_shape=(jax.ShapeDtypeStruct((tok_dev, hid), bf16), jax.ShapeDtypeStruct((2, n_dev, PAIR * cap, half_hid), bf16),
                   jax.ShapeDtypeStruct((2, 2, 4, 2, cap, half_hid), bf16), jax.ShapeDtypeStruct((n_dev, PAIR * cap, hid), bf16),
                   jax.ShapeDtypeStruct((N_FAR, 2, 2, cap, hid), bf16)),
        in_specs=[any_spec, any_spec, any_spec, vmem_spec] + [any_spec] * 6,
        out_specs=(vmem_spec,) + (any_spec,) * 4,
        scratch_shapes=[
            pltpu.VMEM((2, 4, tok_dev, half_hid), bf16),
            pltpu.VMEM((2, 4, n_experts, tok_dev), jnp.float32),
            pltpu.VMEM((2, 2, hid, half_f), bf16),
            pltpu.VMEM((2, 2, hid, half_f), bf16),
            pltpu.VMEM((2, 2, half_f, hid), bf16),
            pltpu.VMEM((2, 2, 8, PAIR * cap, half_hid), bf16),
            pltpu.VMEM((2, 4, PAIR * cap, half_hid), bf16),
            pltpu.VMEM((3, group, PAIR * cap, hid), bf16),
            pltpu.VMEM((group, PAIR * cap, hid), bf16),
            pltpu.VMEM((2, PAIR * cap, hid), bf16),
            pltpu.VMEM((tok_dev, hid), jnp.float32),
            pltpu.VMEM((3, n_experts, tok_dev), jnp.float32),
            dma((6,)), dma((4,)), dma((2,)), dma((2, group)), dma((2,)),
            dma((2, 6)), dma((2, 4, 2)), dma((2, 2, 8)), dma((2, n_dev)), dma((2, 2, 4, 2)), dma((2, 2, 4, 2)),
            dma((3, group)), dma((n_dev,)), dma((N_FAR, 2, 2)), dma((N_FAR, 2, 2)),
        ],
        compiler_params=pltpu.CompilerParams(collective_id=2, has_side_effects=True, vmem_limit_bytes=VMEM_LIMIT),
        cost_estimate=pl.CostEstimate(flops=flops, bytes_accessed=2**27, transcendentals=0),
    )(h_loc, rank_rows, near_rows, gate_rows, w_gate, w_up, w_down, wg_other, wu_other, wd_other)[0]


def routing_rows(ids_loc, gates_loc, n_experts):
    tok_dev = ids_loc.shape[0]
    chosen = ids_loc.T[None, :, :] == jnp.arange(n_experts, dtype=ids_loc.dtype)[:, None, None]
    mask = jnp.any(chosen, axis=1)
    gate_rows = jnp.sum(jnp.where(chosen, gates_loc.T[None, :, :], 0.0), axis=1)
    before = jnp.triu(jnp.ones((tok_dev, tok_dev), jnp.bfloat16), 1)
    rank = jnp.dot(mask.astype(jnp.bfloat16), before, preferred_element_type=jnp.float32)
    return jnp.where(mask, rank, -1.0), gate_rows


def block_of(cp_pos, tp_pos, n_cp, n_tp):
    per_chunk = n_tp // PAIR
    late = tp_pos // per_chunk
    chunk = late * (PAIR * n_cp - 1 - cp_pos) + (1 - late) * cp_pos
    return chunk * per_chunk + tp_pos % per_chunk


def owner_of(block, n_cp, n_tp):
    per_chunk = n_tp // PAIR
    chunk = block // per_chunk
    late = chunk // n_cp
    return late * (PAIR * n_cp - 1 - chunk) + (1 - late) * chunk, late * per_chunk + block % per_chunk


def front_kernel(n_cp, n_tp, x_hbm, w_ref, k_hbm, vt_hbm, q_hbm, x_buf, q_st, k_st, vt_st,
                 own_sem, ring_sem, pair_sem, rx_sem, sk_sem, sv_sem, sq_sem, kv_sem, rq_sem, sf_sem, rf_sem):
    n_x = n_tp // PAIR
    tok_dev, hid = x_hbm.shape
    half = tok_dev // PAIR
    head_dim = k_hbm.shape[1]
    n_loc = q_st.shape[1]
    chunk_len = tok_dev * n_x
    cp_pos, tp_pos = lax.axis_index("cp"), lax.axis_index("tp")
    x_pos, core = tp_pos // PAIR, tp_pos % PAIR
    sibling = PAIR * x_pos + 1 - core
    barrier = pltpu.get_barrier_semaphore()

    def slot_at(off, flip):
        return PAIR * ((x_pos + off + n_x) % n_x) + (core + flip) % PAIR

    own_copy = pltpu.make_async_copy(x_hbm, x_buf.at[tp_pos], own_sem)
    own_copy.start()
    for step in (1, n_x - 1):
        pl.semaphore_signal(barrier, inc=1, device_id=mesh_id(cp_pos, slot_at(step, 0)), device_id_type=MESH)
    for step in range(1, PAIR * n_cp):
        pl.semaphore_signal(barrier, inc=1, device_id=mesh_id((cp_pos + step // PAIR) % n_cp, PAIR * x_pos + (core + step) % PAIR), device_id_type=MESH)
    pl.semaphore_wait(barrier, PAIR * n_cp + 1)

    def own_send(part, to_tp, sem):
        rows = pl.ds(part * half, half)
        return pltpu.make_async_remote_copy(x_hbm.at[rows], x_buf.at[tp_pos, rows], sem, rx_sem.at[tp_pos, part],
                                            device_id=mesh_id(cp_pos, to_tp), device_id_type=MESH)

    def pass_on(slot, part, to_tp, sem):
        rows = pl.ds(pl.multiple_of(part * half, half), half)
        return pltpu.make_async_remote_copy(x_buf.at[slot, rows], x_buf.at[slot, rows], sem, rx_sem.at[slot, part],
                                            device_id=mesh_id(cp_pos, to_tp), device_id_type=MESH)

    for i, (part, off) in enumerate(((0, 1), (1, -1), (1, 1), (0, -1))):
        own_send(part, slot_at(off, 0), ring_sem.at[i]).start()
    for part in BOTH:
        own_send(part, sibling, pair_sem.at[part]).start()

    def place_of(step):
        wave, other, side = step // 4, (step // PAIR) % PAIR, step % PAIR
        near = ((wave + 1) // PAIR) % PAIR
        swap = (wave // PAIR) * (1 - wave // 3)
        off = near * (PAIR * side - 1) + PAIR * (wave // 3)
        return slot_at(off, other), side + swap * (1 - PAIR * side), off

    def outputs_of(step):
        slot, part, _ = place_of(step)
        block = block_of(cp_pos, slot, n_cp, n_tp)
        pos = block * tok_dev + part * half
        q_core = ((block % 4 + 1) // PAIR) % PAIR
        q_pos = (PAIR * (block // 4) + (block % 4) // PAIR) * tok_dev + part * half
        pos, q_pos = pl.multiple_of(pos, half), pl.multiple_of(q_pos, half)
        for i in range(n_loc):
            to_cp = n_loc * core + i
            for src, dst, s_sem, r_sem, to_core in (
                (k_st.at[step, i], k_hbm.at[pl.ds(pos, half)], sk_sem.at[i], kv_sem.at[cp_pos], 0),
                (vt_st.at[step, i], vt_hbm.at[:, pl.ds(pos, half)], sv_sem.at[i], kv_sem.at[cp_pos], 1),
                (q_st.at[step, i], q_hbm.at[pl.ds(q_pos, half)], sq_sem.at[i, q_core], rq_sem.at[cp_pos], q_core),
            ):
                here = jnp.logical_and(to_cp == cp_pos, to_core == core)

                @pl.when(here)
                def _():
                    pltpu.make_async_copy(src, dst, r_sem).start()

                @pl.when(jnp.logical_not(here))
                def _():
                    pltpu.make_async_remote_copy(src, dst, s_sem, r_sem, device_id=mesh_id(to_cp, PAIR * x_pos + to_core),
                                                 device_id_type=MESH).start()

    def project(step, carry):
        slot, part, off = place_of(step)
        wave, other, side = step // 4, (step // PAIR) % PAIR, step % PAIR

        @pl.when(step == 0)
        def _():
            own_copy.wait()

        @pl.when(step > 1)
        def _():
            pass_on(slot, part, sibling, pair_sem.at[0]).wait_recv()

        @pl.when(jnp.logical_and(wave > 0, other == 0))
        def _():
            @pl.when(wave == 1)
            def _():
                pass_on(slot, part, slot_at(-off, 0), ring_sem.at[4 + side]).start()
            pass_on(slot, part, sibling, pair_sem.at[PAIR * wave + side]).start()

        x_rows = x_buf[slot, pl.ds(pl.multiple_of(part * half, half), half), :]
        qkv = jnp.dot(x_rows, w_ref[...], preferred_element_type=jnp.float32)
        for i in range(n_loc):
            q_st[step, i] = qkv[:, i * head_dim:(i + 1) * head_dim].astype(jnp.bfloat16)
            k_st[step, i] = qkv[:, (n_loc + i) * head_dim:(n_loc + i + 1) * head_dim].astype(jnp.bfloat16)
            vt_st[step, i] = qkv[:, (PAIR * n_loc + i) * head_dim:(PAIR * n_loc + i + 1) * head_dim].T.astype(jnp.bfloat16)

        @pl.when(step > 0)
        def _():
            outputs_of(step - 1)
        return carry

    n_steps = PAIR * n_tp
    lax.fori_loop(0, n_steps, project, 0)
    outputs_of(n_steps - 1)

    def whole(ref, count, sem):
        return pltpu.make_async_copy(ref.at[pl.ds(0, count)], ref.at[pl.ds(0, count)], sem)

    def forward(y, place, core_id):
        chunk = y if place == 0 else PAIR * n_cp - 1 - y
        cols = pl.ds(chunk * chunk_len, chunk_len)
        ref = k_hbm.at[cols] if core_id == 0 else vt_hbm.at[:, cols]
        return pltpu.make_async_remote_copy(ref, ref, sf_sem.at[PAIR * y + place], rf_sem.at[PAIR * y + place],
                                            device_id=mesh_id(cp_pos, sibling), device_id_type=MESH)

    for y in range(n_cp):
        whole(k_hbm, PAIR * chunk_len, kv_sem.at[y]).wait()
        for core_id in BOTH:
            @pl.when(core == core_id)
            def _():
                for place in BOTH:
                    forward(y, place, core_id).start()
    for y in range(n_cp):
        whole(q_hbm, chunk_len, rq_sem.at[y]).wait()
    for i in range(4):
        own_send(0, sibling, ring_sem.at[i]).wait_send()
    for i in BOTH:
        own_send(0, sibling, ring_sem.at[4 + i]).wait_send()
    for i in range(8):
        own_send(0, sibling, pair_sem.at[i]).wait_send()
    for i in range(n_loc):
        to_cp = n_loc * core + i
        for sem, to_core, count in ((sk_sem.at[i], 0, PAIR * chunk_len), (sv_sem.at[i], 1, PAIR * chunk_len),
                                    (sq_sem.at[i, 0], 0, chunk_len), (sq_sem.at[i, 1], 1, chunk_len)):
            @pl.when(jnp.logical_not(jnp.logical_and(to_cp == cp_pos, to_core == core)))
            def _():
                whole(k_hbm, count, sem).wait()
    for core_id in BOTH:
        @pl.when(core == core_id)
        def _():
            for y in range(n_cp):
                for place in BOTH:
                    forward(y, place, core_id).wait_send()
                    forward(y, place, 1 - core_id).wait_recv()


def front_call(n_cp, n_tp, x_loc, w_qkv, head_dim, n_loc):
    tok_dev, hid = x_loc.shape
    half = tok_dev // PAIR
    seq = tok_dev * n_cp * n_tp
    any_spec = pl.BlockSpec(memory_space=pl.ANY)
    n_steps = PAIR * n_tp
    return pl.pallas_call(
        functools.partial(front_kernel, n_cp, n_tp),
        name="gather_project",
        out_shape=(jax.ShapeDtypeStruct((seq, head_dim), jnp.bfloat16), jax.ShapeDtypeStruct((head_dim, seq), jnp.bfloat16),
                   jax.ShapeDtypeStruct((seq // PAIR, head_dim), jnp.bfloat16)),
        in_specs=[any_spec, pl.BlockSpec(memory_space=pltpu.VMEM)],
        out_specs=(any_spec, any_spec, any_spec),
        scratch_shapes=[
            pltpu.VMEM((n_tp, tok_dev, hid), jnp.bfloat16),
            pltpu.VMEM((n_steps, n_loc, half, head_dim), jnp.bfloat16),
            pltpu.VMEM((n_steps, n_loc, half, head_dim), jnp.bfloat16),
            pltpu.VMEM((n_steps, n_loc, head_dim, half), jnp.bfloat16),
            pltpu.SemaphoreType.DMA,
            pltpu.SemaphoreType.DMA((6,)),
            pltpu.SemaphoreType.DMA((8,)),
            pltpu.SemaphoreType.DMA((n_tp, 2)),
            pltpu.SemaphoreType.DMA((n_loc,)),
            pltpu.SemaphoreType.DMA((n_loc,)),
            pltpu.SemaphoreType.DMA((n_loc, 2)),
            pltpu.SemaphoreType.DMA((n_cp,)),
            pltpu.SemaphoreType.DMA((n_cp,)),
            pltpu.SemaphoreType.DMA((PAIR * n_cp,)),
            pltpu.SemaphoreType.DMA((PAIR * n_cp,)),
        ],
        compiler_params=pltpu.CompilerParams(collective_id=0, has_side_effects=True, vmem_limit_bytes=VMEM_LIMIT),
        cost_estimate=pl.CostEstimate(flops=PAIR * n_tp * tok_dev * hid * w_qkv.shape[1], bytes_accessed=2**26, transcendentals=0),
    )(x_loc, w_qkv)


def attend_kernel(n_cp, n_tp, k_hbm, vt_hbm, q_hbm, x_hbm, wo_hbm, wg_hbm, wu_hbm, wd_hbm, rank_hbm,
                  h_ref, o_hbm, wgx_hbm, wux_hbm, wdx_hbm, near_hbm,
                  k_buf, vt_buf, q_buf, qt_buf, o_st, o_buf, wo_buf, x_buf, s_even, s_odd, acc, m_ref, l_ref,
                  in_sem, so_sem, ro_sem, swo_sem, rwo_sem, sw_sem, rw_sem, sr_sem, rr_sem, o_sem):
    n_dev = n_cp * n_tp
    n_x = n_tp // PAIR
    tok_dev, hid = x_buf.shape
    head_dim = k_buf.shape[1]
    n_heads = o_buf.shape[0]
    cp_pos, tp_pos = lax.axis_index("cp"), lax.axis_index("tp")
    x_pos, core = tp_pos // PAIR, tp_pos % PAIR
    head = n_cp * x_pos + cp_pos
    scale = (head_dim ** -0.5) * 1.4426950408889634
    loads = [pltpu.make_async_copy(src, dst, in_sem.at[i]) for i, (src, dst) in enumerate(
        ((q_hbm, q_buf), (k_hbm, k_buf), (vt_hbm, vt_buf), (x_hbm, x_buf), (wo_hbm, wo_buf.at[tp_pos])))]
    for one in loads:
        one.start()

    enter_all(n_cp, n_tp)

    def wo_send(step):
        return pltpu.make_async_remote_copy(wo_hbm, wo_buf.at[tp_pos], swo_sem.at[step], rwo_sem.at[step],
                                            device_id=mesh_id(cp_pos, (tp_pos + step) % n_tp), device_id_type=MESH)

    def wo_arrival(step):
        return pltpu.make_async_remote_copy(wo_hbm, wo_buf.at[(tp_pos + n_tp - step) % n_tp], swo_sem.at[step], rwo_sem.at[step],
                                            device_id=mesh_id(cp_pos, tp_pos), device_id_type=MESH)

    keep = wgx_hbm.shape[0]
    swaps = [pltpu.make_async_remote_copy(src.at[pl.ds((1 - core) * keep, keep)], dst, sw_sem.at[i], rw_sem.at[i],
                                          device_id=mesh_id(cp_pos, PAIR * x_pos + 1 - core), device_id_type=MESH)
             for i, (src, dst) in enumerate(((wg_hbm, wgx_hbm), (wu_hbm, wux_hbm), (wd_hbm, wdx_hbm)))]
    ranks = []
    for slot, off in ((1, 1), (2, -1), (3, 2)):
        for part, place in enumerate((((cp_pos + off + n_cp) % n_cp, tp_pos), (cp_pos, PAIR * ((x_pos + off + n_x) % n_x) + core))):
            ranks.append(pltpu.make_async_remote_copy(rank_hbm, near_hbm.at[part, slot], sr_sem.at[part, slot], rr_sem.at[part, slot],
                                                      device_id=mesh_id(*place), device_id_type=MESH))
    for step in range(1, n_tp):
        wo_send(step).start()
    for one in swaps + ranks:
        one.start()
    for one in loads[:3]:
        one.wait()

    def update(s_vals, s_top, v_cols, lo, width):
        cols = pl.ds(lo, width)
        m_old = m_ref[:, cols]
        m_new = jnp.maximum(m_old, s_top)
        prob = jnp.exp2((s_vals - m_new) * scale)
        shrink = jnp.exp2((m_old - m_new) * scale)
        m_ref[:, cols] = m_new
        l_ref[:, cols] = l_ref[:, cols] * shrink + jnp.sum(prob, axis=0, keepdims=True)
        acc[:, cols] = acc[:, cols] * shrink + jnp.dot(v_cols, prob.astype(jnp.bfloat16), preferred_element_type=jnp.float32)

    def keys_at(block):
        return k_buf[pl.ds(pl.multiple_of(block * tok_dev, tok_dev), tok_dev), :]

    def values_at(block):
        return vt_buf[:, pl.ds(pl.multiple_of(block * tok_dev, tok_dev), tok_dev)]

    def query_pair(g, carry):
        q_rows = q_buf[pl.ds(pl.multiple_of(g * PAIR * tok_dev, PAIR * tok_dev), PAIR * tok_dev), :]
        qt_buf[...] = q_rows.astype(jnp.float32).T.astype(jnp.bfloat16)
        m_ref[...] = jnp.full_like(m_ref, -1e30)
        l_ref[...] = jnp.zeros_like(l_ref)
        acc[...] = jnp.zeros_like(acc)
        for r in BOTH:
            lo = r * tok_dev
            inner = (1 - core) * 3 * r + core * (1 + r)

            def near_scores(block):
                return jnp.dot(keys_at(block), qt_buf[:, pl.ds(lo, tok_dev)], preferred_element_type=jnp.float32)

            s_vals = near_scores(4 * g + inner)
            key_id = lax.broadcasted_iota(jnp.int32, s_vals.shape, 0)
            query_id = lax.broadcasted_iota(jnp.int32, s_vals.shape, 1)
            s_vals = jnp.where(key_id <= query_id, s_vals, -1e30)
            update(s_vals, jnp.max(s_vals, axis=0, keepdims=True), values_at(4 * g + inner), lo, tok_dev)

            def near_block(j, inner_carry):
                s_near = near_scores(4 * g + j)
                update(s_near, jnp.max(s_near, axis=0, keepdims=True), values_at(4 * g + j), lo, tok_dev)
                return inner_carry

            lax.fori_loop(0, inner, near_block, 0)

        def far_scores(block, s_ref):
            s_vals = jnp.dot(keys_at(block), qt_buf[...], preferred_element_type=jnp.float32)
            s_ref[...] = s_vals
            return jnp.max(s_vals, axis=0, keepdims=True)

        def far_pair(n, top_even):
            top_odd = far_scores(PAIR * n + 1, s_odd)
            update(s_even[...], top_even, values_at(PAIR * n), 0, PAIR * tok_dev)
            top_next = far_scores(PAIR * n + 2, s_even)
            update(s_odd[...], top_odd, values_at(PAIR * n + 1), 0, PAIR * tok_dev)
            return top_next

        lax.fori_loop(0, PAIR * g, far_pair, far_scores(0, s_even))
        out = (acc[...] / l_ref[...]).T.astype(jnp.bfloat16)
        for r in BOTH:
            o_st[PAIR * g + r] = out[r * tok_dev:(r + 1) * tok_dev]
            o_push(PAIR * g + r, "start")
        return carry

    def o_push(index, what):
        block = 4 * (index // PAIR) + (1 - core) * 3 * (index % PAIR) + core * (1 + index % PAIR)
        to_cp, to_tp = owner_of(block, n_cp, n_tp)
        here = jnp.logical_and(to_cp == cp_pos, to_tp == tp_pos)
        if what == "start":
            @pl.when(here)
            def _():
                pltpu.make_async_copy(o_st.at[index], o_hbm.at[head], ro_sem.at[head]).start()

        @pl.when(jnp.logical_not(here))
        def _():
            copy = pltpu.make_async_remote_copy(o_st.at[index], o_hbm.at[head], so_sem.at[index], ro_sem.at[head],
                                                device_id=mesh_id(to_cp, to_tp), device_id_type=MESH)
            if what == "start":
                copy.start()
            else:
                copy.wait_send()

    lax.fori_loop(0, n_dev // 4, query_pair, 0)

    for step in range(1, n_tp):
        wo_arrival(step).wait_recv()
    for one in loads[3:]:
        one.wait()
    for j in range(n_heads):
        pltpu.make_async_copy(o_hbm.at[j], o_hbm.at[j], ro_sem.at[j]).wait()
    o_load = pltpu.make_async_copy(o_hbm, o_buf, o_sem)
    o_load.start()
    o_load.wait()
    o_rows = jnp.concatenate([o_buf[j] for j in range(n_heads)], axis=1)
    n_cols = min(512, hid // PAIR)

    for col in range(0, hid, n_cols):
        cols = pl.ds(col, n_cols)
        w_cols = wo_buf[:, :, cols].reshape(n_heads * head_dim, n_cols)
        h_cols = (x_buf[:, cols].astype(jnp.float32) + jnp.dot(o_rows, w_cols, preferred_element_type=jnp.float32)).astype(jnp.bfloat16)
        h_ref[PAIR * col // hid, :, pl.ds(col % (hid // PAIR), n_cols)] = h_cols

    for step in range(1, n_tp):
        wo_send(step).wait_send()
    for one in swaps + ranks:
        one.wait()

    def drain(index, carry):
        o_push(index, "wait")
        return carry

    lax.fori_loop(0, n_dev // PAIR, drain, 0)


def attend_call(n_cp, n_tp, k_all, vt_all, q_all, x_loc, wo_loc, w_gate, w_up, w_down, rank_rows):
    n_dev = n_cp * n_tp
    tok_dev, hid = x_loc.shape
    seq, head_dim = k_all.shape
    n_heads = n_tp * wo_loc.shape[0] // head_dim
    keep = w_gate.shape[0] // PAIR
    any_spec = pl.BlockSpec(memory_space=pl.ANY)
    bf16 = jnp.bfloat16
    h_loc, _, wg_other, wu_other, wd_other, near_rows = pl.pallas_call(
        functools.partial(attend_kernel, n_cp, n_tp),
        name="attend_heads",
        out_shape=(jax.ShapeDtypeStruct((2, tok_dev, hid // PAIR), bf16), jax.ShapeDtypeStruct((n_heads, tok_dev, head_dim), bf16))
        + tuple(jax.ShapeDtypeStruct((keep,) + w.shape[1:], bf16) for w in (w_gate, w_up, w_down))
        + (jax.ShapeDtypeStruct((2, 4) + rank_rows.shape, jnp.float32),),
        in_specs=[any_spec] * 9,
        out_specs=(pl.BlockSpec(memory_space=pltpu.VMEM),) + (any_spec,) * 5,
        scratch_shapes=[
            pltpu.VMEM((seq, head_dim), bf16),
            pltpu.VMEM((head_dim, seq), bf16),
            pltpu.VMEM((seq // PAIR, head_dim), bf16),
            pltpu.VMEM((head_dim, PAIR * tok_dev), bf16),
            pltpu.VMEM((n_dev // PAIR, tok_dev, head_dim), bf16),
            pltpu.VMEM((n_heads, tok_dev, head_dim), bf16),
            pltpu.VMEM((n_tp,) + wo_loc.shape, bf16),
            pltpu.VMEM((tok_dev, hid), bf16),
            pltpu.VMEM((tok_dev, PAIR * tok_dev), jnp.float32),
            pltpu.VMEM((tok_dev, PAIR * tok_dev), jnp.float32),
            pltpu.VMEM((head_dim, PAIR * tok_dev), jnp.float32),
            pltpu.VMEM((1, PAIR * tok_dev), jnp.float32),
            pltpu.VMEM((1, PAIR * tok_dev), jnp.float32),
            pltpu.SemaphoreType.DMA((5,)),
            pltpu.SemaphoreType.DMA((n_dev // PAIR,)),
            pltpu.SemaphoreType.DMA((n_heads,)),
            pltpu.SemaphoreType.DMA((n_tp,)),
            pltpu.SemaphoreType.DMA((n_tp,)),
            pltpu.SemaphoreType.DMA((3,)),
            pltpu.SemaphoreType.DMA((3,)),
            pltpu.SemaphoreType.DMA((2, 4)),
            pltpu.SemaphoreType.DMA((2, 4)),
            pltpu.SemaphoreType.DMA,
        ],
        compiler_params=pltpu.CompilerParams(collective_id=1, has_side_effects=True, vmem_limit_bytes=VMEM_LIMIT),
        cost_estimate=pl.CostEstimate(flops=PAIR * seq * seq * head_dim // PAIR, bytes_accessed=2**26, transcendentals=seq * seq // 4),
    )(k_all, vt_all, q_all, x_loc, wo_loc, w_gate, w_up, w_down, rank_rows)
    return h_loc, near_rows, wg_other, wu_other, wd_other


def solution(mesh):
    n_cp = mesh.shape["cp"]
    n_tp = mesh.shape["tp"]
    row_spec = P(("dp", "cp", "tp"), None)
    head_spec = P(None, "tp", None)
    expert_spec = P(("cp", "tp"), None, None)

    def device_step(x_loc, w_q, w_k, w_v, w_o, ids_loc, gates_loc, w_gate, w_up, w_down):
        tok_dev, hid_dim = x_loc.shape
        n_loc, head_dim = w_q.shape[1:]
        n_experts = w_gate.shape[0] * n_cp * n_tp // PAIR
        capacity = ids_loc.shape[1] * tok_dev // n_experts
        w_qkv = jnp.concatenate([w.reshape(hid_dim, n_loc * head_dim) for w in (w_q, w_k, w_v)], axis=1)
        rank_rows, gate_rows = routing_rows(ids_loc, gates_loc, n_experts)
        k_all, vt_all, q_all = front_call(n_cp, n_tp, x_loc, w_qkv, head_dim, n_loc)
        h_loc, near_rows, *others = attend_call(n_cp, n_tp, k_all, vt_all, q_all, x_loc, w_o.reshape(n_loc * head_dim, hid_dim), w_gate, w_up, w_down, rank_rows)
        return moe_call(n_cp, n_tp, capacity, h_loc, rank_rows, near_rows, gate_rows, w_gate, w_up, w_down, *others)

    return jax.shard_map(device_step, mesh=mesh, in_specs=(row_spec, head_spec, head_spec, head_spec, P("tp", None, None), row_spec, row_spec, expert_spec, expert_spec, expert_spec), out_specs=row_spec, check_vma=False)
```

```python
import functools

import jax
import jax.numpy as jnp
from jax import lax
from jax.experimental import pallas as pl
from jax.experimental.pallas import tpu as pltpu
from jax.sharding import PartitionSpec as P

MESH = pl.DeviceIdType.MESH
PAIR = 2
BOTH = range(PAIR)
ROWS_ROWS = (((0,), (0,)), ((), ()))
COLUMN_WISE = {"axis": 0, "keepdims": True}
dma = pltpu.SemaphoreType.DMA
and_, or_, not_ = jnp.logical_and, jnp.logical_or, jnp.logical_not
VMEM_LIMIT = 66_000_000
PLACES = ((0, 0), (0, 1), (1, 0), (0, -1), (-1, 0), (1, 1), (-1, -1), (1, -1), (-1, 1), (0, PAIR), (PAIR, 0), (1, PAIR), (PAIR, 1), (-1, PAIR), (PAIR, -1), (PAIR, PAIR))
N_NEAR, FIRST_FAR = 5, 9
GROUPS = ("1234", "1234", "9a9a", "bcbc", "dede", "0f0f", "5656", "7878")
FLIPS = ("0000", "1111") + ("0011",) * 6
SOURCES = (0, -1, 1, PAIR)


def peer_of(step, cp_pos, tp_pos, n_cp, n_tp):
    n_x = n_tp // PAIR
    off_x = (step // PAIR) % n_x
    off_y = (off_x + step // n_tp) % n_cp
    return (cp_pos + off_y) % n_cp, ((tp_pos // PAIR + off_x) % n_x) * 2 + (tp_pos % PAIR + step % PAIR) % PAIR


def mesh_id(cp_pos, tp_pos):
    return {"cp": cp_pos, "tp": tp_pos}


def enter_all(n_cp, n_tp):
    cp_pos, tp_pos = lax.axis_index("cp"), lax.axis_index("tp")

    def signal_peer(step, carry):
        to_cp, to_tp = peer_of(step, cp_pos, tp_pos, n_cp, n_tp)
        pl.semaphore_signal(pltpu.get_barrier_semaphore(), inc=1, device_id=mesh_id(to_cp, to_tp), device_id_type=MESH)
        return carry

    lax.fori_loop(1, n_cp * n_tp, signal_peer, 0)
    pl.semaphore_wait(pltpu.get_barrier_semaphore(), n_cp * n_tp - 1)


def pick(values, index):
    out = values[-1]
    for k, value in enumerate(values[:-1]):
        out = jnp.where(index == k, value, out)
    return out


def moe_kernel(n_cp, n_tp, group, h_hbm, rank_hbm, near_hbm, gate_ref, wg_hbm, wu_hbm, wd_hbm, wgx_hbm, wux_hbm, wdx_hbm,
               y_ref, rx_hbm, rl_hbm, rz_hbm, zl_hbm,
               h_buf, rank_buf, wg_buf, wu_buf, wd_buf, ring, own_stage, z_ring, x_buf, z_buf, acc, parts,
               w_sem, rank_sem, in_sem, x_sem, z_sem, hs_sem, hr_sem, ss_sem, rx_sem, rl_sem, fl_sem, sz_sem, rz_sem, zl_sem, fz_sem):
    n_x = n_tp // PAIR
    tok_dev, half_hid = h_buf.shape[2:]
    hid = PAIR * half_hid
    cap = ring.shape[3] // PAIR
    cp_pos, tp_pos = lax.axis_index("cp"), lax.axis_index("tp")
    x_pos, core = tp_pos // PAIR, tp_pos % PAIR
    half_tok = tok_dev // PAIR

    def at(off_y, off_x, flip):
        return (cp_pos + off_y + n_cp) % n_cp, PAIR * ((x_pos + off_x + n_x) % n_x) + (core + flip) % PAIR

    def line(place):
        return place[0] * n_tp + place[1]

    def send(src, dst, s_sem, r_sem, place):
        return pltpu.make_async_remote_copy(src, dst, s_sem, r_sem, device_id=mesh_id(*place), device_id_type=MESH)

    def await_bytes(ref, sem):
        pltpu.make_async_copy(ref, ref, sem).wait()

    h_loads = [pltpu.make_async_copy(h_hbm.at[part], h_buf.at[part, 0], in_sem.at[part]) for part in BOTH]
    rank_loads = []
    for part in BOTH:
        rank_loads.append(pltpu.make_async_copy(rank_hbm, rank_buf.at[part, 0], rank_sem.at[PAIR * part]))
        rank_loads.append(pltpu.make_async_copy(near_hbm.at[part, pl.ds(1, 3)], rank_buf.at[part, pl.ds(1, 3)], rank_sem.at[PAIR * part + 1]))
    w_loads = []
    for slot, (own, other, buf) in enumerate(((wg_hbm, wgx_hbm, wg_buf), (wu_hbm, wux_hbm, wu_buf), (wd_hbm, wdx_hbm, wd_buf))):
        w_loads.append(pltpu.make_async_copy(own.at[pl.ds(PAIR * core, PAIR)], buf.at[0], w_sem.at[PAIR * slot]))
        w_loads.append(pltpu.make_async_copy(other, buf.at[1], w_sem.at[PAIR * slot + 1]))
    for one in h_loads + rank_loads:
        one.start()
    enter_all(n_cp, n_tp)

    def along(part, off):
        return at(off, 0, 0) if part == 0 else at(0, off, 0)

    def across(part, off, flip):
        return at(0, off, flip) if part == 0 else at(off, 0, flip)

    def rows_of(piece):
        return pl.ds(piece * half_tok, half_tok)

    def spread(part, i):
        piece, off, slot = ((0, 1, 1), (1, -1, PAIR), (1, 1, 1), (0, -1, PAIR), (0, 1, 3), (1, -1, 3))[i]
        rows = rows_of(piece)
        src = h_hbm.at[part, rows] if i < 4 else h_buf.at[part, 1 if i == 4 else 2, rows]
        return send(src, h_buf.at[part, slot, rows], hs_sem.at[part, i], hr_sem.at[part, slot, piece], along(part, off))

    def await_h(part, slot, piece):
        await_bytes(h_buf.at[part, slot, rows_of(piece)], hr_sem.at[part, slot, piece])

    for i in range(4):
        for part in BOTH:
            spread(part, i).start()
    for one in w_loads:
        one.start()
    for one in h_loads + rank_loads:
        one.wait()

    slots = lax.broadcasted_iota(jnp.int32, (cap, tok_dev), 0).astype(jnp.float32)

    def gather_rows(part, stage, m):
        turn = m // PAIR
        off = turn + (turn // PAIR) * (5 - PAIR * turn)
        first = PAIR * line(across(part, off, m % PAIR))
        chosen = [jnp.where(rank_buf[part, stage, pl.ds(first + i, 1), :] == slots, 1.0, 0.0) for i in BOTH]
        chosen = jnp.concatenate(chosen, axis=0).astype(jnp.bfloat16)
        return jnp.dot(chosen, h_buf[part, stage], preferred_element_type=jnp.float32).astype(jnp.bfloat16)

    def source_line(part, stage, off):
        a = SOURCES[stage]
        return line(at(a, off, 0) if part == 0 else at(off, a, 0))

    def await_ring(part, stage):
        def one(m, carry):
            await_bytes(ring.at[part, stage % PAIR, m], ss_sem.at[part, stage % PAIR, m])
            return carry
        lax.fori_loop(1, 8, one, 0)

    def own_copy(part, stage):
        src_line = source_line(part, stage, 0)
        return pltpu.make_async_copy(own_stage.at[part, stage], rx_hbm.at[part, src_line], rx_sem.at[part, src_line])

    def run_stage(stage):
        side = stage % PAIR
        for part in BOTH:
            if stage >= 2:
                await_ring(part, stage)
            own_stage[part, stage] = gather_rows(part, stage, 0)

            def fill(m, carry):
                ring[part, side, m] = gather_rows(part, stage, m)
                return carry

            lax.fori_loop(1, 8, fill, 0)
        lines = [source_line(part, stage, 0) for part in BOTH]
        for flip in BOTH:
            for way, off in enumerate((1, -1)):
                for part in BOTH:
                    m = 6 + flip
                    send(ring.at[part, side, m, pl.ds(way * cap, cap)], rl_hbm.at[part, way, stage, flip], ss_sem.at[part, side, m],
                         rl_sem.at[part, way, stage, flip], across(part, off, 0)).start()
        for m, off in ((PAIR, 1), (4, -1), (3, 1), (5, -1), (1, 0)):
            for part in BOTH:
                send(ring.at[part, side, m], rx_hbm.at[part, lines[part]], ss_sem.at[part, side, m], rx_sem.at[part, lines[part]],
                     across(part, off, m % PAIR)).start()
        for part in BOTH:
            own_copy(part, stage).start()

    def relay(part, stage, way, flip):
        off = 1 - PAIR * way
        src_line = source_line(part, stage, -off)
        return send(rl_hbm.at[part, way, stage, flip], rx_hbm.at[part, src_line, pl.ds(way * cap, cap)], fl_sem.at[part, way, stage, flip],
                    rx_sem.at[part, src_line], across(part, off, flip))

    def run_relays(stage):
        for flip in BOTH:
            for way in BOTH:
                for part in BOTH:
                    await_bytes(rl_hbm.at[part, way, stage, flip], rl_sem.at[part, way, stage, flip])
                    relay(part, stage, way, flip).start()

    run_stage(0)
    for part in BOTH:
        await_h(part, 1, 0)
        spread(part, 4).start()
    for part in BOTH:
        await_h(part, PAIR, 1)
        spread(part, 5).start()
    for part in BOTH:
        await_h(part, 1, 1)
    run_stage(1)
    gate_all = gate_ref[...]
    high = gate_all.astype(jnp.bfloat16).astype(jnp.float32)
    rest = gate_all - high
    mid = rest.astype(jnp.bfloat16).astype(jnp.float32)
    parts[0] = high
    parts[1] = mid
    parts[2] = rest - mid
    for part in BOTH:
        acc[:, part * half_hid:(part + 1) * half_hid] = h_buf[part, 0].astype(jnp.float32)
    run_relays(0)
    for part in BOTH:
        await_h(part, PAIR, 0)
    run_stage(2)
    run_relays(1)
    for part in BOTH:
        await_h(part, 3, 0)
        await_h(part, 3, 1)
    run_stage(3)
    run_relays(2)
    for one in w_loads:
        one.wait()

    rows = group * cap
    n_cols = min(512, hid)

    def expert_rows(slot, i):
        x_rows = x_buf[:, pl.ds(i * cap, cap), :].reshape(rows, hid)
        hidden = []
        for half in BOTH:
            gate_pre = jnp.dot(x_rows, wg_buf[half, i], preferred_element_type=jnp.float32)
            up_pre = jnp.dot(x_rows, wu_buf[half, i], preferred_element_type=jnp.float32)
            hidden.append((gate_pre * (1.0 / (1.0 + jnp.exp(-gate_pre))) * up_pre).astype(jnp.bfloat16))
        for col in range(0, hid, n_cols):
            z_rows = (jnp.dot(hidden[0], wd_buf[0, i, :, pl.ds(col, n_cols)], preferred_element_type=jnp.float32)
                      + jnp.dot(hidden[1], wd_buf[1, i, :, pl.ds(col, n_cols)], preferred_element_type=jnp.float32))
            z_ring[slot, :, pl.ds(i * cap, cap), pl.ds(col, n_cols)] = z_rows.astype(jnp.bfloat16).reshape(group, cap, n_cols)

    def place_at(g, q):
        places = [int(names[q], 16) for names in GROUPS]
        off_y, off_x = (pick([PLACES[p][k] for p in places], g) for k in BOTH)
        return off_y, off_x, pick([int(flips[q]) for flips in FLIPS], g), pick(places, g)

    my_line = line((cp_pos, tp_pos))

    def await_slot(slot):
        for q in range(group):
            await_bytes(z_ring.at[slot, q], sz_sem.at[slot, q])

    def expert_group(g, carry):
        slot = g % 3

        @pl.when(g == 2)
        def _():
            run_relays(3)

        sources = [line(at(*place_at(g, q)[:3])) for q in range(group)]
        loads = []
        for q in range(group):
            for part in BOTH:
                await_bytes(rx_hbm.at[part, sources[q]], rx_sem.at[part, sources[q]])
                loads.append(pltpu.make_async_copy(rx_hbm.at[part, sources[q]], x_buf.at[q, :, pl.ds(part * half_hid, half_hid)], x_sem.at[part, q]))
                loads[-1].start()

        @pl.when(g >= 3)
        def _():
            await_slot(slot)
        for one in loads:
            one.wait()
        for i in BOTH:
            expert_rows(slot, i)
        for q in range(group):
            off_y, off_x, flip, p = place_at(g, q)
            alone = and_(p == 0, flip == 0)

            @pl.when(alone)
            def _():
                pltpu.make_async_copy(z_ring.at[slot, q], rz_hbm.at[my_line], rz_sem.at[my_line]).start()

            @pl.when(and_(p < FIRST_FAR, not_(alone)))
            def _():
                send(z_ring.at[slot, q], rz_hbm.at[my_line], sz_sem.at[slot, q], rz_sem.at[my_line], at(off_y, off_x, flip)).start()

            @pl.when(p >= FIRST_FAR)
            def _():
                lead_y, lead_x = jnp.where(off_y == 2, 1, 0), jnp.where(off_x == 2, 1, 0)
                for way in BOTH:
                    sign = 1 - PAIR * way
                    send(z_ring.at[slot, q, pl.ds(way * cap, cap)], zl_hbm.at[p - FIRST_FAR, flip, way], sz_sem.at[slot, q],
                         zl_sem.at[p - FIRST_FAR, flip, way], at(sign * lead_y, sign * lead_x, 0)).start()
        return carry

    lax.fori_loop(0, len(GROUPS), expert_group, 0)

    n_far = len(PLACES) - FIRST_FAR

    def z_relay(index, flip, way):
        off_y, off_x = PLACES[FIRST_FAR + index]
        sign = 1 - PAIR * way
        lead_y, lead_x = sign * (off_y == 2), sign * (off_x == 2)
        from_line = line(at(-lead_y, -lead_x, 0))
        to_y = sign if off_y == 2 else off_y
        to_x = sign if off_x == 2 else off_x
        return send(zl_hbm.at[index, flip, way], rz_hbm.at[from_line, pl.ds(way * cap, cap)], fz_sem.at[index, flip, way],
                    rz_sem.at[from_line], at(to_y, to_x, flip))

    def each_relay(*indices):
        return [(index, flip, way) for flip in BOTH for way in BOTH for index in indices]

    def run_z_relays(*indices):
        for key in each_relay(*indices):
            await_bytes(zl_hbm.at[key], zl_sem.at[key])
            z_relay(*key).start()

    def combine(p, carry):
        off_y, off_x = pick([a for a, _ in PLACES], p), pick([b for _, b in PLACES], p)
        homes = [line(at(-off_y, -off_x, q)) for q in BOTH]
        loads = []
        for q in BOTH:
            await_bytes(rz_hbm.at[homes[q]], rz_sem.at[homes[q]])
            loads.append(pltpu.make_async_copy(rz_hbm.at[homes[q]], z_buf.at[q], z_sem.at[q]))
            loads[-1].start()
        weights = [[], [], []]
        for q in BOTH:
            for i in BOTH:
                row = pl.ds(PAIR * homes[q] + i, 1)
                chosen = rank_buf[0, 0, row, :] == slots
                for part in range(3):
                    weights[part].append(jnp.where(chosen, parts[part, row, :], 0.0))
        weights = [jnp.concatenate(w, axis=0).astype(jnp.bfloat16) for w in weights]
        for one in loads:
            one.wait()
        for col in range(0, hid, n_cols):
            z_rows = z_buf[:, :, pl.ds(col, n_cols)].reshape(4 * cap, n_cols)
            total = None
            for part in range(3):
                term = lax.dot_general(weights[part], z_rows, ROWS_ROWS, preferred_element_type=jnp.float32)
                total = term if total is None else total + term
            acc[:, pl.ds(col, n_cols)] += total
        return carry

    run_z_relays(0, 1)
    run_z_relays(PAIR, 3)
    lax.fori_loop(0, N_NEAR, combine, 0)
    run_z_relays(4, 5)
    run_z_relays(6)
    lax.fori_loop(N_NEAR, len(PLACES), combine, 0)
    y_ref[...] = acc[...].astype(jnp.bfloat16)

    for part in BOTH:
        for i in range(6):
            spread(part, i).wait_send()
        for stage in (PAIR, 3):
            await_ring(part, stage)
        for stage in range(4):
            for way in BOTH:
                for flip in BOTH:
                    relay(part, stage, way, flip).wait_send()
    last = len(GROUPS) - 3
    for g in range(last, len(GROUPS)):
        for q in range(group):
            if GROUPS[g][q] + FLIPS[g][q] != "00":
                await_bytes(z_ring.at[g % 3, q], sz_sem.at[g % 3, q])
    for key in each_relay(*range(n_far)):
        z_relay(*key).wait_send()


def moe_call(n_cp, n_tp, cap, h_loc, rank_rows, near_rows, gate_rows, w_gate, w_up, w_down, wg_other, wu_other, wd_other):
    n_dev = n_cp * n_tp
    _, tok_dev, half_hid = h_loc.shape
    hid = PAIR * half_hid
    half_f = w_gate.shape[2]
    n_experts = rank_rows.shape[0]
    group = len(GROUPS[0])
    n_far = len(PLACES) - FIRST_FAR
    bf16 = jnp.bfloat16
    any_spec = pl.BlockSpec(memory_space=pl.ANY)
    vmem_spec = pl.BlockSpec(memory_space=pltpu.VMEM)
    flops = PAIR * n_dev * PAIR * cap * hid * PAIR * half_f * 3
    return pl.pallas_call(
        functools.partial(moe_kernel, n_cp, n_tp, group),
        name="routed_experts",
        out_shape=(jax.ShapeDtypeStruct((tok_dev, hid), bf16), jax.ShapeDtypeStruct((PAIR, n_dev, PAIR * cap, half_hid), bf16),
                   jax.ShapeDtypeStruct((PAIR, PAIR, 4, PAIR, cap, half_hid), bf16), jax.ShapeDtypeStruct((n_dev, PAIR * cap, hid), bf16),
                   jax.ShapeDtypeStruct((n_far, PAIR, 2, cap, hid), bf16)),
        in_specs=[any_spec, any_spec, any_spec, vmem_spec] + [any_spec] * 6,
        out_specs=(vmem_spec,) + (any_spec,) * 4,
        scratch_shapes=[
            pltpu.VMEM((PAIR, 4, tok_dev, half_hid), bf16),
            pltpu.VMEM((PAIR, 4, n_experts, tok_dev), jnp.float32),
            pltpu.VMEM((PAIR, PAIR, hid, half_f), bf16),
            pltpu.VMEM((PAIR, PAIR, hid, half_f), bf16),
            pltpu.VMEM((PAIR, PAIR, half_f, hid), bf16),
            pltpu.VMEM((PAIR, PAIR, 8, PAIR * cap, half_hid), bf16),
            pltpu.VMEM((PAIR, 4, PAIR * cap, half_hid), bf16),
            pltpu.VMEM((3, group, PAIR * cap, hid), bf16),
            pltpu.VMEM((group, PAIR * cap, hid), bf16),
            pltpu.VMEM((PAIR, PAIR * cap, hid), bf16),
            pltpu.VMEM((tok_dev, hid), jnp.float32),
            pltpu.VMEM((3, n_experts, tok_dev), jnp.float32),
            dma((6,)), dma((4,)), dma((PAIR,)), dma((PAIR, group)), dma((PAIR,)),
            dma((PAIR, 6)), dma((PAIR, 4, PAIR)), dma((PAIR, PAIR, 8)), dma((PAIR, n_dev)), dma((PAIR, PAIR, 4, PAIR)), dma((PAIR, PAIR, 4, PAIR)),
            dma((3, group)), dma((n_dev,)), dma((n_far, PAIR, PAIR)), dma((n_far, PAIR, PAIR)),
        ],
        compiler_params=pltpu.CompilerParams(collective_id=2, has_side_effects=True, vmem_limit_bytes=VMEM_LIMIT),
        cost_estimate=pl.CostEstimate(flops=flops, bytes_accessed=2**27, transcendentals=0),
    )(h_loc, rank_rows, near_rows, gate_rows, w_gate, w_up, w_down, wg_other, wu_other, wd_other)[0]


def routing_rows(ids_loc, gates_loc, n_experts):
    tok_dev = ids_loc.shape[0]
    chosen = ids_loc.T[None, :, :] == jnp.arange(n_experts, dtype=ids_loc.dtype)[:, None, None]
    mask = jnp.any(chosen, axis=1)
    gate_rows = jnp.sum(jnp.where(chosen, gates_loc.T[None, :, :], 0.0), axis=1)
    before = jnp.triu(jnp.ones((tok_dev, tok_dev), jnp.bfloat16), 1)
    rank = jnp.dot(mask.astype(jnp.bfloat16), before, preferred_element_type=jnp.float32)
    return jnp.where(mask, rank, -1.0), gate_rows


def block_of(cp_pos, tp_pos, n_cp, n_tp):
    per_chunk = n_tp // PAIR
    late = tp_pos // per_chunk
    chunk = late * (PAIR * n_cp - 1 - cp_pos) + (1 - late) * cp_pos
    return chunk * per_chunk + tp_pos % per_chunk


def owner_of(block, n_cp, n_tp):
    per_chunk = n_tp // PAIR
    chunk = block // per_chunk
    late = chunk // n_cp
    return late * (PAIR * n_cp - 1 - chunk) + (1 - late) * chunk, late * per_chunk + block % per_chunk


def front_kernel(n_cp, n_tp, x_hbm, wq_hbm, wk_hbm, wv_hbm, k_hbm, vt_hbm, q_hbm, x_buf, w_buf, q_st, k_st, vt_st, k_far, vt_far, q_far,
                 own_sem, w_sem, ring_sem, pair_sem, rx_sem, sk_sem, sv_sem, sq_sem, kv_sem, rq_sem, sf_sem, rf_sem, far_sem, pass_sem):
    n_x = n_tp // PAIR
    tok_dev, hid = x_hbm.shape
    half = tok_dev // PAIR
    head_dim = k_hbm.shape[1]
    n_loc = q_st.shape[1]
    chunk_len = tok_dev * n_x
    cp_pos, tp_pos = lax.axis_index("cp"), lax.axis_index("tp")
    x_pos, core = tp_pos // PAIR, tp_pos % PAIR
    sibling = PAIR * x_pos + 1 - core
    barrier = pltpu.get_barrier_semaphore()

    def slot_at(off, flip):
        return PAIR * ((x_pos + off + n_x) % n_x) + (core + flip) % PAIR

    own_copy = pltpu.make_async_copy(x_hbm, x_buf.at[tp_pos], own_sem)
    own_copy.start()
    width = n_loc * head_dim
    w_loads = [pltpu.make_async_copy(w, w_buf.at[:, pl.ds(i * width, width)], w_sem.at[i]) for i, w in enumerate((wq_hbm, wk_hbm, wv_hbm))]
    for one in w_loads:
        one.start()
    for step in (1, n_x - 1):
        pl.semaphore_signal(barrier, inc=1, device_id=mesh_id(cp_pos, slot_at(step, 0)), device_id_type=MESH)
    for step in range(1, PAIR * n_cp):
        pl.semaphore_signal(barrier, inc=1, device_id=mesh_id((cp_pos + step // PAIR) % n_cp, PAIR * x_pos + (core + step) % PAIR), device_id_type=MESH)
    pl.semaphore_wait(barrier, PAIR * n_cp + 1)

    def own_send(part, to_tp, sem):
        rows = pl.ds(part * half, half)
        return pltpu.make_async_remote_copy(x_hbm.at[rows], x_buf.at[tp_pos, rows], sem, rx_sem.at[tp_pos, part],
                                            device_id=mesh_id(cp_pos, to_tp), device_id_type=MESH)

    def pass_on(slot, part, to_tp, sem):
        rows = pl.ds(pl.multiple_of(part * half, half), half)
        return pltpu.make_async_remote_copy(x_buf.at[slot, rows], x_buf.at[slot, rows], sem, rx_sem.at[slot, part],
                                            device_id=mesh_id(cp_pos, to_tp), device_id_type=MESH)

    for i, (part, off) in enumerate(((0, 1), (1, -1), (1, 1), (0, -1))):
        own_send(part, slot_at(off, 0), ring_sem.at[i]).start()
    for part in BOTH:
        own_send(part, sibling, pair_sem.at[part]).start()

    def place_of(step):
        wave, other, side = step // 4, (step // PAIR) % PAIR, step % PAIR
        near = ((wave + 1) // PAIR) % PAIR
        swap = (wave // PAIR) * (1 - wave // 3)
        off = near * (PAIR * side - 1) + PAIR * (wave // 3)
        return slot_at(off, other), side + swap * (1 - PAIR * side), off

    def targets(from_cp, slot, part):
        block = block_of(from_cp, slot, n_cp, n_tp)
        pos = pl.multiple_of(block * tok_dev + part * half, half)
        q_core = ((block % 4 + 1) // PAIR) % PAIR
        q_pos = pl.multiple_of((PAIR * (block // 4) + (block % 4) // PAIR) * tok_dev + part * half, half)
        return ((k_hbm.at[pl.ds(pos, half)], 0, kv_sem.at[from_cp]), (vt_hbm.at[:, pl.ds(pos, half)], 1, kv_sem.at[from_cp]),
                (q_hbm.at[pl.ds(q_pos, half)], q_core, rq_sem.at[from_cp]))

    def remote(src, dst, s_sem, r_sem, to_cp, to_core):
        return pltpu.make_async_remote_copy(src, dst, s_sem, r_sem, device_id=mesh_id((to_cp + n_cp) % n_cp, PAIR * x_pos + to_core), device_id_type=MESH)

    far_refs = (k_far, vt_far, q_far)

    def outputs_of(step):
        slot, part, _ = place_of(step)
        for i in range(n_loc):
            to_cp = n_loc * core + i
            far = (to_cp - cp_pos + n_cp) % n_cp == n_cp // PAIR
            for kind, (src, (dst, to_core, r_sem)) in enumerate(zip((k_st.at[step, i], vt_st.at[step, i], q_st.at[step, i]), targets(cp_pos, slot, part))):
                s_sem = (sk_sem.at[i], sv_sem.at[i], sq_sem.at[i, to_core])[kind]
                here = and_(to_cp == cp_pos, to_core == core)

                @pl.when(here)
                def _():
                    pltpu.make_async_copy(src, dst, r_sem).start()

                @pl.when(far)
                def _():
                    remote(src, far_refs[kind].at[part, slot], s_sem, far_sem.at[kind, part, slot], cp_pos + 1 - PAIR * part, core).start()

                @pl.when(not_(or_(here, far)))
                def _():
                    remote(src, dst, s_sem, r_sem, to_cp, to_core).start()

    def pass_far(step, what):
        slot, part, _ = place_of(step)
        sign = 1 - PAIR * part

        @pl.when((cp_pos + sign + n_cp) % n_cp // n_loc == core)
        def _():
            for kind, (dst, to_core, r_sem) in enumerate(targets((cp_pos - sign + n_cp) % n_cp, slot, part)):
                src = far_refs[kind].at[part, slot]
                copy = remote(src, dst, pass_sem.at[kind, part, slot], r_sem, cp_pos + sign, to_core)
                if what == "start":
                    pltpu.make_async_copy(src, src, far_sem.at[kind, part, slot]).wait()
                    copy.start()
                else:
                    copy.wait_send()

    def project(step, carry):
        slot, part, off = place_of(step)
        wave, other, side = step // 4, (step // PAIR) % PAIR, step % PAIR

        @pl.when(step == 0)
        def _():
            own_copy.wait()
            for one in w_loads:
                one.wait()

        @pl.when(step > 1)
        def _():
            pass_on(slot, part, sibling, pair_sem.at[0]).wait_recv()

        @pl.when(and_(wave > 0, other == 0))
        def _():
            @pl.when(wave == 1)
            def _():
                pass_on(slot, part, slot_at(-off, 0), ring_sem.at[4 + side]).start()
            pass_on(slot, part, sibling, pair_sem.at[PAIR * wave + side]).start()

        x_rows = x_buf[slot, pl.ds(pl.multiple_of(part * half, half), half), :]
        qkv = jnp.dot(x_rows, w_buf[...], preferred_element_type=jnp.float32)
        for i in range(n_loc):
            q_st[step, i] = qkv[:, i * head_dim:(i + 1) * head_dim].astype(jnp.bfloat16)
            k_st[step, i] = qkv[:, (n_loc + i) * head_dim:(n_loc + i + 1) * head_dim].astype(jnp.bfloat16)
            vt_st[step, i] = qkv[:, (PAIR * n_loc + i) * head_dim:(PAIR * n_loc + i + 1) * head_dim].T.astype(jnp.bfloat16)

        @pl.when(step > 0)
        def _():
            outputs_of(step - 1)

        @pl.when(step >= lag)
        def _():
            pass_far(step - lag, "start")
        return carry

    n_steps, lag = PAIR * n_tp, 4
    lax.fori_loop(0, n_steps, project, 0)
    outputs_of(n_steps - 1)

    def pass_late(step, carry):
        pass_far(step, "start")
        return carry

    lax.fori_loop(n_steps - lag, n_steps, pass_late, 0)

    def whole(ref, count, sem):
        return pltpu.make_async_copy(ref.at[pl.ds(0, count)], ref.at[pl.ds(0, count)], sem)

    def forward(y, place, core_id):
        chunk = y if place == 0 else PAIR * n_cp - 1 - y
        cols = pl.ds(chunk * chunk_len, chunk_len)
        ref = k_hbm.at[cols] if core_id == 0 else vt_hbm.at[:, cols]
        return pltpu.make_async_remote_copy(ref, ref, sf_sem.at[PAIR * y + place], rf_sem.at[PAIR * y + place],
                                            device_id=mesh_id(cp_pos, sibling), device_id_type=MESH)

    for y in range(n_cp):
        whole(k_hbm, PAIR * chunk_len, kv_sem.at[y]).wait()
        for core_id in BOTH:
            @pl.when(core == core_id)
            def _():
                for place in BOTH:
                    forward(y, place, core_id).start()
    for y in range(n_cp):
        whole(q_hbm, chunk_len, rq_sem.at[y]).wait()
    for i in range(4):
        own_send(0, sibling, ring_sem.at[i]).wait_send()
    for i in BOTH:
        own_send(0, sibling, ring_sem.at[4 + i]).wait_send()
    for i in range(8):
        own_send(0, sibling, pair_sem.at[i]).wait_send()
    for i in range(n_loc):
        to_cp = n_loc * core + i
        for sem, to_core, count in ((sk_sem.at[i], 0, PAIR * chunk_len), (sv_sem.at[i], 1, PAIR * chunk_len),
                                    (sq_sem.at[i, 0], 0, chunk_len), (sq_sem.at[i, 1], 1, chunk_len)):
            @pl.when(not_(and_(to_cp == cp_pos, to_core == core)))
            def _():
                whole(k_hbm, count, sem).wait()
    def drain(step, carry):
        pass_far(step, "wait")
        return carry

    lax.fori_loop(0, n_steps, drain, 0)
    for core_id in BOTH:
        @pl.when(core == core_id)
        def _():
            for y in range(n_cp):
                for place in BOTH:
                    forward(y, place, core_id).wait_send()
                    forward(y, place, 1 - core_id).wait_recv()


def front_call(n_cp, n_tp, x_loc, w_parts, head_dim, n_loc):
    tok_dev, hid = x_loc.shape
    half = tok_dev // PAIR
    seq = tok_dev * n_cp * n_tp
    any_spec = pl.BlockSpec(memory_space=pl.ANY)
    n_steps = PAIR * n_tp
    return pl.pallas_call(
        functools.partial(front_kernel, n_cp, n_tp),
        name="gather_project",
        out_shape=(jax.ShapeDtypeStruct((seq, head_dim), jnp.bfloat16), jax.ShapeDtypeStruct((head_dim, seq), jnp.bfloat16),
                   jax.ShapeDtypeStruct((seq // PAIR, head_dim), jnp.bfloat16)),
        in_specs=[any_spec] * 4,
        out_specs=(any_spec,) * 3,
        scratch_shapes=[
            pltpu.VMEM((n_tp, tok_dev, hid), jnp.bfloat16),
            pltpu.VMEM((hid, 3 * n_loc * head_dim), jnp.bfloat16),
            pltpu.VMEM((n_steps, n_loc, half, head_dim), jnp.bfloat16),
            pltpu.VMEM((n_steps, n_loc, half, head_dim), jnp.bfloat16),
            pltpu.VMEM((n_steps, n_loc, head_dim, half), jnp.bfloat16),
            pltpu.VMEM((PAIR, n_tp, half, head_dim), jnp.bfloat16),
            pltpu.VMEM((PAIR, n_tp, head_dim, half), jnp.bfloat16),
            pltpu.VMEM((PAIR, n_tp, half, head_dim), jnp.bfloat16),
            dma,
            dma((3,)),
            dma((6,)),
            dma((8,)),
            dma((n_tp, PAIR)),
            dma((n_loc,)),
            dma((n_loc,)),
            dma((n_loc, PAIR)),
            dma((n_cp,)),
            dma((n_cp,)),
            dma((PAIR * n_cp,)),
            dma((PAIR * n_cp,)),
            dma((3, PAIR, n_tp)),
            dma((3, PAIR, n_tp)),
        ],
        compiler_params=pltpu.CompilerParams(collective_id=0, has_side_effects=True, vmem_limit_bytes=VMEM_LIMIT),
        cost_estimate=pl.CostEstimate(flops=PAIR * n_tp * tok_dev * hid * 3 * n_loc * head_dim, bytes_accessed=2**26, transcendentals=0),
    )(x_loc, *w_parts)


def attend_kernel(n_cp, n_tp, k_hbm, vt_hbm, q_hbm, x_hbm, wo_hbm, wg_hbm, wu_hbm, wd_hbm, rank_hbm,
                  h_ref, o_hbm, wgx_hbm, wux_hbm, wdx_hbm, near_hbm,
                  k_buf, vt_buf, q_buf, qt_buf, o_st, o_buf, wo_buf, x_buf, s_even, s_odd, p_even, p_odd, p_near, shrink_even, shrink_odd, acc, m_ref, l_ref,
                  in_sem, so_sem, ro_sem, swo_sem, rwo_sem, sw_sem, rw_sem, sr_sem, rr_sem, o_sem):
    n_dev = n_cp * n_tp
    n_x = n_tp // PAIR
    tok_dev, hid = x_buf.shape
    head_dim = k_buf.shape[1]
    n_heads = o_buf.shape[0]
    cp_pos, tp_pos = lax.axis_index("cp"), lax.axis_index("tp")
    x_pos, core = tp_pos // PAIR, tp_pos % PAIR
    head = n_cp * x_pos + cp_pos
    scale = (head_dim ** -0.5) * 1.4426950408889634
    loads = [pltpu.make_async_copy(src, dst, in_sem.at[i]) for i, (src, dst) in enumerate(
        ((q_hbm, q_buf), (k_hbm, k_buf), (vt_hbm, vt_buf), (x_hbm, x_buf), (wo_hbm, wo_buf.at[tp_pos])))]
    for one in loads:
        one.start()

    enter_all(n_cp, n_tp)

    def wo_send(step):
        return pltpu.make_async_remote_copy(wo_hbm, wo_buf.at[tp_pos], swo_sem.at[step], rwo_sem.at[step],
                                            device_id=mesh_id(cp_pos, (tp_pos + step) % n_tp), device_id_type=MESH)

    def wo_arrival(step):
        return pltpu.make_async_remote_copy(wo_hbm, wo_buf.at[(tp_pos + n_tp - step) % n_tp], swo_sem.at[step], rwo_sem.at[step],
                                            device_id=mesh_id(cp_pos, tp_pos), device_id_type=MESH)

    keep = wgx_hbm.shape[0]
    swaps = [pltpu.make_async_remote_copy(src.at[pl.ds((1 - core) * keep, keep)], dst, sw_sem.at[i], rw_sem.at[i],
                                          device_id=mesh_id(cp_pos, PAIR * x_pos + 1 - core), device_id_type=MESH)
             for i, (src, dst) in enumerate(((wg_hbm, wgx_hbm), (wu_hbm, wux_hbm), (wd_hbm, wdx_hbm)))]
    ranks = []
    for slot, off in ((1, 1), (PAIR, -1), (3, PAIR)):
        for part, place in enumerate((((cp_pos + off + n_cp) % n_cp, tp_pos), (cp_pos, PAIR * ((x_pos + off + n_x) % n_x) + core))):
            ranks.append(pltpu.make_async_remote_copy(rank_hbm, near_hbm.at[part, slot], sr_sem.at[part, slot], rr_sem.at[part, slot],
                                                      device_id=mesh_id(*place), device_id_type=MESH))
    for step in range(1, n_tp):
        wo_send(step).start()
    for one in swaps + ranks:
        one.start()
    for one in loads[:3]:
        one.wait()

    def columns(block):
        return pl.ds(pl.multiple_of(block * tok_dev, tok_dev), tok_dev)

    def scores(block, cols, s_ref, masked):
        s_vals = jnp.dot(k_buf[columns(block), :], qt_buf[:, cols], preferred_element_type=jnp.float32)
        if masked:
            key_id = lax.broadcasted_iota(jnp.int32, s_vals.shape, 0)
            query_id = lax.broadcasted_iota(jnp.int32, s_vals.shape, 1)
            s_vals = jnp.where(key_id <= query_id, s_vals, -1e30)
        s_ref[...] = s_vals
        return jnp.max(s_vals, **COLUMN_WISE)

    def soften(s_ref, s_top, cols, p_ref, shrink_ref):
        m_old = m_ref[:, cols]
        m_new = jnp.maximum(m_old, s_top)
        shrink = jnp.exp2((m_old - m_new) * scale)
        m_ref[:, cols] = m_new
        shrink_ref[...] = shrink
        prob = jnp.exp2((s_ref[...] - m_new) * scale)
        l_ref[:, cols] = l_ref[:, cols] * shrink + jnp.sum(prob, **COLUMN_WISE)
        p_ref[...] = prob.astype(jnp.bfloat16)

    def gather_values(block, cols, p_ref, shrink_ref):
        acc[:, cols] = acc[:, cols] * shrink_ref[...] + jnp.dot(vt_buf[:, columns(block)], p_ref[...], preferred_element_type=jnp.float32)

    def query_pair(turn, carry):
        g = (turn + n_x * (cp_pos % PAIR) + x_pos) % (n_dev // 4)
        q_rows = q_buf[pl.ds(pl.multiple_of(g * PAIR * tok_dev, PAIR * tok_dev), PAIR * tok_dev), :]
        qt_buf[...] = q_rows.astype(jnp.float32).T.astype(jnp.bfloat16)
        m_ref[...] = jnp.full_like(m_ref, -1e30)
        l_ref[...] = jnp.zeros_like(l_ref)
        acc[...] = jnp.zeros_like(acc)
        p_odd[...] = jnp.zeros_like(p_odd)
        shrink_odd[...] = jnp.ones_like(shrink_odd)
        near = ((0, core), (1, 3 - core), (1 - core, 0), (1, 1 - core), (1, 2 - core))
        lanes = [(s_even, p_even, shrink_even, 0), (s_even, p_even, shrink_even, 1), (s_odd, p_near, shrink_odd, 0), (s_odd, p_near, shrink_odd, 1)]
        tops = {}

        def near_refs(i):
            s_ref, p_ref, shrink_ref, place = lanes[i % 4]
            cols = pl.ds(place * tok_dev, tok_dev)
            return s_ref.at[:, cols], p_ref.at[:, cols], shrink_ref.at[:, cols]

        def near_scores(i):
            r, block = near[i]
            tops[i] = scores(4 * g + block, columns(r), near_refs(i)[0], i < 2)

        def near_soften(i):
            s_ref, p_ref, shrink_ref = near_refs(i)
            soften(s_ref, tops[i], columns(near[i][0]), p_ref, shrink_ref)

        def near_values(i):
            _, p_ref, shrink_ref = near_refs(i)
            gather_values(4 * g + near[i][1], columns(near[i][0]), p_ref, shrink_ref)

        for i in range(len(near) + 2):
            if i < len(near):
                near_scores(i)
            if 0 <= i - 1 < len(near):
                near_soften(i - 1)
            if 0 <= i - 2:
                near_values(i - 2)
        shrink_odd[...] = jnp.ones_like(shrink_odd)
        wide = pl.ds(0, PAIR * tok_dev)

        def far_pair(n, top_even):
            top_odd = scores(PAIR * n + 1, wide, s_odd, False)
            soften(s_even, top_even, wide, p_even, shrink_even)
            gather_values(jnp.maximum(PAIR * n - 1, 0), wide, p_odd, shrink_odd)
            top_next = scores(PAIR * n + 2, wide, s_even, False)
            soften(s_odd, top_odd, wide, p_odd, shrink_odd)
            gather_values(PAIR * n, wide, p_even, shrink_even)
            return top_next

        lax.fori_loop(0, PAIR * g, far_pair, scores(0, wide, s_even, False))
        gather_values(jnp.maximum(4 * g - 1, 0), wide, p_odd, shrink_odd)
        out = (acc[...] / l_ref[...]).T.astype(jnp.bfloat16)
        for r in BOTH:
            o_st[PAIR * g + r] = out[r * tok_dev:(r + 1) * tok_dev]
            o_push(PAIR * g + r, "start")
        return carry

    def o_push(index, what):
        block = 4 * (index // PAIR) + (1 - core) * 3 * (index % PAIR) + core * (1 + index % PAIR)
        to_cp, to_tp = owner_of(block, n_cp, n_tp)
        here = and_(to_cp == cp_pos, to_tp == tp_pos)
        if what == "start":
            @pl.when(here)
            def _():
                pltpu.make_async_copy(o_st.at[index], o_hbm.at[head], ro_sem.at[head]).start()

        @pl.when(not_(here))
        def _():
            copy = pltpu.make_async_remote_copy(o_st.at[index], o_hbm.at[head], so_sem.at[index], ro_sem.at[head],
                                                device_id=mesh_id(to_cp, to_tp), device_id_type=MESH)
            if what == "start":
                copy.start()
            else:
                copy.wait_send()

    lax.fori_loop(0, n_dev // 4, query_pair, 0)

    for step in range(1, n_tp):
        wo_arrival(step).wait_recv()
    for one in loads[3:]:
        one.wait()
    for j in range(n_heads):
        pltpu.make_async_copy(o_hbm.at[j], o_hbm.at[j], ro_sem.at[j]).wait()
    o_load = pltpu.make_async_copy(o_hbm, o_buf, o_sem)
    o_load.start()
    o_load.wait()
    o_rows = jnp.concatenate([o_buf[j] for j in range(n_heads)], axis=1)
    n_cols = min(512, hid // PAIR)

    for col in range(0, hid, n_cols):
        cols = pl.ds(col, n_cols)
        w_cols = wo_buf[:, :, cols].reshape(n_heads * head_dim, n_cols)
        h_cols = (x_buf[:, cols].astype(jnp.float32) + jnp.dot(o_rows, w_cols, preferred_element_type=jnp.float32)).astype(jnp.bfloat16)
        h_ref[PAIR * col // hid, :, pl.ds(col % (hid // PAIR), n_cols)] = h_cols

    for step in range(1, n_tp):
        wo_send(step).wait_send()
    for one in swaps + ranks:
        one.wait()

    def drain(index, carry):
        o_push(index, "wait")
        return carry

    lax.fori_loop(0, n_dev // PAIR, drain, 0)


def attend_call(n_cp, n_tp, k_all, vt_all, q_all, x_loc, wo_loc, w_gate, w_up, w_down, rank_rows):
    n_dev = n_cp * n_tp
    tok_dev, hid = x_loc.shape
    seq, head_dim = k_all.shape
    n_heads = n_tp * wo_loc.shape[0] // head_dim
    keep = w_gate.shape[0] // PAIR
    any_spec = pl.BlockSpec(memory_space=pl.ANY)
    bf16 = jnp.bfloat16
    h_loc, _, wg_other, wu_other, wd_other, near_rows = pl.pallas_call(
        functools.partial(attend_kernel, n_cp, n_tp),
        name="attend_heads",
        out_shape=(jax.ShapeDtypeStruct((PAIR, tok_dev, hid // PAIR), bf16), jax.ShapeDtypeStruct((n_heads, tok_dev, head_dim), bf16))
        + tuple(jax.ShapeDtypeStruct((keep,) + w.shape[1:], bf16) for w in (w_gate, w_up, w_down))
        + (jax.ShapeDtypeStruct((PAIR, 4) + rank_rows.shape, jnp.float32),),
        in_specs=[any_spec] * 9,
        out_specs=(pl.BlockSpec(memory_space=pltpu.VMEM),) + (any_spec,) * 5,
        scratch_shapes=[
            pltpu.VMEM((seq, head_dim), bf16),
            pltpu.VMEM((head_dim, seq), bf16),
            pltpu.VMEM((seq // PAIR, head_dim), bf16),
            pltpu.VMEM((head_dim, PAIR * tok_dev), bf16),
            pltpu.VMEM((n_dev // PAIR, tok_dev, head_dim), bf16),
            pltpu.VMEM((n_heads, tok_dev, head_dim), bf16),
            pltpu.VMEM((n_tp,) + wo_loc.shape, bf16),
            pltpu.VMEM((tok_dev, hid), bf16),
            pltpu.VMEM((tok_dev, PAIR * tok_dev), jnp.float32),
            pltpu.VMEM((tok_dev, PAIR * tok_dev), jnp.float32),
            pltpu.VMEM((tok_dev, PAIR * tok_dev), bf16),
            pltpu.VMEM((tok_dev, PAIR * tok_dev), bf16),
            pltpu.VMEM((tok_dev, PAIR * tok_dev), bf16),
            pltpu.VMEM((1, PAIR * tok_dev), jnp.float32),
            pltpu.VMEM((1, PAIR * tok_dev), jnp.float32),
            pltpu.VMEM((head_dim, PAIR * tok_dev), jnp.float32),
            pltpu.VMEM((1, PAIR * tok_dev), jnp.float32),
            pltpu.VMEM((1, PAIR * tok_dev), jnp.float32),
            dma((5,)),
            dma((n_dev // PAIR,)),
            dma((n_heads,)),
            dma((n_tp,)),
            dma((n_tp,)),
            dma((3,)),
            dma((3,)),
            dma((PAIR, 4)),
            dma((PAIR, 4)),
            dma,
        ],
        compiler_params=pltpu.CompilerParams(collective_id=1, has_side_effects=True, vmem_limit_bytes=VMEM_LIMIT),
        cost_estimate=pl.CostEstimate(flops=PAIR * seq * seq * head_dim // PAIR, bytes_accessed=2**26, transcendentals=seq * seq // 4),
    )(k_all, vt_all, q_all, x_loc, wo_loc, w_gate, w_up, w_down, rank_rows)
    return h_loc, near_rows, wg_other, wu_other, wd_other


def solution(mesh):
    n_cp = mesh.shape["cp"]
    n_tp = mesh.shape["tp"]
    row_spec = P(("dp", "cp", "tp"), None)
    head_spec = P(None, "tp", None)
    expert_spec = P(("cp", "tp"), None, None)

    def device_step(x_loc, w_q, w_k, w_v, w_o, ids_loc, gates_loc, w_gate, w_up, w_down):
        tok_dev, hid_dim = x_loc.shape
        n_loc, head_dim = w_q.shape[1:]
        n_experts = w_gate.shape[0] * n_cp * n_tp // PAIR
        capacity = ids_loc.shape[1] * tok_dev // n_experts
        w_parts = [w.reshape(hid_dim, n_loc * head_dim) for w in (w_q, w_k, w_v)]
        rank_rows, gate_rows = routing_rows(ids_loc, gates_loc, n_experts)
        k_all, vt_all, q_all = front_call(n_cp, n_tp, x_loc, w_parts, head_dim, n_loc)
        h_loc, near_rows, *others = attend_call(n_cp, n_tp, k_all, vt_all, q_all, x_loc, w_o.reshape(n_loc * head_dim, hid_dim), w_gate, w_up, w_down, rank_rows)
        return moe_call(n_cp, n_tp, capacity, h_loc, rank_rows, near_rows, gate_rows, w_gate, w_up, w_down, *others)

    return jax.shard_map(device_step, mesh=mesh, in_specs=(row_spec, head_spec, head_spec, head_spec, P("tp", None, None), row_spec, row_spec, expert_spec, expert_spec, expert_spec), out_specs=row_spec, check_vma=False)
```

```python
import functools

import jax
import jax.numpy as jnp
from jax import lax
from jax.experimental import pallas as pl
from jax.experimental.pallas import tpu as pltpu
from jax.sharding import PartitionSpec as P

MESH = pl.DeviceIdType.MESH
PAIR = 2
BOTH = range(PAIR)
ROWS_ROWS = (((0,), (0,)), ((), ()))
COLUMN_WISE = {"axis": 0, "keepdims": True}
dma = pltpu.SemaphoreType.DMA
and_, or_, not_ = jnp.logical_and, jnp.logical_or, jnp.logical_not
VMEM_LIMIT = 66_000_000
PLACES = ((0, 0), (0, 1), (1, 0), (0, -1), (-1, 0), (1, 1), (-1, -1), (1, -1), (-1, 1), (0, PAIR), (PAIR, 0), (1, PAIR), (PAIR, 1), (-1, PAIR), (PAIR, -1), (PAIR, PAIR))
FIRST_FAR = 9
GROUPS = ("5656", "7878", "bcbc", "dede", "9a9a", "0f0f", "1234", "1234")
FLIPS = ("0011",) * 6 + ("0000", "1111")
ADD_ORDER = "05678bcde9a1234f"
SOURCES = (0, -1, 1, PAIR)


def peer_of(step, cp_pos, tp_pos, n_cp, n_tp):
    n_x = n_tp // PAIR
    off_x = (step // PAIR) % n_x
    off_y = (off_x + step // n_tp) % n_cp
    return (cp_pos + off_y) % n_cp, ((tp_pos // PAIR + off_x) % n_x) * 2 + (tp_pos % PAIR + step % PAIR) % PAIR


def mesh_id(cp_pos, tp_pos):
    return {"cp": cp_pos, "tp": tp_pos}


def enter_all(n_cp, n_tp):
    cp_pos, tp_pos = lax.axis_index("cp"), lax.axis_index("tp")

    def signal_peer(step, carry):
        to_cp, to_tp = peer_of(step, cp_pos, tp_pos, n_cp, n_tp)
        pl.semaphore_signal(pltpu.get_barrier_semaphore(), inc=1, device_id=mesh_id(to_cp, to_tp), device_id_type=MESH)
        return carry

    lax.fori_loop(1, n_cp * n_tp, signal_peer, 0)
    pl.semaphore_wait(pltpu.get_barrier_semaphore(), n_cp * n_tp - 1)


def pick(values, index):
    out = values[-1]
    for k, value in enumerate(values[:-1]):
        out = jnp.where(index == k, value, out)
    return out


def moe_kernel(n_cp, n_tp, group, h_hbm, rank_hbm, near_hbm, gate_ref, wg_hbm, wu_hbm, wd_hbm, wgx_hbm, wux_hbm, wdx_hbm,
               y_ref, rx_hbm, rl_hbm, rz_hbm, zl_hbm,
               h_buf, rank_buf, wg_buf, wu_buf, wd_buf, ring, own_stage, z_ring, x_buf, z_buf, acc, parts,
               w_sem, rank_sem, in_sem, x_sem, z_sem, hs_sem, hr_sem, ss_sem, rx_sem, rl_sem, fl_sem, sz_sem, rz_sem, zl_sem, fz_sem):
    n_x = n_tp // PAIR
    tok_dev, half_hid = h_buf.shape[2:]
    hid = PAIR * half_hid
    cap = ring.shape[3] // PAIR
    cp_pos, tp_pos = lax.axis_index("cp"), lax.axis_index("tp")
    x_pos, core = tp_pos // PAIR, tp_pos % PAIR
    half_tok = tok_dev // PAIR

    def at(off_y, off_x, flip):
        return (cp_pos + off_y + n_cp) % n_cp, PAIR * ((x_pos + off_x + n_x) % n_x) + (core + flip) % PAIR

    def line(place):
        return place[0] * n_tp + place[1]

    def send(src, dst, s_sem, r_sem, place):
        return pltpu.make_async_remote_copy(src, dst, s_sem, r_sem, device_id=mesh_id(*place), device_id_type=MESH)

    def await_bytes(ref, sem):
        pltpu.make_async_copy(ref, ref, sem).wait()

    h_loads = [pltpu.make_async_copy(h_hbm.at[part], h_buf.at[part, 0], in_sem.at[part]) for part in BOTH]
    rank_loads = []
    for part in BOTH:
        rank_loads.append(pltpu.make_async_copy(rank_hbm, rank_buf.at[part, 0], rank_sem.at[PAIR * part]))
        rank_loads.append(pltpu.make_async_copy(near_hbm.at[part, pl.ds(1, 3)], rank_buf.at[part, pl.ds(1, 3)], rank_sem.at[PAIR * part + 1]))
    w_loads = []
    for slot, (own, other, buf) in enumerate(((wg_hbm, wgx_hbm, wg_buf), (wu_hbm, wux_hbm, wu_buf), (wd_hbm, wdx_hbm, wd_buf))):
        w_loads.append(pltpu.make_async_copy(own.at[pl.ds(PAIR * core, PAIR)], buf.at[0], w_sem.at[PAIR * slot]))
        w_loads.append(pltpu.make_async_copy(other, buf.at[1], w_sem.at[PAIR * slot + 1]))
    for one in h_loads + rank_loads:
        one.start()
    enter_all(n_cp, n_tp)

    def along(part, off):
        return at(off, 0, 0) if part == 0 else at(0, off, 0)

    def across(part, off, flip):
        return at(0, off, flip) if part == 0 else at(off, 0, flip)

    def rows_of(piece):
        return pl.ds(piece * half_tok, half_tok)

    def spread(part, i):
        piece, off, slot = ((0, 1, 1), (1, -1, PAIR), (1, 1, 1), (0, -1, PAIR), (0, 1, 3), (1, -1, 3))[i]
        rows = rows_of(piece)
        src = h_hbm.at[part, rows] if i < 4 else h_buf.at[part, 1 if i == 4 else 2, rows]
        return send(src, h_buf.at[part, slot, rows], hs_sem.at[part, i], hr_sem.at[part, slot, piece], along(part, off))

    def await_h(part, slot, piece):
        await_bytes(h_buf.at[part, slot, rows_of(piece)], hr_sem.at[part, slot, piece])

    for i in range(4):
        for part in BOTH:
            spread(part, i).start()
    for one in w_loads:
        one.start()
    for one in h_loads + rank_loads:
        one.wait()

    slots = lax.broadcasted_iota(jnp.int32, (cap, tok_dev), 0).astype(jnp.float32)

    def gather_rows(part, stage, m):
        turn = m // PAIR
        off = turn + (turn // PAIR) * (5 - PAIR * turn)
        first = PAIR * line(across(part, off, m % PAIR))
        chosen = [jnp.where(rank_buf[part, stage, pl.ds(first + i, 1), :] == slots, 1.0, 0.0) for i in BOTH]
        chosen = jnp.concatenate(chosen, axis=0).astype(jnp.bfloat16)
        return jnp.dot(chosen, h_buf[part, stage], preferred_element_type=jnp.float32).astype(jnp.bfloat16)

    def source_line(part, stage, off):
        a = SOURCES[stage]
        return line(at(a, off, 0) if part == 0 else at(off, a, 0))

    def await_ring(part, stage):
        def one(m, carry):
            await_bytes(ring.at[part, stage % PAIR, m], ss_sem.at[part, stage % PAIR, m])
            return carry
        lax.fori_loop(1, 8, one, 0)

    def own_copy(part, stage):
        src_line = source_line(part, stage, 0)
        return pltpu.make_async_copy(own_stage.at[part, stage], rx_hbm.at[part, src_line], rx_sem.at[part, src_line])

    def run_stage(stage):
        side = stage % PAIR
        for part in BOTH:
            if stage >= 2:
                await_ring(part, stage)
            own_stage[part, stage] = gather_rows(part, stage, 0)

            def fill(m, carry):
                ring[part, side, m] = gather_rows(part, stage, m)
                return carry

            lax.fori_loop(1, 8, fill, 0)
        lines = [source_line(part, stage, 0) for part in BOTH]
        for flip in BOTH:
            for way, off in enumerate((1, -1)):
                for part in BOTH:
                    m = 6 + flip
                    send(ring.at[part, side, m, pl.ds(way * cap, cap)], rl_hbm.at[part, way, stage, flip], ss_sem.at[part, side, m],
                         rl_sem.at[part, way, stage, flip], across(part, off, 0)).start()
        for m, off in ((PAIR, 1), (4, -1), (3, 1), (5, -1), (1, 0)):
            for part in BOTH:
                send(ring.at[part, side, m], rx_hbm.at[part, lines[part]], ss_sem.at[part, side, m], rx_sem.at[part, lines[part]],
                     across(part, off, m % PAIR)).start()
        for part in BOTH:
            own_copy(part, stage).start()

    def relay(part, stage, way, flip):
        off = 1 - PAIR * way
        src_line = source_line(part, stage, -off)
        return send(rl_hbm.at[part, way, stage, flip], rx_hbm.at[part, src_line, pl.ds(way * cap, cap)], fl_sem.at[part, way, stage, flip],
                    rx_sem.at[part, src_line], across(part, off, flip))

    def run_relays(stage):
        for flip in BOTH:
            for way in BOTH:
                for part in BOTH:
                    await_bytes(rl_hbm.at[part, way, stage, flip], rl_sem.at[part, way, stage, flip])
                    relay(part, stage, way, flip).start()

    run_stage(0)
    for part in BOTH:
        await_h(part, 1, 0)
        spread(part, 4).start()
    for part in BOTH:
        await_h(part, PAIR, 1)
        spread(part, 5).start()
    for part in BOTH:
        await_h(part, 1, 1)
    run_stage(1)
    gate_all = gate_ref[...]
    high = gate_all.astype(jnp.bfloat16).astype(jnp.float32)
    rest = gate_all - high
    mid = rest.astype(jnp.bfloat16).astype(jnp.float32)
    parts[0] = high
    parts[1] = mid
    parts[2] = rest - mid
    for part in BOTH:
        acc[:, part * half_hid:(part + 1) * half_hid] = h_buf[part, 0].astype(jnp.float32)
    run_relays(0)
    for part in BOTH:
        await_h(part, PAIR, 0)
    run_stage(2)
    run_relays(1)
    for part in BOTH:
        await_h(part, 3, 0)
        await_h(part, 3, 1)
    run_stage(3)
    run_relays(2)
    for one in w_loads:
        one.wait()

    rows = group * cap
    n_cols = min(512, hid)

    def expert_rows(slot, i):
        x_rows = x_buf[:, pl.ds(i * cap, cap), :].reshape(rows, hid)
        hidden = []
        for half in BOTH:
            gate_pre = jnp.dot(x_rows, wg_buf[half, i], preferred_element_type=jnp.float32)
            up_pre = jnp.dot(x_rows, wu_buf[half, i], preferred_element_type=jnp.float32)
            hidden.append((gate_pre * (1.0 / (1.0 + jnp.exp(-gate_pre))) * up_pre).astype(jnp.bfloat16))
        for col in range(0, hid, n_cols):
            z_rows = (jnp.dot(hidden[0], wd_buf[0, i, :, pl.ds(col, n_cols)], preferred_element_type=jnp.float32)
                      + jnp.dot(hidden[1], wd_buf[1, i, :, pl.ds(col, n_cols)], preferred_element_type=jnp.float32))
            z_ring[slot, :, pl.ds(i * cap, cap), pl.ds(col, n_cols)] = z_rows.astype(jnp.bfloat16).reshape(group, cap, n_cols)

    def place_at(g, q):
        places = [int(names[q], 16) for names in GROUPS]
        off_y, off_x = (pick([PLACES[p][k] for p in places], g) for k in BOTH)
        return off_y, off_x, pick([int(flips[q]) for flips in FLIPS], g), pick(places, g)

    my_line = line((cp_pos, tp_pos))

    def await_slot(slot):
        for q in range(group):
            await_bytes(z_ring.at[slot, q], sz_sem.at[slot, q])

    n_far = len(PLACES) - FIRST_FAR

    def z_relay(index, flip, way):
        off_y, off_x = PLACES[FIRST_FAR + index]
        sign = 1 - PAIR * way
        lead_y, lead_x = sign * (off_y == 2), sign * (off_x == 2)
        from_line = line(at(-lead_y, -lead_x, 0))
        to_y = sign if off_y == 2 else off_y
        to_x = sign if off_x == 2 else off_x
        return send(zl_hbm.at[index, flip, way], rz_hbm.at[from_line, pl.ds(way * cap, cap)], fz_sem.at[index, flip, way],
                    rz_sem.at[from_line], at(to_y, to_x, flip))

    def each_relay(*indices):
        return [(index, flip, way) for flip in BOTH for way in BOTH for index in indices]

    def run_z_relays(*indices):
        for key in each_relay(*indices):
            await_bytes(zl_hbm.at[key], zl_sem.at[key])
            z_relay(*key).start()

    def expert_group(g, carry):
        slot = g % 3

        @pl.when(g == 2)
        def _():
            run_relays(3)

        sources = [line(at(*place_at(g, q)[:3])) for q in range(group)]
        loads = []
        for q in range(group):
            for part in BOTH:
                await_bytes(rx_hbm.at[part, sources[q]], rx_sem.at[part, sources[q]])
                loads.append(pltpu.make_async_copy(rx_hbm.at[part, sources[q]], x_buf.at[q, :, pl.ds(part * half_hid, half_hid)], x_sem.at[part, q]))
                loads[-1].start()

        @pl.when(g >= 3)
        def _():
            await_slot(slot)
        for one in loads:
            one.wait()
        for i in BOTH:
            expert_rows(slot, i)
        for q in range(group):
            off_y, off_x, flip, p = place_at(g, q)
            alone = and_(p == 0, flip == 0)

            @pl.when(alone)
            def _():
                pltpu.make_async_copy(z_ring.at[slot, q], rz_hbm.at[my_line], rz_sem.at[my_line]).start()

            @pl.when(and_(p < FIRST_FAR, not_(alone)))
            def _():
                send(z_ring.at[slot, q], rz_hbm.at[my_line], sz_sem.at[slot, q], rz_sem.at[my_line], at(off_y, off_x, flip)).start()

            @pl.when(p >= FIRST_FAR)
            def _():
                lead_y, lead_x = jnp.where(off_y == 2, 1, 0), jnp.where(off_x == 2, 1, 0)
                for way in BOTH:
                    sign = 1 - PAIR * way
                    send(z_ring.at[slot, q, pl.ds(way * cap, cap)], zl_hbm.at[p - FIRST_FAR, flip, way], sz_sem.at[slot, q],
                         zl_sem.at[p - FIRST_FAR, flip, way], at(sign * lead_y, sign * lead_x, 0)).start()
        for turn, indices in ((5, (PAIR, 3)), (6, (4, 5)), (7, (0, 1))):
            @pl.when(g == turn)
            def _():
                run_z_relays(*indices)
        return carry

    lax.fori_loop(0, len(GROUPS), expert_group, 0)

    def combine(turn, carry):
        off_y, off_x = (pick([PLACES[int(p, 16)][k] for p in ADD_ORDER], turn) for k in BOTH)
        homes = [line(at(-off_y, -off_x, q)) for q in BOTH]
        loads = []
        for q in BOTH:
            await_bytes(rz_hbm.at[homes[q]], rz_sem.at[homes[q]])
            loads.append(pltpu.make_async_copy(rz_hbm.at[homes[q]], z_buf.at[q], z_sem.at[q]))
            loads[-1].start()
        weights = [[], [], []]
        for q in BOTH:
            for i in BOTH:
                row = pl.ds(PAIR * homes[q] + i, 1)
                chosen = rank_buf[0, 0, row, :] == slots
                for part in range(3):
                    weights[part].append(jnp.where(chosen, parts[part, row, :], 0.0))
        weights = [jnp.concatenate(w, axis=0).astype(jnp.bfloat16) for w in weights]
        for one in loads:
            one.wait()
        for col in range(0, hid, n_cols):
            z_rows = z_buf[:, :, pl.ds(col, n_cols)].reshape(4 * cap, n_cols)
            total = None
            for part in range(3):
                term = lax.dot_general(weights[part], z_rows, ROWS_ROWS, preferred_element_type=jnp.float32)
                total = term if total is None else total + term
            acc[:, pl.ds(col, n_cols)] += total
        return carry

    lax.fori_loop(0, FIRST_FAR - 4, combine, 0)
    run_z_relays(6)
    lax.fori_loop(FIRST_FAR - 4, len(ADD_ORDER), combine, 0)
    y_ref[...] = acc[...].astype(jnp.bfloat16)

    for part in BOTH:
        for i in range(6):
            spread(part, i).wait_send()
        for stage in (PAIR, 3):
            await_ring(part, stage)
        for stage in range(4):
            for way in BOTH:
                for flip in BOTH:
                    relay(part, stage, way, flip).wait_send()
    last = len(GROUPS) - 3
    for g in range(last, len(GROUPS)):
        for q in range(group):
            if GROUPS[g][q] + FLIPS[g][q] != "00":
                await_bytes(z_ring.at[g % 3, q], sz_sem.at[g % 3, q])
    for key in each_relay(*range(n_far)):
        z_relay(*key).wait_send()


def moe_call(n_cp, n_tp, cap, h_loc, rank_rows, near_rows, gate_rows, w_gate, w_up, w_down, wg_other, wu_other, wd_other):
    n_dev = n_cp * n_tp
    _, tok_dev, half_hid = h_loc.shape
    hid = PAIR * half_hid
    half_f = w_gate.shape[2]
    n_experts = rank_rows.shape[0]
    group = len(GROUPS[0])
    n_far = len(PLACES) - FIRST_FAR
    bf16 = jnp.bfloat16
    any_spec = pl.BlockSpec(memory_space=pl.ANY)
    vmem_spec = pl.BlockSpec(memory_space=pltpu.VMEM)
    flops = PAIR * n_dev * PAIR * cap * hid * PAIR * half_f * 3
    return pl.pallas_call(
        functools.partial(moe_kernel, n_cp, n_tp, group),
        name="routed_experts",
        out_shape=(jax.ShapeDtypeStruct((tok_dev, hid), bf16), jax.ShapeDtypeStruct((PAIR, n_dev, PAIR * cap, half_hid), bf16),
                   jax.ShapeDtypeStruct((PAIR, PAIR, 4, PAIR, cap, half_hid), bf16), jax.ShapeDtypeStruct((n_dev, PAIR * cap, hid), bf16),
                   jax.ShapeDtypeStruct((n_far, PAIR, 2, cap, hid), bf16)),
        in_specs=[any_spec, any_spec, any_spec, vmem_spec] + [any_spec] * 6,
        out_specs=(vmem_spec,) + (any_spec,) * 4,
        scratch_shapes=[
            pltpu.VMEM((PAIR, 4, tok_dev, half_hid), bf16),
            pltpu.VMEM((PAIR, 4, n_experts, tok_dev), jnp.float32),
            pltpu.VMEM((PAIR, PAIR, hid, half_f), bf16),
            pltpu.VMEM((PAIR, PAIR, hid, half_f), bf16),
            pltpu.VMEM((PAIR, PAIR, half_f, hid), bf16),
            pltpu.VMEM((PAIR, PAIR, 8, PAIR * cap, half_hid), bf16),
            pltpu.VMEM((PAIR, 4, PAIR * cap, half_hid), bf16),
            pltpu.VMEM((3, group, PAIR * cap, hid), bf16),
            pltpu.VMEM((group, PAIR * cap, hid), bf16),
            pltpu.VMEM((PAIR, PAIR * cap, hid), bf16),
            pltpu.VMEM((tok_dev, hid), jnp.float32),
            pltpu.VMEM((3, n_experts, tok_dev), jnp.float32),
            dma((6,)), dma((4,)), dma((PAIR,)), dma((PAIR, group)), dma((PAIR,)),
            dma((PAIR, 6)), dma((PAIR, 4, PAIR)), dma((PAIR, PAIR, 8)), dma((PAIR, n_dev)), dma((PAIR, PAIR, 4, PAIR)), dma((PAIR, PAIR, 4, PAIR)),
            dma((3, group)), dma((n_dev,)), dma((n_far, PAIR, PAIR)), dma((n_far, PAIR, PAIR)),
        ],
        compiler_params=pltpu.CompilerParams(collective_id=2, has_side_effects=True, vmem_limit_bytes=VMEM_LIMIT),
        cost_estimate=pl.CostEstimate(flops=flops, bytes_accessed=2**27, transcendentals=0),
    )(h_loc, rank_rows, near_rows, gate_rows, w_gate, w_up, w_down, wg_other, wu_other, wd_other)[0]


def routing_rows(ids_loc, gates_loc, n_experts):
    tok_dev = ids_loc.shape[0]
    chosen = ids_loc.T[None, :, :] == jnp.arange(n_experts, dtype=ids_loc.dtype)[:, None, None]
    mask = jnp.any(chosen, axis=1)
    gate_rows = jnp.sum(jnp.where(chosen, gates_loc.T[None, :, :], 0.0), axis=1)
    before = jnp.triu(jnp.ones((tok_dev, tok_dev), jnp.bfloat16), 1)
    rank = jnp.dot(mask.astype(jnp.bfloat16), before, preferred_element_type=jnp.float32)
    return jnp.where(mask, rank, -1.0), gate_rows


def block_of(cp_pos, tp_pos, n_cp, n_tp):
    per_chunk = n_tp // PAIR
    late = tp_pos // per_chunk
    chunk = late * (PAIR * n_cp - 1 - cp_pos) + (1 - late) * cp_pos
    return chunk * per_chunk + tp_pos % per_chunk


def owner_of(block, n_cp, n_tp):
    per_chunk = n_tp // PAIR
    chunk = block // per_chunk
    late = chunk // n_cp
    return late * (PAIR * n_cp - 1 - chunk) + (1 - late) * chunk, late * per_chunk + block % per_chunk


def front_kernel(n_cp, n_tp, n_part, x_hbm, wq_hbm, wk_hbm, wv_hbm, k_hbm, vt_hbm, q_hbm, x_buf, w_buf, q_st, k_st, vt_st, k_far, vt_far, q_far,
                 own_sem, w_sem, ring_sem, pair_sem, rx_sem, sk_sem, sv_sem, sq_sem, kv_sem, rq_sem, sf_sem, rf_sem, far_sem, pass_sem):
    n_x = n_tp // PAIR
    tok_dev, hid = x_hbm.shape
    half = tok_dev // n_part
    head_dim = k_hbm.shape[1]
    n_loc = q_st.shape[1]
    chunk_len = tok_dev * n_x
    cp_pos, tp_pos = lax.axis_index("cp"), lax.axis_index("tp")
    x_pos, core = tp_pos // PAIR, tp_pos % PAIR
    sibling = PAIR * x_pos + 1 - core
    barrier = pltpu.get_barrier_semaphore()

    def slot_at(off, flip):
        return PAIR * ((x_pos + off + n_x) % n_x) + (core + flip) % PAIR

    own_copy = pltpu.make_async_copy(x_hbm, x_buf.at[tp_pos], own_sem)
    own_copy.start()
    width = n_loc * head_dim
    w_loads = [pltpu.make_async_copy(w, w_buf.at[:, pl.ds(i * width, width)], w_sem.at[i]) for i, w in enumerate((wq_hbm, wk_hbm, wv_hbm))]
    for one in w_loads:
        one.start()
    for step in (1, n_x - 1):
        pl.semaphore_signal(barrier, inc=1, device_id=mesh_id(cp_pos, slot_at(step, 0)), device_id_type=MESH)
    for step in range(1, PAIR * n_cp):
        pl.semaphore_signal(barrier, inc=1, device_id=mesh_id((cp_pos + step // PAIR) % n_cp, PAIR * x_pos + (core + step) % PAIR), device_id_type=MESH)
    pl.semaphore_wait(barrier, PAIR * n_cp + 1)

    def own_send(part, to_tp, sem):
        rows = pl.ds(pl.multiple_of(part * half, half), half)
        return pltpu.make_async_remote_copy(x_hbm.at[rows], x_buf.at[tp_pos, rows], sem, rx_sem.at[tp_pos, part],
                                            device_id=mesh_id(cp_pos, to_tp), device_id_type=MESH)

    def pass_on(slot, part, to_tp, sem):
        rows = pl.ds(pl.multiple_of(part * half, half), half)
        return pltpu.make_async_remote_copy(x_buf.at[slot, rows], x_buf.at[slot, rows], sem, rx_sem.at[slot, part],
                                            device_id=mesh_id(cp_pos, to_tp), device_id_type=MESH)

    def ring_send(i, side):
        part = i if side == 0 else n_part - 1 - i
        return own_send(part, slot_at(1 - PAIR * side, 0), ring_sem.at[side, i])

    for i in BOTH:
        for side in BOTH:
            ring_send(i, side).start()
    for part in range(n_part):
        own_send(part, sibling, pair_sem.at[part]).start()
    first = PAIR * n_part

    def place_of(step):
        late = jnp.minimum(step // first, 1)
        wave, other, side = jnp.maximum(step - first, 0) // 4, late * ((step // PAIR) % PAIR) + (1 - late) * (step // n_part), step % PAIR
        piece = pick((0, 1, 0, PAIR, 1, 3), wave)
        through = jnp.where(or_(wave == 2, wave == 4), 1, 0)
        part = late * (piece + side * (n_part - 1 - PAIR * piece)) + (1 - late) * (step % n_part)
        off = late * ((1 - through) * (PAIR * side - 1) + PAIR * through)
        return slot_at(off, other), part, off

    def targets(from_cp, slot, part):
        block = block_of(from_cp, slot, n_cp, n_tp)
        pos = pl.multiple_of(block * tok_dev + part * half, half)
        q_core = ((block % 4 + 1) // PAIR) % PAIR
        q_pos = pl.multiple_of((PAIR * (block // 4) + (block % 4) // PAIR) * tok_dev + part * half, half)
        return ((k_hbm.at[pl.ds(pos, half)], 0, kv_sem.at[from_cp]), (vt_hbm.at[:, pl.ds(pos, half)], 1, kv_sem.at[from_cp]),
                (q_hbm.at[pl.ds(q_pos, half)], q_core, rq_sem.at[from_cp]))

    def remote(src, dst, s_sem, r_sem, to_cp, to_core):
        return pltpu.make_async_remote_copy(src, dst, s_sem, r_sem, device_id=mesh_id((to_cp + n_cp) % n_cp, PAIR * x_pos + to_core), device_id_type=MESH)

    far_refs = (k_far, vt_far, q_far)

    def outputs_of(step):
        slot, part, _ = place_of(step)
        for i in range(n_loc):
            to_cp = n_loc * core + i
            far = (to_cp - cp_pos + n_cp) % n_cp == n_cp // PAIR
            for kind, (src, (dst, to_core, r_sem)) in enumerate(zip((k_st.at[step, i], vt_st.at[step, i], q_st.at[step, i]), targets(cp_pos, slot, part))):
                s_sem = (sk_sem.at[i], sv_sem.at[i], sq_sem.at[i, to_core])[kind]
                here = and_(to_cp == cp_pos, to_core == core)

                @pl.when(here)
                def _():
                    pltpu.make_async_copy(src, dst, r_sem).start()

                @pl.when(far)
                def _():
                    remote(src, far_refs[kind].at[part, slot], s_sem, far_sem.at[kind, part, slot], cp_pos + 1 - part // PAIR * 2, core).start()

                @pl.when(not_(or_(here, far)))
                def _():
                    remote(src, dst, s_sem, r_sem, to_cp, to_core).start()

    def pass_far(step, what):
        slot, part, _ = place_of(step)
        sign = 1 - part // PAIR * 2

        @pl.when((cp_pos + sign + n_cp) % n_cp // n_loc == core)
        def _():
            for kind, (dst, to_core, r_sem) in enumerate(targets((cp_pos - sign + n_cp) % n_cp, slot, part)):
                src = far_refs[kind].at[part, slot]
                copy = remote(src, dst, pass_sem.at[kind, part, slot], r_sem, cp_pos + sign, to_core)
                if what == "start":
                    pltpu.make_async_copy(src, src, far_sem.at[kind, part, slot]).wait()
                    copy.start()
                else:
                    copy.wait_send()

    def project(step, carry):
        slot, part, off = place_of(step)
        wave, other, side = (step - first) // 4, (step // PAIR) % PAIR, step % PAIR

        @pl.when(step == 0)
        def _():
            own_copy.wait()
            for one in w_loads:
                one.wait()

        @pl.when(step >= n_part)
        def _():
            pass_on(slot, part, sibling, pair_sem.at[0]).wait_recv()

        @pl.when(and_(step >= first, other == 0))
        def _():
            @pl.when(wave < 2)
            def _():
                pass_on(slot, part, slot_at(-off, 0), ring_sem.at[side, n_part + wave]).start()
                for i in BOTH:
                    @pl.when(side == i)
                    def _():
                        ring_send(2 + wave, i).start()
            pass_on(slot, part, sibling, pair_sem.at[n_part + PAIR * wave + side]).start()

        x_rows = x_buf[slot, pl.ds(pl.multiple_of(part * half, half), half), :]
        qkv = jnp.dot(x_rows, w_buf[...], preferred_element_type=jnp.float32)
        for i in range(n_loc):
            q_st[step, i] = qkv[:, i * head_dim:(i + 1) * head_dim].astype(jnp.bfloat16)
            k_st[step, i] = qkv[:, (n_loc + i) * head_dim:(n_loc + i + 1) * head_dim].astype(jnp.bfloat16)
            vt_st[step, i] = qkv[:, (PAIR * n_loc + i) * head_dim:(PAIR * n_loc + i + 1) * head_dim].T.astype(jnp.bfloat16)

        @pl.when(step > 0)
        def _():
            outputs_of(step - 1)

        @pl.when(step >= lag)
        def _():
            pass_far(step - lag, "start")
        return carry

    n_steps, lag = n_part * n_tp, 8
    lax.fori_loop(0, n_steps, project, 0)
    outputs_of(n_steps - 1)

    def pass_late(step, carry):
        pass_far(step, "start")
        return carry

    lax.fori_loop(n_steps - lag, n_steps, pass_late, 0)

    def whole(ref, count, sem):
        return pltpu.make_async_copy(ref.at[pl.ds(0, count)], ref.at[pl.ds(0, count)], sem)

    def forward(y, place, core_id):
        chunk = y if place == 0 else PAIR * n_cp - 1 - y
        cols = pl.ds(chunk * chunk_len, chunk_len)
        ref = k_hbm.at[cols] if core_id == 0 else vt_hbm.at[:, cols]
        return pltpu.make_async_remote_copy(ref, ref, sf_sem.at[PAIR * y + place], rf_sem.at[PAIR * y + place],
                                            device_id=mesh_id(cp_pos, sibling), device_id_type=MESH)

    for y in range(n_cp):
        whole(k_hbm, PAIR * chunk_len, kv_sem.at[y]).wait()
        for core_id in BOTH:
            @pl.when(core == core_id)
            def _():
                for place in BOTH:
                    forward(y, place, core_id).start()
    for y in range(n_cp):
        whole(q_hbm, chunk_len, rq_sem.at[y]).wait()
    for side in BOTH:
        for i in range(n_part + 2):
            own_send(0, sibling, ring_sem.at[side, i]).wait_send()
    for i in range(n_part * n_x):
        own_send(0, sibling, pair_sem.at[i]).wait_send()
    for i in range(n_loc):
        to_cp = n_loc * core + i
        for sem, to_core, count in ((sk_sem.at[i], 0, PAIR * chunk_len), (sv_sem.at[i], 1, PAIR * chunk_len),
                                    (sq_sem.at[i, 0], 0, chunk_len), (sq_sem.at[i, 1], 1, chunk_len)):
            @pl.when(not_(and_(to_cp == cp_pos, to_core == core)))
            def _():
                whole(k_hbm, count, sem).wait()
    def drain(step, carry):
        pass_far(step, "wait")
        return carry

    lax.fori_loop(0, n_steps, drain, 0)
    for core_id in BOTH:
        @pl.when(core == core_id)
        def _():
            for y in range(n_cp):
                for place in BOTH:
                    forward(y, place, core_id).wait_send()
                    forward(y, place, 1 - core_id).wait_recv()


def front_call(n_cp, n_tp, x_loc, w_parts, head_dim, n_loc):
    tok_dev, hid = x_loc.shape
    n_part, n_x = 4, n_tp // PAIR
    half = tok_dev // n_part
    seq = tok_dev * n_cp * n_tp
    any_spec = pl.BlockSpec(memory_space=pl.ANY)
    n_steps = n_part * n_tp
    return pl.pallas_call(
        functools.partial(front_kernel, n_cp, n_tp, n_part),
        name="gather_project",
        out_shape=(jax.ShapeDtypeStruct((seq, head_dim), jnp.bfloat16), jax.ShapeDtypeStruct((head_dim, seq), jnp.bfloat16),
                   jax.ShapeDtypeStruct((seq // PAIR, head_dim), jnp.bfloat16)),
        in_specs=[any_spec] * 4,
        out_specs=(any_spec,) * 3,
        scratch_shapes=[
            pltpu.VMEM((n_tp, tok_dev, hid), jnp.bfloat16),
            pltpu.VMEM((hid, 3 * n_loc * head_dim), jnp.bfloat16),
            pltpu.VMEM((n_steps, n_loc, half, head_dim), jnp.bfloat16),
            pltpu.VMEM((n_steps, n_loc, half, head_dim), jnp.bfloat16),
            pltpu.VMEM((n_steps, n_loc, head_dim, half), jnp.bfloat16),
            pltpu.VMEM((n_part, n_tp, half, head_dim), jnp.bfloat16),
            pltpu.VMEM((n_part, n_tp, head_dim, half), jnp.bfloat16),
            pltpu.VMEM((n_part, n_tp, half, head_dim), jnp.bfloat16),
            dma,
            dma((3,)),
            dma((PAIR, n_part + 2)),
            dma((n_part * n_x,)),
            dma((n_tp, n_part)),
            dma((n_loc,)),
            dma((n_loc,)),
            dma((n_loc, PAIR)),
            dma((n_cp,)),
            dma((n_cp,)),
            dma((PAIR * n_cp,)),
            dma((PAIR * n_cp,)),
            dma((3, n_part, n_tp)),
            dma((3, n_part, n_tp)),
        ],
        compiler_params=pltpu.CompilerParams(collective_id=0, has_side_effects=True, vmem_limit_bytes=VMEM_LIMIT),
        cost_estimate=pl.CostEstimate(flops=PAIR * n_tp * tok_dev * hid * 3 * n_loc * head_dim, bytes_accessed=2**26, transcendentals=0),
    )(x_loc, *w_parts)


def attend_kernel(n_cp, n_tp, k_hbm, vt_hbm, q_hbm, x_hbm, wo_hbm, wg_hbm, wu_hbm, wd_hbm, rank_hbm,
                  h_ref, o_hbm, wgx_hbm, wux_hbm, wdx_hbm, near_hbm,
                  k_buf, vt_buf, q_buf, qt_buf, o_st, o_buf, wo_buf, x_buf, s_even, s_odd, p_even, p_odd, p_near, shrink_even, shrink_odd, acc, m_ref, l_ref,
                  in_sem, so_sem, ro_sem, swo_sem, rwo_sem, sw_sem, rw_sem, sr_sem, rr_sem, o_sem):
    n_dev = n_cp * n_tp
    n_x = n_tp // PAIR
    tok_dev, hid = x_buf.shape
    head_dim = k_buf.shape[1]
    n_heads = o_buf.shape[0]
    cp_pos, tp_pos = lax.axis_index("cp"), lax.axis_index("tp")
    x_pos, core = tp_pos // PAIR, tp_pos % PAIR
    head = n_cp * x_pos + cp_pos
    scale = (head_dim ** -0.5) * 1.4426950408889634
    loads = [pltpu.make_async_copy(src, dst, in_sem.at[i]) for i, (src, dst) in enumerate(
        ((q_hbm, q_buf), (k_hbm, k_buf), (vt_hbm, vt_buf), (x_hbm, x_buf), (wo_hbm, wo_buf.at[tp_pos])))]
    for one in loads:
        one.start()

    enter_all(n_cp, n_tp)

    def wo_send(step):
        return pltpu.make_async_remote_copy(wo_hbm, wo_buf.at[tp_pos], swo_sem.at[step], rwo_sem.at[step],
                                            device_id=mesh_id(cp_pos, (tp_pos + step) % n_tp), device_id_type=MESH)

    def wo_arrival(step):
        return pltpu.make_async_remote_copy(wo_hbm, wo_buf.at[(tp_pos + n_tp - step) % n_tp], swo_sem.at[step], rwo_sem.at[step],
                                            device_id=mesh_id(cp_pos, tp_pos), device_id_type=MESH)

    keep = wgx_hbm.shape[0]
    swaps = [pltpu.make_async_remote_copy(src.at[pl.ds((1 - core) * keep, keep)], dst, sw_sem.at[i], rw_sem.at[i],
                                          device_id=mesh_id(cp_pos, PAIR * x_pos + 1 - core), device_id_type=MESH)
             for i, (src, dst) in enumerate(((wg_hbm, wgx_hbm), (wu_hbm, wux_hbm), (wd_hbm, wdx_hbm)))]
    ranks = []
    for slot, off in ((1, 1), (PAIR, -1), (3, PAIR)):
        for part, place in enumerate((((cp_pos + off + n_cp) % n_cp, tp_pos), (cp_pos, PAIR * ((x_pos + off + n_x) % n_x) + core))):
            ranks.append(pltpu.make_async_remote_copy(rank_hbm, near_hbm.at[part, slot], sr_sem.at[part, slot], rr_sem.at[part, slot],
                                                      device_id=mesh_id(*place), device_id_type=MESH))
    for step in range(1, n_tp):
        wo_send(step).start()
    for one in swaps + ranks:
        one.start()
    for one in loads[:3]:
        one.wait()

    def columns(block):
        return pl.ds(pl.multiple_of(block * tok_dev, tok_dev), tok_dev)

    def scores(block, cols, s_ref, masked):
        s_vals = jnp.dot(k_buf[columns(block), :], qt_buf[:, cols], preferred_element_type=jnp.float32)
        if masked:
            key_id = lax.broadcasted_iota(jnp.int32, s_vals.shape, 0)
            query_id = lax.broadcasted_iota(jnp.int32, s_vals.shape, 1)
            s_vals = jnp.where(key_id <= query_id, s_vals, -1e30)
        s_ref[...] = s_vals
        return jnp.max(s_vals, **COLUMN_WISE)

    def soften(s_ref, s_top, cols, p_ref, shrink_ref):
        m_old = m_ref[:, cols]
        m_new = jnp.maximum(m_old, s_top)
        shrink = jnp.exp2((m_old - m_new) * scale)
        m_ref[:, cols] = m_new
        shrink_ref[...] = shrink
        prob = jnp.exp2((s_ref[...] - m_new) * scale)
        l_ref[:, cols] = l_ref[:, cols] * shrink + jnp.sum(prob, **COLUMN_WISE)
        p_ref[...] = prob.astype(jnp.bfloat16)

    def gather_values(block, cols, p_ref, shrink_ref):
        acc[:, cols] = acc[:, cols] * shrink_ref[...] + jnp.dot(vt_buf[:, columns(block)], p_ref[...], preferred_element_type=jnp.float32)

    def query_pair(turn, carry):
        g = (turn + 1 + cp_pos + x_pos // PAIR * (PAIR * n_cp - 1 - PAIR * cp_pos)) % (n_dev // 4)
        q_rows = q_buf[pl.ds(pl.multiple_of(g * PAIR * tok_dev, PAIR * tok_dev), PAIR * tok_dev), :]
        qt_buf[...] = q_rows.astype(jnp.float32).T.astype(jnp.bfloat16)
        m_ref[...] = jnp.full_like(m_ref, -1e30)
        l_ref[...] = jnp.zeros_like(l_ref)
        acc[...] = jnp.zeros_like(acc)
        p_odd[...] = jnp.zeros_like(p_odd)
        shrink_odd[...] = jnp.ones_like(shrink_odd)
        near = ((0, core), (1, 3 - core), (1 - core, 0), (1, 1 - core), (1, 2 - core))
        lanes = [(s_even, p_even, shrink_even, 0), (s_even, p_even, shrink_even, 1), (s_odd, p_near, shrink_odd, 0), (s_odd, p_near, shrink_odd, 1)]
        tops = {}

        def near_refs(i):
            s_ref, p_ref, shrink_ref, place = lanes[i % 4]
            cols = pl.ds(place * tok_dev, tok_dev)
            return s_ref.at[:, cols], p_ref.at[:, cols], shrink_ref.at[:, cols]

        def near_scores(i):
            r, block = near[i]
            tops[i] = scores(4 * g + block, columns(r), near_refs(i)[0], i < 2)

        def near_soften(i):
            s_ref, p_ref, shrink_ref = near_refs(i)
            soften(s_ref, tops[i], columns(near[i][0]), p_ref, shrink_ref)

        def near_values(i):
            _, p_ref, shrink_ref = near_refs(i)
            gather_values(4 * g + near[i][1], columns(near[i][0]), p_ref, shrink_ref)

        for i in range(len(near) + 2):
            if i < len(near):
                near_scores(i)
            if 0 <= i - 1 < len(near):
                near_soften(i - 1)
            if 0 <= i - 2:
                near_values(i - 2)
        shrink_odd[...] = jnp.ones_like(shrink_odd)
        strip = min(256, tok_dev)
        strips = [pl.ds(lo, strip) for lo in range(0, PAIR * tok_dev, strip)]

        def far_step(block, parity, tops):
            s_in, s_out = (s_even, s_odd)[::1 - PAIR * parity]
            p_out, p_in = (p_even, p_odd)[::1 - PAIR * parity]
            shrink_out, shrink_in = (shrink_even, shrink_odd)[::1 - PAIR * parity]
            next_tops = []
            for cols, top in zip(strips, tops):
                next_tops.append(scores(block + 1, cols, s_out.at[:, cols], False))
                soften(s_in.at[:, cols], top, cols, p_out.at[:, cols], shrink_out.at[:, cols])
                gather_values(jnp.maximum(block - 1, 0), cols, p_in.at[:, cols], shrink_in.at[:, cols])
            return next_tops

        def far_blocks(n, tops):
            for j in range(4):
                tops = far_step(4 * n + j, j % PAIR, tops)
            return tops

        lax.fori_loop(0, g, far_blocks, [scores(0, cols, s_even.at[:, cols], False) for cols in strips])
        for cols in strips:
            gather_values(jnp.maximum(4 * g - 1, 0), cols, p_odd.at[:, cols], shrink_odd.at[:, cols])
        out = (acc[...] / l_ref[...]).T.astype(jnp.bfloat16)
        for r in BOTH:
            o_st[PAIR * g + r] = out[r * tok_dev:(r + 1) * tok_dev]
            o_push(PAIR * g + r, "start")
        return carry

    def o_push(index, what):
        block = 4 * (index // PAIR) + (1 - core) * 3 * (index % PAIR) + core * (1 + index % PAIR)
        to_cp, to_tp = owner_of(block, n_cp, n_tp)
        here = and_(to_cp == cp_pos, to_tp == tp_pos)
        if what == "start":
            @pl.when(here)
            def _():
                pltpu.make_async_copy(o_st.at[index], o_hbm.at[head], ro_sem.at[head]).start()

        @pl.when(not_(here))
        def _():
            copy = pltpu.make_async_remote_copy(o_st.at[index], o_hbm.at[head], so_sem.at[index], ro_sem.at[head],
                                                device_id=mesh_id(to_cp, to_tp), device_id_type=MESH)
            if what == "start":
                copy.start()
            else:
                copy.wait_send()

    lax.fori_loop(0, n_dev // 4, query_pair, 0)

    for step in range(1, n_tp):
        wo_arrival(step).wait_recv()
    for one in loads[3:]:
        one.wait()
    for j in range(n_heads):
        pltpu.make_async_copy(o_hbm.at[j], o_hbm.at[j], ro_sem.at[j]).wait()
    o_load = pltpu.make_async_copy(o_hbm, o_buf, o_sem)
    o_load.start()
    o_load.wait()
    o_rows = jnp.concatenate([o_buf[j] for j in range(n_heads)], axis=1)
    n_cols = min(512, hid // PAIR)

    for col in range(0, hid, n_cols):
        cols = pl.ds(col, n_cols)
        w_cols = wo_buf[:, :, cols].reshape(n_heads * head_dim, n_cols)
        h_cols = (x_buf[:, cols].astype(jnp.float32) + jnp.dot(o_rows, w_cols, preferred_element_type=jnp.float32)).astype(jnp.bfloat16)
        h_ref[PAIR * col // hid, :, pl.ds(col % (hid // PAIR), n_cols)] = h_cols

    for step in range(1, n_tp):
        wo_send(step).wait_send()
    for one in swaps + ranks:
        one.wait()

    def drain(index, carry):
        o_push(index, "wait")
        return carry

    lax.fori_loop(0, n_dev // PAIR, drain, 0)


def attend_call(n_cp, n_tp, k_all, vt_all, q_all, x_loc, wo_loc, w_gate, w_up, w_down, rank_rows):
    n_dev = n_cp * n_tp
    tok_dev, hid = x_loc.shape
    seq, head_dim = k_all.shape
    n_heads = n_tp * wo_loc.shape[0] // head_dim
    keep = w_gate.shape[0] // PAIR
    any_spec = pl.BlockSpec(memory_space=pl.ANY)
    bf16 = jnp.bfloat16
    h_loc, _, wg_other, wu_other, wd_other, near_rows = pl.pallas_call(
        functools.partial(attend_kernel, n_cp, n_tp),
        name="attend_heads",
        out_shape=(jax.ShapeDtypeStruct((PAIR, tok_dev, hid // PAIR), bf16), jax.ShapeDtypeStruct((n_heads, tok_dev, head_dim), bf16))
        + tuple(jax.ShapeDtypeStruct((keep,) + w.shape[1:], bf16) for w in (w_gate, w_up, w_down))
        + (jax.ShapeDtypeStruct((PAIR, 4) + rank_rows.shape, jnp.float32),),
        in_specs=[any_spec] * 9,
        out_specs=(pl.BlockSpec(memory_space=pltpu.VMEM),) + (any_spec,) * 5,
        scratch_shapes=[
            pltpu.VMEM((seq, head_dim), bf16),
            pltpu.VMEM((head_dim, seq), bf16),
            pltpu.VMEM((seq // PAIR, head_dim), bf16),
            pltpu.VMEM((head_dim, PAIR * tok_dev), bf16),
            pltpu.VMEM((n_dev // PAIR, tok_dev, head_dim), bf16),
            pltpu.VMEM((n_heads, tok_dev, head_dim), bf16),
            pltpu.VMEM((n_tp,) + wo_loc.shape, bf16),
            pltpu.VMEM((tok_dev, hid), bf16),
            pltpu.VMEM((tok_dev, PAIR * tok_dev), jnp.float32),
            pltpu.VMEM((tok_dev, PAIR * tok_dev), jnp.float32),
            pltpu.VMEM((tok_dev, PAIR * tok_dev), bf16),
            pltpu.VMEM((tok_dev, PAIR * tok_dev), bf16),
            pltpu.VMEM((tok_dev, PAIR * tok_dev), bf16),
            pltpu.VMEM((1, PAIR * tok_dev), jnp.float32),
            pltpu.VMEM((1, PAIR * tok_dev), jnp.float32),
            pltpu.VMEM((head_dim, PAIR * tok_dev), jnp.float32),
            pltpu.VMEM((1, PAIR * tok_dev), jnp.float32),
            pltpu.VMEM((1, PAIR * tok_dev), jnp.float32),
            dma((5,)),
            dma((n_dev // PAIR,)),
            dma((n_heads,)),
            dma((n_tp,)),
            dma((n_tp,)),
            dma((3,)),
            dma((3,)),
            dma((PAIR, 4)),
            dma((PAIR, 4)),
            dma,
        ],
        compiler_params=pltpu.CompilerParams(collective_id=1, has_side_effects=True, vmem_limit_bytes=VMEM_LIMIT),
        cost_estimate=pl.CostEstimate(flops=PAIR * seq * seq * head_dim // PAIR, bytes_accessed=2**26, transcendentals=seq * seq // 4),
    )(k_all, vt_all, q_all, x_loc, wo_loc, w_gate, w_up, w_down, rank_rows)
    return h_loc, near_rows, wg_other, wu_other, wd_other


def solution(mesh):
    n_cp = mesh.shape["cp"]
    n_tp = mesh.shape["tp"]
    row_spec = P(("dp", "cp", "tp"), None)
    head_spec = P(None, "tp", None)
    expert_spec = P(("cp", "tp"), None, None)

    def device_step(x_loc, w_q, w_k, w_v, w_o, ids_loc, gates_loc, w_gate, w_up, w_down):
        tok_dev, hid_dim = x_loc.shape
        n_loc, head_dim = w_q.shape[1:]
        n_experts = w_gate.shape[0] * n_cp * n_tp // PAIR
        capacity = ids_loc.shape[1] * tok_dev // n_experts
        w_parts = [w.reshape(hid_dim, n_loc * head_dim) for w in (w_q, w_k, w_v)]
        rank_rows, gate_rows = routing_rows(ids_loc, gates_loc, n_experts)
        k_all, vt_all, q_all = front_call(n_cp, n_tp, x_loc, w_parts, head_dim, n_loc)
        h_loc, near_rows, *others = attend_call(n_cp, n_tp, k_all, vt_all, q_all, x_loc, w_o.reshape(n_loc * head_dim, hid_dim), w_gate, w_up, w_down, rank_rows)
        return moe_call(n_cp, n_tp, capacity, h_loc, rank_rows, near_rows, gate_rows, w_gate, w_up, w_down, *others)

    return jax.shard_map(device_step, mesh=mesh, in_specs=(row_spec, head_spec, head_spec, head_spec, P("tp", None, None), row_spec, row_spec, expert_spec, expert_spec, expert_spec), out_specs=row_spec, check_vma=False)
```

```python
import functools

import jax
import jax.numpy as jnp
from jax import lax
from jax.experimental import pallas as pl
from jax.experimental.pallas import tpu as pltpu
from jax.sharding import PartitionSpec as P

MESH = pl.DeviceIdType.MESH
PAIR = 2
BOTH = range(PAIR)
ROWS_ROWS = (((0,), (0,)), ((), ()))
COLUMN_WISE = {"axis": 0, "keepdims": True}
dma = pltpu.SemaphoreType.DMA
and_, or_, not_ = jnp.logical_and, jnp.logical_or, jnp.logical_not
VMEM_LIMIT = 66_000_000
PLACES = ((0, 0), (0, 1), (1, 0), (0, -1), (-1, 0), (1, 1), (-1, -1), (1, -1), (-1, 1), (0, PAIR), (PAIR, 0), (1, PAIR), (PAIR, 1), (-1, PAIR), (PAIR, -1), (PAIR, PAIR))
N_NEAR, FIRST_FAR = 5, 9
GROUPS = ("1234", "1234", "9a9a", "bcbc", "dede", "0f0f", "5656", "7878")
FLIPS = ("0000", "1111") + ("0011",) * 6
SOURCES = (0, -1, 1, PAIR)


def peer_of(step, cp_pos, tp_pos, n_cp, n_tp):
    n_x = n_tp // PAIR
    off_x = (step // PAIR) % n_x
    off_y = (off_x + step // n_tp) % n_cp
    return (cp_pos + off_y) % n_cp, ((tp_pos // PAIR + off_x) % n_x) * 2 + (tp_pos % PAIR + step % PAIR) % PAIR


def mesh_id(cp_pos, tp_pos):
    return {"cp": cp_pos, "tp": tp_pos}


def enter_all(n_cp, n_tp):
    cp_pos, tp_pos = lax.axis_index("cp"), lax.axis_index("tp")

    def signal_peer(step, carry):
        to_cp, to_tp = peer_of(step, cp_pos, tp_pos, n_cp, n_tp)
        pl.semaphore_signal(pltpu.get_barrier_semaphore(), inc=1, device_id=mesh_id(to_cp, to_tp), device_id_type=MESH)
        return carry

    lax.fori_loop(1, n_cp * n_tp, signal_peer, 0)
    pl.semaphore_wait(pltpu.get_barrier_semaphore(), n_cp * n_tp - 1)


def pick(values, index):
    out = values[-1]
    for k, value in enumerate(values[:-1]):
        out = jnp.where(index == k, value, out)
    return out


def moe_kernel(n_cp, n_tp, group, h_hbm, rank_hbm, near_hbm, gate_ref, wg_hbm, wu_hbm, wd_hbm, wgx_hbm, wux_hbm, wdx_hbm,
               y_ref, rx_hbm, rl_hbm, rz_hbm, zl_hbm,
               h_buf, rank_buf, wg_buf, wu_buf, wd_buf, ring, own_stage, z_ring, x_buf, z_buf, acc, parts,
               w_sem, rank_sem, in_sem, x_sem, z_sem, hs_sem, hr_sem, ss_sem, rx_sem, rl_sem, fl_sem, sz_sem, rz_sem, zl_sem, fz_sem):
    n_x = n_tp // PAIR
    tok_dev, half_hid = h_buf.shape[2:]
    hid = PAIR * half_hid
    cap = ring.shape[3] // PAIR
    cp_pos, tp_pos = lax.axis_index("cp"), lax.axis_index("tp")
    x_pos, core = tp_pos // PAIR, tp_pos % PAIR
    half_tok = tok_dev // PAIR

    def at(off_y, off_x, flip):
        return (cp_pos + off_y + n_cp) % n_cp, PAIR * ((x_pos + off_x + n_x) % n_x) + (core + flip) % PAIR

    def line(place):
        return place[0] * n_tp + place[1]

    def send(src, dst, s_sem, r_sem, place):
        return pltpu.make_async_remote_copy(src, dst, s_sem, r_sem, device_id=mesh_id(*place), device_id_type=MESH)

    def await_bytes(ref, sem):
        pltpu.make_async_copy(ref, ref, sem).wait()

    h_loads = [pltpu.make_async_copy(h_hbm.at[part], h_buf.at[part, 0], in_sem.at[part]) for part in BOTH]
    rank_loads = []
    for part in BOTH:
        rank_loads.append(pltpu.make_async_copy(rank_hbm, rank_buf.at[part, 0], rank_sem.at[PAIR * part]))
        rank_loads.append(pltpu.make_async_copy(near_hbm.at[part, pl.ds(1, 3)], rank_buf.at[part, pl.ds(1, 3)], rank_sem.at[PAIR * part + 1]))
    w_loads = []
    for slot, (own, other, buf) in enumerate(((wg_hbm, wgx_hbm, wg_buf), (wu_hbm, wux_hbm, wu_buf), (wd_hbm, wdx_hbm, wd_buf))):
        w_loads.append(pltpu.make_async_copy(own.at[pl.ds(PAIR * core, PAIR)], buf.at[0], w_sem.at[PAIR * slot]))
        w_loads.append(pltpu.make_async_copy(other, buf.at[1], w_sem.at[PAIR * slot + 1]))
    for one in h_loads + rank_loads:
        one.start()
    enter_all(n_cp, n_tp)

    def along(part, off):
        return at(off, 0, 0) if part == 0 else at(0, off, 0)

    def across(part, off, flip):
        return at(0, off, flip) if part == 0 else at(off, 0, flip)

    def rows_of(piece):
        return pl.ds(piece * half_tok, half_tok)

    def spread(part, i):
        piece, off, slot = ((0, 1, 1), (1, -1, PAIR), (1, 1, 1), (0, -1, PAIR), (0, 1, 3), (1, -1, 3))[i]
        rows = rows_of(piece)
        src = h_hbm.at[part, rows] if i < 4 else h_buf.at[part, 1 if i == 4 else 2, rows]
        return send(src, h_buf.at[part, slot, rows], hs_sem.at[part, i], hr_sem.at[part, slot, piece], along(part, off))

    def await_h(part, slot, piece):
        await_bytes(h_buf.at[part, slot, rows_of(piece)], hr_sem.at[part, slot, piece])

    for i in range(4):
        for part in BOTH:
            spread(part, i).start()
    for one in w_loads:
        one.start()
    for one in h_loads + rank_loads:
        one.wait()

    slots = lax.broadcasted_iota(jnp.int32, (cap, tok_dev), 0).astype(jnp.float32)

    def gather_rows(part, stage, m):
        turn = m // PAIR
        off = turn + (turn // PAIR) * (5 - PAIR * turn)
        first = PAIR * line(across(part, off, m % PAIR))
        chosen = [jnp.where(rank_buf[part, stage, pl.ds(first + i, 1), :] == slots, 1.0, 0.0) for i in BOTH]
        chosen = jnp.concatenate(chosen, axis=0).astype(jnp.bfloat16)
        return jnp.dot(chosen, h_buf[part, stage], preferred_element_type=jnp.float32).astype(jnp.bfloat16)

    def source_line(part, stage, off):
        a = SOURCES[stage]
        return line(at(a, off, 0) if part == 0 else at(off, a, 0))

    def await_ring(part, stage):
        def one(m, carry):
            await_bytes(ring.at[part, stage % PAIR, m], ss_sem.at[part, stage % PAIR, m])
            return carry
        lax.fori_loop(1, 8, one, 0)

    def own_copy(part, stage):
        src_line = source_line(part, stage, 0)
        return pltpu.make_async_copy(own_stage.at[part, stage], rx_hbm.at[part, src_line], rx_sem.at[part, src_line])

    def run_stage(stage):
        side = stage % PAIR
        for part in BOTH:
            if stage >= 2:
                await_ring(part, stage)
            own_stage[part, stage] = gather_rows(part, stage, 0)

            def fill(m, carry):
                ring[part, side, m] = gather_rows(part, stage, m)
                return carry

            lax.fori_loop(1, 8, fill, 0)
        lines = [source_line(part, stage, 0) for part in BOTH]
        for flip in BOTH:
            for way, off in enumerate((1, -1)):
                for part in BOTH:
                    m = 6 + flip
                    send(ring.at[part, side, m, pl.ds(way * cap, cap)], rl_hbm.at[part, way, stage, flip], ss_sem.at[part, side, m],
                         rl_sem.at[part, way, stage, flip], across(part, off, 0)).start()
        for m, off in ((PAIR, 1), (4, -1), (3, 1), (5, -1), (1, 0)):
            for part in BOTH:
                send(ring.at[part, side, m], rx_hbm.at[part, lines[part]], ss_sem.at[part, side, m], rx_sem.at[part, lines[part]],
                     across(part, off, m % PAIR)).start()
        for part in BOTH:
            own_copy(part, stage).start()

    def relay(part, stage, way, flip):
        off = 1 - PAIR * way
        src_line = source_line(part, stage, -off)
        return send(rl_hbm.at[part, way, stage, flip], rx_hbm.at[part, src_line, pl.ds(way * cap, cap)], fl_sem.at[part, way, stage, flip],
                    rx_sem.at[part, src_line], across(part, off, flip))

    def run_relays(stage):
        for flip in BOTH:
            for way in BOTH:
                for part in BOTH:
                    await_bytes(rl_hbm.at[part, way, stage, flip], rl_sem.at[part, way, stage, flip])
                    relay(part, stage, way, flip).start()

    run_stage(0)
    for part in BOTH:
        await_h(part, 1, 0)
        spread(part, 4).start()
    for part in BOTH:
        await_h(part, PAIR, 1)
        spread(part, 5).start()
    for part in BOTH:
        await_h(part, 1, 1)
    run_stage(1)
    gate_all = gate_ref[...]
    high = gate_all.astype(jnp.bfloat16).astype(jnp.float32)
    rest = gate_all - high
    mid = rest.astype(jnp.bfloat16).astype(jnp.float32)
    parts[0] = high
    parts[1] = mid
    parts[2] = rest - mid
    for part in BOTH:
        acc[:, part * half_hid:(part + 1) * half_hid] = h_buf[part, 0].astype(jnp.float32)
    run_relays(0)
    for part in BOTH:
        await_h(part, PAIR, 0)
    run_stage(2)
    run_relays(1)
    for part in BOTH:
        await_h(part, 3, 0)
        await_h(part, 3, 1)
    run_stage(3)
    run_relays(2)
    for one in w_loads:
        one.wait()

    rows = group * cap
    n_cols = min(512, hid)

    def expert_rows(slot, i):
        x_rows = x_buf[:, pl.ds(i * cap, cap), :].reshape(rows, hid)
        hidden = []
        for half in BOTH:
            gate_pre = jnp.dot(x_rows, wg_buf[half, i], preferred_element_type=jnp.float32)
            up_pre = jnp.dot(x_rows, wu_buf[half, i], preferred_element_type=jnp.float32)
            hidden.append((gate_pre * (1.0 / (1.0 + jnp.exp(-gate_pre))) * up_pre).astype(jnp.bfloat16))
        for col in range(0, hid, n_cols):
            z_rows = (jnp.dot(hidden[0], wd_buf[0, i, :, pl.ds(col, n_cols)], preferred_element_type=jnp.float32)
                      + jnp.dot(hidden[1], wd_buf[1, i, :, pl.ds(col, n_cols)], preferred_element_type=jnp.float32))
            z_ring[slot, :, pl.ds(i * cap, cap), pl.ds(col, n_cols)] = z_rows.astype(jnp.bfloat16).reshape(group, cap, n_cols)

    def place_at(g, q):
        places = [int(names[q], 16) for names in GROUPS]
        off_y, off_x = (pick([PLACES[p][k] for p in places], g) for k in BOTH)
        return off_y, off_x, pick([int(flips[q]) for flips in FLIPS], g), pick(places, g)

    my_line = line((cp_pos, tp_pos))

    def await_slot(slot):
        for q in range(group):
            await_bytes(z_ring.at[slot, q], sz_sem.at[slot, q])

    def expert_group(g, carry):
        slot = g % 3

        @pl.when(g == 2)
        def _():
            run_relays(3)

        sources = [line(at(*place_at(g, q)[:3])) for q in range(group)]
        loads = []
        for q in range(group):
            for part in BOTH:
                await_bytes(rx_hbm.at[part, sources[q]], rx_sem.at[part, sources[q]])
                loads.append(pltpu.make_async_copy(rx_hbm.at[part, sources[q]], x_buf.at[q, :, pl.ds(part * half_hid, half_hid)], x_sem.at[part, q]))
                loads[-1].start()

        @pl.when(g >= 3)
        def _():
            await_slot(slot)
        for one in loads:
            one.wait()
        for i in BOTH:
            expert_rows(slot, i)
        for q in range(group):
            off_y, off_x, flip, p = place_at(g, q)
            alone = and_(p == 0, flip == 0)

            @pl.when(alone)
            def _():
                pltpu.make_async_copy(z_ring.at[slot, q], rz_hbm.at[my_line], rz_sem.at[my_line]).start()

            @pl.when(and_(p < FIRST_FAR, not_(alone)))
            def _():
                send(z_ring.at[slot, q], rz_hbm.at[my_line], sz_sem.at[slot, q], rz_sem.at[my_line], at(off_y, off_x, flip)).start()

            @pl.when(p >= FIRST_FAR)
            def _():
                lead_y, lead_x = jnp.where(off_y == 2, 1, 0), jnp.where(off_x == 2, 1, 0)
                for way in BOTH:
                    sign = 1 - PAIR * way
                    send(z_ring.at[slot, q, pl.ds(way * cap, cap)], zl_hbm.at[p - FIRST_FAR, flip, way], sz_sem.at[slot, q],
                         zl_sem.at[p - FIRST_FAR, flip, way], at(sign * lead_y, sign * lead_x, 0)).start()
        return carry

    lax.fori_loop(0, len(GROUPS), expert_group, 0)

    n_far = len(PLACES) - FIRST_FAR

    def z_relay(index, flip, way):
        off_y, off_x = PLACES[FIRST_FAR + index]
        sign = 1 - PAIR * way
        lead_y, lead_x = sign * (off_y == 2), sign * (off_x == 2)
        from_line = line(at(-lead_y, -lead_x, 0))
        to_y = sign if off_y == 2 else off_y
        to_x = sign if off_x == 2 else off_x
        return send(zl_hbm.at[index, flip, way], rz_hbm.at[from_line, pl.ds(way * cap, cap)], fz_sem.at[index, flip, way],
                    rz_sem.at[from_line], at(to_y, to_x, flip))

    def each_relay(*indices):
        return [(index, flip, way) for flip in BOTH for way in BOTH for index in indices]

    def run_z_relays(*indices):
        for key in each_relay(*indices):
            await_bytes(zl_hbm.at[key], zl_sem.at[key])
            z_relay(*key).start()

    def combine(p, carry):
        off_y, off_x = pick([a for a, _ in PLACES], p), pick([b for _, b in PLACES], p)
        homes = [line(at(-off_y, -off_x, q)) for q in BOTH]
        loads = []
        for q in BOTH:
            await_bytes(rz_hbm.at[homes[q]], rz_sem.at[homes[q]])
            loads.append(pltpu.make_async_copy(rz_hbm.at[homes[q]], z_buf.at[q], z_sem.at[q]))
            loads[-1].start()
        weights = [[], [], []]
        for q in BOTH:
            for i in BOTH:
                row = pl.ds(PAIR * homes[q] + i, 1)
                chosen = rank_buf[0, 0, row, :] == slots
                for part in range(3):
                    weights[part].append(jnp.where(chosen, parts[part, row, :], 0.0))
        weights = [jnp.concatenate(w, axis=0).astype(jnp.bfloat16) for w in weights]
        for one in loads:
            one.wait()
        for col in range(0, hid, n_cols):
            z_rows = z_buf[:, :, pl.ds(col, n_cols)].reshape(4 * cap, n_cols)
            total = None
            for part in range(3):
                term = lax.dot_general(weights[part], z_rows, ROWS_ROWS, preferred_element_type=jnp.float32)
                total = term if total is None else total + term
            acc[:, pl.ds(col, n_cols)] += total
        return carry

    run_z_relays(0, 1)
    run_z_relays(PAIR, 3)
    lax.fori_loop(0, N_NEAR, combine, 0)
    run_z_relays(4, 5)
    run_z_relays(6)
    lax.fori_loop(N_NEAR, len(PLACES), combine, 0)
    y_ref[...] = acc[...].astype(jnp.bfloat16)

    for part in BOTH:
        for i in range(6):
            spread(part, i).wait_send()
        for stage in (PAIR, 3):
            await_ring(part, stage)
        for stage in range(4):
            for way in BOTH:
                for flip in BOTH:
                    relay(part, stage, way, flip).wait_send()
    last = len(GROUPS) - 3
    for g in range(last, len(GROUPS)):
        for q in range(group):
            if GROUPS[g][q] + FLIPS[g][q] != "00":
                await_bytes(z_ring.at[g % 3, q], sz_sem.at[g % 3, q])
    for key in each_relay(*range(n_far)):
        z_relay(*key).wait_send()


def moe_call(n_cp, n_tp, cap, h_loc, rank_rows, near_rows, gate_rows, w_gate, w_up, w_down, wg_other, wu_other, wd_other):
    n_dev = n_cp * n_tp
    _, tok_dev, half_hid = h_loc.shape
    hid = PAIR * half_hid
    half_f = w_gate.shape[2]
    n_experts = rank_rows.shape[0]
    group = len(GROUPS[0])
    n_far = len(PLACES) - FIRST_FAR
    bf16 = jnp.bfloat16
    any_spec = pl.BlockSpec(memory_space=pl.ANY)
    vmem_spec = pl.BlockSpec(memory_space=pltpu.VMEM)
    flops = PAIR * n_dev * PAIR * cap * hid * PAIR * half_f * 3
    return pl.pallas_call(
        functools.partial(moe_kernel, n_cp, n_tp, group),
        name="routed_experts",
        out_shape=(jax.ShapeDtypeStruct((tok_dev, hid), bf16), jax.ShapeDtypeStruct((PAIR, n_dev, PAIR * cap, half_hid), bf16),
                   jax.ShapeDtypeStruct((PAIR, PAIR, 4, PAIR, cap, half_hid), bf16), jax.ShapeDtypeStruct((n_dev, PAIR * cap, hid), bf16),
                   jax.ShapeDtypeStruct((n_far, PAIR, 2, cap, hid), bf16)),
        in_specs=[any_spec, any_spec, any_spec, vmem_spec] + [any_spec] * 6,
        out_specs=(vmem_spec,) + (any_spec,) * 4,
        scratch_shapes=[
            pltpu.VMEM((PAIR, 4, tok_dev, half_hid), bf16),
            pltpu.VMEM((PAIR, 4, n_experts, tok_dev), jnp.float32),
            pltpu.VMEM((PAIR, PAIR, hid, half_f), bf16),
            pltpu.VMEM((PAIR, PAIR, hid, half_f), bf16),
            pltpu.VMEM((PAIR, PAIR, half_f, hid), bf16),
            pltpu.VMEM((PAIR, PAIR, 8, PAIR * cap, half_hid), bf16),
            pltpu.VMEM((PAIR, 4, PAIR * cap, half_hid), bf16),
            pltpu.VMEM((3, group, PAIR * cap, hid), bf16),
            pltpu.VMEM((group, PAIR * cap, hid), bf16),
            pltpu.VMEM((PAIR, PAIR * cap, hid), bf16),
            pltpu.VMEM((tok_dev, hid), jnp.float32),
            pltpu.VMEM((3, n_experts, tok_dev), jnp.float32),
            dma((6,)), dma((4,)), dma((PAIR,)), dma((PAIR, group)), dma((PAIR,)),
            dma((PAIR, 6)), dma((PAIR, 4, PAIR)), dma((PAIR, PAIR, 8)), dma((PAIR, n_dev)), dma((PAIR, PAIR, 4, PAIR)), dma((PAIR, PAIR, 4, PAIR)),
            dma((3, group)), dma((n_dev,)), dma((n_far, PAIR, PAIR)), dma((n_far, PAIR, PAIR)),
        ],
        compiler_params=pltpu.CompilerParams(collective_id=2, has_side_effects=True, vmem_limit_bytes=VMEM_LIMIT),
        cost_estimate=pl.CostEstimate(flops=flops, bytes_accessed=2**27, transcendentals=0),
    )(h_loc, rank_rows, near_rows, gate_rows, w_gate, w_up, w_down, wg_other, wu_other, wd_other)[0]


def routing_rows(ids_loc, gates_loc, n_experts):
    tok_dev = ids_loc.shape[0]
    chosen = ids_loc.T[None, :, :] == jnp.arange(n_experts, dtype=ids_loc.dtype)[:, None, None]
    mask = jnp.any(chosen, axis=1)
    gate_rows = jnp.sum(jnp.where(chosen, gates_loc.T[None, :, :], 0.0), axis=1)
    before = jnp.triu(jnp.ones((tok_dev, tok_dev), jnp.bfloat16), 1)
    rank = jnp.dot(mask.astype(jnp.bfloat16), before, preferred_element_type=jnp.float32)
    return jnp.where(mask, rank, -1.0), gate_rows


def block_of(cp_pos, tp_pos, n_cp, n_tp):
    per_chunk = n_tp // PAIR
    late = tp_pos // per_chunk
    chunk = late * (PAIR * n_cp - 1 - cp_pos) + (1 - late) * cp_pos
    return chunk * per_chunk + tp_pos % per_chunk


def owner_of(block, n_cp, n_tp):
    per_chunk = n_tp // PAIR
    chunk = block // per_chunk
    late = chunk // n_cp
    return late * (PAIR * n_cp - 1 - chunk) + (1 - late) * chunk, late * per_chunk + block % per_chunk


def front_kernel(n_cp, n_tp, n_part, x_hbm, wq_hbm, wk_hbm, wv_hbm, k_hbm, vt_hbm, q_hbm, x_buf, w_buf, q_st, k_st, vt_st, k_far, vt_far, q_far,
                 own_sem, w_sem, ring_sem, pair_sem, rx_sem, sk_sem, sv_sem, sq_sem, kv_sem, rq_sem, sf_sem, rf_sem, far_sem, pass_sem):
    n_x = n_tp // PAIR
    tok_dev, hid = x_hbm.shape
    half = tok_dev // n_part
    head_dim = k_hbm.shape[1]
    n_loc = q_st.shape[1]
    chunk_len = tok_dev * n_x
    cp_pos, tp_pos = lax.axis_index("cp"), lax.axis_index("tp")
    x_pos, core = tp_pos // PAIR, tp_pos % PAIR
    sibling = PAIR * x_pos + 1 - core
    barrier = pltpu.get_barrier_semaphore()

    def slot_at(off, flip):
        return PAIR * ((x_pos + off + n_x) % n_x) + (core + flip) % PAIR

    own_copy = pltpu.make_async_copy(x_hbm, x_buf.at[tp_pos], own_sem)
    own_copy.start()
    width = n_loc * head_dim
    w_loads = [pltpu.make_async_copy(w, w_buf.at[:, pl.ds(i * width, width)], w_sem.at[i]) for i, w in enumerate((wq_hbm, wk_hbm, wv_hbm))]
    for one in w_loads:
        one.start()
    for step in (1, n_x - 1):
        pl.semaphore_signal(barrier, inc=1, device_id=mesh_id(cp_pos, slot_at(step, 0)), device_id_type=MESH)
    for step in range(1, PAIR * n_cp):
        pl.semaphore_signal(barrier, inc=1, device_id=mesh_id((cp_pos + step // PAIR) % n_cp, PAIR * x_pos + (core + step) % PAIR), device_id_type=MESH)
    pl.semaphore_wait(barrier, PAIR * n_cp + 1)

    def own_send(part, to_tp, sem):
        rows = pl.ds(pl.multiple_of(part * half, half), half)
        return pltpu.make_async_remote_copy(x_hbm.at[rows], x_buf.at[tp_pos, rows], sem, rx_sem.at[tp_pos, part],
                                            device_id=mesh_id(cp_pos, to_tp), device_id_type=MESH)

    def pass_on(slot, part, to_tp, sem):
        rows = pl.ds(pl.multiple_of(part * half, half), half)
        return pltpu.make_async_remote_copy(x_buf.at[slot, rows], x_buf.at[slot, rows], sem, rx_sem.at[slot, part],
                                            device_id=mesh_id(cp_pos, to_tp), device_id_type=MESH)

    def ring_send(i, side):
        part = i if side == 0 else n_part - 1 - i
        return own_send(part, slot_at(1 - PAIR * side, 0), ring_sem.at[side, i])

    for i in BOTH:
        for side in BOTH:
            ring_send(i, side).start()
    for part in range(n_part):
        own_send(part, sibling, pair_sem.at[part]).start()
    first = PAIR * n_part

    def place_of(step):
        late = jnp.minimum(step // first, 1)
        wave, other, side = jnp.maximum(step - first, 0) // 4, late * ((step // PAIR) % PAIR) + (1 - late) * (step // n_part), step % PAIR
        piece = pick((0, 1, 0, PAIR, 1, 3), wave)
        through = jnp.where(or_(wave == 2, wave == 4), 1, 0)
        part = late * (piece + side * (n_part - 1 - PAIR * piece)) + (1 - late) * (step % n_part)
        off = late * ((1 - through) * (PAIR * side - 1) + PAIR * through)
        return slot_at(off, other), part, off

    def targets(from_cp, slot, part):
        block = block_of(from_cp, slot, n_cp, n_tp)
        pos = pl.multiple_of(block * tok_dev + part * half, half)
        q_core = ((block % 4 + 1) // PAIR) % PAIR
        q_pos = pl.multiple_of((PAIR * (block // 4) + (block % 4) // PAIR) * tok_dev + part * half, half)
        return ((k_hbm.at[pl.ds(pos, half)], 0, kv_sem.at[from_cp]), (vt_hbm.at[:, pl.ds(pos, half)], 1, kv_sem.at[from_cp]),
                (q_hbm.at[pl.ds(q_pos, half)], q_core, rq_sem.at[from_cp]))

    def remote(src, dst, s_sem, r_sem, to_cp, to_core):
        return pltpu.make_async_remote_copy(src, dst, s_sem, r_sem, device_id=mesh_id((to_cp + n_cp) % n_cp, PAIR * x_pos + to_core), device_id_type=MESH)

    far_refs = (k_far, vt_far, q_far)

    def outputs_of(step):
        slot, part, _ = place_of(step)
        for i in range(n_loc):
            to_cp = n_loc * core + i
            far = (to_cp - cp_pos + n_cp) % n_cp == n_cp // PAIR
            for kind, (src, (dst, to_core, r_sem)) in enumerate(zip((k_st.at[step, i], vt_st.at[step, i], q_st.at[step, i]), targets(cp_pos, slot, part))):
                s_sem = (sk_sem.at[i], sv_sem.at[i], sq_sem.at[i, to_core])[kind]
                here = and_(to_cp == cp_pos, to_core == core)

                @pl.when(here)
                def _():
                    pltpu.make_async_copy(src, dst, r_sem).start()

                @pl.when(far)
                def _():
                    remote(src, far_refs[kind].at[part, slot], s_sem, far_sem.at[kind, part, slot], cp_pos + 1 - part // PAIR * 2, core).start()

                @pl.when(not_(or_(here, far)))
                def _():
                    remote(src, dst, s_sem, r_sem, to_cp, to_core).start()

    def pass_far(step, what):
        slot, part, _ = place_of(step)
        sign = 1 - part // PAIR * 2

        @pl.when((cp_pos + sign + n_cp) % n_cp // n_loc == core)
        def _():
            for kind, (dst, to_core, r_sem) in enumerate(targets((cp_pos - sign + n_cp) % n_cp, slot, part)):
                src = far_refs[kind].at[part, slot]
                copy = remote(src, dst, pass_sem.at[kind, part, slot], r_sem, cp_pos + sign, to_core)
                if what == "start":
                    pltpu.make_async_copy(src, src, far_sem.at[kind, part, slot]).wait()
                    copy.start()
                else:
                    copy.wait_send()

    def project(step, carry):
        slot, part, off = place_of(step)
        wave, other, side = (step - first) // 4, (step // PAIR) % PAIR, step % PAIR

        @pl.when(step == 0)
        def _():
            own_copy.wait()
            for one in w_loads:
                one.wait()

        @pl.when(step >= n_part)
        def _():
            pass_on(slot, part, sibling, pair_sem.at[0]).wait_recv()

        @pl.when(and_(step >= first, other == 0))
        def _():
            @pl.when(wave < 2)
            def _():
                pass_on(slot, part, slot_at(-off, 0), ring_sem.at[side, n_part + wave]).start()
                for i in BOTH:
                    @pl.when(side == i)
                    def _():
                        ring_send(2 + wave, i).start()
            pass_on(slot, part, sibling, pair_sem.at[n_part + PAIR * wave + side]).start()

        x_rows = x_buf[slot, pl.ds(pl.multiple_of(part * half, half), half), :]
        qkv = jnp.dot(x_rows, w_buf[...], preferred_element_type=jnp.float32)
        for i in range(n_loc):
            q_st[step, i] = qkv[:, i * head_dim:(i + 1) * head_dim].astype(jnp.bfloat16)
            k_st[step, i] = qkv[:, (n_loc + i) * head_dim:(n_loc + i + 1) * head_dim].astype(jnp.bfloat16)
            vt_st[step, i] = qkv[:, (PAIR * n_loc + i) * head_dim:(PAIR * n_loc + i + 1) * head_dim].T.astype(jnp.bfloat16)

        @pl.when(step > 0)
        def _():
            outputs_of(step - 1)

        @pl.when(step >= lag)
        def _():
            pass_far(step - lag, "start")
        return carry

    n_steps, lag = n_part * n_tp, 8
    lax.fori_loop(0, n_steps, project, 0)
    outputs_of(n_steps - 1)

    def pass_late(step, carry):
        pass_far(step, "start")
        return carry

    lax.fori_loop(n_steps - lag, n_steps, pass_late, 0)

    def whole(ref, count, sem):
        return pltpu.make_async_copy(ref.at[pl.ds(0, count)], ref.at[pl.ds(0, count)], sem)

    def forward(y, place, core_id):
        chunk = y if place == 0 else PAIR * n_cp - 1 - y
        cols = pl.ds(chunk * chunk_len, chunk_len)
        ref = k_hbm.at[cols] if core_id == 0 else vt_hbm.at[:, cols]
        return pltpu.make_async_remote_copy(ref, ref, sf_sem.at[PAIR * y + place], rf_sem.at[PAIR * y + place],
                                            device_id=mesh_id(cp_pos, sibling), device_id_type=MESH)

    for y in range(n_cp):
        whole(k_hbm, PAIR * chunk_len, kv_sem.at[y]).wait()
        for core_id in BOTH:
            @pl.when(core == core_id)
            def _():
                for place in BOTH:
                    forward(y, place, core_id).start()
    for y in range(n_cp):
        whole(q_hbm, chunk_len, rq_sem.at[y]).wait()
    for side in BOTH:
        for i in range(n_part + 2):
            own_send(0, sibling, ring_sem.at[side, i]).wait_send()
    for i in range(n_part * n_x):
        own_send(0, sibling, pair_sem.at[i]).wait_send()
    for i in range(n_loc):
        to_cp = n_loc * core + i
        for sem, to_core, count in ((sk_sem.at[i], 0, PAIR * chunk_len), (sv_sem.at[i], 1, PAIR * chunk_len),
                                    (sq_sem.at[i, 0], 0, chunk_len), (sq_sem.at[i, 1], 1, chunk_len)):
            @pl.when(not_(and_(to_cp == cp_pos, to_core == core)))
            def _():
                whole(k_hbm, count, sem).wait()
    def drain(step, carry):
        pass_far(step, "wait")
        return carry

    lax.fori_loop(0, n_steps, drain, 0)
    for core_id in BOTH:
        @pl.when(core == core_id)
        def _():
            for y in range(n_cp):
                for place in BOTH:
                    forward(y, place, core_id).wait_send()
                    forward(y, place, 1 - core_id).wait_recv()


def front_call(n_cp, n_tp, x_loc, w_parts, head_dim, n_loc):
    tok_dev, hid = x_loc.shape
    n_part, n_x = 4, n_tp // PAIR
    half = tok_dev // n_part
    seq = tok_dev * n_cp * n_tp
    any_spec = pl.BlockSpec(memory_space=pl.ANY)
    n_steps = n_part * n_tp
    return pl.pallas_call(
        functools.partial(front_kernel, n_cp, n_tp, n_part),
        name="gather_project",
        out_shape=(jax.ShapeDtypeStruct((seq, head_dim), jnp.bfloat16), jax.ShapeDtypeStruct((head_dim, seq), jnp.bfloat16),
                   jax.ShapeDtypeStruct((seq // PAIR, head_dim), jnp.bfloat16)),
        in_specs=[any_spec] * 4,
        out_specs=(any_spec,) * 3,
        scratch_shapes=[
            pltpu.VMEM((n_tp, tok_dev, hid), jnp.bfloat16),
            pltpu.VMEM((hid, 3 * n_loc * head_dim), jnp.bfloat16),
            pltpu.VMEM((n_steps, n_loc, half, head_dim), jnp.bfloat16),
            pltpu.VMEM((n_steps, n_loc, half, head_dim), jnp.bfloat16),
            pltpu.VMEM((n_steps, n_loc, head_dim, half), jnp.bfloat16),
            pltpu.VMEM((n_part, n_tp, half, head_dim), jnp.bfloat16),
            pltpu.VMEM((n_part, n_tp, head_dim, half), jnp.bfloat16),
            pltpu.VMEM((n_part, n_tp, half, head_dim), jnp.bfloat16),
            dma,
            dma((3,)),
            dma((PAIR, n_part + 2)),
            dma((n_part * n_x,)),
            dma((n_tp, n_part)),
            dma((n_loc,)),
            dma((n_loc,)),
            dma((n_loc, PAIR)),
            dma((n_cp,)),
            dma((n_cp,)),
            dma((PAIR * n_cp,)),
            dma((PAIR * n_cp,)),
            dma((3, n_part, n_tp)),
            dma((3, n_part, n_tp)),
        ],
        compiler_params=pltpu.CompilerParams(collective_id=0, has_side_effects=True, vmem_limit_bytes=VMEM_LIMIT),
        cost_estimate=pl.CostEstimate(flops=PAIR * n_tp * tok_dev * hid * 3 * n_loc * head_dim, bytes_accessed=2**26, transcendentals=0),
    )(x_loc, *w_parts)


def attend_kernel(n_cp, n_tp, k_hbm, vt_hbm, q_hbm, x_hbm, wo_hbm, wg_hbm, wu_hbm, wd_hbm, rank_hbm,
                  h_ref, o_hbm, wgx_hbm, wux_hbm, wdx_hbm, near_hbm,
                  k_buf, vt_buf, q_buf, qt_buf, o_st, o_buf, wo_buf, x_buf, s_even, s_odd, p_even, p_odd, p_near, shrink_even, shrink_odd, acc, m_ref, l_ref,
                  in_sem, so_sem, ro_sem, swo_sem, rwo_sem, sw_sem, rw_sem, sr_sem, rr_sem, o_sem):
    n_dev = n_cp * n_tp
    n_x = n_tp // PAIR
    tok_dev, hid = x_buf.shape
    head_dim = k_buf.shape[1]
    n_heads = o_buf.shape[0]
    cp_pos, tp_pos = lax.axis_index("cp"), lax.axis_index("tp")
    x_pos, core = tp_pos // PAIR, tp_pos % PAIR
    head = n_cp * x_pos + cp_pos
    scale = (head_dim ** -0.5) * 1.4426950408889634
    loads = [pltpu.make_async_copy(src, dst, in_sem.at[i]) for i, (src, dst) in enumerate(
        ((q_hbm, q_buf), (k_hbm, k_buf), (vt_hbm, vt_buf), (x_hbm, x_buf), (wo_hbm, wo_buf.at[tp_pos])))]
    for one in loads:
        one.start()

    enter_all(n_cp, n_tp)

    sibling = PAIR * x_pos + 1 - core

    def wo_copy(src, slot, sem, to_tp):
        return pltpu.make_async_remote_copy(src, wo_buf.at[slot], swo_sem.at[sem], rwo_sem.at[sem], device_id=mesh_id(cp_pos, to_tp),
                                            device_id_type=MESH)

    def wo_send(step):
        to_tp = PAIR * ((x_pos + step) % n_x) + core if step else sibling
        return wo_copy(wo_hbm, tp_pos, step, to_tp)

    def wo_pass(step):
        slot = PAIR * ((x_pos + n_x - step) % n_x) + core
        return wo_copy(wo_buf.at[slot], slot, n_x + step, sibling)

    def run_wo_passes():
        for step in range(1, n_x):
            wo_send(step).wait_recv()
            wo_pass(step).start()

    keep = wgx_hbm.shape[0]
    swaps = [pltpu.make_async_remote_copy(src.at[pl.ds((1 - core) * keep, keep)], dst, sw_sem.at[i], rw_sem.at[i],
                                          device_id=mesh_id(cp_pos, PAIR * x_pos + 1 - core), device_id_type=MESH)
             for i, (src, dst) in enumerate(((wg_hbm, wgx_hbm), (wu_hbm, wux_hbm), (wd_hbm, wdx_hbm)))]
    ranks = []
    for slot, off in ((1, 1), (PAIR, -1), (3, PAIR)):
        for part, place in enumerate((((cp_pos + off + n_cp) % n_cp, tp_pos), (cp_pos, PAIR * ((x_pos + off + n_x) % n_x) + core))):
            ranks.append(pltpu.make_async_remote_copy(rank_hbm, near_hbm.at[part, slot], sr_sem.at[part, slot], rr_sem.at[part, slot],
                                                      device_id=mesh_id(*place), device_id_type=MESH))
    for step in range(n_x):
        wo_send(step).start()
    for one in swaps + ranks:
        one.start()
    for one in loads[:3]:
        one.wait()

    def columns(block):
        return pl.ds(pl.multiple_of(block * tok_dev, tok_dev), tok_dev)

    def scores(block, cols, s_ref, masked):
        s_vals = jnp.dot(k_buf[columns(block), :], qt_buf[:, cols], preferred_element_type=jnp.float32)
        if masked:
            key_id = lax.broadcasted_iota(jnp.int32, s_vals.shape, 0)
            query_id = lax.broadcasted_iota(jnp.int32, s_vals.shape, 1)
            s_vals = jnp.where(key_id <= query_id, s_vals, -1e30)
        s_ref[...] = s_vals
        return jnp.max(s_vals, **COLUMN_WISE)

    def soften(s_ref, s_top, cols, p_ref, shrink_ref):
        m_old = m_ref[:, cols]
        m_new = jnp.maximum(m_old, s_top)
        shrink = jnp.exp2((m_old - m_new) * scale)
        m_ref[:, cols] = m_new
        shrink_ref[...] = shrink
        prob = jnp.exp2((s_ref[...] - m_new) * scale)
        l_ref[:, cols] = l_ref[:, cols] * shrink + jnp.sum(prob, **COLUMN_WISE)
        p_ref[...] = prob.astype(jnp.bfloat16)

    def gather_values(block, cols, p_ref, shrink_ref):
        acc[:, cols] = acc[:, cols] * shrink_ref[...] + jnp.dot(vt_buf[:, columns(block)], p_ref[...], preferred_element_type=jnp.float32)

    def query_pair(turn, carry):
        g = (turn + 1 + cp_pos + x_pos // PAIR * (PAIR * n_cp - 1 - PAIR * cp_pos)) % (n_dev // 4)

        @pl.when(turn == n_dev // 4 - 2)
        def _():
            run_wo_passes()
        q_rows = q_buf[pl.ds(pl.multiple_of(g * PAIR * tok_dev, PAIR * tok_dev), PAIR * tok_dev), :]
        qt_buf[...] = q_rows.astype(jnp.float32).T.astype(jnp.bfloat16)
        m_ref[...] = jnp.full_like(m_ref, -1e30)
        l_ref[...] = jnp.zeros_like(l_ref)
        acc[...] = jnp.zeros_like(acc)
        p_odd[...] = jnp.zeros_like(p_odd)
        shrink_odd[...] = jnp.ones_like(shrink_odd)
        near = ((0, core), (1, 3 - core), (1 - core, 0), (1, 1 - core), (1, 2 - core))
        lanes = [(s_even, p_even, shrink_even, 0), (s_even, p_even, shrink_even, 1), (s_odd, p_near, shrink_odd, 0), (s_odd, p_near, shrink_odd, 1)]
        tops = {}

        def near_refs(i):
            s_ref, p_ref, shrink_ref, place = lanes[i % 4]
            cols = pl.ds(place * tok_dev, tok_dev)
            return s_ref.at[:, cols], p_ref.at[:, cols], shrink_ref.at[:, cols]

        def near_scores(i):
            r, block = near[i]
            tops[i] = scores(4 * g + block, columns(r), near_refs(i)[0], i < 2)

        def near_soften(i):
            s_ref, p_ref, shrink_ref = near_refs(i)
            soften(s_ref, tops[i], columns(near[i][0]), p_ref, shrink_ref)

        def near_values(i):
            _, p_ref, shrink_ref = near_refs(i)
            gather_values(4 * g + near[i][1], columns(near[i][0]), p_ref, shrink_ref)

        for i in range(len(near) + 2):
            if i < len(near):
                near_scores(i)
            if 0 <= i - 1 < len(near):
                near_soften(i - 1)
            if 0 <= i - 2:
                near_values(i - 2)
        shrink_odd[...] = jnp.ones_like(shrink_odd)
        strip = min(256, tok_dev)
        strips = [pl.ds(lo, strip) for lo in range(0, PAIR * tok_dev, strip)]

        def far_step(block, parity, tops):
            s_in, s_out = (s_even, s_odd)[::1 - PAIR * parity]
            p_out, p_in = (p_even, p_odd)[::1 - PAIR * parity]
            shrink_out, shrink_in = (shrink_even, shrink_odd)[::1 - PAIR * parity]
            next_tops = []
            for cols, top in zip(strips, tops):
                next_tops.append(scores(block + 1, cols, s_out.at[:, cols], False))
                soften(s_in.at[:, cols], top, cols, p_out.at[:, cols], shrink_out.at[:, cols])
                gather_values(jnp.maximum(block - 1, 0), cols, p_in.at[:, cols], shrink_in.at[:, cols])
            return next_tops

        def far_blocks(n, tops):
            for j in range(4):
                tops = far_step(4 * n + j, j % PAIR, tops)
            return tops

        lax.fori_loop(0, g, far_blocks, [scores(0, cols, s_even.at[:, cols], False) for cols in strips])
        for cols in strips:
            gather_values(jnp.maximum(4 * g - 1, 0), cols, p_odd.at[:, cols], shrink_odd.at[:, cols])
        out = (acc[...] / l_ref[...]).T.astype(jnp.bfloat16)
        for r in BOTH:
            o_st[PAIR * g + r] = out[r * tok_dev:(r + 1) * tok_dev]
            o_push(PAIR * g + r, "start")
        return carry

    def o_push(index, what):
        block = 4 * (index // PAIR) + (1 - core) * 3 * (index % PAIR) + core * (1 + index % PAIR)
        to_cp, to_tp = owner_of(block, n_cp, n_tp)
        here = and_(to_cp == cp_pos, to_tp == tp_pos)
        if what == "start":
            @pl.when(here)
            def _():
                pltpu.make_async_copy(o_st.at[index], o_hbm.at[head], ro_sem.at[head]).start()

        @pl.when(not_(here))
        def _():
            copy = pltpu.make_async_remote_copy(o_st.at[index], o_hbm.at[head], so_sem.at[index], ro_sem.at[head],
                                                device_id=mesh_id(to_cp, to_tp), device_id_type=MESH)
            if what == "start":
                copy.start()
            else:
                copy.wait_send()

    lax.fori_loop(0, n_dev // 4, query_pair, 0)

    wo_send(0).wait_recv()
    for step in range(1, n_x):
        wo_pass(step).wait_recv()
    for one in loads[3:]:
        one.wait()
    for j in range(n_heads):
        pltpu.make_async_copy(o_hbm.at[j], o_hbm.at[j], ro_sem.at[j]).wait()
    o_load = pltpu.make_async_copy(o_hbm, o_buf, o_sem)
    o_load.start()
    o_load.wait()
    o_rows = jnp.concatenate([o_buf[j] for j in range(n_heads)], axis=1)
    n_cols = min(512, hid // PAIR)

    for col in range(0, hid, n_cols):
        cols = pl.ds(col, n_cols)
        w_cols = wo_buf[:, :, cols].reshape(n_heads * head_dim, n_cols)
        h_cols = (x_buf[:, cols].astype(jnp.float32) + jnp.dot(o_rows, w_cols, preferred_element_type=jnp.float32)).astype(jnp.bfloat16)
        h_ref[PAIR * col // hid, :, pl.ds(col % (hid // PAIR), n_cols)] = h_cols

    for step in range(n_x):
        wo_send(step).wait_send()
    for step in range(1, n_x):
        wo_pass(step).wait_send()
    for one in swaps + ranks:
        one.wait()

    def drain(index, carry):
        o_push(index, "wait")
        return carry

    lax.fori_loop(0, n_dev // PAIR, drain, 0)


def attend_call(n_cp, n_tp, k_all, vt_all, q_all, x_loc, wo_loc, w_gate, w_up, w_down, rank_rows):
    n_dev = n_cp * n_tp
    tok_dev, hid = x_loc.shape
    seq, head_dim = k_all.shape
    n_heads = n_tp * wo_loc.shape[0] // head_dim
    keep = w_gate.shape[0] // PAIR
    any_spec = pl.BlockSpec(memory_space=pl.ANY)
    bf16 = jnp.bfloat16
    h_loc, _, wg_other, wu_other, wd_other, near_rows = pl.pallas_call(
        functools.partial(attend_kernel, n_cp, n_tp),
        name="attend_heads",
        out_shape=(jax.ShapeDtypeStruct((PAIR, tok_dev, hid // PAIR), bf16), jax.ShapeDtypeStruct((n_heads, tok_dev, head_dim), bf16))
        + tuple(jax.ShapeDtypeStruct((keep,) + w.shape[1:], bf16) for w in (w_gate, w_up, w_down))
        + (jax.ShapeDtypeStruct((PAIR, 4) + rank_rows.shape, jnp.float32),),
        in_specs=[any_spec] * 9,
        out_specs=(pl.BlockSpec(memory_space=pltpu.VMEM),) + (any_spec,) * 5,
        scratch_shapes=[
            pltpu.VMEM((seq, head_dim), bf16),
            pltpu.VMEM((head_dim, seq), bf16),
            pltpu.VMEM((seq // PAIR, head_dim), bf16),
            pltpu.VMEM((head_dim, PAIR * tok_dev), bf16),
            pltpu.VMEM((n_dev // PAIR, tok_dev, head_dim), bf16),
            pltpu.VMEM((n_heads, tok_dev, head_dim), bf16),
            pltpu.VMEM((n_tp,) + wo_loc.shape, bf16),
            pltpu.VMEM((tok_dev, hid), bf16),
            pltpu.VMEM((tok_dev, PAIR * tok_dev), jnp.float32),
            pltpu.VMEM((tok_dev, PAIR * tok_dev), jnp.float32),
            pltpu.VMEM((tok_dev, PAIR * tok_dev), bf16),
            pltpu.VMEM((tok_dev, PAIR * tok_dev), bf16),
            pltpu.VMEM((tok_dev, PAIR * tok_dev), bf16),
            pltpu.VMEM((1, PAIR * tok_dev), jnp.float32),
            pltpu.VMEM((1, PAIR * tok_dev), jnp.float32),
            pltpu.VMEM((head_dim, PAIR * tok_dev), jnp.float32),
            pltpu.VMEM((1, PAIR * tok_dev), jnp.float32),
            pltpu.VMEM((1, PAIR * tok_dev), jnp.float32),
            dma((5,)),
            dma((n_dev // PAIR,)),
            dma((n_heads,)),
            dma((n_tp,)),
            dma((n_tp,)),
            dma((3,)),
            dma((3,)),
            dma((PAIR, 4)),
            dma((PAIR, 4)),
            dma,
        ],
        compiler_params=pltpu.CompilerParams(collective_id=1, has_side_effects=True, vmem_limit_bytes=VMEM_LIMIT),
        cost_estimate=pl.CostEstimate(flops=PAIR * seq * seq * head_dim // PAIR, bytes_accessed=2**26, transcendentals=seq * seq // 4),
    )(k_all, vt_all, q_all, x_loc, wo_loc, w_gate, w_up, w_down, rank_rows)
    return h_loc, near_rows, wg_other, wu_other, wd_other


def solution(mesh):
    n_cp = mesh.shape["cp"]
    n_tp = mesh.shape["tp"]
    row_spec = P(("dp", "cp", "tp"), None)
    head_spec = P(None, "tp", None)
    expert_spec = P(("cp", "tp"), None, None)

    def device_step(x_loc, w_q, w_k, w_v, w_o, ids_loc, gates_loc, w_gate, w_up, w_down):
        tok_dev, hid_dim = x_loc.shape
        n_loc, head_dim = w_q.shape[1:]
        n_experts = w_gate.shape[0] * n_cp * n_tp // PAIR
        capacity = ids_loc.shape[1] * tok_dev // n_experts
        w_parts = [w.reshape(hid_dim, n_loc * head_dim) for w in (w_q, w_k, w_v)]
        rank_rows, gate_rows = routing_rows(ids_loc, gates_loc, n_experts)
        k_all, vt_all, q_all = front_call(n_cp, n_tp, x_loc, w_parts, head_dim, n_loc)
        h_loc, near_rows, *others = attend_call(n_cp, n_tp, k_all, vt_all, q_all, x_loc, w_o.reshape(n_loc * head_dim, hid_dim), w_gate, w_up, w_down, rank_rows)
        return moe_call(n_cp, n_tp, capacity, h_loc, rank_rows, near_rows, gate_rows, w_gate, w_up, w_down, *others)

    return jax.shard_map(device_step, mesh=mesh, in_specs=(row_spec, head_spec, head_spec, head_spec, P("tp", None, None), row_spec, row_spec, expert_spec, expert_spec, expert_spec), out_specs=row_spec, check_vma=False)
```

```python
import functools

import jax
import jax.numpy as jnp
from jax import lax
from jax.experimental import pallas as pl
from jax.experimental.pallas import tpu as pltpu
from jax.sharding import PartitionSpec as P

MESH = pl.DeviceIdType.MESH
PAIR = 2
BOTH = range(PAIR)
ROWS_ROWS = (((0,), (0,)), ((), ()))
COLUMN_WISE = {"axis": 0, "keepdims": True}
dma = pltpu.SemaphoreType.DMA
and_, or_, not_ = jnp.logical_and, jnp.logical_or, jnp.logical_not
VMEM_LIMIT = 66_000_000
PLACES = ((0, 0), (0, 1), (1, 0), (0, -1), (-1, 0), (1, 1), (-1, -1), (1, -1), (-1, 1), (0, PAIR), (PAIR, 0), (1, PAIR), (PAIR, 1), (-1, PAIR), (PAIR, -1), (PAIR, PAIR))
N_NEAR, FIRST_FAR = 5, 9
GROUPS = ("1234", "1234", "9a9a", "bcbc", "dede", "0f0f", "5656", "7878")
FLIPS = ("0000", "1111") + ("0011",) * 6
SOURCES = (0, -1, 1, PAIR)


def peer_of(step, cp_pos, tp_pos, n_cp, n_tp):
    n_x = n_tp // PAIR
    off_x = (step // PAIR) % n_x
    off_y = (off_x + step // n_tp) % n_cp
    return (cp_pos + off_y) % n_cp, ((tp_pos // PAIR + off_x) % n_x) * 2 + (tp_pos % PAIR + step % PAIR) % PAIR


def mesh_id(cp_pos, tp_pos):
    return {"cp": cp_pos, "tp": tp_pos}


def enter_all(n_cp, n_tp):
    cp_pos, tp_pos = lax.axis_index("cp"), lax.axis_index("tp")

    def signal_peer(step, carry):
        to_cp, to_tp = peer_of(step, cp_pos, tp_pos, n_cp, n_tp)
        pl.semaphore_signal(pltpu.get_barrier_semaphore(), inc=1, device_id=mesh_id(to_cp, to_tp), device_id_type=MESH)
        return carry

    lax.fori_loop(1, n_cp * n_tp, signal_peer, 0)
    pl.semaphore_wait(pltpu.get_barrier_semaphore(), n_cp * n_tp - 1)


def pick(values, index):
    out = values[-1]
    for k, value in enumerate(values[:-1]):
        out = jnp.where(index == k, value, out)
    return out


def moe_kernel(n_cp, n_tp, group, h_hbm, rank_hbm, near_hbm, gate_ref, wg_hbm, wu_hbm, wd_hbm, wgx_hbm, wux_hbm, wdx_hbm,
               y_ref, rx_hbm, rl_hbm, rz_hbm, zl_hbm,
               h_buf, rank_buf, wg_buf, wu_buf, wd_buf, ring, own_stage, z_ring, x_buf, z_buf, acc, parts,
               w_sem, rank_sem, in_sem, x_sem, z_sem, hs_sem, hr_sem, ss_sem, rx_sem, rl_sem, fl_sem, sz_sem, rz_sem, zl_sem, fz_sem):
    n_x = n_tp // PAIR
    tok_dev, half_hid = h_buf.shape[2:]
    hid = PAIR * half_hid
    cap = ring.shape[3] // PAIR
    cp_pos, tp_pos = lax.axis_index("cp"), lax.axis_index("tp")
    x_pos, core = tp_pos // PAIR, tp_pos % PAIR
    half_tok = tok_dev // PAIR

    def at(off_y, off_x, flip):
        return (cp_pos + off_y + n_cp) % n_cp, PAIR * ((x_pos + off_x + n_x) % n_x) + (core + flip) % PAIR

    def line(place):
        return place[0] * n_tp + place[1]

    def send(src, dst, s_sem, r_sem, place):
        return pltpu.make_async_remote_copy(src, dst, s_sem, r_sem, device_id=mesh_id(*place), device_id_type=MESH)

    def await_bytes(ref, sem):
        pltpu.make_async_copy(ref, ref, sem).wait()

    h_loads = [pltpu.make_async_copy(h_hbm.at[part], h_buf.at[part, 0], in_sem.at[part]) for part in BOTH]
    rank_loads = []
    for part in BOTH:
        rank_loads.append(pltpu.make_async_copy(rank_hbm, rank_buf.at[part, 0], rank_sem.at[PAIR * part]))
        rank_loads.append(pltpu.make_async_copy(near_hbm.at[part, pl.ds(1, 3)], rank_buf.at[part, pl.ds(1, 3)], rank_sem.at[PAIR * part + 1]))
    w_loads = []
    for slot, (own, other, buf) in enumerate(((wg_hbm, wgx_hbm, wg_buf), (wu_hbm, wux_hbm, wu_buf), (wd_hbm, wdx_hbm, wd_buf))):
        w_loads.append(pltpu.make_async_copy(own.at[pl.ds(PAIR * core, PAIR)], buf.at[0], w_sem.at[PAIR * slot]))
        w_loads.append(pltpu.make_async_copy(other, buf.at[1], w_sem.at[PAIR * slot + 1]))
    for one in h_loads + rank_loads:
        one.start()
    enter_all(n_cp, n_tp)

    def along(part, off):
        return at(off, 0, 0) if part == 0 else at(0, off, 0)

    def across(part, off, flip):
        return at(0, off, flip) if part == 0 else at(off, 0, flip)

    def rows_of(piece):
        return pl.ds(piece * half_tok, half_tok)

    def spread(part, i):
        piece, off, slot = ((0, 1, 1), (1, -1, PAIR), (1, 1, 1), (0, -1, PAIR), (0, 1, 3), (1, -1, 3))[i]
        rows = rows_of(piece)
        src = h_hbm.at[part, rows] if i < 4 else h_buf.at[part, 1 if i == 4 else 2, rows]
        return send(src, h_buf.at[part, slot, rows], hs_sem.at[part, i], hr_sem.at[part, slot, piece], along(part, off))

    def await_h(part, slot, piece):
        await_bytes(h_buf.at[part, slot, rows_of(piece)], hr_sem.at[part, slot, piece])

    for i in range(4):
        for part in BOTH:
            spread(part, i).start()
    for one in w_loads:
        one.start()
    for one in h_loads + rank_loads:
        one.wait()

    slots = lax.broadcasted_iota(jnp.int32, (cap, tok_dev), 0).astype(jnp.float32)

    def gather_rows(part, stage, m):
        turn = m // PAIR
        off = turn + (turn // PAIR) * (5 - PAIR * turn)
        first = PAIR * line(across(part, off, m % PAIR))
        chosen = [jnp.where(rank_buf[part, stage, pl.ds(first + i, 1), :] == slots, 1.0, 0.0) for i in BOTH]
        chosen = jnp.concatenate(chosen, axis=0).astype(jnp.bfloat16)
        return jnp.dot(chosen, h_buf[part, stage], preferred_element_type=jnp.float32).astype(jnp.bfloat16)

    def source_line(part, stage, off):
        a = SOURCES[stage]
        return line(at(a, off, 0) if part == 0 else at(off, a, 0))

    def await_ring(part, stage):
        def one(m, carry):
            await_bytes(ring.at[part, stage % PAIR, m], ss_sem.at[part, stage % PAIR, m])
            return carry
        lax.fori_loop(1, 8, one, 0)

    def own_copy(part, stage):
        src_line = source_line(part, stage, 0)
        return pltpu.make_async_copy(own_stage.at[part, stage], rx_hbm.at[part, src_line], rx_sem.at[part, src_line])

    def run_stage(stage):
        side = stage % PAIR
        for part in BOTH:
            if stage >= 2:
                await_ring(part, stage)
            own_stage[part, stage] = gather_rows(part, stage, 0)

            def fill(m, carry):
                ring[part, side, m] = gather_rows(part, stage, m)
                return carry

            lax.fori_loop(1, 8, fill, 0)
        lines = [source_line(part, stage, 0) for part in BOTH]
        for flip in BOTH:
            for way, off in enumerate((1, -1)):
                for part in BOTH:
                    m = 6 + flip
                    send(ring.at[part, side, m, pl.ds(way * cap, cap)], rl_hbm.at[part, way, stage, flip], ss_sem.at[part, side, m],
                         rl_sem.at[part, way, stage, flip], across(part, off, 0)).start()
        for m, off in ((PAIR, 1), (4, -1), (3, 1), (5, -1), (1, 0)):
            for part in BOTH:
                send(ring.at[part, side, m], rx_hbm.at[part, lines[part]], ss_sem.at[part, side, m], rx_sem.at[part, lines[part]],
                     across(part, off, m % PAIR)).start()
        for part in BOTH:
            own_copy(part, stage).start()

    def relay(part, stage, way, flip):
        off = 1 - PAIR * way
        src_line = source_line(part, stage, -off)
        return send(rl_hbm.at[part, way, stage, flip], rx_hbm.at[part, src_line, pl.ds(way * cap, cap)], fl_sem.at[part, way, stage, flip],
                    rx_sem.at[part, src_line], across(part, off, flip))

    def run_relays(stage):
        for flip in BOTH:
            for way in BOTH:
                for part in BOTH:
                    await_bytes(rl_hbm.at[part, way, stage, flip], rl_sem.at[part, way, stage, flip])
                    relay(part, stage, way, flip).start()

    run_stage(0)
    for part in BOTH:
        await_h(part, 1, 0)
        spread(part, 4).start()
    for part in BOTH:
        await_h(part, PAIR, 1)
        spread(part, 5).start()
    for part in BOTH:
        await_h(part, 1, 1)
    run_stage(1)
    gate_all = gate_ref[...]
    high = gate_all.astype(jnp.bfloat16).astype(jnp.float32)
    rest = gate_all - high
    mid = rest.astype(jnp.bfloat16).astype(jnp.float32)
    parts[0] = high
    parts[1] = mid
    parts[2] = rest - mid
    for part in BOTH:
        acc[:, part * half_hid:(part + 1) * half_hid] = h_buf[part, 0].astype(jnp.float32)
    run_relays(0)
    for part in BOTH:
        await_h(part, PAIR, 0)
    run_stage(2)
    run_relays(1)
    for part in BOTH:
        await_h(part, 3, 0)
        await_h(part, 3, 1)
    run_stage(3)
    run_relays(2)
    for one in w_loads:
        one.wait()

    rows = group * cap
    n_cols = min(512, hid)

    def expert_rows(slot, i):
        x_rows = x_buf[:, pl.ds(i * cap, cap), :].reshape(rows, hid)
        hidden = []
        for half in BOTH:
            gate_pre = jnp.dot(x_rows, wg_buf[half, i], preferred_element_type=jnp.float32)
            up_pre = jnp.dot(x_rows, wu_buf[half, i], preferred_element_type=jnp.float32)
            hidden.append((gate_pre * (1.0 / (1.0 + jnp.exp(-gate_pre))) * up_pre).astype(jnp.bfloat16))
        for col in range(0, hid, n_cols):
            z_rows = (jnp.dot(hidden[0], wd_buf[0, i, :, pl.ds(col, n_cols)], preferred_element_type=jnp.float32)
                      + jnp.dot(hidden[1], wd_buf[1, i, :, pl.ds(col, n_cols)], preferred_element_type=jnp.float32))
            z_ring[slot, :, pl.ds(i * cap, cap), pl.ds(col, n_cols)] = z_rows.astype(jnp.bfloat16).reshape(group, cap, n_cols)

    def place_at(g, q):
        places = [int(names[q], 16) for names in GROUPS]
        off_y, off_x = (pick([PLACES[p][k] for p in places], g) for k in BOTH)
        return off_y, off_x, pick([int(flips[q]) for flips in FLIPS], g), pick(places, g)

    my_line = line((cp_pos, tp_pos))

    def await_slot(slot):
        for q in range(group):
            await_bytes(z_ring.at[slot, q], sz_sem.at[slot, q])

    def expert_group(g, carry):
        slot = g % 3

        @pl.when(g == 2)
        def _():
            run_relays(3)

        sources = [line(at(*place_at(g, q)[:3])) for q in range(group)]
        loads = []
        for q in range(group):
            for part in BOTH:
                await_bytes(rx_hbm.at[part, sources[q]], rx_sem.at[part, sources[q]])
                loads.append(pltpu.make_async_copy(rx_hbm.at[part, sources[q]], x_buf.at[q, :, pl.ds(part * half_hid, half_hid)], x_sem.at[part, q]))
                loads[-1].start()

        @pl.when(g >= 3)
        def _():
            await_slot(slot)
        for one in loads:
            one.wait()
        for i in BOTH:
            expert_rows(slot, i)
        for q in range(group):
            off_y, off_x, flip, p = place_at(g, q)
            alone = and_(p == 0, flip == 0)

            @pl.when(alone)
            def _():
                pltpu.make_async_copy(z_ring.at[slot, q], rz_hbm.at[my_line], rz_sem.at[my_line]).start()

            @pl.when(and_(p < FIRST_FAR, not_(alone)))
            def _():
                send(z_ring.at[slot, q], rz_hbm.at[my_line], sz_sem.at[slot, q], rz_sem.at[my_line], at(off_y, off_x, flip)).start()

            @pl.when(p >= FIRST_FAR)
            def _():
                lead_y, lead_x = jnp.where(off_y == 2, 1, 0), jnp.where(off_x == 2, 1, 0)
                for way in BOTH:
                    sign = 1 - PAIR * way
                    send(z_ring.at[slot, q, pl.ds(way * cap, cap)], zl_hbm.at[p - FIRST_FAR, flip, way], sz_sem.at[slot, q],
                         zl_sem.at[p - FIRST_FAR, flip, way], at(sign * lead_y, sign * lead_x, 0)).start()
        return carry

    lax.fori_loop(0, len(GROUPS), expert_group, 0)

    n_far = len(PLACES) - FIRST_FAR

    def z_relay(index, flip, way):
        off_y, off_x = PLACES[FIRST_FAR + index]
        sign = 1 - PAIR * way
        lead_y, lead_x = sign * (off_y == 2), sign * (off_x == 2)
        from_line = line(at(-lead_y, -lead_x, 0))
        to_y = sign if off_y == 2 else off_y
        to_x = sign if off_x == 2 else off_x
        return send(zl_hbm.at[index, flip, way], rz_hbm.at[from_line, pl.ds(way * cap, cap)], fz_sem.at[index, flip, way],
                    rz_sem.at[from_line], at(to_y, to_x, flip))

    def each_relay(*indices):
        return [(index, flip, way) for flip in BOTH for way in BOTH for index in indices]

    def run_z_relays(*indices):
        for key in each_relay(*indices):
            await_bytes(zl_hbm.at[key], zl_sem.at[key])
            z_relay(*key).start()

    def combine(p, carry):
        off_y, off_x = pick([a for a, _ in PLACES], p), pick([b for _, b in PLACES], p)
        homes = [line(at(-off_y, -off_x, q)) for q in BOTH]
        loads = []
        for q in BOTH:
            await_bytes(rz_hbm.at[homes[q]], rz_sem.at[homes[q]])
            loads.append(pltpu.make_async_copy(rz_hbm.at[homes[q]], z_buf.at[q], z_sem.at[q]))
            loads[-1].start()
        weights = [[], [], []]
        for q in BOTH:
            for i in BOTH:
                row = pl.ds(PAIR * homes[q] + i, 1)
                chosen = rank_buf[0, 0, row, :] == slots
                for part in range(3):
                    weights[part].append(jnp.where(chosen, parts[part, row, :], 0.0))
        weights = [jnp.concatenate(w, axis=0).astype(jnp.bfloat16) for w in weights]
        for one in loads:
            one.wait()
        for col in range(0, hid, n_cols):
            z_rows = z_buf[:, :, pl.ds(col, n_cols)].reshape(4 * cap, n_cols)
            total = None
            for part in range(3):
                term = lax.dot_general(weights[part], z_rows, ROWS_ROWS, preferred_element_type=jnp.float32)
                total = term if total is None else total + term
            acc[:, pl.ds(col, n_cols)] += total
        return carry

    run_z_relays(0, 1)
    run_z_relays(PAIR, 3)
    lax.fori_loop(0, N_NEAR, combine, 0)
    run_z_relays(4, 5)
    run_z_relays(6)
    lax.fori_loop(N_NEAR, len(PLACES), combine, 0)
    y_ref[...] = acc[...].astype(jnp.bfloat16)

    for part in BOTH:
        for i in range(6):
            spread(part, i).wait_send()
        for stage in (PAIR, 3):
            await_ring(part, stage)
        for stage in range(4):
            for way in BOTH:
                for flip in BOTH:
                    relay(part, stage, way, flip).wait_send()
    last = len(GROUPS) - 3
    for g in range(last, len(GROUPS)):
        for q in range(group):
            if GROUPS[g][q] + FLIPS[g][q] != "00":
                await_bytes(z_ring.at[g % 3, q], sz_sem.at[g % 3, q])
    for key in each_relay(*range(n_far)):
        z_relay(*key).wait_send()


def moe_call(n_cp, n_tp, cap, h_loc, rank_rows, near_rows, gate_rows, w_gate, w_up, w_down, wg_other, wu_other, wd_other):
    n_dev = n_cp * n_tp
    _, tok_dev, half_hid = h_loc.shape
    hid = PAIR * half_hid
    half_f = w_gate.shape[2]
    n_experts = rank_rows.shape[0]
    group = len(GROUPS[0])
    n_far = len(PLACES) - FIRST_FAR
    bf16 = jnp.bfloat16
    any_spec = pl.BlockSpec(memory_space=pl.ANY)
    vmem_spec = pl.BlockSpec(memory_space=pltpu.VMEM)
    flops = PAIR * n_dev * PAIR * cap * hid * PAIR * half_f * 3
    return pl.pallas_call(
        functools.partial(moe_kernel, n_cp, n_tp, group),
        name="routed_experts",
        out_shape=(jax.ShapeDtypeStruct((tok_dev, hid), bf16), jax.ShapeDtypeStruct((PAIR, n_dev, PAIR * cap, half_hid), bf16),
                   jax.ShapeDtypeStruct((PAIR, PAIR, 4, PAIR, cap, half_hid), bf16), jax.ShapeDtypeStruct((n_dev, PAIR * cap, hid), bf16),
                   jax.ShapeDtypeStruct((n_far, PAIR, 2, cap, hid), bf16)),
        in_specs=[any_spec, any_spec, any_spec, vmem_spec] + [any_spec] * 6,
        out_specs=(vmem_spec,) + (any_spec,) * 4,
        scratch_shapes=[
            pltpu.VMEM((PAIR, 4, tok_dev, half_hid), bf16),
            pltpu.VMEM((PAIR, 4, n_experts, tok_dev), jnp.float32),
            pltpu.VMEM((PAIR, PAIR, hid, half_f), bf16),
            pltpu.VMEM((PAIR, PAIR, hid, half_f), bf16),
            pltpu.VMEM((PAIR, PAIR, half_f, hid), bf16),
            pltpu.VMEM((PAIR, PAIR, 8, PAIR * cap, half_hid), bf16),
            pltpu.VMEM((PAIR, 4, PAIR * cap, half_hid), bf16),
            pltpu.VMEM((3, group, PAIR * cap, hid), bf16),
            pltpu.VMEM((group, PAIR * cap, hid), bf16),
            pltpu.VMEM((PAIR, PAIR * cap, hid), bf16),
            pltpu.VMEM((tok_dev, hid), jnp.float32),
            pltpu.VMEM((3, n_experts, tok_dev), jnp.float32),
            dma((6,)), dma((4,)), dma((PAIR,)), dma((PAIR, group)), dma((PAIR,)),
            dma((PAIR, 6)), dma((PAIR, 4, PAIR)), dma((PAIR, PAIR, 8)), dma((PAIR, n_dev)), dma((PAIR, PAIR, 4, PAIR)), dma((PAIR, PAIR, 4, PAIR)),
            dma((3, group)), dma((n_dev,)), dma((n_far, PAIR, PAIR)), dma((n_far, PAIR, PAIR)),
        ],
        compiler_params=pltpu.CompilerParams(collective_id=2, has_side_effects=True, vmem_limit_bytes=VMEM_LIMIT),
        cost_estimate=pl.CostEstimate(flops=flops, bytes_accessed=2**27, transcendentals=0),
    )(h_loc, rank_rows, near_rows, gate_rows, w_gate, w_up, w_down, wg_other, wu_other, wd_other)[0]


def routing_rows(ids_ref, gates_ref, rank_ref, gate_ref):
    top_k, tok_dev = ids_ref.shape
    ids, gates = ids_ref[...].astype(jnp.float32), gates_ref[...]
    expert = lax.broadcasted_iota(jnp.int32, rank_ref.shape, 0).astype(jnp.float32)
    chosen, weight = jnp.zeros_like(expert), jnp.zeros_like(expert)
    for k in range(top_k):
        hit = ids[k:k + 1] == expert
        chosen = jnp.where(hit, 1.0, chosen)
        weight = jnp.where(hit, gates[k:k + 1], weight)
    token = lax.broadcasted_iota(jnp.int32, (tok_dev, tok_dev), 0)
    before = jnp.where(token < lax.broadcasted_iota(jnp.int32, (tok_dev, tok_dev), 1), 1.0, 0.0).astype(jnp.bfloat16)
    rank = jnp.dot(chosen.astype(jnp.bfloat16), before, preferred_element_type=jnp.float32)
    rank_ref[...] = jnp.where(chosen > 0.0, rank, -1.0)
    gate_ref[...] = weight


def block_of(cp_pos, tp_pos, n_cp, n_tp):
    per_chunk = n_tp // PAIR
    late = tp_pos // per_chunk
    chunk = late * (PAIR * n_cp - 1 - cp_pos) + (1 - late) * cp_pos
    return chunk * per_chunk + tp_pos % per_chunk


def owner_of(block, n_cp, n_tp):
    per_chunk = n_tp // PAIR
    chunk = block // per_chunk
    late = chunk // n_cp
    return late * (PAIR * n_cp - 1 - chunk) + (1 - late) * chunk, late * per_chunk + block % per_chunk


def front_kernel(n_cp, n_tp, n_part, x_hbm, wq_hbm, wk_hbm, wv_hbm, ids_ref, gates_ref, k_hbm, vt_hbm, q_hbm, rank_ref, gate_ref,
                 x_buf, w_raw, w_buf, q_st, k_st, vt_st, k_far, vt_far, q_far,
                 own_sem, w_sem, ring_sem, pair_sem, rx_sem, sk_sem, sv_sem, sq_sem, kv_sem, rq_sem, sf_sem, rf_sem, far_sem, pass_sem):
    n_x = n_tp // PAIR
    tok_dev, hid = x_hbm.shape
    half = tok_dev // n_part
    head_dim = k_hbm.shape[1]
    n_loc = q_st.shape[1]
    chunk_len = tok_dev * n_x
    cp_pos, tp_pos = lax.axis_index("cp"), lax.axis_index("tp")
    x_pos, core = tp_pos // PAIR, tp_pos % PAIR
    sibling = PAIR * x_pos + 1 - core
    barrier = pltpu.get_barrier_semaphore()

    def slot_at(off, flip):
        return PAIR * ((x_pos + off + n_x) % n_x) + (core + flip) % PAIR

    own_copy = pltpu.make_async_copy(x_hbm, x_buf.at[tp_pos], own_sem)
    own_copy.start()
    width = n_loc * head_dim
    w_loads = [pltpu.make_async_copy(w, w_raw.at[i], w_sem.at[i]) for i, w in enumerate((wq_hbm, wk_hbm, wv_hbm))]
    for one in w_loads:
        one.start()
    for step in (1, n_x - 1):
        pl.semaphore_signal(barrier, inc=1, device_id=mesh_id(cp_pos, slot_at(step, 0)), device_id_type=MESH)
    for step in range(1, PAIR * n_cp):
        pl.semaphore_signal(barrier, inc=1, device_id=mesh_id((cp_pos + step // PAIR) % n_cp, PAIR * x_pos + (core + step) % PAIR), device_id_type=MESH)
    pl.semaphore_wait(barrier, PAIR * n_cp + 1)

    def own_send(part, to_tp, sem):
        rows = pl.ds(pl.multiple_of(part * half, half), half)
        return pltpu.make_async_remote_copy(x_hbm.at[rows], x_buf.at[tp_pos, rows], sem, rx_sem.at[tp_pos, part],
                                            device_id=mesh_id(cp_pos, to_tp), device_id_type=MESH)

    def pass_on(slot, part, to_tp, sem):
        rows = pl.ds(pl.multiple_of(part * half, half), half)
        return pltpu.make_async_remote_copy(x_buf.at[slot, rows], x_buf.at[slot, rows], sem, rx_sem.at[slot, part],
                                            device_id=mesh_id(cp_pos, to_tp), device_id_type=MESH)

    def ring_send(i, side):
        part = i if side == 0 else n_part - 1 - i
        return own_send(part, slot_at(1 - PAIR * side, 0), ring_sem.at[side, i])

    for i in BOTH:
        for side in BOTH:
            ring_send(i, side).start()
    for part in range(n_part):
        own_send(part, sibling, pair_sem.at[part]).start()
    first = PAIR * n_part
    for one in w_loads:
        one.wait()
    rows_once = min(256, hid)

    def widen(r, carry):
        rows = pl.ds(pl.multiple_of(r * rows_once, rows_once), rows_once)
        for i in range(len(w_loads)):
            w_buf[rows, pl.ds(i * width, width)] = w_raw[i, rows].reshape(rows_once, width)
        return carry

    lax.fori_loop(0, hid // rows_once, widen, 0)
    routing_rows(ids_ref, gates_ref, rank_ref, gate_ref)

    def place_of(step):
        late = jnp.minimum(step // first, 1)
        wave, other, side = jnp.maximum(step - first, 0) // 4, late * ((step // PAIR) % PAIR) + (1 - late) * (step // n_part), step % PAIR
        piece = pick((0, 1, 0, PAIR, 1, 3), wave)
        through = jnp.where(or_(wave == 2, wave == 4), 1, 0)
        part = late * (piece + side * (n_part - 1 - PAIR * piece)) + (1 - late) * (step % n_part)
        off = late * ((1 - through) * (PAIR * side - 1) + PAIR * through)
        return slot_at(off, other), part, off

    def targets(from_cp, slot, part):
        block = block_of(from_cp, slot, n_cp, n_tp)
        pos = pl.multiple_of(block * tok_dev + part * half, half)
        q_core = ((block % 4 + 1) // PAIR) % PAIR
        q_pos = pl.multiple_of((PAIR * (block // 4) + (block % 4) // PAIR) * tok_dev + part * half, half)
        return ((k_hbm.at[pl.ds(pos, half)], 0, kv_sem.at[from_cp]), (vt_hbm.at[:, pl.ds(pos, half)], 1, kv_sem.at[from_cp]),
                (q_hbm.at[pl.ds(q_pos, half)], q_core, rq_sem.at[from_cp]))

    def remote(src, dst, s_sem, r_sem, to_cp, to_core):
        return pltpu.make_async_remote_copy(src, dst, s_sem, r_sem, device_id=mesh_id((to_cp + n_cp) % n_cp, PAIR * x_pos + to_core), device_id_type=MESH)

    far_refs = (k_far, vt_far, q_far)

    def outputs_of(step):
        slot, part, _ = place_of(step)
        for i in range(n_loc):
            to_cp = n_loc * core + i
            far = (to_cp - cp_pos + n_cp) % n_cp == n_cp // PAIR
            for kind, (src, (dst, to_core, r_sem)) in enumerate(zip((k_st.at[step, i], vt_st.at[step, i], q_st.at[step, i]), targets(cp_pos, slot, part))):
                s_sem = (sk_sem.at[i], sv_sem.at[i], sq_sem.at[i, to_core])[kind]
                here = and_(to_cp == cp_pos, to_core == core)

                @pl.when(here)
                def _():
                    pltpu.make_async_copy(src, dst, r_sem).start()

                @pl.when(far)
                def _():
                    remote(src, far_refs[kind].at[part, slot], s_sem, far_sem.at[kind, part, slot], cp_pos + 1 - part // PAIR * 2, core).start()

                @pl.when(not_(or_(here, far)))
                def _():
                    remote(src, dst, s_sem, r_sem, to_cp, to_core).start()

    def pass_far(step, what):
        slot, part, _ = place_of(step)
        sign = 1 - part // PAIR * 2

        @pl.when((cp_pos + sign + n_cp) % n_cp // n_loc == core)
        def _():
            for kind, (dst, to_core, r_sem) in enumerate(targets((cp_pos - sign + n_cp) % n_cp, slot, part)):
                src = far_refs[kind].at[part, slot]
                copy = remote(src, dst, pass_sem.at[kind, part, slot], r_sem, cp_pos + sign, to_core)
                if what == "start":
                    pltpu.make_async_copy(src, src, far_sem.at[kind, part, slot]).wait()
                    copy.start()
                else:
                    copy.wait_send()

    def project(step, carry):
        slot, part, off = place_of(step)
        wave, other, side = (step - first) // 4, (step // PAIR) % PAIR, step % PAIR

        @pl.when(step == 0)
        def _():
            own_copy.wait()

        @pl.when(step >= n_part)
        def _():
            pass_on(slot, part, sibling, pair_sem.at[0]).wait_recv()

        @pl.when(and_(step >= first, other == 0))
        def _():
            @pl.when(wave < 2)
            def _():
                pass_on(slot, part, slot_at(-off, 0), ring_sem.at[side, n_part + wave]).start()
                for i in BOTH:
                    @pl.when(side == i)
                    def _():
                        ring_send(2 + wave, i).start()
            pass_on(slot, part, sibling, pair_sem.at[n_part + PAIR * wave + side]).start()

        x_rows = x_buf[slot, pl.ds(pl.multiple_of(part * half, half), half), :]
        qkv = jnp.dot(x_rows, w_buf[...], preferred_element_type=jnp.float32)
        for i in range(n_loc):
            q_st[step, i] = qkv[:, i * head_dim:(i + 1) * head_dim].astype(jnp.bfloat16)
            k_st[step, i] = qkv[:, (n_loc + i) * head_dim:(n_loc + i + 1) * head_dim].astype(jnp.bfloat16)
            vt_st[step, i] = qkv[:, (PAIR * n_loc + i) * head_dim:(PAIR * n_loc + i + 1) * head_dim].T.astype(jnp.bfloat16)

        @pl.when(step > 0)
        def _():
            outputs_of(step - 1)

        @pl.when(step >= lag)
        def _():
            pass_far(step - lag, "start")
        return carry

    n_steps, lag = n_part * n_tp, 8
    lax.fori_loop(0, n_steps, project, 0)
    outputs_of(n_steps - 1)

    def pass_late(step, carry):
        pass_far(step, "start")
        return carry

    lax.fori_loop(n_steps - lag, n_steps, pass_late, 0)

    def whole(ref, count, sem):
        return pltpu.make_async_copy(ref.at[pl.ds(0, count)], ref.at[pl.ds(0, count)], sem)

    def forward(y, place, core_id):
        chunk = y if place == 0 else PAIR * n_cp - 1 - y
        cols = pl.ds(chunk * chunk_len, chunk_len)
        ref = k_hbm.at[cols] if core_id == 0 else vt_hbm.at[:, cols]
        return pltpu.make_async_remote_copy(ref, ref, sf_sem.at[PAIR * y + place], rf_sem.at[PAIR * y + place],
                                            device_id=mesh_id(cp_pos, sibling), device_id_type=MESH)

    for y in range(n_cp):
        whole(k_hbm, PAIR * chunk_len, kv_sem.at[y]).wait()
        for core_id in BOTH:
            @pl.when(core == core_id)
            def _():
                for place in BOTH:
                    forward(y, place, core_id).start()
    for y in range(n_cp):
        whole(q_hbm, chunk_len, rq_sem.at[y]).wait()
    for side in BOTH:
        for i in range(n_part + 2):
            own_send(0, sibling, ring_sem.at[side, i]).wait_send()
    for i in range(n_part * n_x):
        own_send(0, sibling, pair_sem.at[i]).wait_send()
    for i in range(n_loc):
        to_cp = n_loc * core + i
        for sem, to_core, count in ((sk_sem.at[i], 0, PAIR * chunk_len), (sv_sem.at[i], 1, PAIR * chunk_len),
                                    (sq_sem.at[i, 0], 0, chunk_len), (sq_sem.at[i, 1], 1, chunk_len)):
            @pl.when(not_(and_(to_cp == cp_pos, to_core == core)))
            def _():
                whole(k_hbm, count, sem).wait()
    def drain(step, carry):
        pass_far(step, "wait")
        return carry

    lax.fori_loop(0, n_steps, drain, 0)
    for core_id in BOTH:
        @pl.when(core == core_id)
        def _():
            for y in range(n_cp):
                for place in BOTH:
                    forward(y, place, core_id).wait_send()
                    forward(y, place, 1 - core_id).wait_recv()


def front_call(n_cp, n_tp, x_loc, w_parts, ids_loc, gates_loc, n_experts):
    _, n_loc, head_dim = w_parts[0].shape
    tok_dev, hid = x_loc.shape
    n_part, n_x = 4, n_tp // PAIR
    half = tok_dev // n_part
    seq = tok_dev * n_cp * n_tp
    any_spec = pl.BlockSpec(memory_space=pl.ANY)
    n_steps = n_part * n_tp
    vmem_spec = pl.BlockSpec(memory_space=pltpu.VMEM)
    return pl.pallas_call(
        functools.partial(front_kernel, n_cp, n_tp, n_part),
        name="gather_project",
        out_shape=(jax.ShapeDtypeStruct((seq, head_dim), jnp.bfloat16), jax.ShapeDtypeStruct((head_dim, seq), jnp.bfloat16),
                   jax.ShapeDtypeStruct((seq // PAIR, head_dim), jnp.bfloat16)) + (jax.ShapeDtypeStruct((n_experts, tok_dev), jnp.float32),) * 2,
        in_specs=[any_spec] * 4 + [vmem_spec] * 2,
        out_specs=(any_spec,) * 3 + (vmem_spec,) * 2,
        scratch_shapes=[
            pltpu.VMEM((n_tp, tok_dev, hid), jnp.bfloat16),
            pltpu.VMEM((3, hid, n_loc, head_dim), jnp.bfloat16),
            pltpu.VMEM((hid, 3 * n_loc * head_dim), jnp.bfloat16),
            pltpu.VMEM((n_steps, n_loc, half, head_dim), jnp.bfloat16),
            pltpu.VMEM((n_steps, n_loc, half, head_dim), jnp.bfloat16),
            pltpu.VMEM((n_steps, n_loc, head_dim, half), jnp.bfloat16),
            pltpu.VMEM((n_part, n_tp, half, head_dim), jnp.bfloat16),
            pltpu.VMEM((n_part, n_tp, head_dim, half), jnp.bfloat16),
            pltpu.VMEM((n_part, n_tp, half, head_dim), jnp.bfloat16),
            dma,
            dma((3,)),
            dma((PAIR, n_part + 2)),
            dma((n_part * n_x,)),
            dma((n_tp, n_part)),
            dma((n_loc,)),
            dma((n_loc,)),
            dma((n_loc, PAIR)),
            dma((n_cp,)),
            dma((n_cp,)),
            dma((PAIR * n_cp,)),
            dma((PAIR * n_cp,)),
            dma((3, n_part, n_tp)),
            dma((3, n_part, n_tp)),
        ],
        compiler_params=pltpu.CompilerParams(collective_id=0, has_side_effects=True, vmem_limit_bytes=VMEM_LIMIT),
        cost_estimate=pl.CostEstimate(flops=PAIR * n_tp * tok_dev * hid * 3 * n_loc * head_dim, bytes_accessed=2**26, transcendentals=0),
    )(x_loc, *w_parts, ids_loc, gates_loc)


def attend_kernel(n_cp, n_tp, k_hbm, vt_hbm, q_hbm, x_hbm, wo_hbm, wg_hbm, wu_hbm, wd_hbm, rank_hbm,
                  h_ref, o_hbm, wgx_hbm, wux_hbm, wdx_hbm, near_hbm,
                  k_buf, vt_buf, q_buf, qt_buf, o_st, o_buf, wo_buf, x_buf, s_even, s_odd, p_even, p_odd, p_near, shrink_even, shrink_odd, acc, m_ref, l_ref,
                  in_sem, so_sem, ro_sem, swo_sem, rwo_sem, sw_sem, rw_sem, sr_sem, rr_sem, o_sem):
    n_dev = n_cp * n_tp
    n_x = n_tp // PAIR
    tok_dev, hid = x_buf.shape
    head_dim = k_buf.shape[1]
    n_heads = o_buf.shape[0]
    cp_pos, tp_pos = lax.axis_index("cp"), lax.axis_index("tp")
    x_pos, core = tp_pos // PAIR, tp_pos % PAIR
    head = n_cp * x_pos + cp_pos
    scale = (head_dim ** -0.5) * 1.4426950408889634
    loads = [pltpu.make_async_copy(src, dst, in_sem.at[i]) for i, (src, dst) in enumerate(
        ((q_hbm, q_buf), (k_hbm, k_buf), (vt_hbm, vt_buf), (x_hbm, x_buf), (wo_hbm, wo_buf.at[tp_pos])))]
    for one in loads:
        one.start()

    enter_all(n_cp, n_tp)

    sibling = PAIR * x_pos + 1 - core

    def wo_copy(src, slot, sem, to_tp):
        return pltpu.make_async_remote_copy(src, wo_buf.at[slot], swo_sem.at[sem], rwo_sem.at[sem], device_id=mesh_id(cp_pos, to_tp),
                                            device_id_type=MESH)

    def wo_send(step):
        to_tp = PAIR * ((x_pos + step) % n_x) + core if step else sibling
        return wo_copy(wo_hbm, tp_pos, step, to_tp)

    def wo_pass(step):
        slot = PAIR * ((x_pos + n_x - step) % n_x) + core
        return wo_copy(wo_buf.at[slot], slot, n_x + step, sibling)

    def run_wo_passes():
        for step in range(1, n_x):
            wo_send(step).wait_recv()
            wo_pass(step).start()

    keep = wgx_hbm.shape[0]
    swaps = [pltpu.make_async_remote_copy(src.at[pl.ds((1 - core) * keep, keep)], dst, sw_sem.at[i], rw_sem.at[i],
                                          device_id=mesh_id(cp_pos, PAIR * x_pos + 1 - core), device_id_type=MESH)
             for i, (src, dst) in enumerate(((wg_hbm, wgx_hbm), (wu_hbm, wux_hbm), (wd_hbm, wdx_hbm)))]
    ranks = []
    for slot, off in ((1, 1), (PAIR, -1), (3, PAIR)):
        for part, place in enumerate((((cp_pos + off + n_cp) % n_cp, tp_pos), (cp_pos, PAIR * ((x_pos + off + n_x) % n_x) + core))):
            ranks.append(pltpu.make_async_remote_copy(rank_hbm, near_hbm.at[part, slot], sr_sem.at[part, slot], rr_sem.at[part, slot],
                                                      device_id=mesh_id(*place), device_id_type=MESH))
    for step in range(n_x):
        wo_send(step).start()
    for one in swaps + ranks:
        one.start()
    for one in loads[:3]:
        one.wait()

    def columns(block):
        return pl.ds(pl.multiple_of(block * tok_dev, tok_dev), tok_dev)

    def scores(block, cols, s_ref, masked):
        s_vals = jnp.dot(k_buf[columns(block), :], qt_buf[:, cols], preferred_element_type=jnp.float32)
        if masked:
            key_id = lax.broadcasted_iota(jnp.int32, s_vals.shape, 0)
            query_id = lax.broadcasted_iota(jnp.int32, s_vals.shape, 1)
            s_vals = jnp.where(key_id <= query_id, s_vals, -1e30)
        s_ref[...] = s_vals
        return jnp.max(s_vals, **COLUMN_WISE)

    def soften(s_ref, s_top, cols, p_ref, shrink_ref):
        m_old = m_ref[:, cols]
        m_new = jnp.maximum(m_old, s_top)
        shrink = jnp.exp2((m_old - m_new) * scale)
        m_ref[:, cols] = m_new
        shrink_ref[...] = shrink
        prob = jnp.exp2((s_ref[...] - m_new) * scale)
        l_ref[:, cols] = l_ref[:, cols] * shrink + jnp.sum(prob, **COLUMN_WISE)
        p_ref[...] = prob.astype(jnp.bfloat16)

    def gather_values(block, cols, p_ref, shrink_ref):
        acc[:, cols] = acc[:, cols] * shrink_ref[...] + jnp.dot(vt_buf[:, columns(block)], p_ref[...], preferred_element_type=jnp.float32)

    def query_pair(turn, carry):
        g = (turn + 1 + cp_pos + x_pos // PAIR * (PAIR * n_cp - 1 - PAIR * cp_pos)) % (n_dev // 4)

        @pl.when(turn == n_dev // 4 - 2)
        def _():
            run_wo_passes()
        q_rows = q_buf[pl.ds(pl.multiple_of(g * PAIR * tok_dev, PAIR * tok_dev), PAIR * tok_dev), :]
        qt_buf[...] = q_rows.astype(jnp.float32).T.astype(jnp.bfloat16)
        m_ref[...] = jnp.full_like(m_ref, -1e30)
        l_ref[...] = jnp.zeros_like(l_ref)
        acc[...] = jnp.zeros_like(acc)
        p_odd[...] = jnp.zeros_like(p_odd)
        shrink_odd[...] = jnp.ones_like(shrink_odd)
        near = ((0, core), (1, 3 - core), (1 - core, 0), (1, 1 - core), (1, 2 - core))
        lanes = [(s_even, p_even, shrink_even, 0), (s_even, p_even, shrink_even, 1), (s_odd, p_near, shrink_odd, 0), (s_odd, p_near, shrink_odd, 1)]
        tops = {}

        def near_refs(i):
            s_ref, p_ref, shrink_ref, place = lanes[i % 4]
            cols = pl.ds(place * tok_dev, tok_dev)
            return s_ref.at[:, cols], p_ref.at[:, cols], shrink_ref.at[:, cols]

        def near_scores(i):
            r, block = near[i]
            tops[i] = scores(4 * g + block, columns(r), near_refs(i)[0], i < 2)

        def near_soften(i):
            s_ref, p_ref, shrink_ref = near_refs(i)
            soften(s_ref, tops[i], columns(near[i][0]), p_ref, shrink_ref)

        def near_values(i):
            _, p_ref, shrink_ref = near_refs(i)
            gather_values(4 * g + near[i][1], columns(near[i][0]), p_ref, shrink_ref)

        for i in range(len(near) + 2):
            if i < len(near):
                near_scores(i)
            if 0 <= i - 1 < len(near):
                near_soften(i - 1)
            if 0 <= i - 2:
                near_values(i - 2)
        shrink_odd[...] = jnp.ones_like(shrink_odd)
        strip = min(256, tok_dev)
        strips = [pl.ds(lo, strip) for lo in range(0, PAIR * tok_dev, strip)]

        def far_step(block, parity, tops):
            s_in, s_out = (s_even, s_odd)[::1 - PAIR * parity]
            p_out, p_in = (p_even, p_odd)[::1 - PAIR * parity]
            shrink_out, shrink_in = (shrink_even, shrink_odd)[::1 - PAIR * parity]
            next_tops = []
            for cols, top in zip(strips, tops):
                next_tops.append(scores(block + 1, cols, s_out.at[:, cols], False))
                soften(s_in.at[:, cols], top, cols, p_out.at[:, cols], shrink_out.at[:, cols])
                gather_values(jnp.maximum(block - 1, 0), cols, p_in.at[:, cols], shrink_in.at[:, cols])
            return next_tops

        def far_blocks(n, tops):
            for j in range(4):
                tops = far_step(4 * n + j, j % PAIR, tops)
            return tops

        lax.fori_loop(0, g, far_blocks, [scores(0, cols, s_even.at[:, cols], False) for cols in strips])
        for cols in strips:
            gather_values(jnp.maximum(4 * g - 1, 0), cols, p_odd.at[:, cols], shrink_odd.at[:, cols])
        out = (acc[...] / l_ref[...]).T.astype(jnp.bfloat16)
        for r in BOTH:
            o_st[PAIR * g + r] = out[r * tok_dev:(r + 1) * tok_dev]
            o_push(PAIR * g + r, "start")
        return carry

    def o_push(index, what):
        block = 4 * (index // PAIR) + (1 - core) * 3 * (index % PAIR) + core * (1 + index % PAIR)
        to_cp, to_tp = owner_of(block, n_cp, n_tp)
        here = and_(to_cp == cp_pos, to_tp == tp_pos)
        if what == "start":
            @pl.when(here)
            def _():
                pltpu.make_async_copy(o_st.at[index], o_hbm.at[head], ro_sem.at[head]).start()

        @pl.when(not_(here))
        def _():
            copy = pltpu.make_async_remote_copy(o_st.at[index], o_hbm.at[head], so_sem.at[index], ro_sem.at[head],
                                                device_id=mesh_id(to_cp, to_tp), device_id_type=MESH)
            if what == "start":
                copy.start()
            else:
                copy.wait_send()

    lax.fori_loop(0, n_dev // 4, query_pair, 0)

    wo_send(0).wait_recv()
    for step in range(1, n_x):
        wo_pass(step).wait_recv()
    for one in loads[3:]:
        one.wait()
    for j in range(n_heads):
        pltpu.make_async_copy(o_hbm.at[j], o_hbm.at[j], ro_sem.at[j]).wait()
    o_load = pltpu.make_async_copy(o_hbm, o_buf, o_sem)
    o_load.start()
    o_load.wait()
    o_rows = jnp.concatenate([o_buf[j] for j in range(n_heads)], axis=1)
    n_cols = min(512, hid // PAIR)

    for col in range(0, hid, n_cols):
        cols = pl.ds(col, n_cols)
        w_cols = wo_buf[:, :, cols].reshape(n_heads * head_dim, n_cols)
        h_cols = (x_buf[:, cols].astype(jnp.float32) + jnp.dot(o_rows, w_cols, preferred_element_type=jnp.float32)).astype(jnp.bfloat16)
        h_ref[PAIR * col // hid, :, pl.ds(col % (hid // PAIR), n_cols)] = h_cols

    for step in range(n_x):
        wo_send(step).wait_send()
    for step in range(1, n_x):
        wo_pass(step).wait_send()
    for one in swaps + ranks:
        one.wait()

    def drain(index, carry):
        o_push(index, "wait")
        return carry

    lax.fori_loop(0, n_dev // PAIR, drain, 0)


def attend_call(n_cp, n_tp, k_all, vt_all, q_all, x_loc, wo_loc, w_gate, w_up, w_down, rank_rows):
    n_dev = n_cp * n_tp
    tok_dev, hid = x_loc.shape
    seq, head_dim = k_all.shape
    n_heads = n_tp * wo_loc.shape[0] // head_dim
    keep = w_gate.shape[0] // PAIR
    any_spec = pl.BlockSpec(memory_space=pl.ANY)
    bf16 = jnp.bfloat16
    h_loc, _, wg_other, wu_other, wd_other, near_rows = pl.pallas_call(
        functools.partial(attend_kernel, n_cp, n_tp),
        name="attend_heads",
        out_shape=(jax.ShapeDtypeStruct((PAIR, tok_dev, hid // PAIR), bf16), jax.ShapeDtypeStruct((n_heads, tok_dev, head_dim), bf16))
        + tuple(jax.ShapeDtypeStruct((keep,) + w.shape[1:], bf16) for w in (w_gate, w_up, w_down))
        + (jax.ShapeDtypeStruct((PAIR, 4) + rank_rows.shape, jnp.float32),),
        in_specs=[any_spec] * 9,
        out_specs=(pl.BlockSpec(memory_space=pltpu.VMEM),) + (any_spec,) * 5,
        scratch_shapes=[
            pltpu.VMEM((seq, head_dim), bf16),
            pltpu.VMEM((head_dim, seq), bf16),
            pltpu.VMEM((seq // PAIR, head_dim), bf16),
            pltpu.VMEM((head_dim, PAIR * tok_dev), bf16),
            pltpu.VMEM((n_dev // PAIR, tok_dev, head_dim), bf16),
            pltpu.VMEM((n_heads, tok_dev, head_dim), bf16),
            pltpu.VMEM((n_tp,) + wo_loc.shape, bf16),
            pltpu.VMEM((tok_dev, hid), bf16),
            pltpu.VMEM((tok_dev, PAIR * tok_dev), jnp.float32),
            pltpu.VMEM((tok_dev, PAIR * tok_dev), jnp.float32),
            pltpu.VMEM((tok_dev, PAIR * tok_dev), bf16),
            pltpu.VMEM((tok_dev, PAIR * tok_dev), bf16),
            pltpu.VMEM((tok_dev, PAIR * tok_dev), bf16),
            pltpu.VMEM((1, PAIR * tok_dev), jnp.float32),
            pltpu.VMEM((1, PAIR * tok_dev), jnp.float32),
            pltpu.VMEM((head_dim, PAIR * tok_dev), jnp.float32),
            pltpu.VMEM((1, PAIR * tok_dev), jnp.float32),
            pltpu.VMEM((1, PAIR * tok_dev), jnp.float32),
            dma((5,)),
            dma((n_dev // PAIR,)),
            dma((n_heads,)),
            dma((n_tp,)),
            dma((n_tp,)),
            dma((3,)),
            dma((3,)),
            dma((PAIR, 4)),
            dma((PAIR, 4)),
            dma,
        ],
        compiler_params=pltpu.CompilerParams(collective_id=1, has_side_effects=True, vmem_limit_bytes=VMEM_LIMIT),
        cost_estimate=pl.CostEstimate(flops=PAIR * seq * seq * head_dim // PAIR, bytes_accessed=2**26, transcendentals=seq * seq // 4),
    )(k_all, vt_all, q_all, x_loc, wo_loc, w_gate, w_up, w_down, rank_rows)
    return h_loc, near_rows, wg_other, wu_other, wd_other


def solution(mesh):
    n_cp = mesh.shape["cp"]
    n_tp = mesh.shape["tp"]
    row_spec = P(("dp", "cp", "tp"), None)
    head_spec = P(None, "tp", None)
    expert_spec = P(("cp", "tp"), None, None)

    def device_step(x_loc, w_q, w_k, w_v, w_o, ids_loc, gates_loc, w_gate, w_up, w_down):
        tok_dev, hid_dim = x_loc.shape
        n_loc, head_dim = w_q.shape[1:]
        n_experts = w_gate.shape[0] * n_cp * n_tp // PAIR
        capacity = ids_loc.shape[1] * tok_dev // n_experts
        k_all, vt_all, q_all, rank_rows, gate_rows = front_call(n_cp, n_tp, x_loc, (w_q, w_k, w_v), ids_loc.T, gates_loc.T, n_experts)
        h_loc, near_rows, *others = attend_call(n_cp, n_tp, k_all, vt_all, q_all, x_loc, w_o.reshape(n_loc * head_dim, hid_dim), w_gate, w_up, w_down, rank_rows)
        return moe_call(n_cp, n_tp, capacity, h_loc, rank_rows, near_rows, gate_rows, w_gate, w_up, w_down, *others)

    return jax.shard_map(device_step, mesh=mesh, in_specs=(row_spec, head_spec, head_spec, head_spec, P("tp", None, None), row_spec, row_spec, expert_spec, expert_spec, expert_spec), out_specs=row_spec, check_vma=False)
```

```python
import functools

import jax
import jax.numpy as jnp
from jax import lax
from jax.experimental import pallas as pl
from jax.experimental.pallas import tpu as pltpu
from jax.sharding import PartitionSpec as P

MESH = pl.DeviceIdType.MESH
PAIR = 2
BOTH = range(PAIR)
ROWS_ROWS = (((0,), (0,)), ((), ()))
COLUMN_WISE = {"axis": 0, "keepdims": True}
dma = pltpu.SemaphoreType.DMA
and_, or_, not_ = jnp.logical_and, jnp.logical_or, jnp.logical_not
VMEM_LIMIT = 66_000_000
PLACES = ((0, 0), (0, 1), (1, 0), (0, -1), (-1, 0), (1, 1), (-1, -1), (1, -1), (-1, 1), (0, PAIR), (PAIR, 0), (1, PAIR), (PAIR, 1), (-1, PAIR), (PAIR, -1), (PAIR, PAIR))
N_NEAR, FIRST_FAR = 5, 9
GROUPS = ("1234", "9a9a", "5656", "bcbc", "1234", "dede", "7878", "0f0f")
FLIPS = ("0000", "0011", "0011", "0011", "1111", "0011", "0011", "0011")
SOURCES = (0, -1, 1, PAIR)


def peer_of(step, cp_pos, tp_pos, n_cp, n_tp):
    n_x = n_tp // PAIR
    off_x = (step // PAIR) % n_x
    off_y = (off_x + step // n_tp) % n_cp
    return (cp_pos + off_y) % n_cp, ((tp_pos // PAIR + off_x) % n_x) * 2 + (tp_pos % PAIR + step % PAIR) % PAIR


def mesh_id(cp_pos, tp_pos):
    return {"cp": cp_pos, "tp": tp_pos}


def enter_all(n_cp, n_tp):
    cp_pos, tp_pos = lax.axis_index("cp"), lax.axis_index("tp")

    def signal_peer(step, carry):
        to_cp, to_tp = peer_of(step, cp_pos, tp_pos, n_cp, n_tp)
        pl.semaphore_signal(pltpu.get_barrier_semaphore(), inc=1, device_id=mesh_id(to_cp, to_tp), device_id_type=MESH)
        return carry

    lax.fori_loop(1, n_cp * n_tp, signal_peer, 0)
    pl.semaphore_wait(pltpu.get_barrier_semaphore(), n_cp * n_tp - 1)


def pick(values, index):
    out = values[-1]
    for k, value in enumerate(values[:-1]):
        out = jnp.where(index == k, value, out)
    return out


def moe_kernel(n_cp, n_tp, group, h_hbm, rank_hbm, near_hbm, gate_ref, wg_hbm, wu_hbm, wd_hbm, wgx_hbm, wux_hbm, wdx_hbm,
               y_ref, rx_hbm, rl_hbm, rz_hbm, zl_hbm,
               h_buf, rank_buf, wg_buf, wu_buf, wd_buf, ring, own_stage, z_ring, x_buf, z_buf, acc, parts,
               w_sem, rank_sem, in_sem, x_sem, z_sem, hs_sem, hr_sem, ss_sem, rx_sem, rl_sem, fl_sem, sz_sem, rz_sem, zl_sem, fz_sem):
    n_x = n_tp // PAIR
    tok_dev, half_hid = h_buf.shape[2:]
    hid = PAIR * half_hid
    cap = ring.shape[3] // PAIR
    cp_pos, tp_pos = lax.axis_index("cp"), lax.axis_index("tp")
    x_pos, core = tp_pos // PAIR, tp_pos % PAIR
    half_tok = tok_dev // PAIR

    def at(off_y, off_x, flip):
        return (cp_pos + off_y + n_cp) % n_cp, PAIR * ((x_pos + off_x + n_x) % n_x) + (core + flip) % PAIR

    def line(place):
        return place[0] * n_tp + place[1]

    def send(src, dst, s_sem, r_sem, place):
        return pltpu.make_async_remote_copy(src, dst, s_sem, r_sem, device_id=mesh_id(*place), device_id_type=MESH)

    def await_bytes(ref, sem):
        pltpu.make_async_copy(ref, ref, sem).wait()

    h_loads = [pltpu.make_async_copy(h_hbm.at[part], h_buf.at[part, 0], in_sem.at[part]) for part in BOTH]
    rank_loads = []
    for part in BOTH:
        rank_loads.append(pltpu.make_async_copy(rank_hbm, rank_buf.at[part, 0], rank_sem.at[PAIR * part]))
        rank_loads.append(pltpu.make_async_copy(near_hbm.at[part, pl.ds(1, 3)], rank_buf.at[part, pl.ds(1, 3)], rank_sem.at[PAIR * part + 1]))
    w_loads = []
    for slot, (own, other, buf) in enumerate(((wg_hbm, wgx_hbm, wg_buf), (wu_hbm, wux_hbm, wu_buf), (wd_hbm, wdx_hbm, wd_buf))):
        w_loads.append(pltpu.make_async_copy(own.at[pl.ds(PAIR * core, PAIR)], buf.at[0], w_sem.at[PAIR * slot]))
        w_loads.append(pltpu.make_async_copy(other, buf.at[1], w_sem.at[PAIR * slot + 1]))
    for one in h_loads + rank_loads:
        one.start()
    enter_all(n_cp, n_tp)

    def along(part, off):
        return at(off, 0, 0) if part == 0 else at(0, off, 0)

    def across(part, off, flip):
        return at(0, off, flip) if part == 0 else at(off, 0, flip)

    def rows_of(piece):
        return pl.ds(piece * half_tok, half_tok)

    def spread(part, i):
        piece, off, slot = ((0, 1, 1), (1, -1, PAIR), (1, 1, 1), (0, -1, PAIR), (0, 1, 3), (1, -1, 3))[i]
        rows = rows_of(piece)
        src = h_hbm.at[part, rows] if i < 4 else h_buf.at[part, 1 if i == 4 else 2, rows]
        return send(src, h_buf.at[part, slot, rows], hs_sem.at[part, i], hr_sem.at[part, slot, piece], along(part, off))

    def await_h(part, slot, piece):
        await_bytes(h_buf.at[part, slot, rows_of(piece)], hr_sem.at[part, slot, piece])

    for i in range(4):
        for part in BOTH:
            spread(part, i).start()
    for one in w_loads:
        one.start()
    for one in h_loads + rank_loads:
        one.wait()

    slots = lax.broadcasted_iota(jnp.int32, (cap, tok_dev), 0).astype(jnp.float32)

    def gather_rows(part, stage, m):
        turn = m // PAIR
        off = turn + (turn // PAIR) * (5 - PAIR * turn)
        first = PAIR * line(across(part, off, m % PAIR))
        chosen = [jnp.where(rank_buf[part, stage, pl.ds(first + i, 1), :] == slots, 1.0, 0.0) for i in BOTH]
        chosen = jnp.concatenate(chosen, axis=0).astype(jnp.bfloat16)
        return jnp.dot(chosen, h_buf[part, stage], preferred_element_type=jnp.float32).astype(jnp.bfloat16)

    def source_line(part, stage, off):
        a = SOURCES[stage]
        return line(at(a, off, 0) if part == 0 else at(off, a, 0))

    def await_ring(part, stage):
        def one(m, carry):
            await_bytes(ring.at[part, stage % PAIR, m], ss_sem.at[part, stage % PAIR, m])
            return carry
        lax.fori_loop(1, 8, one, 0)

    def own_copy(part, stage):
        src_line = source_line(part, stage, 0)
        return pltpu.make_async_copy(own_stage.at[part, stage], rx_hbm.at[part, src_line], rx_sem.at[part, src_line])

    def run_stage(stage):
        side = stage % PAIR
        for part in BOTH:
            if stage >= 2:
                await_ring(part, stage)
            own_stage[part, stage] = gather_rows(part, stage, 0)

            def fill(m, carry):
                ring[part, side, m] = gather_rows(part, stage, m)
                return carry

            lax.fori_loop(1, 8, fill, 0)
        lines = [source_line(part, stage, 0) for part in BOTH]
        for flip in BOTH:
            for way, off in enumerate((1, -1)):
                for part in BOTH:
                    m = 6 + flip
                    send(ring.at[part, side, m, pl.ds(way * cap, cap)], rl_hbm.at[part, way, stage, flip], ss_sem.at[part, side, m],
                         rl_sem.at[part, way, stage, flip], across(part, off, 0)).start()
        for m, off in ((PAIR, 1), (4, -1), (3, 1), (5, -1), (1, 0)):
            for part in BOTH:
                send(ring.at[part, side, m], rx_hbm.at[part, lines[part]], ss_sem.at[part, side, m], rx_sem.at[part, lines[part]],
                     across(part, off, m % PAIR)).start()
        for part in BOTH:
            own_copy(part, stage).start()

    def relay(part, stage, way, flip):
        off = 1 - PAIR * way
        src_line = source_line(part, stage, -off)
        return send(rl_hbm.at[part, way, stage, flip], rx_hbm.at[part, src_line, pl.ds(way * cap, cap)], fl_sem.at[part, way, stage, flip],
                    rx_sem.at[part, src_line], across(part, off, flip))

    def run_relays(stage):
        for flip in BOTH:
            for way in BOTH:
                for part in BOTH:
                    await_bytes(rl_hbm.at[part, way, stage, flip], rl_sem.at[part, way, stage, flip])
                    relay(part, stage, way, flip).start()

    run_stage(0)
    for part in BOTH:
        await_h(part, 1, 0)
        spread(part, 4).start()
    for part in BOTH:
        await_h(part, PAIR, 1)
        spread(part, 5).start()
    for part in BOTH:
        await_h(part, 1, 1)
    run_stage(1)
    gate_all = gate_ref[...]
    high = gate_all.astype(jnp.bfloat16).astype(jnp.float32)
    rest = gate_all - high
    mid = rest.astype(jnp.bfloat16).astype(jnp.float32)
    parts[0] = high
    parts[1] = mid
    parts[2] = rest - mid
    for part in BOTH:
        acc[:, part * half_hid:(part + 1) * half_hid] = h_buf[part, 0].astype(jnp.float32)
    run_relays(0)
    for part in BOTH:
        await_h(part, PAIR, 0)
    run_stage(2)
    run_relays(1)
    for part in BOTH:
        await_h(part, 3, 0)
        await_h(part, 3, 1)
    run_stage(3)
    run_relays(2)
    for one in w_loads:
        one.wait()

    rows = group * cap
    n_cols = min(512, hid)

    def expert_rows(slot, i):
        x_rows = x_buf[:, pl.ds(i * cap, cap), :].reshape(rows, hid)
        hidden = []
        for half in BOTH:
            gate_pre = jnp.dot(x_rows, wg_buf[half, i], preferred_element_type=jnp.float32)
            up_pre = jnp.dot(x_rows, wu_buf[half, i], preferred_element_type=jnp.float32)
            hidden.append((gate_pre * (1.0 / (1.0 + jnp.exp(-gate_pre))) * up_pre).astype(jnp.bfloat16))
        for col in range(0, hid, n_cols):
            z_rows = (jnp.dot(hidden[0], wd_buf[0, i, :, pl.ds(col, n_cols)], preferred_element_type=jnp.float32)
                      + jnp.dot(hidden[1], wd_buf[1, i, :, pl.ds(col, n_cols)], preferred_element_type=jnp.float32))
            z_ring[slot, :, pl.ds(i * cap, cap), pl.ds(col, n_cols)] = z_rows.astype(jnp.bfloat16).reshape(group, cap, n_cols)

    def place_at(g, q):
        places = [int(names[q], 16) for names in GROUPS]
        off_y, off_x = (pick([PLACES[p][k] for p in places], g) for k in BOTH)
        return off_y, off_x, pick([int(flips[q]) for flips in FLIPS], g), pick(places, g)

    my_line = line((cp_pos, tp_pos))

    def await_slot(slot):
        for q in range(group):
            await_bytes(z_ring.at[slot, q], sz_sem.at[slot, q])

    def expert_group(g, carry):
        slot = g % 3

        @pl.when(g == 2)
        def _():
            run_relays(3)

        sources = [line(at(*place_at(g, q)[:3])) for q in range(group)]
        loads = []
        for q in range(group):
            for part in BOTH:
                await_bytes(rx_hbm.at[part, sources[q]], rx_sem.at[part, sources[q]])
                loads.append(pltpu.make_async_copy(rx_hbm.at[part, sources[q]], x_buf.at[q, :, pl.ds(part * half_hid, half_hid)], x_sem.at[part, q]))
                loads[-1].start()

        @pl.when(g >= 3)
        def _():
            await_slot(slot)
        for one in loads:
            one.wait()
        for i in BOTH:
            expert_rows(slot, i)
        for q in range(group):
            off_y, off_x, flip, p = place_at(g, q)
            alone = and_(p == 0, flip == 0)

            @pl.when(alone)
            def _():
                pltpu.make_async_copy(z_ring.at[slot, q], rz_hbm.at[my_line], rz_sem.at[my_line]).start()

            @pl.when(and_(p < FIRST_FAR, not_(alone)))
            def _():
                send(z_ring.at[slot, q], rz_hbm.at[my_line], sz_sem.at[slot, q], rz_sem.at[my_line], at(off_y, off_x, flip)).start()

            @pl.when(p >= FIRST_FAR)
            def _():
                lead_y, lead_x = jnp.where(off_y == 2, 1, 0), jnp.where(off_x == 2, 1, 0)
                for way in BOTH:
                    sign = 1 - PAIR * way
                    send(z_ring.at[slot, q, pl.ds(way * cap, cap)], zl_hbm.at[p - FIRST_FAR, flip, way], sz_sem.at[slot, q],
                         zl_sem.at[p - FIRST_FAR, flip, way], at(sign * lead_y, sign * lead_x, 0)).start()
        return carry

    lax.fori_loop(0, len(GROUPS), expert_group, 0)

    n_far = len(PLACES) - FIRST_FAR

    def z_relay(index, flip, way):
        off_y, off_x = PLACES[FIRST_FAR + index]
        sign = 1 - PAIR * way
        lead_y, lead_x = sign * (off_y == 2), sign * (off_x == 2)
        from_line = line(at(-lead_y, -lead_x, 0))
        to_y = sign if off_y == 2 else off_y
        to_x = sign if off_x == 2 else off_x
        return send(zl_hbm.at[index, flip, way], rz_hbm.at[from_line, pl.ds(way * cap, cap)], fz_sem.at[index, flip, way],
                    rz_sem.at[from_line], at(to_y, to_x, flip))

    def each_relay(*indices):
        return [(index, flip, way) for flip in BOTH for way in BOTH for index in indices]

    def run_z_relays(*indices):
        for key in each_relay(*indices):
            await_bytes(zl_hbm.at[key], zl_sem.at[key])
            z_relay(*key).start()

    def combine(p, carry):
        off_y, off_x = pick([a for a, _ in PLACES], p), pick([b for _, b in PLACES], p)
        homes = [line(at(-off_y, -off_x, q)) for q in BOTH]
        loads = []
        for q in BOTH:
            await_bytes(rz_hbm.at[homes[q]], rz_sem.at[homes[q]])
            loads.append(pltpu.make_async_copy(rz_hbm.at[homes[q]], z_buf.at[q], z_sem.at[q]))
            loads[-1].start()
        weights = [[], [], []]
        for q in BOTH:
            for i in BOTH:
                row = pl.ds(PAIR * homes[q] + i, 1)
                chosen = rank_buf[0, 0, row, :] == slots
                for part in range(3):
                    weights[part].append(jnp.where(chosen, parts[part, row, :], 0.0))
        weights = [jnp.concatenate(w, axis=0).astype(jnp.bfloat16) for w in weights]
        for one in loads:
            one.wait()
        for col in range(0, hid, n_cols):
            z_rows = z_buf[:, :, pl.ds(col, n_cols)].reshape(4 * cap, n_cols)
            total = None
            for part in range(3):
                term = lax.dot_general(weights[part], z_rows, ROWS_ROWS, preferred_element_type=jnp.float32)
                total = term if total is None else total + term
            acc[:, pl.ds(col, n_cols)] += total
        return carry

    run_z_relays(0, 1)
    run_z_relays(PAIR, 3)
    lax.fori_loop(0, N_NEAR, combine, 0)
    run_z_relays(4, 5)
    run_z_relays(6)
    lax.fori_loop(N_NEAR, len(PLACES), combine, 0)
    y_ref[...] = acc[...].astype(jnp.bfloat16)

    for part in BOTH:
        for i in range(6):
            spread(part, i).wait_send()
        for stage in (PAIR, 3):
            await_ring(part, stage)
        for stage in range(4):
            for way in BOTH:
                for flip in BOTH:
                    relay(part, stage, way, flip).wait_send()
    last = len(GROUPS) - 3
    for g in range(last, len(GROUPS)):
        for q in range(group):
            if GROUPS[g][q] + FLIPS[g][q] != "00":
                await_bytes(z_ring.at[g % 3, q], sz_sem.at[g % 3, q])
    for key in each_relay(*range(n_far)):
        z_relay(*key).wait_send()


def moe_call(n_cp, n_tp, cap, h_loc, rank_rows, near_rows, gate_rows, w_gate, w_up, w_down, wg_other, wu_other, wd_other):
    n_dev = n_cp * n_tp
    _, tok_dev, half_hid = h_loc.shape
    hid = PAIR * half_hid
    half_f = w_gate.shape[2]
    n_experts = rank_rows.shape[0]
    group = len(GROUPS[0])
    n_far = len(PLACES) - FIRST_FAR
    bf16 = jnp.bfloat16
    any_spec = pl.BlockSpec(memory_space=pl.ANY)
    vmem_spec = pl.BlockSpec(memory_space=pltpu.VMEM)
    flops = PAIR * n_dev * PAIR * cap * hid * PAIR * half_f * 3
    return pl.pallas_call(
        functools.partial(moe_kernel, n_cp, n_tp, group),
        name="routed_experts",
        out_shape=(jax.ShapeDtypeStruct((tok_dev, hid), bf16), jax.ShapeDtypeStruct((PAIR, n_dev, PAIR * cap, half_hid), bf16),
                   jax.ShapeDtypeStruct((PAIR, PAIR, 4, PAIR, cap, half_hid), bf16), jax.ShapeDtypeStruct((n_dev, PAIR * cap, hid), bf16),
                   jax.ShapeDtypeStruct((n_far, PAIR, 2, cap, hid), bf16)),
        in_specs=[any_spec, any_spec, any_spec, vmem_spec] + [any_spec] * 6,
        out_specs=(vmem_spec,) + (any_spec,) * 4,
        scratch_shapes=[
            pltpu.VMEM((PAIR, 4, tok_dev, half_hid), bf16),
            pltpu.VMEM((PAIR, 4, n_experts, tok_dev), jnp.float32),
            pltpu.VMEM((PAIR, PAIR, hid, half_f), bf16),
            pltpu.VMEM((PAIR, PAIR, hid, half_f), bf16),
            pltpu.VMEM((PAIR, PAIR, half_f, hid), bf16),
            pltpu.VMEM((PAIR, PAIR, 8, PAIR * cap, half_hid), bf16),
            pltpu.VMEM((PAIR, 4, PAIR * cap, half_hid), bf16),
            pltpu.VMEM((3, group, PAIR * cap, hid), bf16),
            pltpu.VMEM((group, PAIR * cap, hid), bf16),
            pltpu.VMEM((PAIR, PAIR * cap, hid), bf16),
            pltpu.VMEM((tok_dev, hid), jnp.float32),
            pltpu.VMEM((3, n_experts, tok_dev), jnp.float32),
            dma((6,)), dma((4,)), dma((PAIR,)), dma((PAIR, group)), dma((PAIR,)),
            dma((PAIR, 6)), dma((PAIR, 4, PAIR)), dma((PAIR, PAIR, 8)), dma((PAIR, n_dev)), dma((PAIR, PAIR, 4, PAIR)), dma((PAIR, PAIR, 4, PAIR)),
            dma((3, group)), dma((n_dev,)), dma((n_far, PAIR, PAIR)), dma((n_far, PAIR, PAIR)),
        ],
        compiler_params=pltpu.CompilerParams(collective_id=2, has_side_effects=True, vmem_limit_bytes=VMEM_LIMIT),
        cost_estimate=pl.CostEstimate(flops=flops, bytes_accessed=2**27, transcendentals=0),
    )(h_loc, rank_rows, near_rows, gate_rows, w_gate, w_up, w_down, wg_other, wu_other, wd_other)[0]


def routing_rows(ids_ref, gates_ref, rank_ref, gate_ref):
    top_k, tok_dev = ids_ref.shape
    ids, gates = ids_ref[...].astype(jnp.float32), gates_ref[...]
    expert = lax.broadcasted_iota(jnp.int32, rank_ref.shape, 0).astype(jnp.float32)
    chosen, weight = jnp.zeros_like(expert), jnp.zeros_like(expert)
    for k in range(top_k):
        hit = ids[k:k + 1] == expert
        chosen = jnp.where(hit, 1.0, chosen)
        weight = jnp.where(hit, gates[k:k + 1], weight)
    token = lax.broadcasted_iota(jnp.int32, (tok_dev, tok_dev), 0)
    before = jnp.where(token < lax.broadcasted_iota(jnp.int32, (tok_dev, tok_dev), 1), 1.0, 0.0).astype(jnp.bfloat16)
    rank = jnp.dot(chosen.astype(jnp.bfloat16), before, preferred_element_type=jnp.float32)
    rank_ref[...] = jnp.where(chosen > 0.0, rank, -1.0)
    gate_ref[...] = weight


def block_of(cp_pos, tp_pos, n_cp, n_tp):
    per_chunk = n_tp // PAIR
    late = tp_pos // per_chunk
    chunk = late * (PAIR * n_cp - 1 - cp_pos) + (1 - late) * cp_pos
    return chunk * per_chunk + tp_pos % per_chunk


def owner_of(block, n_cp, n_tp):
    per_chunk = n_tp // PAIR
    chunk = block // per_chunk
    late = chunk // n_cp
    return late * (PAIR * n_cp - 1 - chunk) + (1 - late) * chunk, late * per_chunk + block % per_chunk


def front_kernel(n_cp, n_tp, n_part, x_hbm, wq_hbm, wk_hbm, wv_hbm, ids_ref, gates_ref, k_hbm, vt_hbm, q_hbm, rank_ref, gate_ref,
                 x_buf, w_raw, w_buf, q_st, k_st, vt_st, k_far, vt_far, q_far,
                 own_sem, w_sem, ring_sem, pair_sem, rx_sem, sk_sem, sv_sem, sq_sem, kv_sem, rq_sem, sf_sem, rf_sem, far_sem, pass_sem):
    n_x = n_tp // PAIR
    tok_dev, hid = x_hbm.shape
    half = tok_dev // n_part
    head_dim = k_hbm.shape[1]
    n_loc = q_st.shape[1]
    chunk_len = tok_dev * n_x
    cp_pos, tp_pos = lax.axis_index("cp"), lax.axis_index("tp")
    x_pos, core = tp_pos // PAIR, tp_pos % PAIR
    sibling = PAIR * x_pos + 1 - core
    barrier = pltpu.get_barrier_semaphore()

    def slot_at(off, flip):
        return PAIR * ((x_pos + off + n_x) % n_x) + (core + flip) % PAIR

    own_copy = pltpu.make_async_copy(x_hbm, x_buf.at[tp_pos], own_sem)
    own_copy.start()
    width = n_loc * head_dim
    w_loads = [pltpu.make_async_copy(w, w_raw.at[i], w_sem.at[i]) for i, w in enumerate((wq_hbm, wk_hbm, wv_hbm))]
    for one in w_loads:
        one.start()
    for step in (1, n_x - 1):
        pl.semaphore_signal(barrier, inc=1, device_id=mesh_id(cp_pos, slot_at(step, 0)), device_id_type=MESH)
    for step in range(1, PAIR * n_cp):
        pl.semaphore_signal(barrier, inc=1, device_id=mesh_id((cp_pos + step // PAIR) % n_cp, PAIR * x_pos + (core + step) % PAIR), device_id_type=MESH)
    pl.semaphore_wait(barrier, PAIR * n_cp + 1)

    def own_send(part, to_tp, sem):
        rows = pl.ds(pl.multiple_of(part * half, half), half)
        return pltpu.make_async_remote_copy(x_hbm.at[rows], x_buf.at[tp_pos, rows], sem, rx_sem.at[tp_pos, part],
                                            device_id=mesh_id(cp_pos, to_tp), device_id_type=MESH)

    def pass_on(slot, part, to_tp, sem):
        rows = pl.ds(pl.multiple_of(part * half, half), half)
        return pltpu.make_async_remote_copy(x_buf.at[slot, rows], x_buf.at[slot, rows], sem, rx_sem.at[slot, part],
                                            device_id=mesh_id(cp_pos, to_tp), device_id_type=MESH)

    def ring_send(i, side):
        part = i if side == 0 else n_part - 1 - i
        return own_send(part, slot_at(1 - PAIR * side, 0), ring_sem.at[side, i])

    for i in BOTH:
        for side in BOTH:
            ring_send(i, side).start()
    for part in range(n_part):
        own_send(part, sibling, pair_sem.at[part]).start()
    first = PAIR * n_part
    for one in w_loads:
        one.wait()
    rows_once = min(256, hid)

    def widen(r, carry):
        rows = pl.ds(pl.multiple_of(r * rows_once, rows_once), rows_once)
        for i in range(len(w_loads)):
            w_buf[rows, pl.ds(i * width, width)] = w_raw[i, rows].reshape(rows_once, width)
        return carry

    lax.fori_loop(0, hid // rows_once, widen, 0)
    routing_rows(ids_ref, gates_ref, rank_ref, gate_ref)

    def place_of(step):
        late = jnp.minimum(step // first, 1)
        wave, other, side = jnp.maximum(step - first, 0) // 4, late * ((step // PAIR) % PAIR) + (1 - late) * (step // n_part), step % PAIR
        piece = pick((0, 1, 0, PAIR, 1, 3), wave)
        through = jnp.where(or_(wave == 2, wave == 4), 1, 0)
        part = late * (piece + side * (n_part - 1 - PAIR * piece)) + (1 - late) * (step % n_part)
        off = late * ((1 - through) * (PAIR * side - 1) + PAIR * through)
        return slot_at(off, other), part, off

    def targets(from_cp, slot, part):
        block = block_of(from_cp, slot, n_cp, n_tp)
        pos = pl.multiple_of(block * tok_dev + part * half, half)
        q_core = ((block % 4 + 1) // PAIR) % PAIR
        q_pos = pl.multiple_of((PAIR * (block // 4) + (block % 4) // PAIR) * tok_dev + part * half, half)
        return ((k_hbm.at[pl.ds(pos, half)], 0, kv_sem.at[from_cp]), (vt_hbm.at[:, pl.ds(pos, half)], 1, kv_sem.at[from_cp]),
                (q_hbm.at[pl.ds(q_pos, half)], q_core, rq_sem.at[from_cp]))

    def remote(src, dst, s_sem, r_sem, to_cp, to_core):
        return pltpu.make_async_remote_copy(src, dst, s_sem, r_sem, device_id=mesh_id((to_cp + n_cp) % n_cp, PAIR * x_pos + to_core), device_id_type=MESH)

    far_refs = (k_far, vt_far, q_far)

    def outputs_of(step):
        slot, part, _ = place_of(step)
        for i in range(n_loc):
            to_cp = n_loc * core + i
            far = (to_cp - cp_pos + n_cp) % n_cp == n_cp // PAIR
            for kind, (src, (dst, to_core, r_sem)) in enumerate(zip((k_st.at[step, i], vt_st.at[step, i], q_st.at[step, i]), targets(cp_pos, slot, part))):
                s_sem = (sk_sem.at[i], sv_sem.at[i], sq_sem.at[i, to_core])[kind]
                here = and_(to_cp == cp_pos, to_core == core)

                @pl.when(here)
                def _():
                    pltpu.make_async_copy(src, dst, r_sem).start()

                @pl.when(far)
                def _():
                    remote(src, far_refs[kind].at[part, slot], s_sem, far_sem.at[kind, part, slot], cp_pos + 1 - part // PAIR * 2, core).start()

                @pl.when(not_(or_(here, far)))
                def _():
                    remote(src, dst, s_sem, r_sem, to_cp, to_core).start()

    def pass_far(step, what):
        slot, part, _ = place_of(step)
        sign = 1 - part // PAIR * 2

        @pl.when((cp_pos + sign + n_cp) % n_cp // n_loc == core)
        def _():
            for kind, (dst, to_core, r_sem) in enumerate(targets((cp_pos - sign + n_cp) % n_cp, slot, part)):
                src = far_refs[kind].at[part, slot]
                copy = remote(src, dst, pass_sem.at[kind, part, slot], r_sem, cp_pos + sign, to_core)
                if what == "start":
                    pltpu.make_async_copy(src, src, far_sem.at[kind, part, slot]).wait()
                    copy.start()
                else:
                    copy.wait_send()

    def project(step, carry):
        slot, part, off = place_of(step)
        wave, other, side = (step - first) // 4, (step // PAIR) % PAIR, step % PAIR

        @pl.when(step == 0)
        def _():
            own_copy.wait()

        @pl.when(step >= n_part)
        def _():
            pass_on(slot, part, sibling, pair_sem.at[0]).wait_recv()

        @pl.when(and_(step >= first, other == 0))
        def _():
            @pl.when(wave < 2)
            def _():
                pass_on(slot, part, slot_at(-off, 0), ring_sem.at[side, n_part + wave]).start()
                for i in BOTH:
                    @pl.when(side == i)
                    def _():
                        ring_send(2 + wave, i).start()
            pass_on(slot, part, sibling, pair_sem.at[n_part + PAIR * wave + side]).start()

        x_rows = x_buf[slot, pl.ds(pl.multiple_of(part * half, half), half), :]
        qkv = jnp.dot(x_rows, w_buf[...], preferred_element_type=jnp.float32)
        for i in range(n_loc):
            q_st[step, i] = qkv[:, i * head_dim:(i + 1) * head_dim].astype(jnp.bfloat16)
            k_st[step, i] = qkv[:, (n_loc + i) * head_dim:(n_loc + i + 1) * head_dim].astype(jnp.bfloat16)
            vt_st[step, i] = qkv[:, (PAIR * n_loc + i) * head_dim:(PAIR * n_loc + i + 1) * head_dim].T.astype(jnp.bfloat16)

        @pl.when(step > 0)
        def _():
            outputs_of(step - 1)

        @pl.when(step >= lag)
        def _():
            pass_far(step - lag, "start")
        return carry

    n_steps, lag = n_part * n_tp, 8
    lax.fori_loop(0, n_steps, project, 0)
    outputs_of(n_steps - 1)

    def pass_late(step, carry):
        pass_far(step, "start")
        return carry

    lax.fori_loop(n_steps - lag, n_steps, pass_late, 0)

    def whole(ref, count, sem):
        return pltpu.make_async_copy(ref.at[pl.ds(0, count)], ref.at[pl.ds(0, count)], sem)

    def forward(y, place, core_id):
        chunk = y if place == 0 else PAIR * n_cp - 1 - y
        cols = pl.ds(chunk * chunk_len, chunk_len)
        ref = k_hbm.at[cols] if core_id == 0 else vt_hbm.at[:, cols]
        return pltpu.make_async_remote_copy(ref, ref, sf_sem.at[PAIR * y + place], rf_sem.at[PAIR * y + place],
                                            device_id=mesh_id(cp_pos, sibling), device_id_type=MESH)

    for y in range(n_cp):
        whole(k_hbm, PAIR * chunk_len, kv_sem.at[y]).wait()
        for core_id in BOTH:
            @pl.when(core == core_id)
            def _():
                for place in BOTH:
                    forward(y, place, core_id).start()
    for y in range(n_cp):
        whole(q_hbm, chunk_len, rq_sem.at[y]).wait()
    for side in BOTH:
        for i in range(n_part + 2):
            own_send(0, sibling, ring_sem.at[side, i]).wait_send()
    for i in range(n_part * n_x):
        own_send(0, sibling, pair_sem.at[i]).wait_send()
    for i in range(n_loc):
        to_cp = n_loc * core + i
        for sem, to_core, count in ((sk_sem.at[i], 0, PAIR * chunk_len), (sv_sem.at[i], 1, PAIR * chunk_len),
                                    (sq_sem.at[i, 0], 0, chunk_len), (sq_sem.at[i, 1], 1, chunk_len)):
            @pl.when(not_(and_(to_cp == cp_pos, to_core == core)))
            def _():
                whole(k_hbm, count, sem).wait()
    def drain(step, carry):
        pass_far(step, "wait")
        return carry

    lax.fori_loop(0, n_steps, drain, 0)
    for core_id in BOTH:
        @pl.when(core == core_id)
        def _():
            for y in range(n_cp):
                for place in BOTH:
                    forward(y, place, core_id).wait_send()
                    forward(y, place, 1 - core_id).wait_recv()


def front_call(n_cp, n_tp, x_loc, w_parts, ids_loc, gates_loc, n_experts):
    _, n_loc, head_dim = w_parts[0].shape
    tok_dev, hid = x_loc.shape
    n_part, n_x = 4, n_tp // PAIR
    half = tok_dev // n_part
    seq = tok_dev * n_cp * n_tp
    any_spec = pl.BlockSpec(memory_space=pl.ANY)
    n_steps = n_part * n_tp
    vmem_spec = pl.BlockSpec(memory_space=pltpu.VMEM)
    return pl.pallas_call(
        functools.partial(front_kernel, n_cp, n_tp, n_part),
        name="gather_project",
        out_shape=(jax.ShapeDtypeStruct((seq, head_dim), jnp.bfloat16), jax.ShapeDtypeStruct((head_dim, seq), jnp.bfloat16),
                   jax.ShapeDtypeStruct((seq // PAIR, head_dim), jnp.bfloat16)) + (jax.ShapeDtypeStruct((n_experts, tok_dev), jnp.float32),) * 2,
        in_specs=[any_spec] * 4 + [vmem_spec] * 2,
        out_specs=(any_spec,) * 3 + (vmem_spec,) * 2,
        scratch_shapes=[
            pltpu.VMEM((n_tp, tok_dev, hid), jnp.bfloat16),
            pltpu.VMEM((3, hid, n_loc, head_dim), jnp.bfloat16),
            pltpu.VMEM((hid, 3 * n_loc * head_dim), jnp.bfloat16),
            pltpu.VMEM((n_steps, n_loc, half, head_dim), jnp.bfloat16),
            pltpu.VMEM((n_steps, n_loc, half, head_dim), jnp.bfloat16),
            pltpu.VMEM((n_steps, n_loc, head_dim, half), jnp.bfloat16),
            pltpu.VMEM((n_part, n_tp, half, head_dim), jnp.bfloat16),
            pltpu.VMEM((n_part, n_tp, head_dim, half), jnp.bfloat16),
            pltpu.VMEM((n_part, n_tp, half, head_dim), jnp.bfloat16),
            dma,
            dma((3,)),
            dma((PAIR, n_part + 2)),
            dma((n_part * n_x,)),
            dma((n_tp, n_part)),
            dma((n_loc,)),
            dma((n_loc,)),
            dma((n_loc, PAIR)),
            dma((n_cp,)),
            dma((n_cp,)),
            dma((PAIR * n_cp,)),
            dma((PAIR * n_cp,)),
            dma((3, n_part, n_tp)),
            dma((3, n_part, n_tp)),
        ],
        compiler_params=pltpu.CompilerParams(collective_id=0, has_side_effects=True, vmem_limit_bytes=VMEM_LIMIT),
        cost_estimate=pl.CostEstimate(flops=PAIR * n_tp * tok_dev * hid * 3 * n_loc * head_dim, bytes_accessed=2**26, transcendentals=0),
    )(x_loc, *w_parts, ids_loc, gates_loc)


def attend_kernel(n_cp, n_tp, k_hbm, vt_hbm, q_hbm, x_hbm, wo_hbm, wg_hbm, wu_hbm, wd_hbm, rank_hbm,
                  h_ref, o_hbm, wgx_hbm, wux_hbm, wdx_hbm, near_hbm,
                  k_buf, vt_buf, q_buf, qt_buf, o_st, o_buf, wo_buf, x_buf, s_even, s_odd, p_even, p_odd, p_near, shrink_even, shrink_odd, acc, m_ref, l_ref,
                  in_sem, so_sem, ro_sem, swo_sem, rwo_sem, sw_sem, rw_sem, sr_sem, rr_sem, o_sem):
    n_dev = n_cp * n_tp
    n_x = n_tp // PAIR
    tok_dev, hid = x_buf.shape
    head_dim = k_buf.shape[1]
    n_heads = o_buf.shape[0]
    cp_pos, tp_pos = lax.axis_index("cp"), lax.axis_index("tp")
    x_pos, core = tp_pos // PAIR, tp_pos % PAIR
    head = n_cp * x_pos + cp_pos
    scale = (head_dim ** -0.5) * 1.4426950408889634
    loads = [pltpu.make_async_copy(src, dst, in_sem.at[i]) for i, (src, dst) in enumerate(
        ((q_hbm, q_buf), (k_hbm, k_buf), (vt_hbm, vt_buf), (x_hbm, x_buf), (wo_hbm, wo_buf.at[tp_pos])))]
    for one in loads:
        one.start()

    enter_all(n_cp, n_tp)

    sibling = PAIR * x_pos + 1 - core

    def wo_copy(src, slot, sem, to_tp):
        return pltpu.make_async_remote_copy(src, wo_buf.at[slot], swo_sem.at[sem], rwo_sem.at[sem], device_id=mesh_id(cp_pos, to_tp),
                                            device_id_type=MESH)

    def wo_send(step):
        to_tp = PAIR * ((x_pos + step) % n_x) + core if step else sibling
        return wo_copy(wo_hbm, tp_pos, step, to_tp)

    def wo_pass(step):
        slot = PAIR * ((x_pos + n_x - step) % n_x) + core
        return wo_copy(wo_buf.at[slot], slot, n_x + step, sibling)

    def run_wo_passes():
        for step in range(1, n_x):
            wo_send(step).wait_recv()
            wo_pass(step).start()

    keep = wgx_hbm.shape[0]
    swaps = [pltpu.make_async_remote_copy(src.at[pl.ds((1 - core) * keep, keep)], dst, sw_sem.at[i], rw_sem.at[i],
                                          device_id=mesh_id(cp_pos, PAIR * x_pos + 1 - core), device_id_type=MESH)
             for i, (src, dst) in enumerate(((wg_hbm, wgx_hbm), (wu_hbm, wux_hbm), (wd_hbm, wdx_hbm)))]
    ranks = []
    for slot, off in ((1, 1), (PAIR, -1), (3, PAIR)):
        for part, place in enumerate((((cp_pos + off + n_cp) % n_cp, tp_pos), (cp_pos, PAIR * ((x_pos + off + n_x) % n_x) + core))):
            ranks.append(pltpu.make_async_remote_copy(rank_hbm, near_hbm.at[part, slot], sr_sem.at[part, slot], rr_sem.at[part, slot],
                                                      device_id=mesh_id(*place), device_id_type=MESH))
    for step in range(n_x):
        wo_send(step).start()
    for one in swaps + ranks:
        one.start()
    for one in loads[:3]:
        one.wait()

    def columns(block):
        return pl.ds(pl.multiple_of(block * tok_dev, tok_dev), tok_dev)

    def scores(block, cols, s_ref, masked):
        s_vals = jnp.dot(k_buf[columns(block), :], qt_buf[:, cols], preferred_element_type=jnp.float32)
        if masked:
            key_id = lax.broadcasted_iota(jnp.int32, s_vals.shape, 0)
            query_id = lax.broadcasted_iota(jnp.int32, s_vals.shape, 1)
            s_vals = jnp.where(key_id <= query_id, s_vals, -1e30)
        s_ref[...] = s_vals
        return jnp.max(s_vals, **COLUMN_WISE)

    def soften(s_ref, s_top, cols, p_ref, shrink_ref):
        m_old = m_ref[:, cols]
        m_new = jnp.maximum(m_old, s_top)
        shrink = jnp.exp2((m_old - m_new) * scale)
        m_ref[:, cols] = m_new
        shrink_ref[...] = shrink
        prob = jnp.exp2((s_ref[...] - m_new) * scale)
        l_ref[:, cols] = l_ref[:, cols] * shrink + jnp.sum(prob, **COLUMN_WISE)
        p_ref[...] = prob.astype(jnp.bfloat16)

    def gather_values(block, cols, p_ref, shrink_ref):
        acc[:, cols] = acc[:, cols] * shrink_ref[...] + jnp.dot(vt_buf[:, columns(block)], p_ref[...], preferred_element_type=jnp.float32)

    def query_pair(turn, carry):
        g = (turn + 1 + cp_pos + x_pos // PAIR * (PAIR * n_cp - 1 - PAIR * cp_pos)) % (n_dev // 4)

        @pl.when(turn == n_dev // 4 - 2)
        def _():
            run_wo_passes()
        q_rows = q_buf[pl.ds(pl.multiple_of(g * PAIR * tok_dev, PAIR * tok_dev), PAIR * tok_dev), :]
        qt_buf[...] = q_rows.astype(jnp.float32).T.astype(jnp.bfloat16)
        m_ref[...] = jnp.full_like(m_ref, -1e30)
        l_ref[...] = jnp.zeros_like(l_ref)
        acc[...] = jnp.zeros_like(acc)
        p_odd[...] = jnp.zeros_like(p_odd)
        shrink_odd[...] = jnp.ones_like(shrink_odd)
        near = ((0, core), (1, 3 - core), (1 - core, 0), (1, 1 - core), (1, 2 - core))
        lanes = [(s_even, p_even, shrink_even, 0), (s_even, p_even, shrink_even, 1), (s_odd, p_near, shrink_odd, 0), (s_odd, p_near, shrink_odd, 1)]
        tops = {}

        def near_refs(i):
            s_ref, p_ref, shrink_ref, place = lanes[i % 4]
            cols = pl.ds(place * tok_dev, tok_dev)
            return s_ref.at[:, cols], p_ref.at[:, cols], shrink_ref.at[:, cols]

        def near_scores(i):
            r, block = near[i]
            tops[i] = scores(4 * g + block, columns(r), near_refs(i)[0], i < 2)

        def near_soften(i):
            s_ref, p_ref, shrink_ref = near_refs(i)
            soften(s_ref, tops[i], columns(near[i][0]), p_ref, shrink_ref)

        def near_values(i):
            _, p_ref, shrink_ref = near_refs(i)
            gather_values(4 * g + near[i][1], columns(near[i][0]), p_ref, shrink_ref)

        for i in range(len(near) + 2):
            if i < len(near):
                near_scores(i)
            if 0 <= i - 1 < len(near):
                near_soften(i - 1)
            if 0 <= i - 2:
                near_values(i - 2)
        shrink_odd[...] = jnp.ones_like(shrink_odd)
        strip = min(512, tok_dev)
        strips = [pl.ds(lo, strip) for lo in range(0, PAIR * tok_dev, strip)]

        def far_step(block, parity, tops):
            s_in, s_out = (s_even, s_odd)[::1 - PAIR * parity]
            p_out, p_in = (p_even, p_odd)[::1 - PAIR * parity]
            shrink_out, shrink_in = (shrink_even, shrink_odd)[::1 - PAIR * parity]
            next_tops = []
            for cols, top in zip(strips, tops):
                next_tops.append(scores(block + 1, cols, s_out.at[:, cols], False))
                soften(s_in.at[:, cols], top, cols, p_out.at[:, cols], shrink_out.at[:, cols])
                gather_values(jnp.maximum(block - 1, 0), cols, p_in.at[:, cols], shrink_in.at[:, cols])
            return next_tops

        def far_blocks(n, tops):
            for j in range(4):
                tops = far_step(4 * n + j, j % PAIR, tops)
            return tops

        lax.fori_loop(0, g, far_blocks, [scores(0, cols, s_even.at[:, cols], False) for cols in strips])
        for cols in strips:
            gather_values(jnp.maximum(4 * g - 1, 0), cols, p_odd.at[:, cols], shrink_odd.at[:, cols])
        out = (acc[...] / l_ref[...]).T.astype(jnp.bfloat16)
        for r in BOTH:
            o_st[PAIR * g + r] = out[r * tok_dev:(r + 1) * tok_dev]
            o_push(PAIR * g + r, "start")
        return carry

    def o_push(index, what):
        block = 4 * (index // PAIR) + (1 - core) * 3 * (index % PAIR) + core * (1 + index % PAIR)
        to_cp, to_tp = owner_of(block, n_cp, n_tp)
        here = and_(to_cp == cp_pos, to_tp == tp_pos)
        if what == "start":
            @pl.when(here)
            def _():
                pltpu.make_async_copy(o_st.at[index], o_hbm.at[head], ro_sem.at[head]).start()

        @pl.when(not_(here))
        def _():
            copy = pltpu.make_async_remote_copy(o_st.at[index], o_hbm.at[head], so_sem.at[index], ro_sem.at[head],
                                                device_id=mesh_id(to_cp, to_tp), device_id_type=MESH)
            if what == "start":
                copy.start()
            else:
                copy.wait_send()

    lax.fori_loop(0, n_dev // 4, query_pair, 0)

    wo_send(0).wait_recv()
    for step in range(1, n_x):
        wo_pass(step).wait_recv()
    for one in loads[3:]:
        one.wait()
    for j in range(n_heads):
        pltpu.make_async_copy(o_hbm.at[j], o_hbm.at[j], ro_sem.at[j]).wait()
    o_load = pltpu.make_async_copy(o_hbm, o_buf, o_sem)
    o_load.start()
    o_load.wait()
    o_rows = jnp.concatenate([o_buf[j] for j in range(n_heads)], axis=1)
    n_cols = min(512, hid // PAIR)

    for col in range(0, hid, n_cols):
        cols = pl.ds(col, n_cols)
        w_cols = wo_buf[:, :, cols].reshape(n_heads * head_dim, n_cols)
        h_cols = (x_buf[:, cols].astype(jnp.float32) + jnp.dot(o_rows, w_cols, preferred_element_type=jnp.float32)).astype(jnp.bfloat16)
        h_ref[PAIR * col // hid, :, pl.ds(col % (hid // PAIR), n_cols)] = h_cols

    for step in range(n_x):
        wo_send(step).wait_send()
    for step in range(1, n_x):
        wo_pass(step).wait_send()
    for one in swaps + ranks:
        one.wait()

    def drain(index, carry):
        o_push(index, "wait")
        return carry

    lax.fori_loop(0, n_dev // PAIR, drain, 0)


def attend_call(n_cp, n_tp, k_all, vt_all, q_all, x_loc, wo_loc, w_gate, w_up, w_down, rank_rows):
    n_dev = n_cp * n_tp
    tok_dev, hid = x_loc.shape
    seq, head_dim = k_all.shape
    n_heads = n_tp * wo_loc.shape[0] // head_dim
    keep = w_gate.shape[0] // PAIR
    any_spec = pl.BlockSpec(memory_space=pl.ANY)
    bf16 = jnp.bfloat16
    h_loc, _, wg_other, wu_other, wd_other, near_rows = pl.pallas_call(
        functools.partial(attend_kernel, n_cp, n_tp),
        name="attend_heads",
        out_shape=(jax.ShapeDtypeStruct((PAIR, tok_dev, hid // PAIR), bf16), jax.ShapeDtypeStruct((n_heads, tok_dev, head_dim), bf16))
        + tuple(jax.ShapeDtypeStruct((keep,) + w.shape[1:], bf16) for w in (w_gate, w_up, w_down))
        + (jax.ShapeDtypeStruct((PAIR, 4) + rank_rows.shape, jnp.float32),),
        in_specs=[any_spec] * 9,
        out_specs=(pl.BlockSpec(memory_space=pltpu.VMEM),) + (any_spec,) * 5,
        scratch_shapes=[
            pltpu.VMEM((seq, head_dim), bf16),
            pltpu.VMEM((head_dim, seq), bf16),
            pltpu.VMEM((seq // PAIR, head_dim), bf16),
            pltpu.VMEM((head_dim, PAIR * tok_dev), bf16),
            pltpu.VMEM((n_dev // PAIR, tok_dev, head_dim), bf16),
            pltpu.VMEM((n_heads, tok_dev, head_dim), bf16),
            pltpu.VMEM((n_tp,) + wo_loc.shape, bf16),
            pltpu.VMEM((tok_dev, hid), bf16),
            pltpu.VMEM((tok_dev, PAIR * tok_dev), jnp.float32),
            pltpu.VMEM((tok_dev, PAIR * tok_dev), jnp.float32),
            pltpu.VMEM((tok_dev, PAIR * tok_dev), bf16),
            pltpu.VMEM((tok_dev, PAIR * tok_dev), bf16),
            pltpu.VMEM((tok_dev, PAIR * tok_dev), bf16),
            pltpu.VMEM((1, PAIR * tok_dev), jnp.float32),
            pltpu.VMEM((1, PAIR * tok_dev), jnp.float32),
            pltpu.VMEM((head_dim, PAIR * tok_dev), jnp.float32),
            pltpu.VMEM((1, PAIR * tok_dev), jnp.float32),
            pltpu.VMEM((1, PAIR * tok_dev), jnp.float32),
            dma((5,)),
            dma((n_dev // PAIR,)),
            dma((n_heads,)),
            dma((n_tp,)),
            dma((n_tp,)),
            dma((3,)),
            dma((3,)),
            dma((PAIR, 4)),
            dma((PAIR, 4)),
            dma,
        ],
        compiler_params=pltpu.CompilerParams(collective_id=1, has_side_effects=True, vmem_limit_bytes=VMEM_LIMIT),
        cost_estimate=pl.CostEstimate(flops=PAIR * seq * seq * head_dim // PAIR, bytes_accessed=2**26, transcendentals=seq * seq // 4),
    )(k_all, vt_all, q_all, x_loc, wo_loc, w_gate, w_up, w_down, rank_rows)
    return h_loc, near_rows, wg_other, wu_other, wd_other


def solution(mesh):
    n_cp = mesh.shape["cp"]
    n_tp = mesh.shape["tp"]
    row_spec = P(("dp", "cp", "tp"), None)
    head_spec = P(None, "tp", None)
    expert_spec = P(("cp", "tp"), None, None)

    def device_step(x_loc, w_q, w_k, w_v, w_o, ids_loc, gates_loc, w_gate, w_up, w_down):
        tok_dev, hid_dim = x_loc.shape
        n_loc, head_dim = w_q.shape[1:]
        n_experts = w_gate.shape[0] * n_cp * n_tp // PAIR
        capacity = ids_loc.shape[1] * tok_dev // n_experts
        k_all, vt_all, q_all, rank_rows, gate_rows = front_call(n_cp, n_tp, x_loc, (w_q, w_k, w_v), ids_loc.T, gates_loc.T, n_experts)
        h_loc, near_rows, *others = attend_call(n_cp, n_tp, k_all, vt_all, q_all, x_loc, w_o.reshape(n_loc * head_dim, hid_dim), w_gate, w_up, w_down, rank_rows)
        return moe_call(n_cp, n_tp, capacity, h_loc, rank_rows, near_rows, gate_rows, w_gate, w_up, w_down, *others)

    return jax.shard_map(device_step, mesh=mesh, in_specs=(row_spec, head_spec, head_spec, head_spec, P("tp", None, None), row_spec, row_spec, expert_spec, expert_spec, expert_spec), out_specs=row_spec, check_vma=False)
```

```python
import functools

import jax
import jax.numpy as jnp
from jax import lax
from jax.experimental import pallas as pl
from jax.experimental.pallas import tpu as pltpu
from jax.sharding import PartitionSpec as P

MESH = pl.DeviceIdType.MESH
PAIR = 2
BOTH = range(PAIR)
ROWS_ROWS = (((0,), (0,)), ((), ()))
COLUMN_WISE = {"axis": 0, "keepdims": True}
dma = pltpu.SemaphoreType.DMA
and_, or_, not_ = jnp.logical_and, jnp.logical_or, jnp.logical_not
VMEM_LIMIT = 66_000_000
PLACES = ((0, 0), (0, 1), (1, 0), (0, -1), (-1, 0), (1, 1), (-1, -1), (1, -1), (-1, 1), (0, PAIR), (PAIR, 0), (1, PAIR), (PAIR, 1), (-1, PAIR), (PAIR, -1), (PAIR, PAIR))
N_NEAR, FIRST_FAR = 5, 9
GROUPS = ("1234", "bcbc", "5656", "dede", "7878", "0f0f", "9a9a", "1234")
FLIPS = ("0000",) + ("0011",) * 6 + ("1111",)
SOURCES = (0, -1, 1, PAIR)


def peer_of(step, cp_pos, tp_pos, n_cp, n_tp):
    n_x = n_tp // PAIR
    off_x = (step // PAIR) % n_x
    off_y = (off_x + step // n_tp) % n_cp
    return (cp_pos + off_y) % n_cp, ((tp_pos // PAIR + off_x) % n_x) * 2 + (tp_pos % PAIR + step % PAIR) % PAIR


def mesh_id(cp_pos, tp_pos):
    return {"cp": cp_pos, "tp": tp_pos}


def enter_all(n_cp, n_tp):
    cp_pos, tp_pos = lax.axis_index("cp"), lax.axis_index("tp")

    def signal_peer(step, carry):
        to_cp, to_tp = peer_of(step, cp_pos, tp_pos, n_cp, n_tp)
        pl.semaphore_signal(pltpu.get_barrier_semaphore(), inc=1, device_id=mesh_id(to_cp, to_tp), device_id_type=MESH)
        return carry

    lax.fori_loop(1, n_cp * n_tp, signal_peer, 0)
    pl.semaphore_wait(pltpu.get_barrier_semaphore(), n_cp * n_tp - 1)


def pick(values, index):
    out = values[-1]
    for k, value in enumerate(values[:-1]):
        out = jnp.where(index == k, value, out)
    return out


def moe_kernel(n_cp, n_tp, group, h_hbm, rank_hbm, near_hbm, gate_ref, wg_hbm, wu_hbm, wd_hbm, wgx_hbm, wux_hbm, wdx_hbm,
               y_ref, rx_hbm, rl_hbm, rz_hbm, zl_hbm,
               h_buf, rank_buf, wg_buf, wu_buf, wd_buf, ring, own_stage, z_ring, x_buf, z_buf, acc, parts,
               w_sem, rank_sem, in_sem, x_sem, z_sem, hs_sem, hr_sem, ss_sem, rx_sem, rl_sem, fl_sem, sz_sem, rz_sem, zl_sem, fz_sem):
    n_x = n_tp // PAIR
    tok_dev, half_hid = h_buf.shape[2:]
    hid = PAIR * half_hid
    cap = ring.shape[3] // PAIR
    cp_pos, tp_pos = lax.axis_index("cp"), lax.axis_index("tp")
    x_pos, core = tp_pos // PAIR, tp_pos % PAIR
    half_tok = tok_dev // PAIR

    def at(off_y, off_x, flip):
        return (cp_pos + off_y + n_cp) % n_cp, PAIR * ((x_pos + off_x + n_x) % n_x) + (core + flip) % PAIR

    def line(place):
        return place[0] * n_tp + place[1]

    def send(src, dst, s_sem, r_sem, place):
        return pltpu.make_async_remote_copy(src, dst, s_sem, r_sem, device_id=mesh_id(*place), device_id_type=MESH)

    def await_bytes(ref, sem):
        pltpu.make_async_copy(ref, ref, sem).wait()

    h_loads = [pltpu.make_async_copy(h_hbm.at[part], h_buf.at[part, 0], in_sem.at[part]) for part in BOTH]
    rank_loads = []
    for part in BOTH:
        rank_loads.append(pltpu.make_async_copy(rank_hbm, rank_buf.at[part, 0], rank_sem.at[PAIR * part]))
        rank_loads.append(pltpu.make_async_copy(near_hbm.at[part, pl.ds(1, 3)], rank_buf.at[part, pl.ds(1, 3)], rank_sem.at[PAIR * part + 1]))
    w_loads = []
    for slot, (own, other, buf) in enumerate(((wg_hbm, wgx_hbm, wg_buf), (wu_hbm, wux_hbm, wu_buf), (wd_hbm, wdx_hbm, wd_buf))):
        w_loads.append(pltpu.make_async_copy(own.at[pl.ds(PAIR * core, PAIR)], buf.at[0], w_sem.at[PAIR * slot]))
        w_loads.append(pltpu.make_async_copy(other, buf.at[1], w_sem.at[PAIR * slot + 1]))
    for one in h_loads + rank_loads:
        one.start()
    enter_all(n_cp, n_tp)

    def along(part, off):
        return at(off, 0, 0) if part == 0 else at(0, off, 0)

    def across(part, off, flip):
        return at(0, off, flip) if part == 0 else at(off, 0, flip)

    def rows_of(piece):
        return pl.ds(piece * half_tok, half_tok)

    def spread(part, i):
        piece, off, slot = ((0, 1, 1), (1, -1, PAIR), (1, 1, 1), (0, -1, PAIR), (0, 1, 3), (1, -1, 3))[i]
        rows = rows_of(piece)
        src = h_hbm.at[part, rows] if i < 4 else h_buf.at[part, 1 if i == 4 else 2, rows]
        return send(src, h_buf.at[part, slot, rows], hs_sem.at[part, i], hr_sem.at[part, slot, piece], along(part, off))

    def await_h(part, slot, piece):
        await_bytes(h_buf.at[part, slot, rows_of(piece)], hr_sem.at[part, slot, piece])

    for i in range(4):
        for part in BOTH:
            spread(part, i).start()
    for one in w_loads:
        one.start()
    for one in h_loads + rank_loads:
        one.wait()

    slots = lax.broadcasted_iota(jnp.int32, (cap, tok_dev), 0).astype(jnp.float32)

    def gather_rows(part, stage, m):
        turn = m // PAIR
        off = turn + (turn // PAIR) * (5 - PAIR * turn)
        first = PAIR * line(across(part, off, m % PAIR))
        chosen = [jnp.where(rank_buf[part, stage, pl.ds(first + i, 1), :] == slots, 1.0, 0.0) for i in BOTH]
        chosen = jnp.concatenate(chosen, axis=0).astype(jnp.bfloat16)
        return jnp.dot(chosen, h_buf[part, stage], preferred_element_type=jnp.float32).astype(jnp.bfloat16)

    def source_line(part, stage, off):
        a = SOURCES[stage]
        return line(at(a, off, 0) if part == 0 else at(off, a, 0))

    def await_ring(part, stage):
        def one(m, carry):
            await_bytes(ring.at[part, stage % PAIR, m], ss_sem.at[part, stage % PAIR, m])
            return carry
        lax.fori_loop(1, 8, one, 0)

    def own_copy(part, stage):
        src_line = source_line(part, stage, 0)
        return pltpu.make_async_copy(own_stage.at[part, stage], rx_hbm.at[part, src_line], rx_sem.at[part, src_line])

    def run_stage(stage):
        side = stage % PAIR
        for part in BOTH:
            if stage >= 2:
                await_ring(part, stage)
            own_stage[part, stage] = gather_rows(part, stage, 0)

            def fill(m, carry):
                ring[part, side, m] = gather_rows(part, stage, m)
                return carry

            lax.fori_loop(1, 8, fill, 0)
        lines = [source_line(part, stage, 0) for part in BOTH]
        for flip in BOTH:
            for way, off in enumerate((1, -1)):
                for part in BOTH:
                    m = 6 + flip
                    send(ring.at[part, side, m, pl.ds(way * cap, cap)], rl_hbm.at[part, way, stage, flip], ss_sem.at[part, side, m],
                         rl_sem.at[part, way, stage, flip], across(part, off, 0)).start()
        for m, off in ((PAIR, 1), (4, -1), (3, 1), (5, -1), (1, 0)):
            for part in BOTH:
                send(ring.at[part, side, m], rx_hbm.at[part, lines[part]], ss_sem.at[part, side, m], rx_sem.at[part, lines[part]],
                     across(part, off, m % PAIR)).start()
        for part in BOTH:
            own_copy(part, stage).start()

    def relay(part, stage, way, flip):
        off = 1 - PAIR * way
        src_line = source_line(part, stage, -off)
        return send(rl_hbm.at[part, way, stage, flip], rx_hbm.at[part, src_line, pl.ds(way * cap, cap)], fl_sem.at[part, way, stage, flip],
                    rx_sem.at[part, src_line], across(part, off, flip))

    def run_relays(stage):
        for flip in BOTH:
            for way in BOTH:
                for part in BOTH:
                    await_bytes(rl_hbm.at[part, way, stage, flip], rl_sem.at[part, way, stage, flip])
                    relay(part, stage, way, flip).start()

    run_stage(0)
    for part in BOTH:
        await_h(part, 1, 0)
        spread(part, 4).start()
    for part in BOTH:
        await_h(part, PAIR, 1)
        spread(part, 5).start()
    for part in BOTH:
        await_h(part, 1, 1)
    run_stage(1)
    gate_all = gate_ref[...]
    high = gate_all.astype(jnp.bfloat16).astype(jnp.float32)
    rest = gate_all - high
    mid = rest.astype(jnp.bfloat16).astype(jnp.float32)
    parts[0] = high
    parts[1] = mid
    parts[2] = rest - mid
    for part in BOTH:
        acc[:, part * half_hid:(part + 1) * half_hid] = h_buf[part, 0].astype(jnp.float32)
    run_relays(0)
    for part in BOTH:
        await_h(part, PAIR, 0)
    run_stage(2)
    run_relays(1)
    for part in BOTH:
        await_h(part, 3, 0)
        await_h(part, 3, 1)
    run_stage(3)
    run_relays(2)
    for one in w_loads:
        one.wait()

    rows = group * cap
    n_cols = min(512, hid)

    def expert_rows(slot, i):
        x_rows = x_buf[:, pl.ds(i * cap, cap), :].reshape(rows, hid)
        hidden = []
        for half in BOTH:
            gate_pre = jnp.dot(x_rows, wg_buf[half, i], preferred_element_type=jnp.float32)
            up_pre = jnp.dot(x_rows, wu_buf[half, i], preferred_element_type=jnp.float32)
            hidden.append((gate_pre * (1.0 / (1.0 + jnp.exp(-gate_pre))) * up_pre).astype(jnp.bfloat16))
        for col in range(0, hid, n_cols):
            z_rows = (jnp.dot(hidden[0], wd_buf[0, i, :, pl.ds(col, n_cols)], preferred_element_type=jnp.float32)
                      + jnp.dot(hidden[1], wd_buf[1, i, :, pl.ds(col, n_cols)], preferred_element_type=jnp.float32))
            z_ring[slot, :, pl.ds(i * cap, cap), pl.ds(col, n_cols)] = z_rows.astype(jnp.bfloat16).reshape(group, cap, n_cols)

    def place_at(g, q):
        places = [int(names[q], 16) for names in GROUPS]
        off_y, off_x = (pick([PLACES[p][k] for p in places], g) for k in BOTH)
        return off_y, off_x, pick([int(flips[q]) for flips in FLIPS], g), pick(places, g)

    my_line = line((cp_pos, tp_pos))

    def await_slot(slot):
        for q in range(group):
            await_bytes(z_ring.at[slot, q], sz_sem.at[slot, q])

    def expert_group(g, carry):
        slot = g % 3

        @pl.when(g == 2)
        def _():
            run_relays(3)

        sources = [line(at(*place_at(g, q)[:3])) for q in range(group)]
        loads = []
        for q in range(group):
            for part in BOTH:
                await_bytes(rx_hbm.at[part, sources[q]], rx_sem.at[part, sources[q]])
                loads.append(pltpu.make_async_copy(rx_hbm.at[part, sources[q]], x_buf.at[q, :, pl.ds(part * half_hid, half_hid)], x_sem.at[part, q]))
                loads[-1].start()

        @pl.when(g >= 3)
        def _():
            await_slot(slot)
        for one in loads:
            one.wait()
        for i in BOTH:
            expert_rows(slot, i)
        for q in range(group):
            off_y, off_x, flip, p = place_at(g, q)
            alone = and_(p == 0, flip == 0)

            @pl.when(alone)
            def _():
                pltpu.make_async_copy(z_ring.at[slot, q], rz_hbm.at[my_line], rz_sem.at[my_line]).start()

            @pl.when(and_(p < FIRST_FAR, not_(alone)))
            def _():
                send(z_ring.at[slot, q], rz_hbm.at[my_line], sz_sem.at[slot, q], rz_sem.at[my_line], at(off_y, off_x, flip)).start()

            @pl.when(p >= FIRST_FAR)
            def _():
                lead_y, lead_x = jnp.where(off_y == 2, 1, 0), jnp.where(off_x == 2, 1, 0)
                for way in BOTH:
                    sign = 1 - PAIR * way
                    send(z_ring.at[slot, q, pl.ds(way * cap, cap)], zl_hbm.at[p - FIRST_FAR, flip, way], sz_sem.at[slot, q],
                         zl_sem.at[p - FIRST_FAR, flip, way], at(sign * lead_y, sign * lead_x, 0)).start()
        return carry

    lax.fori_loop(0, len(GROUPS), expert_group, 0)

    n_far = len(PLACES) - FIRST_FAR

    def z_relay(index, flip, way):
        off_y, off_x = PLACES[FIRST_FAR + index]
        sign = 1 - PAIR * way
        lead_y, lead_x = sign * (off_y == 2), sign * (off_x == 2)
        from_line = line(at(-lead_y, -lead_x, 0))
        to_y = sign if off_y == 2 else off_y
        to_x = sign if off_x == 2 else off_x
        return send(zl_hbm.at[index, flip, way], rz_hbm.at[from_line, pl.ds(way * cap, cap)], fz_sem.at[index, flip, way],
                    rz_sem.at[from_line], at(to_y, to_x, flip))

    def each_relay(*indices):
        return [(index, flip, way) for flip in BOTH for way in BOTH for index in indices]

    def run_z_relays(*indices):
        for key in each_relay(*indices):
            await_bytes(zl_hbm.at[key], zl_sem.at[key])
            z_relay(*key).start()

    def combine(p, carry):
        off_y, off_x = pick([a for a, _ in PLACES], p), pick([b for _, b in PLACES], p)
        homes = [line(at(-off_y, -off_x, q)) for q in BOTH]
        loads = []
        for q in BOTH:
            await_bytes(rz_hbm.at[homes[q]], rz_sem.at[homes[q]])
            loads.append(pltpu.make_async_copy(rz_hbm.at[homes[q]], z_buf.at[q], z_sem.at[q]))
            loads[-1].start()
        weights = [[], [], []]
        for q in BOTH:
            for i in BOTH:
                row = pl.ds(PAIR * homes[q] + i, 1)
                chosen = rank_buf[0, 0, row, :] == slots
                for part in range(3):
                    weights[part].append(jnp.where(chosen, parts[part, row, :], 0.0))
        weights = [jnp.concatenate(w, axis=0).astype(jnp.bfloat16) for w in weights]
        for one in loads:
            one.wait()
        for col in range(0, hid, n_cols):
            z_rows = z_buf[:, :, pl.ds(col, n_cols)].reshape(4 * cap, n_cols)
            total = None
            for part in range(3):
                term = lax.dot_general(weights[part], z_rows, ROWS_ROWS, preferred_element_type=jnp.float32)
                total = term if total is None else total + term
            acc[:, pl.ds(col, n_cols)] += total
        return carry

    run_z_relays(PAIR, 3)
    run_z_relays(4, 5)
    lax.fori_loop(0, N_NEAR, combine, 0)
    run_z_relays(6)
    run_z_relays(0, 1)
    lax.fori_loop(N_NEAR, len(PLACES), combine, 0)
    y_ref[...] = acc[...].astype(jnp.bfloat16)

    for part in BOTH:
        for i in range(6):
            spread(part, i).wait_send()
        for stage in (PAIR, 3):
            await_ring(part, stage)
        for stage in range(4):
            for way in BOTH:
                for flip in BOTH:
                    relay(part, stage, way, flip).wait_send()
    last = len(GROUPS) - 3
    for g in range(last, len(GROUPS)):
        for q in range(group):
            if GROUPS[g][q] + FLIPS[g][q] != "00":
                await_bytes(z_ring.at[g % 3, q], sz_sem.at[g % 3, q])
    for key in each_relay(*range(n_far)):
        z_relay(*key).wait_send()


def moe_call(n_cp, n_tp, cap, h_loc, rank_rows, near_rows, gate_rows, w_gate, w_up, w_down, wg_other, wu_other, wd_other):
    n_dev = n_cp * n_tp
    _, tok_dev, half_hid = h_loc.shape
    hid = PAIR * half_hid
    half_f = w_gate.shape[2]
    n_experts = rank_rows.shape[0]
    group = len(GROUPS[0])
    n_far = len(PLACES) - FIRST_FAR
    bf16 = jnp.bfloat16
    any_spec = pl.BlockSpec(memory_space=pl.ANY)
    vmem_spec = pl.BlockSpec(memory_space=pltpu.VMEM)
    flops = PAIR * n_dev * PAIR * cap * hid * PAIR * half_f * 3
    return pl.pallas_call(
        functools.partial(moe_kernel, n_cp, n_tp, group),
        name="routed_experts",
        out_shape=(jax.ShapeDtypeStruct((tok_dev, hid), bf16), jax.ShapeDtypeStruct((PAIR, n_dev, PAIR * cap, half_hid), bf16),
                   jax.ShapeDtypeStruct((PAIR, PAIR, 4, PAIR, cap, half_hid), bf16), jax.ShapeDtypeStruct((n_dev, PAIR * cap, hid), bf16),
                   jax.ShapeDtypeStruct((n_far, PAIR, 2, cap, hid), bf16)),
        in_specs=[any_spec, any_spec, any_spec, vmem_spec] + [any_spec] * 6,
        out_specs=(vmem_spec,) + (any_spec,) * 4,
        scratch_shapes=[
            pltpu.VMEM((PAIR, 4, tok_dev, half_hid), bf16),
            pltpu.VMEM((PAIR, 4, n_experts, tok_dev), jnp.float32),
            pltpu.VMEM((PAIR, PAIR, hid, half_f), bf16),
            pltpu.VMEM((PAIR, PAIR, hid, half_f), bf16),
            pltpu.VMEM((PAIR, PAIR, half_f, hid), bf16),
            pltpu.VMEM((PAIR, PAIR, 8, PAIR * cap, half_hid), bf16),
            pltpu.VMEM((PAIR, 4, PAIR * cap, half_hid), bf16),
            pltpu.VMEM((3, group, PAIR * cap, hid), bf16),
            pltpu.VMEM((group, PAIR * cap, hid), bf16),
            pltpu.VMEM((PAIR, PAIR * cap, hid), bf16),
            pltpu.VMEM((tok_dev, hid), jnp.float32),
            pltpu.VMEM((3, n_experts, tok_dev), jnp.float32),
            dma((6,)), dma((4,)), dma((PAIR,)), dma((PAIR, group)), dma((PAIR,)),
            dma((PAIR, 6)), dma((PAIR, 4, PAIR)), dma((PAIR, PAIR, 8)), dma((PAIR, n_dev)), dma((PAIR, PAIR, 4, PAIR)), dma((PAIR, PAIR, 4, PAIR)),
            dma((3, group)), dma((n_dev,)), dma((n_far, PAIR, PAIR)), dma((n_far, PAIR, PAIR)),
        ],
        compiler_params=pltpu.CompilerParams(collective_id=2, has_side_effects=True, vmem_limit_bytes=VMEM_LIMIT),
        cost_estimate=pl.CostEstimate(flops=flops, bytes_accessed=2**27, transcendentals=0),
    )(h_loc, rank_rows, near_rows, gate_rows, w_gate, w_up, w_down, wg_other, wu_other, wd_other)[0]


def routing_rows(ids_ref, gates_ref, rank_ref, gate_ref):
    top_k, tok_dev = ids_ref.shape
    ids, gates = ids_ref[...].astype(jnp.float32), gates_ref[...]
    expert = lax.broadcasted_iota(jnp.int32, rank_ref.shape, 0).astype(jnp.float32)
    chosen, weight = jnp.zeros_like(expert), jnp.zeros_like(expert)
    for k in range(top_k):
        hit = ids[k:k + 1] == expert
        chosen = jnp.where(hit, 1.0, chosen)
        weight = jnp.where(hit, gates[k:k + 1], weight)
    token = lax.broadcasted_iota(jnp.int32, (tok_dev, tok_dev), 0)
    before = jnp.where(token < lax.broadcasted_iota(jnp.int32, (tok_dev, tok_dev), 1), 1.0, 0.0).astype(jnp.bfloat16)
    rank = jnp.dot(chosen.astype(jnp.bfloat16), before, preferred_element_type=jnp.float32)
    rank_ref[...] = jnp.where(chosen > 0.0, rank, -1.0)
    gate_ref[...] = weight


def block_of(cp_pos, tp_pos, n_cp, n_tp):
    per_chunk = n_tp // PAIR
    late = tp_pos // per_chunk
    chunk = late * (PAIR * n_cp - 1 - cp_pos) + (1 - late) * cp_pos
    return chunk * per_chunk + tp_pos % per_chunk


def owner_of(block, n_cp, n_tp):
    per_chunk = n_tp // PAIR
    chunk = block // per_chunk
    late = chunk // n_cp
    return late * (PAIR * n_cp - 1 - chunk) + (1 - late) * chunk, late * per_chunk + block % per_chunk


def front_kernel(n_cp, n_tp, n_part, x_hbm, wq_hbm, wk_hbm, wv_hbm, ids_ref, gates_ref, k_hbm, vt_hbm, q_hbm, rank_ref, gate_ref,
                 x_buf, w_raw, w_buf, q_st, k_st, vt_st, k_far, vt_far, q_far,
                 own_sem, w_sem, ring_sem, pair_sem, rx_sem, sk_sem, sv_sem, sq_sem, kv_sem, rq_sem, sf_sem, rf_sem, far_sem, pass_sem):
    n_x = n_tp // PAIR
    tok_dev, hid = x_hbm.shape
    half = tok_dev // n_part
    head_dim = k_hbm.shape[1]
    n_loc = q_st.shape[1]
    chunk_len = tok_dev * n_x
    cp_pos, tp_pos = lax.axis_index("cp"), lax.axis_index("tp")
    x_pos, core = tp_pos // PAIR, tp_pos % PAIR
    sibling = PAIR * x_pos + 1 - core
    barrier = pltpu.get_barrier_semaphore()

    def slot_at(off, flip):
        return PAIR * ((x_pos + off + n_x) % n_x) + (core + flip) % PAIR

    own_copy = pltpu.make_async_copy(x_hbm, x_buf.at[tp_pos], own_sem)
    own_copy.start()
    width = n_loc * head_dim
    w_loads = [pltpu.make_async_copy(w, w_raw.at[i], w_sem.at[i]) for i, w in enumerate((wq_hbm, wk_hbm, wv_hbm))]
    for one in w_loads:
        one.start()
    for step in (1, n_x - 1):
        pl.semaphore_signal(barrier, inc=1, device_id=mesh_id(cp_pos, slot_at(step, 0)), device_id_type=MESH)
    for step in range(1, PAIR * n_cp):
        pl.semaphore_signal(barrier, inc=1, device_id=mesh_id((cp_pos + step // PAIR) % n_cp, PAIR * x_pos + (core + step) % PAIR), device_id_type=MESH)
    pl.semaphore_wait(barrier, PAIR * n_cp + 1)

    def own_send(part, to_tp, sem):
        rows = pl.ds(pl.multiple_of(part * half, half), half)
        return pltpu.make_async_remote_copy(x_hbm.at[rows], x_buf.at[tp_pos, rows], sem, rx_sem.at[tp_pos, part],
                                            device_id=mesh_id(cp_pos, to_tp), device_id_type=MESH)

    def pass_on(slot, part, to_tp, sem):
        rows = pl.ds(pl.multiple_of(part * half, half), half)
        return pltpu.make_async_remote_copy(x_buf.at[slot, rows], x_buf.at[slot, rows], sem, rx_sem.at[slot, part],
                                            device_id=mesh_id(cp_pos, to_tp), device_id_type=MESH)

    def ring_send(i, side):
        part = i if side == 0 else n_part - 1 - i
        return own_send(part, slot_at(1 - PAIR * side, 0), ring_sem.at[side, i])

    for i in BOTH:
        for side in BOTH:
            ring_send(i, side).start()
    for part in range(n_part):
        own_send(part, sibling, pair_sem.at[part]).start()
    first = PAIR * n_part
    for one in w_loads:
        one.wait()
    rows_once = min(256, hid)

    def widen(r, carry):
        rows = pl.ds(pl.multiple_of(r * rows_once, rows_once), rows_once)
        for i in range(len(w_loads)):
            w_buf[rows, pl.ds(i * width, width)] = w_raw[i, rows].reshape(rows_once, width)
        return carry

    lax.fori_loop(0, hid // rows_once, widen, 0)
    routing_rows(ids_ref, gates_ref, rank_ref, gate_ref)

    def place_of(step):
        late = jnp.minimum(step // first, 1)
        wave, other, side = jnp.maximum(step - first, 0) // 4, late * ((step // PAIR) % PAIR) + (1 - late) * (step // n_part), step % PAIR
        piece = pick((0, 1, 0, PAIR, 1, 3), wave)
        through = jnp.where(or_(wave == 2, wave == 4), 1, 0)
        part = late * (piece + side * (n_part - 1 - PAIR * piece)) + (1 - late) * (step % n_part)
        off = late * ((1 - through) * (PAIR * side - 1) + PAIR * through)
        return slot_at(off, other), part, off

    def targets(from_cp, slot, part):
        block = block_of(from_cp, slot, n_cp, n_tp)
        pos = pl.multiple_of(block * tok_dev + part * half, half)
        q_core = ((block % 4 + 1) // PAIR) % PAIR
        q_pos = pl.multiple_of((PAIR * (block // 4) + (block % 4) // PAIR) * tok_dev + part * half, half)
        return ((k_hbm.at[pl.ds(pos, half)], 0, kv_sem.at[from_cp]), (vt_hbm.at[:, pl.ds(pos, half)], 1, kv_sem.at[from_cp]),
                (q_hbm.at[pl.ds(q_pos, half)], q_core, rq_sem.at[from_cp]))

    def remote(src, dst, s_sem, r_sem, to_cp, to_core):
        return pltpu.make_async_remote_copy(src, dst, s_sem, r_sem, device_id=mesh_id((to_cp + n_cp) % n_cp, PAIR * x_pos + to_core), device_id_type=MESH)

    far_refs = (k_far, vt_far, q_far)

    def outputs_of(step):
        slot, part, _ = place_of(step)
        for i in range(n_loc):
            to_cp = n_loc * core + i
            far = (to_cp - cp_pos + n_cp) % n_cp == n_cp // PAIR
            for kind, (src, (dst, to_core, r_sem)) in enumerate(zip((k_st.at[step, i], vt_st.at[step, i], q_st.at[step, i]), targets(cp_pos, slot, part))):
                s_sem = (sk_sem.at[i], sv_sem.at[i], sq_sem.at[i, to_core])[kind]
                here = and_(to_cp == cp_pos, to_core == core)

                @pl.when(here)
                def _():
                    pltpu.make_async_copy(src, dst, r_sem).start()

                @pl.when(far)
                def _():
                    remote(src, far_refs[kind].at[part, slot], s_sem, far_sem.at[kind, part, slot], cp_pos + 1 - part // PAIR * 2, core).start()

                @pl.when(not_(or_(here, far)))
                def _():
                    remote(src, dst, s_sem, r_sem, to_cp, to_core).start()

    def pass_far(step, what):
        slot, part, _ = place_of(step)
        sign = 1 - part // PAIR * 2

        @pl.when((cp_pos + sign + n_cp) % n_cp // n_loc == core)
        def _():
            for kind, (dst, to_core, r_sem) in enumerate(targets((cp_pos - sign + n_cp) % n_cp, slot, part)):
                src = far_refs[kind].at[part, slot]
                copy = remote(src, dst, pass_sem.at[kind, part, slot], r_sem, cp_pos + sign, to_core)
                if what == "start":
                    pltpu.make_async_copy(src, src, far_sem.at[kind, part, slot]).wait()
                    copy.start()
                else:
                    copy.wait_send()

    def project(step, carry):
        slot, part, off = place_of(step)
        wave, other, side = (step - first) // 4, (step // PAIR) % PAIR, step % PAIR

        @pl.when(step == 0)
        def _():
            own_copy.wait()

        @pl.when(step >= n_part)
        def _():
            pass_on(slot, part, sibling, pair_sem.at[0]).wait_recv()

        @pl.when(and_(step >= first, other == 0))
        def _():
            @pl.when(wave < 2)
            def _():
                pass_on(slot, part, slot_at(-off, 0), ring_sem.at[side, n_part + wave]).start()
                for i in BOTH:
                    @pl.when(side == i)
                    def _():
                        ring_send(2 + wave, i).start()
            pass_on(slot, part, sibling, pair_sem.at[n_part + PAIR * wave + side]).start()

        x_rows = x_buf[slot, pl.ds(pl.multiple_of(part * half, half), half), :]
        qkv = jnp.dot(x_rows, w_buf[...], preferred_element_type=jnp.float32)
        for i in range(n_loc):
            q_st[step, i] = qkv[:, i * head_dim:(i + 1) * head_dim].astype(jnp.bfloat16)
            k_st[step, i] = qkv[:, (n_loc + i) * head_dim:(n_loc + i + 1) * head_dim].astype(jnp.bfloat16)
            vt_st[step, i] = qkv[:, (PAIR * n_loc + i) * head_dim:(PAIR * n_loc + i + 1) * head_dim].T.astype(jnp.bfloat16)

        @pl.when(step > 0)
        def _():
            outputs_of(step - 1)

        @pl.when(step >= lag)
        def _():
            pass_far(step - lag, "start")
        return carry

    n_steps, lag = n_part * n_tp, 8
    lax.fori_loop(0, n_steps, project, 0)
    outputs_of(n_steps - 1)

    def pass_late(step, carry):
        pass_far(step, "start")
        return carry

    lax.fori_loop(n_steps - lag, n_steps, pass_late, 0)

    def whole(ref, count, sem):
        return pltpu.make_async_copy(ref.at[pl.ds(0, count)], ref.at[pl.ds(0, count)], sem)

    def forward(y, place, core_id):
        chunk = y if place == 0 else PAIR * n_cp - 1 - y
        cols = pl.ds(chunk * chunk_len, chunk_len)
        ref = k_hbm.at[cols] if core_id == 0 else vt_hbm.at[:, cols]
        return pltpu.make_async_remote_copy(ref, ref, sf_sem.at[PAIR * y + place], rf_sem.at[PAIR * y + place],
                                            device_id=mesh_id(cp_pos, sibling), device_id_type=MESH)

    for y in range(n_cp):
        whole(k_hbm, PAIR * chunk_len, kv_sem.at[y]).wait()
        for core_id in BOTH:
            @pl.when(core == core_id)
            def _():
                for place in BOTH:
                    forward(y, place, core_id).start()
    for y in range(n_cp):
        whole(q_hbm, chunk_len, rq_sem.at[y]).wait()
    for side in BOTH:
        for i in range(n_part + 2):
            own_send(0, sibling, ring_sem.at[side, i]).wait_send()
    for i in range(n_part * n_x):
        own_send(0, sibling, pair_sem.at[i]).wait_send()
    for i in range(n_loc):
        to_cp = n_loc * core + i
        for sem, to_core, count in ((sk_sem.at[i], 0, PAIR * chunk_len), (sv_sem.at[i], 1, PAIR * chunk_len),
                                    (sq_sem.at[i, 0], 0, chunk_len), (sq_sem.at[i, 1], 1, chunk_len)):
            @pl.when(not_(and_(to_cp == cp_pos, to_core == core)))
            def _():
                whole(k_hbm, count, sem).wait()
    def drain(step, carry):
        pass_far(step, "wait")
        return carry

    lax.fori_loop(0, n_steps, drain, 0)
    for core_id in BOTH:
        @pl.when(core == core_id)
        def _():
            for y in range(n_cp):
                for place in BOTH:
                    forward(y, place, core_id).wait_send()
                    forward(y, place, 1 - core_id).wait_recv()


def front_call(n_cp, n_tp, x_loc, w_parts, ids_loc, gates_loc, n_experts):
    _, n_loc, head_dim = w_parts[0].shape
    tok_dev, hid = x_loc.shape
    n_part, n_x = 4, n_tp // PAIR
    half = tok_dev // n_part
    seq = tok_dev * n_cp * n_tp
    any_spec = pl.BlockSpec(memory_space=pl.ANY)
    n_steps = n_part * n_tp
    vmem_spec = pl.BlockSpec(memory_space=pltpu.VMEM)
    return pl.pallas_call(
        functools.partial(front_kernel, n_cp, n_tp, n_part),
        name="gather_project",
        out_shape=(jax.ShapeDtypeStruct((seq, head_dim), jnp.bfloat16), jax.ShapeDtypeStruct((head_dim, seq), jnp.bfloat16),
                   jax.ShapeDtypeStruct((seq // PAIR, head_dim), jnp.bfloat16)) + (jax.ShapeDtypeStruct((n_experts, tok_dev), jnp.float32),) * 2,
        in_specs=[any_spec] * 4 + [vmem_spec] * 2,
        out_specs=(any_spec,) * 3 + (vmem_spec,) * 2,
        scratch_shapes=[
            pltpu.VMEM((n_tp, tok_dev, hid), jnp.bfloat16),
            pltpu.VMEM((3, hid, n_loc, head_dim), jnp.bfloat16),
            pltpu.VMEM((hid, 3 * n_loc * head_dim), jnp.bfloat16),
            pltpu.VMEM((n_steps, n_loc, half, head_dim), jnp.bfloat16),
            pltpu.VMEM((n_steps, n_loc, half, head_dim), jnp.bfloat16),
            pltpu.VMEM((n_steps, n_loc, head_dim, half), jnp.bfloat16),
            pltpu.VMEM((n_part, n_tp, half, head_dim), jnp.bfloat16),
            pltpu.VMEM((n_part, n_tp, head_dim, half), jnp.bfloat16),
            pltpu.VMEM((n_part, n_tp, half, head_dim), jnp.bfloat16),
            dma,
            dma((3,)),
            dma((PAIR, n_part + 2)),
            dma((n_part * n_x,)),
            dma((n_tp, n_part)),
            dma((n_loc,)),
            dma((n_loc,)),
            dma((n_loc, PAIR)),
            dma((n_cp,)),
            dma((n_cp,)),
            dma((PAIR * n_cp,)),
            dma((PAIR * n_cp,)),
            dma((3, n_part, n_tp)),
            dma((3, n_part, n_tp)),
        ],
        compiler_params=pltpu.CompilerParams(collective_id=0, has_side_effects=True, vmem_limit_bytes=VMEM_LIMIT),
        cost_estimate=pl.CostEstimate(flops=PAIR * n_tp * tok_dev * hid * 3 * n_loc * head_dim, bytes_accessed=2**26, transcendentals=0),
    )(x_loc, *w_parts, ids_loc, gates_loc)


def attend_kernel(n_cp, n_tp, k_hbm, vt_hbm, q_hbm, x_hbm, wo_hbm, wg_hbm, wu_hbm, wd_hbm, rank_hbm,
                  h_ref, o_hbm, wgx_hbm, wux_hbm, wdx_hbm, near_hbm,
                  k_buf, vt_buf, q_buf, qt_buf, o_st, o_buf, wo_buf, x_buf, s_even, s_odd, p_even, p_odd, p_near, shrink_even, shrink_odd, acc, m_ref, l_ref,
                  in_sem, so_sem, ro_sem, swo_sem, rwo_sem, sw_sem, rw_sem, sr_sem, rr_sem, o_sem):
    n_dev = n_cp * n_tp
    n_x = n_tp // PAIR
    tok_dev, hid = x_buf.shape
    head_dim = k_buf.shape[1]
    n_heads = o_buf.shape[0]
    cp_pos, tp_pos = lax.axis_index("cp"), lax.axis_index("tp")
    x_pos, core = tp_pos // PAIR, tp_pos % PAIR
    head = n_cp * x_pos + cp_pos
    scale = (head_dim ** -0.5) * 1.4426950408889634
    loads = [pltpu.make_async_copy(src, dst, in_sem.at[i]) for i, (src, dst) in enumerate(
        ((q_hbm, q_buf), (k_hbm, k_buf), (vt_hbm, vt_buf), (x_hbm, x_buf), (wo_hbm, wo_buf.at[tp_pos])))]
    for one in loads:
        one.start()

    enter_all(n_cp, n_tp)

    sibling = PAIR * x_pos + 1 - core

    def wo_copy(src, slot, sem, to_tp):
        return pltpu.make_async_remote_copy(src, wo_buf.at[slot], swo_sem.at[sem], rwo_sem.at[sem], device_id=mesh_id(cp_pos, to_tp),
                                            device_id_type=MESH)

    def wo_send(step):
        to_tp = PAIR * ((x_pos + step) % n_x) + core if step else sibling
        return wo_copy(wo_hbm, tp_pos, step, to_tp)

    def wo_pass(step):
        slot = PAIR * ((x_pos + n_x - step) % n_x) + core
        return wo_copy(wo_buf.at[slot], slot, n_x + step, sibling)

    def run_wo_passes():
        for step in range(1, n_x):
            wo_send(step).wait_recv()
            wo_pass(step).start()

    keep = wgx_hbm.shape[0]
    swaps = [pltpu.make_async_remote_copy(src.at[pl.ds((1 - core) * keep, keep)], dst, sw_sem.at[i], rw_sem.at[i],
                                          device_id=mesh_id(cp_pos, PAIR * x_pos + 1 - core), device_id_type=MESH)
             for i, (src, dst) in enumerate(((wg_hbm, wgx_hbm), (wu_hbm, wux_hbm), (wd_hbm, wdx_hbm)))]
    ranks = []
    for slot, off in ((1, 1), (PAIR, -1), (3, PAIR)):
        for part, place in enumerate((((cp_pos + off + n_cp) % n_cp, tp_pos), (cp_pos, PAIR * ((x_pos + off + n_x) % n_x) + core))):
            ranks.append(pltpu.make_async_remote_copy(rank_hbm, near_hbm.at[part, slot], sr_sem.at[part, slot], rr_sem.at[part, slot],
                                                      device_id=mesh_id(*place), device_id_type=MESH))
    for step in range(n_x):
        wo_send(step).start()
    for one in swaps + ranks:
        one.start()
    for one in loads[:3]:
        one.wait()

    def columns(block):
        return pl.ds(pl.multiple_of(block * tok_dev, tok_dev), tok_dev)

    def scores(block, cols, s_ref, masked):
        s_vals = jnp.dot(k_buf[columns(block), :], qt_buf[:, cols], preferred_element_type=jnp.float32)
        if masked:
            key_id = lax.broadcasted_iota(jnp.int32, s_vals.shape, 0)
            query_id = lax.broadcasted_iota(jnp.int32, s_vals.shape, 1)
            s_vals = jnp.where(key_id <= query_id, s_vals, -1e30)
        s_ref[...] = s_vals
        return jnp.max(s_vals, **COLUMN_WISE)

    def soften(s_ref, s_top, cols, p_ref, shrink_ref):
        m_old = m_ref[:, cols]
        m_new = jnp.maximum(m_old, s_top)
        shrink = jnp.exp2((m_old - m_new) * scale)
        m_ref[:, cols] = m_new
        shrink_ref[...] = shrink
        prob = jnp.exp2((s_ref[...] - m_new) * scale)
        l_ref[:, cols] = l_ref[:, cols] * shrink + jnp.sum(prob, **COLUMN_WISE)
        p_ref[...] = prob.astype(jnp.bfloat16)

    def gather_values(block, cols, p_ref, shrink_ref):
        acc[:, cols] = acc[:, cols] * shrink_ref[...] + jnp.dot(vt_buf[:, columns(block)], p_ref[...], preferred_element_type=jnp.float32)

    def query_pair(turn, carry):
        g = (turn + 1 + cp_pos + x_pos // PAIR * (PAIR * n_cp - 1 - PAIR * cp_pos)) % (n_dev // 4)

        @pl.when(turn == n_dev // 4 - 2)
        def _():
            run_wo_passes()
        q_rows = q_buf[pl.ds(pl.multiple_of(g * PAIR * tok_dev, PAIR * tok_dev), PAIR * tok_dev), :]
        qt_buf[...] = q_rows.astype(jnp.float32).T.astype(jnp.bfloat16)
        m_ref[...] = jnp.full_like(m_ref, -1e30)
        l_ref[...] = jnp.zeros_like(l_ref)
        acc[...] = jnp.zeros_like(acc)
        p_odd[...] = jnp.zeros_like(p_odd)
        shrink_odd[...] = jnp.ones_like(shrink_odd)
        near = ((0, core), (1, 3 - core), (1 - core, 0), (1, 1 - core), (1, 2 - core))
        lanes = [(s_even, p_even, shrink_even, 0), (s_even, p_even, shrink_even, 1), (s_odd, p_near, shrink_odd, 0), (s_odd, p_near, shrink_odd, 1)]
        tops = {}

        def near_refs(i):
            s_ref, p_ref, shrink_ref, place = lanes[i % 4]
            cols = pl.ds(place * tok_dev, tok_dev)
            return s_ref.at[:, cols], p_ref.at[:, cols], shrink_ref.at[:, cols]

        def near_scores(i):
            r, block = near[i]
            tops[i] = scores(4 * g + block, columns(r), near_refs(i)[0], i < 2)

        def near_soften(i):
            s_ref, p_ref, shrink_ref = near_refs(i)
            soften(s_ref, tops[i], columns(near[i][0]), p_ref, shrink_ref)

        def near_values(i):
            _, p_ref, shrink_ref = near_refs(i)
            gather_values(4 * g + near[i][1], columns(near[i][0]), p_ref, shrink_ref)

        for i in range(len(near) + 2):
            if i < len(near):
                near_scores(i)
            if 0 <= i - 1 < len(near):
                near_soften(i - 1)
            if 0 <= i - 2:
                near_values(i - 2)
        shrink_odd[...] = jnp.ones_like(shrink_odd)
        strip = min(512, tok_dev)
        strips = [pl.ds(lo, strip) for lo in range(0, PAIR * tok_dev, strip)]

        def far_step(block, parity, tops):
            s_in, s_out = (s_even, s_odd)[::1 - PAIR * parity]
            p_out, p_in = (p_even, p_odd)[::1 - PAIR * parity]
            shrink_out, shrink_in = (shrink_even, shrink_odd)[::1 - PAIR * parity]
            next_tops = []
            for cols, top in zip(strips, tops):
                next_tops.append(scores(block + 1, cols, s_out.at[:, cols], False))
                soften(s_in.at[:, cols], top, cols, p_out.at[:, cols], shrink_out.at[:, cols])
                gather_values(jnp.maximum(block - 1, 0), cols, p_in.at[:, cols], shrink_in.at[:, cols])
            return next_tops

        def far_blocks(n, tops):
            for j in range(4):
                tops = far_step(4 * n + j, j % PAIR, tops)
            return tops

        lax.fori_loop(0, g, far_blocks, [scores(0, cols, s_even.at[:, cols], False) for cols in strips])
        for cols in strips:
            gather_values(jnp.maximum(4 * g - 1, 0), cols, p_odd.at[:, cols], shrink_odd.at[:, cols])
        out = (acc[...] / l_ref[...]).T.astype(jnp.bfloat16)
        for r in BOTH:
            o_st[PAIR * g + r] = out[r * tok_dev:(r + 1) * tok_dev]
            o_push(PAIR * g + r, "start")
        return carry

    def o_push(index, what):
        block = 4 * (index // PAIR) + (1 - core) * 3 * (index % PAIR) + core * (1 + index % PAIR)
        to_cp, to_tp = owner_of(block, n_cp, n_tp)
        here = and_(to_cp == cp_pos, to_tp == tp_pos)
        if what == "start":
            @pl.when(here)
            def _():
                pltpu.make_async_copy(o_st.at[index], o_hbm.at[head], ro_sem.at[head]).start()

        @pl.when(not_(here))
        def _():
            copy = pltpu.make_async_remote_copy(o_st.at[index], o_hbm.at[head], so_sem.at[index], ro_sem.at[head],
                                                device_id=mesh_id(to_cp, to_tp), device_id_type=MESH)
            if what == "start":
                copy.start()
            else:
                copy.wait_send()

    lax.fori_loop(0, n_dev // 4, query_pair, 0)

    wo_send(0).wait_recv()
    for step in range(1, n_x):
        wo_pass(step).wait_recv()
    for one in loads[3:]:
        one.wait()
    for j in range(n_heads):
        pltpu.make_async_copy(o_hbm.at[j], o_hbm.at[j], ro_sem.at[j]).wait()
    o_load = pltpu.make_async_copy(o_hbm, o_buf, o_sem)
    o_load.start()
    o_load.wait()
    o_rows = jnp.concatenate([o_buf[j] for j in range(n_heads)], axis=1)
    n_cols = min(512, hid // PAIR)

    for col in range(0, hid, n_cols):
        cols = pl.ds(col, n_cols)
        w_cols = wo_buf[:, :, cols].reshape(n_heads * head_dim, n_cols)
        h_cols = (x_buf[:, cols].astype(jnp.float32) + jnp.dot(o_rows, w_cols, preferred_element_type=jnp.float32)).astype(jnp.bfloat16)
        h_ref[PAIR * col // hid, :, pl.ds(col % (hid // PAIR), n_cols)] = h_cols

    for step in range(n_x):
        wo_send(step).wait_send()
    for step in range(1, n_x):
        wo_pass(step).wait_send()
    for one in swaps + ranks:
        one.wait()

    def drain(index, carry):
        o_push(index, "wait")
        return carry

    lax.fori_loop(0, n_dev // PAIR, drain, 0)


def attend_call(n_cp, n_tp, k_all, vt_all, q_all, x_loc, wo_loc, w_gate, w_up, w_down, rank_rows):
    n_dev = n_cp * n_tp
    tok_dev, hid = x_loc.shape
    seq, head_dim = k_all.shape
    n_heads = n_tp * wo_loc.shape[0] // head_dim
    keep = w_gate.shape[0] // PAIR
    any_spec = pl.BlockSpec(memory_space=pl.ANY)
    bf16 = jnp.bfloat16
    h_loc, _, wg_other, wu_other, wd_other, near_rows = pl.pallas_call(
        functools.partial(attend_kernel, n_cp, n_tp),
        name="attend_heads",
        out_shape=(jax.ShapeDtypeStruct((PAIR, tok_dev, hid // PAIR), bf16), jax.ShapeDtypeStruct((n_heads, tok_dev, head_dim), bf16))
        + tuple(jax.ShapeDtypeStruct((keep,) + w.shape[1:], bf16) for w in (w_gate, w_up, w_down))
        + (jax.ShapeDtypeStruct((PAIR, 4) + rank_rows.shape, jnp.float32),),
        in_specs=[any_spec] * 9,
        out_specs=(pl.BlockSpec(memory_space=pltpu.VMEM),) + (any_spec,) * 5,
        scratch_shapes=[
            pltpu.VMEM((seq, head_dim), bf16),
            pltpu.VMEM((head_dim, seq), bf16),
            pltpu.VMEM((seq // PAIR, head_dim), bf16),
            pltpu.VMEM((head_dim, PAIR * tok_dev), bf16),
            pltpu.VMEM((n_dev // PAIR, tok_dev, head_dim), bf16),
            pltpu.VMEM((n_heads, tok_dev, head_dim), bf16),
            pltpu.VMEM((n_tp,) + wo_loc.shape, bf16),
            pltpu.VMEM((tok_dev, hid), bf16),
            pltpu.VMEM((tok_dev, PAIR * tok_dev), jnp.float32),
            pltpu.VMEM((tok_dev, PAIR * tok_dev), jnp.float32),
            pltpu.VMEM((tok_dev, PAIR * tok_dev), bf16),
            pltpu.VMEM((tok_dev, PAIR * tok_dev), bf16),
            pltpu.VMEM((tok_dev, PAIR * tok_dev), bf16),
            pltpu.VMEM((1, PAIR * tok_dev), jnp.float32),
            pltpu.VMEM((1, PAIR * tok_dev), jnp.float32),
            pltpu.VMEM((head_dim, PAIR * tok_dev), jnp.float32),
            pltpu.VMEM((1, PAIR * tok_dev), jnp.float32),
            pltpu.VMEM((1, PAIR * tok_dev), jnp.float32),
            dma((5,)),
            dma((n_dev // PAIR,)),
            dma((n_heads,)),
            dma((n_tp,)),
            dma((n_tp,)),
            dma((3,)),
            dma((3,)),
            dma((PAIR, 4)),
            dma((PAIR, 4)),
            dma,
        ],
        compiler_params=pltpu.CompilerParams(collective_id=1, has_side_effects=True, vmem_limit_bytes=VMEM_LIMIT),
        cost_estimate=pl.CostEstimate(flops=PAIR * seq * seq * head_dim // PAIR, bytes_accessed=2**26, transcendentals=seq * seq // 4),
    )(k_all, vt_all, q_all, x_loc, wo_loc, w_gate, w_up, w_down, rank_rows)
    return h_loc, near_rows, wg_other, wu_other, wd_other


def solution(mesh):
    n_cp = mesh.shape["cp"]
    n_tp = mesh.shape["tp"]
    row_spec = P(("dp", "cp", "tp"), None)
    head_spec = P(None, "tp", None)
    expert_spec = P(("cp", "tp"), None, None)

    def device_step(x_loc, w_q, w_k, w_v, w_o, ids_loc, gates_loc, w_gate, w_up, w_down):
        tok_dev, hid_dim = x_loc.shape
        n_loc, head_dim = w_q.shape[1:]
        n_experts = w_gate.shape[0] * n_cp * n_tp // PAIR
        capacity = ids_loc.shape[1] * tok_dev // n_experts
        k_all, vt_all, q_all, rank_rows, gate_rows = front_call(n_cp, n_tp, x_loc, (w_q, w_k, w_v), ids_loc.T, gates_loc.T, n_experts)
        h_loc, near_rows, *others = attend_call(n_cp, n_tp, k_all, vt_all, q_all, x_loc, w_o.reshape(n_loc * head_dim, hid_dim), w_gate, w_up, w_down, rank_rows)
        return moe_call(n_cp, n_tp, capacity, h_loc, rank_rows, near_rows, gate_rows, w_gate, w_up, w_down, *others)

    return jax.shard_map(device_step, mesh=mesh, in_specs=(row_spec, head_spec, head_spec, head_spec, P("tp", None, None), row_spec, row_spec, expert_spec, expert_spec, expert_spec), out_specs=row_spec, check_vma=False)
```
